32 devices in a mesh: dp: 8 (over z, core), tensor: 4 (over y, x).
Axes of the slice: x: 2, y: 2, z: 4, core: 2. Of those that a mesh axis runs over, the one named last changes fastest.
Arguments:
- token_ids: int32 [8, 1024], P('dp', 'tensor'), may hold values from 0 to 30527
- lengths: int32 [8], P('dp'), may hold values from 256 to 1024, as said below
- teacher_bins: int32 [8], P('dp'), may hold values from 0 to 127
- embed_table: bfloat16 [30528, 1024], P('tensor'), may hold values from -6 to 6
- query_key_value_matrix: bfloat16 [1024, 3, 1024], P('dp', None, 'tensor'), may hold values from -2 to 2
- output_matrix: bfloat16 [1024, 1024], P('tensor', 'dp'), may hold values from -0.1875 to 0.1875
- up_matrix: bfloat16 [1024, 4096], P('dp', 'tensor'), may hold values from -0.1875 to 0.1875
- down_matrix: bfloat16 [4096, 1024], P('tensor', 'dp'), may hold values from -0.09375 to 0.09375
- w_head: bfloat16 [1024, 128], P('dp'), may hold values from -64 to 64
Outputs:
- loss: float32 [], replicated
- query_key_value_gradient: float32 [1024, 3, 1024], P('dp', None, 'tensor')
- output_weight_gradient: float32 [1024, 1024], P('tensor', 'dp')
- up_weight_gradient: float32 [1024, 4096], P('dp', 'tensor')
- down_weight_gradient: float32 [4096, 1024], P('tensor', 'dp')
- grad_head: float32 [1024, 128], P('dp')
The draws below stay inside these ranges and needn't reach their ends.
Inputs may be any that keep to these rules, and one draw needn't show every extreme that they name: lengths[0] is 1024.
All inputs are finite; a program needn't handle non-finite values.
Results may differ from the reference program's by a relative error of at most 0.02.
Values may be sent and summed in bfloat16 or wider, within the bound.
A program may use at most 128 MiB of HBM per device.

```python
import math
import jax
import jax.numpy as jnp
import numpy as np
from jax import lax

D = 1024
HEAD_COUNT = 16
HEAD_WIDTH = 64
FF = 4096
VOCAB = 30528
NBINS = 128
LEN = 1024
SEQS = 8
N_TENSOR = 4


def draw_lengths(key, part):
    values = jax.random.randint(jax.random.fold_in(key, 11), (SEQS,), LEN // 4, LEN + 1, dtype=jnp.int32)
    return values.at[0].set(LEN)


def draw_embed_table(key, part):
    normal_rows = jax.random.normal(jax.random.fold_in(key, 21), (VOCAB, D), jnp.float32)
    values = normal_rows
    return jnp.clip(values, -6.0, 6.0).astype(jnp.bfloat16)


def draw_query_key_value_matrix(key, part):
    scaled = jnp.clip(jax.random.normal(jax.random.fold_in(key, 31), (D, 3, D), jnp.float32), -6.0, 6.0) * (1.0 / math.sqrt(D))
    return jnp.clip(scaled, -2.0, 2.0).astype(jnp.bfloat16)


def draw_w_head(key, part):
    drawn_cols = jnp.clip(jax.random.normal(jax.random.fold_in(key, 41), (D, NBINS), jnp.float32), -6.0, 6.0) * 0.1
    return jnp.clip(drawn_cols, -64.0, 64.0).astype(jnp.bfloat16)


def plant(entries, rng, least, top_value):
    longest = entries.shape.index(max(entries.shape))
    spots = []
    for shift in (0, 1):
        where = [jax.random.randint(jax.random.fold_in(rng, axis), (), 0, length) for axis, length in enumerate(entries.shape)]
        where[longest] = (where[longest] + shift) % entries.shape[longest]
        spots.append(tuple(where))
    return entries.at[spots[0]].set(least).at[spots[1]].set(top_value)


def shard_levels(own_key, extent, cuts, smallest, high):
    def one(axis_at, parts):
        heights = jax.random.uniform(jax.random.fold_in(jax.random.fold_in(own_key, 6), axis_at), (parts,), jnp.float32, smallest / len(cuts), high / len(cuts))
        return jnp.repeat(jnp.exp(heights), extent[axis_at] // parts).reshape((-1,) + (1,) * (len(extent) - axis_at - 1))

    loudness = one(*cuts[0])
    for cut in cuts[1:]:
        loudness = loudness * one(*cut)
    return loudness


def rank_table(amount, slope):
    portions = [(1 << 20) // math.isqrt(standing ** slope) + 1 for standing in range(1, amount + 1)]
    scale = 1 + sum(portions) // (1 << 30)
    return np.cumsum(np.array([max(1, weight // scale) for weight in portions]))


def skewed_ids(stream_key, extent, amount, lean):
    listing = rank_table(amount, lean)
    ticket = jax.random.randint(jax.random.fold_in(stream_key, 1), extent, 0, int(listing[amount - 1]))
    rank = jnp.searchsorted(jnp.asarray(listing, jnp.int32), ticket, side="right")
    return jax.random.permutation(jax.random.fold_in(stream_key, 2), amount)[rank].astype(jnp.int32)


def normal_values(key, shape, scale, reach, shards=(), held_as=jnp.bfloat16):
    values = jax.random.normal(key, shape, jnp.float32) * scale
    if len(shards) > 0:
        values = shard_levels(key, shape, shards, -0.22, 0.18) * values
    return jnp.clip(values, min=-reach, max=reach).astype(held_as)


def setup_inputs(seed: int = 0) -> dict:
    streams_of = jax.random.split(jax.random.key(seed), 10)
    token_ids = plant(skewed_ids(streams_of[0], (SEQS, LEN), VOCAB, 2), jax.random.fold_in(streams_of[0], 3), 0, VOCAB - 1).astype(jnp.int32)
    lengths = draw_lengths(jax.random.fold_in(streams_of[9], 71), 0)
    teacher_bins = plant(jax.random.randint(streams_of[2], (SEQS,), 0, NBINS), jax.random.fold_in(streams_of[2], 1), 0, NBINS - 1).astype(jnp.int32)
    embed_table = draw_embed_table(jax.random.fold_in(streams_of[9], 71), 0)
    query_key_value_matrix = draw_query_key_value_matrix(jax.random.fold_in(streams_of[9], 71), 0)
    output_matrix = normal_values(streams_of[5], (D, D), D ** -0.5, 0.1875, ((0, 4), (1, 8)))
    up_matrix = normal_values(streams_of[6], (D, FF), D ** -0.5, 0.1875, ((0, 8), (1, 4)))
    down_matrix = normal_values(streams_of[7], (FF, D), FF ** -0.5, 0.09375, ((0, 4), (1, 8)))
    w_head = draw_w_head(jax.random.fold_in(streams_of[9], 71), 0)
    return dict(token_ids=token_ids, lengths=lengths, teacher_bins=teacher_bins, embed_table=embed_table, query_key_value_matrix=query_key_value_matrix, output_matrix=output_matrix, up_matrix=up_matrix, down_matrix=down_matrix, w_head=w_head)


EPS = 1e-05

def normalize(values):
    mean = lax.optimization_barrier(jnp.mean(values, axis=-1, keepdims=True))
    centered = values - mean
    return centered * lax.rsqrt(lax.optimization_barrier(jnp.mean(centered * centered, axis=-1, keepdims=True)) + EPS)

def gelu_tanh(values):
    return 0.5 * values * (1.0 + jnp.tanh(0.7978845608028654 * (values + 0.044715 * values * values * values)))

def attend(query, keys, values_in, lengths):
    scale = query.shape[-1] ** (-0.5)
    scores = jnp.einsum('sqhe,skhe->shqk', query, keys) * scale
    visible = jnp.arange(keys.shape[1], dtype=jnp.int32)[None, :] < lengths[:, None]
    scores = jnp.where(visible[:, None, None, :], scores, -1e+30)
    top = lax.optimization_barrier(jnp.max(scores, axis=-1, keepdims=True))
    expo = jnp.exp(scores - top)
    probs = expo / lax.optimization_barrier(jnp.sum(expo, axis=-1, keepdims=True))
    rounded = lax.optimization_barrier(probs.astype(jnp.bfloat16)).astype(jnp.float32)
    return jnp.einsum('shqk,skhe->sqhe', rounded, values_in)

def rounded_sum(left_operand, right_operand, blocks, inner_value):
    total = None
    for layer_block in range(blocks):
        slice_portion = jnp.einsum('wou,ue->woe', left_operand[:, :, layer_block * inner_value:(layer_block + 1) * inner_value].astype(jnp.float32), right_operand[layer_block * inner_value:(layer_block + 1) * inner_value].astype(jnp.float32))
        slice_portion = lax.optimization_barrier(slice_portion.astype(jnp.bfloat16)).astype(jnp.float32)
        total = slice_portion if total is None else total + slice_portion
    return total

def reference(token_ids, lengths, teacher_bins, embed_table, query_key_value_matrix, output_matrix, up_matrix, down_matrix, w_head):
    sequence_batch, sequence_length = token_ids.shape
    width = embed_table.shape[1]
    first = jnp.take(embed_table, token_ids, axis=0)
    first_normed_rows = normalize(first.astype(jnp.float32)).astype(jnp.bfloat16)
    mixed_output = jnp.einsum('fxw,wvr->fxvr', first_normed_rows.astype(jnp.float32), query_key_value_matrix.astype(jnp.float32)).astype(jnp.bfloat16)
    split = mixed_output.astype(jnp.float32).reshape(sequence_batch, sequence_length, 3, HEAD_COUNT, HEAD_WIDTH)

    def forward_one(item):
        query, keys, vals, count = item
        return attend(query[None], keys[None], vals[None], count[None])[0]
    attended_rows = lax.map(forward_one, (split[:, :, 0], split[:, :, 1], split[:, :, 2], lengths))
    attended_rows = attended_rows.astype(jnp.bfloat16).reshape(sequence_batch, sequence_length, width)
    attn = rounded_sum(attended_rows, output_matrix, N_TENSOR, width // N_TENSOR)
    second = (first.astype(jnp.float32) + attn).astype(jnp.bfloat16)
    second_normed_rows = normalize(second.astype(jnp.float32)).astype(jnp.bfloat16)
    hidden_preactivation = jnp.einsum('ntp,pk->ntk', second_normed_rows.astype(jnp.float32), up_matrix.astype(jnp.float32))
    hidden_activated = gelu_tanh(hidden_preactivation).astype(jnp.bfloat16)
    ffn = rounded_sum(hidden_activated, down_matrix, N_TENSOR, FF // N_TENSOR)
    third = second.astype(jnp.float32) + ffn
    live = (jnp.arange(sequence_length, dtype=jnp.int32)[None, :] < lengths[:, None]).astype(jnp.float32)
    counts = lengths.astype(jnp.float32)[:, None]
    pooled = lax.optimization_barrier(jnp.sum(third * live[:, :, None], axis=1)) / counts
    final, final_back = jax.vjp(normalize, pooled)
    head = w_head.astype(jnp.float32)
    logits = jnp.dot(final, head, precision=lax.Precision.HIGHEST)
    top = lax.optimization_barrier(jnp.max(logits, axis=-1, keepdims=True))
    total_exp = jnp.log(lax.optimization_barrier(jnp.sum(jnp.exp(logits - top), axis=-1, keepdims=True))) + top
    labels = (teacher_bins[:, None] == jnp.arange(logits.shape[1], dtype=jnp.int32)[None, :]).astype(jnp.float32)
    losses = total_exp[:, 0] - lax.optimization_barrier(jnp.sum(logits * labels, axis=-1))
    loss = jnp.sum(losses) / sequence_batch
    g_logits = (jnp.exp(logits - total_exp) - labels) / sequence_batch
    grad_head = jnp.dot(final.T, g_logits, precision=lax.Precision.HIGHEST)
    g_final = jnp.dot(g_logits, head.T, precision=lax.Precision.HIGHEST)
    g_pooled = final_back(g_final)[0]
    per_token = g_pooled / counts
    g_third = per_token[:, None, :] * live[:, :, None]
    third_gradient_batch = g_third.astype(jnp.bfloat16)
    down_weight_gradient = jnp.einsum('omi,omy->iy', hidden_activated.astype(jnp.float32), third_gradient_batch.astype(jnp.float32))
    hidden_gradient = jnp.einsum('tpu,bu->tpb', third_gradient_batch.astype(jnp.float32), down_matrix.astype(jnp.float32))
    gelu_back = jax.vjp(gelu_tanh, hidden_preactivation)[1]
    preact_gradient = gelu_back(hidden_gradient)[0].astype(jnp.bfloat16)
    up_weight_gradient = jnp.einsum('qon,qom->nm', second_normed_rows.astype(jnp.float32), preact_gradient.astype(jnp.float32))
    g_normed_two = rounded_sum(preact_gradient, up_matrix.T, N_TENSOR, FF // N_TENSOR)
    norm_back = jax.vjp(normalize, second.astype(jnp.float32))[1]
    second_gradient = (g_third + norm_back(g_normed_two)[0]).astype(jnp.bfloat16)
    output_weight_gradient = jnp.einsum('jxm,jxn->mn', attended_rows.astype(jnp.float32), second_gradient.astype(jnp.float32))
    attended_gradient = jnp.einsum('kmi,qi->kmq', second_gradient.astype(jnp.float32), output_matrix.astype(jnp.float32)).reshape(sequence_batch, sequence_length, HEAD_COUNT, HEAD_WIDTH)

    def backward_one(item):
        query, keys, vals, count, grad = item
        back = jax.vjp(lambda a, b, c: attend(a[None], b[None], c[None], count[None])[0], query, keys, vals)[1]
        return back(grad)
    g_query, g_keys, g_vals = lax.map(backward_one, (split[:, :, 0], split[:, :, 1], split[:, :, 2], lengths, attended_gradient))
    mixed_gradient = jnp.stack([g_query, g_keys, g_vals], axis=2).reshape(sequence_batch, sequence_length, 3, width).astype(jnp.bfloat16)
    query_key_value_gradient = jnp.einsum('rvt,rvzx->tzx', first_normed_rows.astype(jnp.float32), mixed_gradient.astype(jnp.float32))
    return (loss, query_key_value_gradient, output_weight_gradient, up_weight_gradient, down_weight_gradient, grad_head)
```

```python
import functools

import jax
import jax.numpy as jnp
from jax import lax
from jax.experimental import pallas as pl
from jax.experimental.pallas import tpu as pltpu
from jax.sharding import PartitionSpec as P

HEAD_WIDTH = 64
EPS = 1e-05
BF = jnp.bfloat16
F32 = jnp.float32
MESH = pl.DeviceIdType.MESH
VMEM = pltpu.VMEM
BIG = 60 * 1024 * 1024


def normalize(values):
    mean = jnp.mean(values, axis=-1, keepdims=True)
    centered = values - mean
    return centered * lax.rsqrt(jnp.mean(centered * centered, axis=-1, keepdims=True) + EPS)


def vmem_spec():
    return pl.BlockSpec(memory_space=pltpu.VMEM)


def greet(axis, count):
    me = lax.axis_index(axis)
    barrier = pltpu.get_barrier_semaphore()
    for step in range(1, count):
        pl.semaphore_signal(
            barrier, inc=1, device_id={axis: lax.rem(me + step, count)}, device_id_type=MESH
        )
    pl.semaphore_wait(barrier, count - 1)
    return me


def gather_body(axis, count, x_ref, out_ref, send_sem, recv_sem):
    me = greet(axis, count)
    copies = []
    for step in range(1, count):
        copy = pltpu.make_async_remote_copy(
            src_ref=x_ref,
            dst_ref=out_ref.at[me],
            send_sem=send_sem.at[step - 1],
            recv_sem=recv_sem.at[step - 1],
            device_id={axis: lax.rem(me + step, count)},
            device_id_type=MESH,
        )
        copy.start()
        copies.append(copy)
    out_ref[me] = x_ref[...]
    for copy in copies:
        copy.wait()


def relay_gather(axis, me, src, out, send_sem, recv_sem):
    across = me + 1 - 2 * lax.rem(me, 2)
    over = lax.rem(me + 2, 4)
    half = src.shape[0] // 2
    low, high = pl.ds(0, half), pl.ds(half, half)

    def copy(index, src_part, block, part, device):
        return pltpu.make_async_remote_copy(
            src_ref=src_part,
            dst_ref=out.at[block, part],
            send_sem=send_sem.at[index],
            recv_sem=recv_sem.at[index],
            device_id={axis: device},
            device_id_type=MESH,
        )

    first_a = copy(0, src.at[low], me, low, across)
    first_b = copy(1, src.at[high], me, high, over)
    second_a = copy(2, src.at[high], me, high, across)
    second_b = copy(3, src.at[low], me, low, over)
    for one in (first_a, first_b, second_a, second_b):
        one.start()
    first_a.wait_recv()
    pass_b = copy(4, out.at[across, low], across, low, over)
    pass_b.start()
    first_b.wait_recv()
    pass_a = copy(5, out.at[over, high], over, high, across)
    pass_a.start()
    second_a.wait_recv()
    second_b.wait_recv()
    pass_b.wait_recv()
    pass_a.wait_recv()
    for one in (first_a, first_b, second_a, second_b, pass_b, pass_a):
        one.wait_send()


def relay_body(axis, x_ref, out_ref, send_sem, recv_sem):
    me = greet(axis, 4)
    relay_gather(axis, me, x_ref, out_ref, send_sem, recv_sem)
    out_ref[me] = x_ref[...]


def gather_blocks(x, axis, count, ident):
    if count != 4:
        return gather_all(x, axis, count, ident)
    return pl.pallas_call(
        functools.partial(relay_body, axis),
        out_shape=jax.ShapeDtypeStruct((count,) + x.shape, x.dtype),
        in_specs=[vmem_spec()],
        out_specs=vmem_spec(),
        scratch_shapes=[pltpu.SemaphoreType.DMA((6,)), pltpu.SemaphoreType.DMA((6,))],
        compiler_params=pltpu.CompilerParams(collective_id=ident, has_side_effects=True),
        name="gather_blocks",
    )(x)


def gather_all(x, axis, count, ident):
    return pl.pallas_call(
        functools.partial(gather_body, axis, count),
        out_shape=jax.ShapeDtypeStruct((count,) + x.shape, x.dtype),
        in_specs=[vmem_spec()],
        out_specs=vmem_spec(),
        scratch_shapes=[
            pltpu.SemaphoreType.DMA((count - 1,)),
            pltpu.SemaphoreType.DMA((count - 1,)),
        ],
        compiler_params=pltpu.CompilerParams(collective_id=ident, has_side_effects=True),
        name="gather_all",
    )(x)


def scatter_copies(axis, count, me, x_ref, held, send_sem, recv_sem):
    copies = []
    for step in range(1, count):
        peer = lax.rem(me + step, count)
        copies.append(
            pltpu.make_async_remote_copy(
                src_ref=x_ref.at[peer],
                dst_ref=held.at[step - 1],
                send_sem=send_sem.at[step - 1],
                recv_sem=recv_sem.at[step - 1],
                device_id={axis: peer},
                device_id_type=MESH,
            )
        )
    return copies


def scatter_start(*args):
    for copy in scatter_copies(*args):
        copy.start()


def scatter_finish(axis, count, me, x_ref, held, send_sem, recv_sem, put):
    for copy in scatter_copies(axis, count, me, x_ref, held, send_sem, recv_sem):
        copy.wait()

    def body(at):
        total = x_ref[me, at].astype(F32)
        for step in range(1, count):
            total = total + held[step - 1, at].astype(F32)
        put(at, total)

    add_tiles(x_ref.shape[1], 32, body)


def add_tiles(rows, tile, body):
    def step(index, carry):
        body(pl.ds(pl.multiple_of(index * tile, tile), tile))
        return carry

    lax.fori_loop(0, rows // tile, step, 0)


class GroupSum:
    def __init__(self, x_ref, out_ref, pair, mine, far, sems):
        self.x, self.out, self.pair, self.mine, self.far = x_ref, out_ref, pair, mine, far
        self.sems = sems
        self.groups = x_ref.shape[0]
        self.chips = self.groups // 2
        self.rows = x_ref.shape[1]
        me = lax.axis_index("dp")
        self.core = lax.rem(me, 2)
        self.chip = me // 2
        self.near = self.chip * 2 + 1 - self.core

    @staticmethod
    def scratch(shape, dtype):
        groups, rows, columns = shape
        chips = groups // 2
        return [
            VMEM((chips, rows, columns), dtype),
            VMEM((chips, rows, columns), dtype),
            VMEM((chips - 1, rows, columns), dtype),
            pltpu.SemaphoreType.DMA((chips,)),
            pltpu.SemaphoreType.DMA((chips,)),
            pltpu.SemaphoreType.DMA((6 if chips == 4 else chips - 1,)),
            pltpu.SemaphoreType.DMA((6 if chips == 4 else chips - 1,)),
        ]

    def signal(self, barrier):
        pl.semaphore_signal(
            barrier, inc=1, device_id={"dp": self.near}, device_id_type=MESH
        )
        for step in range(1, self.chips):
            pl.semaphore_signal(
                barrier, inc=1, device_id={"dp": self.owner(step)}, device_id_type=MESH
            )
        return self.chips

    def owner(self, step):
        return lax.rem(self.chip + step, self.chips) * 2 + self.core

    def pair_copies(self):
        copies = []
        for chip in range(self.chips):
            copies.append(
                pltpu.make_async_remote_copy(
                    src_ref=self.x.at[chip * 2 + 1 - self.core],
                    dst_ref=self.pair.at[chip],
                    send_sem=self.sems[0].at[chip],
                    recv_sem=self.sems[1].at[chip],
                    device_id={"dp": self.near},
                    device_id_type=MESH,
                )
            )
        return copies

    def far_copies(self):
        copies = []
        for step in range(1, self.chips):
            copies.append(
                pltpu.make_async_remote_copy(
                    src_ref=self.mine.at[lax.rem(self.chip + step, self.chips)],
                    dst_ref=self.far.at[step - 1],
                    send_sem=self.sems[2].at[step - 1],
                    recv_sem=self.sems[3].at[step - 1],
                    device_id={"dp": self.owner(step)},
                    device_id_type=MESH,
                )
            )
        return copies

    def ring_copies(self):
        right, left = lax.rem(self.chip + 1, 4), lax.rem(self.chip + 3, 4)
        opposite = lax.rem(self.chip + 2, 4)
        half = self.rows // 2
        low, high = pl.ds(0, half), pl.ds(half, half)

        def copy(index, block, part, slot, chip):
            return pltpu.make_async_remote_copy(
                src_ref=self.mine.at[block, part],
                dst_ref=self.far.at[slot, part],
                send_sem=self.sems[2].at[index],
                recv_sem=self.sems[3].at[index],
                device_id={"dp": chip * 2 + self.core},
                device_id_type=MESH,
            )

        return (
            copy(0, opposite, low, 2, right),
            copy(1, opposite, high, 2, left),
            copy(2, right, high, 0, right),
            copy(3, left, low, 1, left),
            copy(4, right, low, 0, right),
            copy(5, left, high, 1, left),
        )

    def relay(self):
        if self.chips != 4:
            return
        copies = self.ring_copies()
        half = self.rows // 2
        for index, step, base in ((0, 1, 0), (1, 3, half)):
            copies[index].wait_recv()
            block = lax.rem(self.chip + step, 4)

            def body(at, block=block, base=base):
                here = pl.ds(base + at.start, at.size)
                self.mine[block, here] = (
                    self.mine[block, here].astype(F32) + self.far[2, here].astype(F32)
                ).astype(self.mine.dtype)

            add_tiles(half, 32, body)
            copies[index + 4].start()

    def start(self):
        for copy in self.pair_copies():
            copy.start()

    def middle(self):
        for copy in self.pair_copies():
            copy.wait()

        for chip in range(self.chips):

            def body(at, chip=chip):
                self.mine[chip, at] = (
                    self.x[chip * 2 + self.core, at].astype(F32)
                    + self.pair[chip, at].astype(F32)
                ).astype(self.mine.dtype)

            add_tiles(self.rows, 32, body)
        copies = self.ring_copies()[:4] if self.chips == 4 else self.far_copies()
        for copy in copies:
            copy.start()

    def finish(self):
        if self.chips == 4:
            copies = self.ring_copies()
            for copy in copies[2:]:
                copy.wait()
            for copy in copies[:2]:
                copy.wait_send()
        else:
            for copy in self.far_copies():
                copy.wait()

        def body(at):
            total = self.mine[self.chip, at].astype(F32)
            for step in range(2 if self.chips == 4 else self.chips - 1):
                total = total + self.far[step, at].astype(F32)
            self.out[at] = total

        add_tiles(self.rows, 32, body)


def scatter_and_group_body(
    count, x_ref, up_ref, small_ref, out_ref, up_out, small_out, held, send_sem, recv_sem, *rest
):
    up = GroupSum(up_ref, up_out, rest[0], rest[1], rest[2], rest[3:7])
    small_send, small_recv = rest[7:]
    groups = small_out.shape[0]
    group = lax.axis_index("dp")
    barrier = pltpu.get_barrier_semaphore()
    me = lax.axis_index("tensor")
    for step in range(1, count):
        pl.semaphore_signal(
            barrier, inc=1, device_id={"tensor": lax.rem(me + step, count)}, device_id_type=MESH
        )
    for step in range(1, groups):
        pl.semaphore_signal(
            barrier, inc=1, device_id={"dp": lax.rem(group + step, groups)}, device_id_type=MESH
        )
    pl.semaphore_wait(barrier, count + groups - 2)
    smalls = []
    for step in range(1, groups):
        smalls.append(
            pltpu.make_async_remote_copy(
                src_ref=small_ref,
                dst_ref=small_out.at[group],
                send_sem=small_send.at[step - 1],
                recv_sem=small_recv.at[step - 1],
                device_id={"dp": lax.rem(group + step, groups)},
                device_id_type=MESH,
            )
        )

    def put(at, total):
        out_ref[at] = total.astype(out_ref.dtype)

    up.start()
    scatter_start("tensor", count, me, x_ref, held, send_sem, recv_sem)
    up.middle()
    for copy in smalls:
        copy.start()
    small_out[group] = small_ref[...]
    up.relay()
    scatter_finish("tensor", count, me, x_ref, held, send_sem, recv_sem, put)
    up.finish()
    for copy in smalls:
        copy.wait()


def scatter_and_group(x, up, small, count, ident):
    return pl.pallas_call(
        functools.partial(scatter_and_group_body, count),
        out_shape=(
            jax.ShapeDtypeStruct(x.shape[1:], x.dtype),
            jax.ShapeDtypeStruct(up.shape[1:], F32),
            jax.ShapeDtypeStruct(up.shape[:1] + small.shape, F32),
        ),
        in_specs=[vmem_spec()] * 3,
        out_specs=(vmem_spec(),) * 3,
        scratch_shapes=[
            VMEM((count - 1,) + x.shape[1:], x.dtype),
            pltpu.SemaphoreType.DMA((count - 1,)),
            pltpu.SemaphoreType.DMA((count - 1,)),
        ]
        + GroupSum.scratch(up.shape, up.dtype)
        + [pltpu.SemaphoreType.DMA((up.shape[0] - 1,))] * 2,
        compiler_params=pltpu.CompilerParams(
            collective_id=ident, has_side_effects=True, vmem_limit_bytes=BIG
        ),
        name="scatter_and_group",
    )(x, up, small)


def group_sum_body(number, *refs):
    xs, outs, rest = refs[:number], refs[number : 2 * number], refs[2 * number :]
    sums = [
        GroupSum(x, out, *rest[7 * i : 7 * i + 3], rest[7 * i + 3 : 7 * i + 7])
        for i, (x, out) in enumerate(zip(xs, outs))
    ]
    barrier = pltpu.get_barrier_semaphore()
    pl.semaphore_wait(barrier, sums[0].signal(barrier))
    for one in sums:
        one.start()
    for one in sums:
        one.middle()
    for one in sums:
        one.relay()
    for one in sums:
        one.finish()


def group_sum(arrays, ident):
    number = len(arrays)
    scratch = []
    for array in arrays:
        scratch += GroupSum.scratch(array.shape, array.dtype)
    return pl.pallas_call(
        functools.partial(group_sum_body, number),
        out_shape=tuple(jax.ShapeDtypeStruct(a.shape[1:], F32) for a in arrays),
        in_specs=[vmem_spec()] * number,
        out_specs=(vmem_spec(),) * number,
        scratch_shapes=scratch,
        compiler_params=pltpu.CompilerParams(
            collective_id=ident, has_side_effects=True, vmem_limit_bytes=BIG
        ),
        name="group_sum",
    )(*arrays)


def sum_all_body(axis, count, x_ref, out_ref, held, send_sem, recv_sem, send_two, recv_two):
    me = greet(axis, count)

    def put(at, total):
        out_ref[me, at] = total.astype(out_ref.dtype)

    scatter_start(axis, count, me, x_ref, held, send_sem, recv_sem)
    scatter_finish(axis, count, me, x_ref, held, send_sem, recv_sem, put)
    if count == 4:
        relay_gather(axis, me, out_ref.at[me], out_ref, send_two, recv_two)
        return
    copies = []
    for step in range(1, count):
        copy = pltpu.make_async_remote_copy(
            src_ref=out_ref.at[me],
            dst_ref=out_ref.at[me],
            send_sem=send_two.at[step - 1],
            recv_sem=recv_two.at[step - 1],
            device_id={axis: lax.rem(me + step, count)},
            device_id_type=MESH,
        )
        copy.start()
        copies.append(copy)
    for copy in copies:
        copy.wait()


def sum_all(x, axis, count, ident):
    return pl.pallas_call(
        functools.partial(sum_all_body, axis, count),
        out_shape=jax.ShapeDtypeStruct(x.shape, x.dtype),
        in_specs=[vmem_spec()],
        out_specs=vmem_spec(),
        scratch_shapes=[VMEM((count - 1,) + x.shape[1:], x.dtype)]
        + [pltpu.SemaphoreType.DMA((count - 1,))] * 2
        + [pltpu.SemaphoreType.DMA((6 if count == 4 else count - 1,))] * 2,
        compiler_params=pltpu.CompilerParams(collective_id=ident, has_side_effects=True),
        name="sum_all",
    )(x)


def contract(left, right, dims):
    return lax.dot_general(left, right, ((dims[:1], dims[1:]), ((), ())), preferred_element_type=F32)


def masked_scores(keys, query, length):
    scores = contract(keys, query, (0, 0))
    position = lax.broadcasted_iota(jnp.int32, scores.shape, 0)
    return jnp.where(position < length, scores, -1e30)


def attend_body(chunk, length_ref, qkv_ref, out_ref, lse_ref):
    length = length_ref[0]
    keys, vals = qkv_ref[1], qkv_ref[2]
    scale = HEAD_WIDTH ** (-0.5)
    for at in range(0, qkv_ref.shape[2], chunk):
        query = (qkv_ref[0, :, at : at + chunk].astype(F32) * scale).astype(BF)
        scores = masked_scores(keys, query, length)
        top = jnp.max(scores, axis=0, keepdims=True)
        expo = jnp.exp(scores - top)
        total = jnp.sum(expo, axis=0, keepdims=True)
        mixed = contract(vals, expo.astype(BF), (1, 0))
        out_ref[:, at : at + chunk] = (mixed * (1.0 / total)).astype(BF)
        lse_ref[0, :, at : at + chunk] = top + jnp.log(total)


def attend(qkv, lengths, chunk):
    _, width, length = qkv.shape
    heads = width // HEAD_WIDTH
    return pl.pallas_call(
        functools.partial(attend_body, chunk),
        grid=(heads,),
        out_shape=(
            jax.ShapeDtypeStruct((width, length), BF),
            jax.ShapeDtypeStruct((heads, 1, length), F32),
        ),
        in_specs=[
            pl.BlockSpec(memory_space=pltpu.SMEM),
            pl.BlockSpec((3, HEAD_WIDTH, length), lambda h: (0, h, 0)),
        ],
        out_specs=(
            pl.BlockSpec((HEAD_WIDTH, length), lambda h: (h, 0)),
            pl.BlockSpec((1, 1, length), lambda h: (h, 0, 0)),
        ),
        cost_estimate=pl.CostEstimate(
            flops=4 * width * length * length,
            bytes_accessed=8 * width * length,
            transcendentals=heads * length * length,
        ),
        compiler_params=pltpu.CompilerParams(vmem_limit_bytes=BIG),
        name="attend",
    )(lengths, qkv)


def attend_back_body(
    chunk, ranks, length_ref, qkv_ref, lse_ref, grad_ref, x_ref, out_ref, x_out, held, send_sem, recv_sem
):
    me = lax.axis_index("tensor")
    args = ("tensor", ranks, me, x_ref, held, send_sem, recv_sem)

    @pl.when(pl.program_id(0) == 0)
    def _():
        greet("tensor", ranks)
        scatter_start(*args)

    attend_back_head(chunk, length_ref, qkv_ref, lse_ref, grad_ref, out_ref)

    @pl.when(pl.program_id(0) == pl.num_programs(0) - 1)
    def _():
        piece = x_out.shape[2]

        def put(at, total):
            for group in range(x_out.shape[0]):
                x_out[group, at] = total[:, group * piece : (group + 1) * piece].astype(BF)

        scatter_finish(*args, put)


def attend_back_head(chunk, length_ref, qkv_ref, lse_ref, grad_ref, out_ref):
    length = length_ref[0]
    keys, vals = qkv_ref[1], qkv_ref[2]
    scale = HEAD_WIDTH ** (-0.5)
    span = qkv_ref.shape[2]
    g_keys = jnp.zeros((HEAD_WIDTH, span), F32)
    g_vals = jnp.zeros((HEAD_WIDTH, span), F32)
    for at in range(0, span, chunk):
        here = slice(at, at + chunk)
        query = (qkv_ref[0, :, here].astype(F32) * scale).astype(BF)
        grad = grad_ref[:, here]
        probs = jnp.exp(masked_scores(keys, query, length) - lse_ref[0, :, here])
        g_probs = contract(vals, grad, (0, 0))
        weighted = probs * g_probs
        inner = jnp.sum(weighted, axis=0, keepdims=True)
        g_scores = (weighted - probs * inner).astype(BF)
        out_ref[0, :, here] = (contract(keys, g_scores, (1, 0)) * scale).astype(BF)
        g_keys += contract(query, g_scores, (1, 1))
        g_vals += contract(grad, probs.astype(BF), (1, 1))
    out_ref[1] = g_keys.astype(BF)
    out_ref[2] = g_vals.astype(BF)


def attend_back(qkv, lengths, lse, grad, x, groups, chunk, ident):
    _, width, length = qkv.shape
    heads = width // HEAD_WIDTH
    return pl.pallas_call(
        functools.partial(attend_back_body, chunk, x.shape[0]),
        grid=(heads,),
        out_shape=(
            jax.ShapeDtypeStruct(qkv.shape, BF),
            jax.ShapeDtypeStruct((groups, x.shape[1], x.shape[2] // groups), BF),
        ),
        in_specs=[
            pl.BlockSpec(memory_space=pltpu.SMEM),
            pl.BlockSpec((3, HEAD_WIDTH, length), lambda h: (0, h, 0)),
            pl.BlockSpec((1, 1, length), lambda h: (h, 0, 0)),
            pl.BlockSpec((HEAD_WIDTH, length), lambda h: (h, 0)),
            vmem_spec(),
        ],
        out_specs=(
            pl.BlockSpec((3, HEAD_WIDTH, length), lambda h: (0, h, 0)),
            vmem_spec(),
        ),
        scratch_shapes=[
            VMEM((x.shape[0] - 1,) + x.shape[1:], x.dtype),
            pltpu.SemaphoreType.DMA((x.shape[0] - 1,)),
            pltpu.SemaphoreType.DMA((x.shape[0] - 1,)),
        ],
        cost_estimate=pl.CostEstimate(
            flops=10 * width * length * length,
            bytes_accessed=14 * width * length,
            transcendentals=heads * length * length,
        ),
        compiler_params=pltpu.CompilerParams(
            collective_id=ident, has_side_effects=True, vmem_limit_bytes=BIG
        ),
        name="attend_back",
    )(lengths, qkv, lse, grad, x)


def hidden_body(length_ref, normed_ref, up_ref, slope_ref, sum_ref):
    pre = jnp.dot(normed_ref[...], up_ref[...], preferred_element_type=F32)
    live = lax.broadcasted_iota(jnp.int32, pre.shape, 0) < length_ref[0]
    square = pre * pre
    bend = jnp.tanh(0.7978845608028654 * (pre * (1.0 + 0.044715 * square)))
    half = 0.5 * (1.0 + bend)
    act = (pre * half).astype(BF).astype(F32)
    sum_ref[...] = jnp.sum(jnp.where(live, act, 0.0), axis=0, keepdims=True)
    inner = 0.7978845608028654 * (1.0 + 3 * 0.044715 * square)
    slope = half + 0.5 * pre * (1.0 - bend * bend) * inner
    slope_ref[...] = jnp.where(live, slope, 0.0).astype(BF)


def hidden(normed, up, lengths, chunk):
    length, width = normed.shape
    units = up.shape[1]
    return pl.pallas_call(
        hidden_body,
        grid=(units // chunk,),
        out_shape=(
            jax.ShapeDtypeStruct((length, units), BF),
            jax.ShapeDtypeStruct((1, units), F32),
        ),
        in_specs=[
            pl.BlockSpec(memory_space=pltpu.SMEM),
            pl.BlockSpec((length, width), lambda f: (0, 0)),
            pl.BlockSpec((width, chunk), lambda f: (0, f)),
        ],
        out_specs=(
            pl.BlockSpec((length, chunk), lambda f: (0, f)),
            pl.BlockSpec((1, chunk), lambda f: (0, f)),
        ),
        cost_estimate=pl.CostEstimate(
            flops=2 * length * width * units,
            bytes_accessed=6 * length * units,
            transcendentals=length * units,
        ),
        compiler_params=pltpu.CompilerParams(vmem_limit_bytes=BIG),
        name="hidden",
    )(lengths, normed, up)


def per_device(
    token_ids,
    lengths,
    teacher_bins,
    embed_table,
    query_key_value_matrix,
    output_matrix,
    up_matrix,
    down_matrix,
    w_head,
):
    ranks = lax.axis_size("tensor")
    groups = lax.axis_size("dp")
    rank = lax.axis_index("tensor")
    group = lax.axis_index("dp")
    assert token_ids.shape[0] == 1
    local_len = token_ids.shape[1]
    span = local_len * ranks
    vocab_local, width = embed_table.shape
    d_local, _, e_local = query_key_value_matrix.shape
    f_local = up_matrix.shape[1]
    bins = w_head.shape[1]
    exact = lax.Precision.HIGHEST

    qkv_full = lax.all_gather(
        query_key_value_matrix.reshape(d_local, 3 * e_local), "dp", axis=0, tiled=True
    )
    out_parts = lax.all_gather(output_matrix, ("tensor", "dp"), axis=0, tiled=False)
    out_full = (
        out_parts.reshape(ranks, groups, e_local, d_local)
        .transpose(0, 2, 1, 3)
        .reshape(ranks * e_local, width)
    )
    up_full = lax.all_gather(up_matrix, "dp", axis=0, tiled=True)
    low = lax.all_gather(
        jnp.concatenate([down_matrix, w_head.reshape(bins, d_local)], axis=0), "dp", axis=0, tiled=False
    )
    down_full = low[:, :f_local]
    head_wide = low[:, f_local:].reshape(width, bins).astype(F32)

    all_ids = gather_all(token_ids, "tensor", ranks, 1).reshape(ranks, local_len)
    shifted = all_ids - rank * vocab_local
    inside = (shifted >= 0) & (shifted < vocab_local)
    rows = jnp.take(embed_table, jnp.clip(shifted, 0, vocab_local - 1), axis=0)
    first = sum_all(
        jnp.where(inside[..., None], rows, jnp.zeros((), BF)), "tensor", ranks, 2
    ).reshape(span, width)
    normed_one = normalize(first.astype(F32)).astype(BF)
    qkv = (
        lax.dot_general(qkv_full, normed_one, (((0,), (1,)), ((), ())), preferred_element_type=F32)
        .astype(BF)
        .reshape(3, e_local, span)
    )
    chunk = min(256, span)
    context, lse = attend(qkv, lengths, chunk)
    context_all = gather_blocks(context, "tensor", ranks, 3).reshape(ranks * e_local, span)
    attn = lax.dot_general(
        context_all, out_full, (((0,), (0,)), ((), ())), preferred_element_type=F32
    )
    second = (first.astype(F32) + attn).astype(BF)
    normed_f, norm_back = jax.vjp(normalize, second.astype(F32))
    normed_two = normed_f.astype(BF)
    slope, hidden_sum = hidden(normed_two, up_full, lengths, min(256, f_local))

    live = (jnp.arange(span, dtype=jnp.int32) < lengths[0]).astype(F32)
    count = lengths.astype(F32)[:, None]
    ffn_part = jnp.einsum(
        "of,jfd->ojd", hidden_sum, down_full.astype(F32), precision=exact
    ).reshape(1, width)
    ffn_all = gather_all(ffn_part, "tensor", ranks, 4)
    second_sum = jnp.sum(second.astype(F32) * live[:, None], axis=0, keepdims=True)
    pooled = (second_sum + jnp.sum(ffn_all, axis=0)) / count
    final, final_back = jax.vjp(normalize, pooled)
    logits = jnp.dot(final, head_wide, precision=exact)
    top = jnp.max(logits, axis=-1, keepdims=True)
    total_exp = jnp.log(jnp.sum(jnp.exp(logits - top), axis=-1, keepdims=True)) + top
    labels = (teacher_bins[:, None] == jnp.arange(bins, dtype=jnp.int32)[None, :]).astype(F32)
    loss_here = total_exp - jnp.sum(logits * labels, axis=-1, keepdims=True)
    g_logits = (jnp.exp(logits - total_exp) - labels) / groups
    g_final = jnp.dot(g_logits, head_wide.T, precision=exact)
    per_token = final_back(g_final)[0] / count
    rounded = per_token.astype(BF).astype(F32)
    g_hidden = jnp.einsum(
        "ojd,jfd->of",
        rounded.reshape(1, groups, d_local),
        down_full.astype(F32),
        precision=exact,
    )

    packed = jnp.concatenate(
        [hidden_sum, rounded, final, g_logits, jnp.broadcast_to(loss_here, (1, 128))], axis=1
    )

    over_seqs = (((0,), (0,)), ((), ()))
    up_base = lax.dot_general(normed_two, slope, over_seqs, preferred_element_type=F32)
    up_term = (up_base * g_hidden).astype(BF).reshape(groups, d_local, f_local)
    g_pre = (slope.astype(F32) * g_hidden).astype(BF)
    g_normed = lax.dot_general(
        g_pre, up_full, (((1,), (1,)), ((), ())), preferred_element_type=F32
    )
    g_second = (
        norm_back(g_normed)[0] + live[:, None] * (per_token / ranks)
    ).astype(BF)
    spread = lax.dot_general(
        out_full, g_second, (((1,), (1,)), ((), ())), preferred_element_type=F32
    ).astype(BF)
    g_context, up_weight_gradient, every = scatter_and_group(
        spread.reshape(ranks, e_local, span), up_term, packed, ranks, 6
    )
    every = every[:, 0]
    hidden_every = every[:, :f_local]
    rounded_every = every[:, f_local : f_local + width]
    final_every = every[:, f_local + width : f_local + 2 * width]
    rest = every[:, f_local + 2 * width :]
    loss = jnp.sum(rest[:, bins]) / groups
    mine = group * d_local
    down_weight_gradient = lax.dot_general(
        hidden_every,
        lax.dynamic_slice_in_dim(rounded_every, mine, d_local, axis=1),
        over_seqs,
        precision=exact,
    )
    grad_head = lax.dot_general(
        lax.dynamic_slice_in_dim(final_every, mine, d_local, axis=1),
        rest[:, :bins],
        over_seqs,
        precision=exact,
    )

    out_term = (
        jnp.dot(context_all, g_second, preferred_element_type=F32)
        .astype(BF)
        .reshape(ranks, e_local, width)
    )
    g_qkv, out_mine = attend_back(qkv, lengths, lse, g_context, out_term, groups, chunk, 7)
    qkv_term = lax.dot_general(
        normed_one,
        g_qkv.reshape(3 * e_local, span),
        (((0,), (1,)), ((), ())),
        preferred_element_type=F32,
    )
    qkv_gradient, output_weight_gradient = group_sum(
        [qkv_term.astype(BF).reshape(groups, d_local, 3 * e_local), out_mine], 8
    )
    query_key_value_gradient = qkv_gradient.reshape(d_local, 3, e_local)
    return (
        loss,
        query_key_value_gradient,
        output_weight_gradient,
        up_weight_gradient,
        down_weight_gradient,
        grad_head,
    )


def remote(src, dst, sems, index, device):
    return pltpu.make_async_remote_copy(
        src_ref=src,
        dst_ref=dst,
        send_sem=sems[0].at[index],
        recv_sem=sems[1].at[index],
        device_id=device,
        device_id_type=MESH,
    )


class Place:
    def __init__(self):
        self.rank = lax.axis_index("tensor")
        self.across = self.rank + 1 - 2 * lax.rem(self.rank, 2)
        self.over = lax.rem(self.rank + 2, 4)
        self.diag = 3 - self.rank
        self.group = lax.axis_index("dp")
        self.core = lax.rem(self.group, 2)
        self.chip = self.group // 2
        self.near = self.chip * 2 + 1 - self.core

    def turn(self, step):
        return lax.rem(self.chip + step, 4)

    def same(self, chip):
        return chip * 2 + self.core

    def greet(self, tensor, dp, everyone=False):
        barrier = pltpu.get_barrier_semaphore()
        peers = []
        if tensor:
            peers += [{"tensor": one} for one in (self.across, self.over, self.diag)]
        if everyone:
            peers += [{"dp": lax.rem(self.group + step, 8)} for step in range(1, 8)]
        elif dp:
            peers += [
                {"dp": self.near},
                {"dp": self.same(self.turn(1))},
                {"dp": self.same(self.turn(3))},
            ]
        for peer in peers:
            pl.semaphore_signal(barrier, inc=1, device_id=peer, device_id_type=MESH)
        pl.semaphore_wait(barrier, len(peers))


class RingGather:
    def __init__(self, at, src, own, slot, sems):
        self.at, self.src, self.own, self.slot = at, src, own, slot
        self.sems, self.local = sems[:2], sems[2]

    @staticmethod
    def scratch():
        return [
            pltpu.SemaphoreType.DMA((10,)),
            pltpu.SemaphoreType.DMA((10,)),
            pltpu.SemaphoreType.DMA((1,)),
        ]

    def copies(self):
        at = self.at
        right, left, far = at.turn(1), at.turn(3), at.turn(2)
        me, to_right, to_left = at.group, {"dp": at.same(right)}, {"dp": at.same(left)}
        near = {"dp": at.near}

        def held(index, chip, half, device):
            ref = self.slot(at.same(chip), half)
            return remote(ref, ref, self.sems, index, device)

        def first(index, half, device):
            return remote(self.own(half), self.slot(me, half), self.sems, index, device)

        return (
            first(0, 0, to_right),
            first(1, 1, to_left),
            first(2, 1, to_right),
            first(3, 0, to_left),
            held(4, left, 0, to_right),
            held(5, right, 1, to_left),
            remote(self.src, self.slot(me, None), self.sems, 6, near),
            held(7, left, None, near),
            held(8, right, None, near),
            held(9, far, None, near),
        )

    def keep(self):
        return pltpu.make_async_copy(self.src, self.slot(self.at.group, None), self.local.at[0])

    def start(self):
        copies = self.copies()
        for index in (0, 1, 2, 3, 6):
            copies[index].start()
        self.keep().start()

    def relay(self):
        copies = self.copies()
        copies[0].wait_recv()
        copies[4].start()
        copies[1].wait_recv()
        copies[5].start()

    def spread(self):
        copies = self.copies()
        copies[2].wait_recv()
        copies[7].start()
        copies[3].wait_recv()
        copies[8].start()
        copies[4].wait_recv()
        copies[5].wait_recv()
        copies[9].start()

    def finish(self):
        copies = self.copies()
        for index in (6, 7, 8, 9):
            copies[index].wait_recv()
        for copy in copies:
            copy.wait_send()
        self.keep().wait()


def rows_of(ref, block, half, size, axis=0):
    lead = (slice(None),) * axis
    if half is None:
        return ref.at[lead + (pl.ds(pl.multiple_of(block * size, size), size),)]
    part = size // 2
    return ref.at[lead + (pl.ds(pl.multiple_of(block * size + half * part, part), part),)]


def half_rows(ref, half, axis=0):
    part = ref.shape[axis] // 2
    return ref.at[(slice(None),) * axis + (pl.ds(half * part, part),)]


def ids_body(ids_ref, out_ref, ids_all, out_all, send, recv):
    at = Place()
    at.greet(True, False)
    copies = []
    for index, peer in enumerate((at.across, at.over, at.diag)):
        copies.append(
            remote(ids_ref, ids_all.at[at.rank], (send, recv), index, {"tensor": peer})
        )
    for index, peer in enumerate((at.across, at.over, at.diag)):
        copies.append(
            remote(out_ref, out_all.at[at.rank], (send, recv), 3 + index, {"tensor": peer})
        )
    for copy in copies:
        copy.start()
    ids_all[at.rank] = ids_ref[...]
    out_all[at.rank] = out_ref[...]
    for copy in copies:
        copy.wait()


def share_ids(ids, out, ident):
    return pl.pallas_call(
        ids_body,
        out_shape=(
            jax.ShapeDtypeStruct((4,) + ids.shape, ids.dtype),
            jax.ShapeDtypeStruct((4,) + out.shape, out.dtype),
        ),
        in_specs=[vmem_spec()] * 2,
        out_specs=(vmem_spec(),) * 2,
        scratch_shapes=[pltpu.SemaphoreType.DMA((6,))] * 2,
        compiler_params=pltpu.CompilerParams(collective_id=ident, has_side_effects=True),
        name="share_ids",
    )(ids, out)


def any_spec():
    return pl.BlockSpec(memory_space=pl.ANY)


class Stream:
    def __init__(self, at, x_ref, acc, held, last, whole, sems, index, rows, x_first):
        self.at, self.x, self.acc, self.held, self.last, self.whole = at, x_ref, acc, held, last, whole
        self.sems, self.index, self.rows = sems, index * 6, rows
        self.one, self.two = (at.across, at.over) if x_first else (at.over, at.across)

    def copies(self):
        at, rows, base, sems = self.at, self.rows, self.index, self.sems
        one, two = {"tensor": self.one}, {"tensor": self.two}
        return (
            remote(self.x.at[at.diag, rows], self.held.at[1, rows], sems, base, one),
            remote(self.x.at[self.one, rows], self.held.at[0, rows], sems, base + 1, one),
            remote(self.acc.at[rows], self.last.at[rows], sems, base + 2, two),
            remote(self.whole.at[at.rank, rows], self.whole.at[at.rank, rows], sems, base + 3, two),
            remote(self.whole.at[at.rank, rows], self.whole.at[at.rank, rows], sems, base + 4, one),
            remote(self.whole.at[self.two, rows], self.whole.at[self.two, rows], sems, base + 5, one),
        )

    def start(self):
        copies = self.copies()
        copies[0].start()
        copies[1].start()

    def second(self):
        copies = self.copies()
        copies[0].wait_recv()

        def body(at):
            here = pl.ds(self.rows.start + at.start, at.size)
            self.acc[here] = self.x[self.two, here] + self.held[1, here]

        add_tiles(self.rows.size, 32, body)
        copies[2].start()

    def third(self):
        copies = self.copies()
        copies[1].wait_recv()
        copies[2].wait_recv()

        def body(at):
            here = pl.ds(self.rows.start + at.start, at.size)
            self.whole[self.at.rank, here] = (
                self.x[self.at.rank, here] + self.held[0, here] + self.last[here]
            )

        add_tiles(self.rows.size, 32, body)
        copies[3].start()
        copies[4].start()

    def relay(self):
        copies = self.copies()
        copies[3].wait_recv()
        copies[5].start()

    def beside(self):
        self.copies()[4].wait_recv()

    def opposite(self):
        self.copies()[5].wait_recv()

    def finish(self):
        for copy in self.copies():
            copy.wait_send()


def embed_body(
    x_ref, w_ref, up_ref, first_out, normed_out, qkv_ref, up_out,
    acc, held, last, whole, normed, w_full, w_turn, send, recv, saved, *rest,
):
    at = Place()
    at.greet(True, True)
    d_local = w_ref.shape[1]
    local = x_ref.shape[1]
    weights = RingGather(
        at, w_ref, lambda half: half_rows(w_ref, half, 1),
        lambda block, half: rows_of(w_full, block, half, d_local, 1), rest[:3],
    )
    ups = RingGather(
        at, up_ref, lambda half: half_rows(up_ref, half),
        lambda block, half: rows_of(up_out, block, half, d_local), rest[3:],
    )
    weights.start()
    part = local // 4
    streams = [
        Stream(
            at, x_ref, acc, held, last, whole, (send, recv), index,
            pl.ds((index % 2) * (local // 2) + (index // 2) * part, part), index % 2 == 0,
        )
        for index in range(4)
    ]
    for one in streams:
        one.start()
    for one in streams:
        one.second()
    weights.relay()
    ups.start()
    for one in streams:
        one.third()
    weights.spread()
    weights.finish()
    for index in range(3):
        w_turn[index] = w_full[index].T

    def project(block, slot):
        def tile(here):
            normed[block, here] = normalize(whole[block, here].astype(F32)).astype(BF)

        add_tiles(local, 32, tile)
        base = pl.multiple_of(block * local, local)

        def matrix(index, carry):
            qkv_ref[index, :, pl.ds(base, local)] = contract(
                w_turn[index], normed[block], (1, 1)
            ).astype(BF)
            return carry

        lax.fori_loop(0, 3, matrix, 0)
        pltpu.make_async_copy(whole.at[block], first_out.at[block], saved.at[slot, 0]).start()
        pltpu.make_async_copy(normed.at[block], normed_out.at[block], saved.at[slot, 1]).start()

    for one in streams[:2]:
        one.relay()
    project(at.rank, 0)
    for one in streams[2:]:
        one.relay()
    ups.relay()
    for one in streams:
        one.beside()
    project(at.across, 1)
    project(at.over, 2)
    ups.spread()
    for one in streams:
        one.opposite()
    project(at.diag, 3)
    ups.finish()
    for one in streams:
        one.finish()
    for slot, block in enumerate((at.rank, at.across, at.over, at.diag)):
        pltpu.make_async_copy(whole.at[block], first_out.at[block], saved.at[slot, 0]).wait()
        pltpu.make_async_copy(normed.at[block], normed_out.at[block], saved.at[slot, 1]).wait()


def embed(x, w, up, ident):
    ranks, local, width = x.shape
    kinds, d_local, e_local = w.shape
    f_local = up.shape[1]
    return pl.pallas_call(
        embed_body,
        out_shape=(
            jax.ShapeDtypeStruct(x.shape, BF),
            jax.ShapeDtypeStruct(x.shape, BF),
            jax.ShapeDtypeStruct((kinds, e_local, ranks * local), BF),
            jax.ShapeDtypeStruct((width, f_local), BF),
        ),
        in_specs=[vmem_spec()] * 3,
        out_specs=(any_spec(), any_spec(), vmem_spec(), any_spec()),
        scratch_shapes=[
            VMEM((local, width), BF),
            VMEM((2, local, width), BF),
            VMEM((local, width), BF),
            VMEM(x.shape, BF),
            VMEM(x.shape, BF),
            VMEM((kinds, width, e_local), BF),
            VMEM((kinds, e_local, width), BF),
            pltpu.SemaphoreType.DMA((24,)),
            pltpu.SemaphoreType.DMA((24,)),
            pltpu.SemaphoreType.DMA((4, 2)),
        ]
        + RingGather.scratch()
        + RingGather.scratch(),
        compiler_params=pltpu.CompilerParams(
            collective_id=ident, has_side_effects=True, vmem_limit_bytes=BIG
        ),
        name="embed",
    )(x, w, up)


def attend_send_body(
    chunk, length_ref, qkv_ref, col_ref, ctx_out, lse_ref, out_full, ctx_ref, saved, send, recv, *rest
):
    at = Place()
    head = pl.program_id(0)
    last = pl.num_programs(0) - 1
    size = HEAD_WIDTH // 2
    d_local = col_ref.shape[1]
    e_rows = col_ref.shape[0]

    def columns(block, half):
        lanes = pl.ds(pl.multiple_of(block * d_local, d_local), d_local)
        if half is None:
            return out_full.at[:, lanes]
        return out_full.at[pl.ds(half * (e_rows // 2), e_rows // 2), lanes]

    outs = RingGather(at, col_ref, lambda half: half_rows(col_ref, half), columns, rest)

    def copies(one):
        def copy(index, block, half, peer):
            ref = ctx_ref.at[block, pl.ds(pl.multiple_of(one * HEAD_WIDTH + half * size, size), size)]
            return pltpu.make_async_remote_copy(
                src_ref=ref,
                dst_ref=ref,
                send_sem=send.at[one, index],
                recv_sem=recv.at[one, index],
                device_id={"tensor": peer},
                device_id_type=MESH,
            )

        return (
            copy(0, at.rank, 0, at.across),
            copy(1, at.rank, 1, at.over),
            copy(2, at.rank, 1, at.across),
            copy(3, at.rank, 0, at.over),
            copy(4, at.across, 0, at.over),
            copy(5, at.over, 1, at.across),
        )

    def relay(one):
        group = copies(one)
        group[0].wait_recv()
        group[4].start()
        group[1].wait_recv()
        group[5].start()

    @pl.when(head == 0)
    def _():
        at.greet(True, True)
        outs.start()

    length = length_ref[0]
    keys, vals = qkv_ref[1], qkv_ref[2]
    scale = HEAD_WIDTH ** (-0.5)
    for start in range(0, qkv_ref.shape[2], chunk):
        here = slice(start, start + chunk)
        query = (qkv_ref[0, :, here].astype(F32) * scale).astype(BF)
        scores = masked_scores(keys, query, length)
        top = jnp.max(scores, axis=0, keepdims=True)
        expo = jnp.exp(scores - top)
        total = jnp.sum(expo, axis=0, keepdims=True)
        mixed = contract(vals, expo.astype(BF), (1, 0))
        ctx_ref[at.rank, pl.ds(pl.multiple_of(head * HEAD_WIDTH, HEAD_WIDTH), HEAD_WIDTH), here] = (
            mixed * (1.0 / total)
        ).astype(BF)
        lse_ref[0, :, here] = top + jnp.log(total)

    @pl.when(head > 0)
    def _():
        relay(head - 1)

    for copy in copies(head)[:4]:
        copy.start()

    @pl.when(head == 1)
    def _():
        outs.relay()

    @pl.when(head == last)
    def _():
        relay(last)
        outs.spread()

        def save(one):
            here = pl.ds(pl.multiple_of(one * HEAD_WIDTH, HEAD_WIDTH), HEAD_WIDTH)
            return pltpu.make_async_copy(ctx_ref.at[:, here], ctx_out.at[:, here], saved.at[one])

        def drain(one, carry):
            group = copies(one)
            for copy in group[2:]:
                copy.wait_recv()
            for copy in group:
                copy.wait_send()
            save(one).start()
            return carry

        lax.fori_loop(0, last + 1, drain, 0)
        outs.finish()

        def store(one, carry):
            save(one).wait()
            return carry

        lax.fori_loop(0, last + 1, store, 0)


def attend_send(qkv, lengths, column, chunk, ident):
    _, width, length = qkv.shape
    heads = width // HEAD_WIDTH
    assert heads > 1
    return pl.pallas_call(
        functools.partial(attend_send_body, chunk),
        grid=(heads,),
        out_shape=(
            jax.ShapeDtypeStruct((4, width, length), BF),
            jax.ShapeDtypeStruct((heads, 1, length), F32),
            jax.ShapeDtypeStruct((column.shape[0], 8 * column.shape[1]), BF),
        ),
        in_specs=[
            pl.BlockSpec(memory_space=pltpu.SMEM),
            pl.BlockSpec((3, HEAD_WIDTH, length), lambda h: (0, h, 0)),
            vmem_spec(),
        ],
        out_specs=(
            any_spec(),
            pl.BlockSpec((1, 1, length), lambda h: (h, 0, 0)),
            any_spec(),
        ),
        scratch_shapes=[VMEM((4, width, length), BF), pltpu.SemaphoreType.DMA((heads,))]
        + [pltpu.SemaphoreType.DMA((heads, 6))] * 2
        + RingGather.scratch(),
        compiler_params=pltpu.CompilerParams(
            collective_id=ident, has_side_effects=True, vmem_limit_bytes=BIG
        ),
        name="attend_send",
    )(lengths, qkv, column)


def exact_dot(row, matrix, dims):
    high = row.astype(BF).astype(F32)
    middle = (row - high).astype(BF).astype(F32)
    low = row - high - middle
    shape = (8, row.shape[1])
    index = lax.broadcasted_iota(jnp.int32, shape, 0)
    stacked = jnp.where(
        index == 0, jnp.broadcast_to(high, shape),
        jnp.where(
            index == 1, jnp.broadcast_to(middle, shape),
            jnp.where(index == 2, jnp.broadcast_to(low, shape), 0.0),
        ),
    ).astype(BF)
    return jnp.sum(contract(stacked, matrix, dims), axis=0, keepdims=True)


def classify_body(
    length_ref, bin_ref, normed_ref, up_ref, base_ref, down_ref, head_ref,
    slope_ref, small_ref, hidden_ref, token_ref,
    sums, down_full, head_full, parts, send, recv, *rest,
):
    at = Place()
    step = pl.program_id(0)
    last = pl.num_programs(0) - 1
    units, width = down_full.shape
    chunk = up_ref.shape[1]
    d_local = down_ref.shape[1]
    bins = head_ref.shape[1]

    def columns(block, half):
        lanes = pl.ds(pl.multiple_of(block * d_local, d_local), d_local)
        if half is None:
            return down_full.at[:, lanes]
        return down_full.at[pl.ds(half * (units // 2), units // 2), lanes]

    downs = RingGather(at, down_ref, lambda half: half_rows(down_ref, half), columns, rest[:3])
    heads = RingGather(
        at, head_ref, lambda half: half_rows(head_ref, half),
        lambda block, half: rows_of(head_full, block, half, d_local), rest[3:],
    )

    @pl.when(step == 0)
    def _():
        at.greet(True, True)
        downs.start()
        heads.start()

    pre = jnp.dot(normed_ref[...], up_ref[...], preferred_element_type=F32)
    live = lax.broadcasted_iota(jnp.int32, pre.shape, 0) < length_ref[0]
    square = pre * pre
    bend = jnp.tanh(0.7978845608028654 * (pre * (1.0 + 0.044715 * square)))
    half = 0.5 * (1.0 + bend)
    act = (pre * half).astype(BF).astype(F32)
    sums[:, pl.ds(pl.multiple_of(step * chunk, chunk), chunk)] = jnp.sum(
        jnp.where(live, act, 0.0), axis=0, keepdims=True
    )
    inner = 0.7978845608028654 * (1.0 + 3 * 0.044715 * square)
    slope = half + 0.5 * pre * (1.0 - bend * bend) * inner
    slope_ref[...] = jnp.where(live, slope, 0.0).astype(BF)

    @pl.when(step == last)
    def _():
        downs.relay()
        heads.relay()
        downs.spread()
        heads.spread()
        downs.finish()
        heads.finish()
        hidden_sum = sums[...]
        parts[at.rank] = exact_dot(hidden_sum, down_full[...], (1, 0))
        copies = [
            remote(parts.at[at.rank], parts.at[at.rank], (send, recv), index, {"tensor": peer})
            for index, peer in enumerate((at.across, at.over, at.diag))
        ]
        for copy in copies:
            copy.start()
        for copy in copies:
            copy.wait()
        count = jnp.full((1, 1), length_ref[0], jnp.int32).astype(F32)
        total = base_ref[...]
        for index in range(4):
            total = total + parts[index]
        pooled = total / count
        mean = jnp.mean(pooled, axis=-1, keepdims=True)
        centered = pooled - mean
        scale = lax.rsqrt(jnp.mean(centered * centered, axis=-1, keepdims=True) + EPS)
        final = centered * scale
        logits = exact_dot(final, head_full[...], (1, 0))
        top = jnp.max(logits, axis=-1, keepdims=True)
        total_exp = jnp.log(jnp.sum(jnp.exp(logits - top), axis=-1, keepdims=True)) + top
        labels = (lax.broadcasted_iota(jnp.int32, logits.shape, 1) == bin_ref[0]).astype(F32)
        loss = total_exp - jnp.sum(logits * labels, axis=-1, keepdims=True)
        g_logits = (jnp.exp(logits - total_exp) - labels) / 8.0
        g_final = exact_dot(g_logits, head_full[...], (1, 1))
        g_pooled = scale * (
            g_final
            - jnp.mean(g_final, axis=-1, keepdims=True)
            - final * jnp.mean(g_final * final, axis=-1, keepdims=True)
        )
        per_token = g_pooled / count
        rounded = per_token.astype(BF)
        token_ref[...] = per_token
        hidden_ref[...] = contract(
            jnp.broadcast_to(rounded.astype(F32), (8, width)).astype(BF), down_full[...], (1, 1)
        )[:1]
        small_ref[:, :units] = hidden_sum
        small_ref[:, units : units + width] = rounded.astype(F32)
        small_ref[:, units + width : units + 2 * width] = final
        small_ref[:, units + 2 * width : units + 2 * width + bins] = g_logits
        small_ref[:, units + 2 * width + bins :] = jnp.broadcast_to(loss, (1, 128))


def classify(normed, up, base, down, head, lengths, bins_at, chunk, ident):
    length, width = normed.shape
    units = up.shape[1]
    bins = head.shape[1]
    return pl.pallas_call(
        classify_body,
        grid=(units // chunk,),
        out_shape=(
            jax.ShapeDtypeStruct((length, units), BF),
            jax.ShapeDtypeStruct((1, units + 2 * width + bins + 128), F32),
            jax.ShapeDtypeStruct((1, units), F32),
            jax.ShapeDtypeStruct((1, width), F32),
        ),
        in_specs=[
            pl.BlockSpec(memory_space=pltpu.SMEM),
            pl.BlockSpec(memory_space=pltpu.SMEM),
            vmem_spec(),
            pl.BlockSpec((width, chunk), lambda f: (0, f)),
            vmem_spec(),
            vmem_spec(),
            vmem_spec(),
        ],
        out_specs=(
            pl.BlockSpec((length, chunk), lambda f: (0, f)),
            vmem_spec(),
            vmem_spec(),
            vmem_spec(),
        ),
        scratch_shapes=[
            VMEM((1, units), F32),
            VMEM((units, width), BF),
            VMEM((width, bins), BF),
            VMEM((4, 1, width), F32),
            pltpu.SemaphoreType.DMA((3,)),
            pltpu.SemaphoreType.DMA((3,)),
        ]
        + RingGather.scratch()
        + RingGather.scratch(),
        compiler_params=pltpu.CompilerParams(
            collective_id=ident, has_side_effects=True, vmem_limit_bytes=BIG
        ),
        name="classify",
    )(lengths, bins_at, normed, up, base, down, head)


def per_device_block(
    token_ids,
    lengths,
    teacher_bins,
    embed_table,
    query_key_value_matrix,
    output_matrix,
    up_matrix,
    down_matrix,
    w_head,
):
    ranks = lax.axis_size("tensor")
    groups = lax.axis_size("dp")
    rank = lax.axis_index("tensor")
    group = lax.axis_index("dp")
    assert token_ids.shape[0] == 1
    local_len = token_ids.shape[1]
    span = local_len * ranks
    vocab_local, width = embed_table.shape
    d_local, _, e_local = query_key_value_matrix.shape
    f_local = up_matrix.shape[1]
    bins = w_head.shape[1]
    exact = lax.Precision.HIGHEST

    all_ids, out_columns = share_ids(token_ids, output_matrix, 11)
    all_ids = all_ids.reshape(ranks, local_len)
    shifted = all_ids - rank * vocab_local
    inside = (shifted >= 0) & (shifted < vocab_local)
    rows = jnp.take(embed_table, jnp.clip(shifted, 0, vocab_local - 1), axis=0)
    first, normed_one, qkv, up_full = embed(
        jnp.where(inside[..., None], rows, jnp.zeros((), BF)),
        query_key_value_matrix.transpose(1, 0, 2),
        up_matrix,
        12,
    )
    first = first.reshape(span, width)
    normed_one = normed_one.reshape(span, width)
    chunk = min(256, span)
    context, lse, out_full = attend_send(
        qkv, lengths, out_columns.reshape(ranks * e_local, d_local), chunk, 13
    )
    context_all = context.reshape(ranks * e_local, span)
    attn = lax.dot_general(
        context_all, out_full, (((0,), (0,)), ((), ())), preferred_element_type=F32
    )
    second = (first.astype(F32) + attn).astype(BF)
    normed_f, norm_back = jax.vjp(normalize, second.astype(F32))
    normed_two = normed_f.astype(BF)
    live = (jnp.arange(span, dtype=jnp.int32) < lengths[0]).astype(F32)
    second_sum = jnp.sum(second.astype(F32) * live[:, None], axis=0, keepdims=True)
    slope, packed, g_hidden, per_token = classify(
        normed_two, up_full, second_sum, down_matrix, w_head, lengths, teacher_bins,
        min(256, f_local), 14,
    )

    over_seqs = (((0,), (0,)), ((), ()))
    up_base = lax.dot_general(normed_two, slope, over_seqs, preferred_element_type=F32)
    up_term = (up_base * g_hidden).astype(BF).reshape(groups, d_local, f_local)
    g_pre = (slope.astype(F32) * g_hidden).astype(BF)
    g_normed = lax.dot_general(
        g_pre, up_full, (((1,), (1,)), ((), ())), preferred_element_type=F32
    )
    g_second = (
        norm_back(g_normed)[0] + live[:, None] * (per_token / ranks)
    ).astype(BF)
    spread = lax.dot_general(
        out_full, g_second, (((1,), (1,)), ((), ())), preferred_element_type=F32
    ).astype(BF)
    g_context, up_weight_gradient, every = scatter_and_group(
        spread.reshape(ranks, e_local, span), up_term, packed, ranks, 6
    )
    every = every[:, 0]
    hidden_every = every[:, :f_local]
    rounded_every = every[:, f_local : f_local + width]
    final_every = every[:, f_local + width : f_local + 2 * width]
    rest = every[:, f_local + 2 * width :]
    loss = jnp.sum(rest[:, bins]) / groups
    mine = group * d_local
    down_weight_gradient = lax.dot_general(
        hidden_every,
        lax.dynamic_slice_in_dim(rounded_every, mine, d_local, axis=1),
        over_seqs,
        precision=exact,
    )
    grad_head = lax.dot_general(
        lax.dynamic_slice_in_dim(final_every, mine, d_local, axis=1),
        rest[:, :bins],
        over_seqs,
        precision=exact,
    )

    out_term = (
        jnp.dot(context_all, g_second, preferred_element_type=F32)
        .astype(BF)
        .reshape(ranks, e_local, width)
    )
    g_qkv, out_mine = attend_back(qkv, lengths, lse, g_context, out_term, groups, chunk, 7)
    qkv_term = lax.dot_general(
        normed_one,
        g_qkv.reshape(3 * e_local, span),
        (((0,), (1,)), ((), ())),
        preferred_element_type=F32,
    )
    qkv_gradient, output_weight_gradient = group_sum(
        [qkv_term.astype(BF).reshape(groups, d_local, 3 * e_local), out_mine], 8
    )
    query_key_value_gradient = qkv_gradient.reshape(d_local, 3, e_local)
    return (
        loss,
        query_key_value_gradient,
        output_weight_gradient,
        up_weight_gradient,
        down_weight_gradient,
        grad_head,
    )


def solution(mesh):
    placed = (
        P("dp", "tensor"),
        P("dp"),
        P("dp"),
        P("tensor", None),
        P("dp", None, "tensor"),
        P("tensor", "dp"),
        P("dp", "tensor"),
        P("tensor", "dp"),
        P("dp", None),
    )
    return jax.shard_map(
        per_device_block if (mesh.shape["tensor"], mesh.shape["dp"]) == (4, 8) else per_device,
        mesh=mesh,
        in_specs=placed,
        out_specs=(
            P(),
            P("dp", None, "tensor"),
            P("tensor", "dp"),
            P("dp", "tensor"),
            P("tensor", "dp"),
            P("dp", None),
        ),
        check_vma=False,
    )
```

```python
import functools

import jax
import jax.numpy as jnp
from jax import lax
from jax.experimental import pallas as pl
from jax.experimental.pallas import tpu as pltpu
from jax.sharding import PartitionSpec as P

HEAD_WIDTH = 64
EPS = 1e-05
BF = jnp.bfloat16
F32 = jnp.float32
MESH = pl.DeviceIdType.MESH
VMEM = pltpu.VMEM
BIG = 60 * 1024 * 1024


def normalize(values):
    mean = jnp.mean(values, axis=-1, keepdims=True)
    centered = values - mean
    return centered * lax.rsqrt(jnp.mean(centered * centered, axis=-1, keepdims=True) + EPS)


def vmem_spec():
    return pl.BlockSpec(memory_space=pltpu.VMEM)


def greet(axis, count):
    me = lax.axis_index(axis)
    barrier = pltpu.get_barrier_semaphore()
    for step in range(1, count):
        pl.semaphore_signal(
            barrier, inc=1, device_id={axis: lax.rem(me + step, count)}, device_id_type=MESH
        )
    pl.semaphore_wait(barrier, count - 1)
    return me


def gather_body(axis, count, x_ref, out_ref, send_sem, recv_sem):
    me = greet(axis, count)
    copies = []
    for step in range(1, count):
        copy = pltpu.make_async_remote_copy(
            src_ref=x_ref,
            dst_ref=out_ref.at[me],
            send_sem=send_sem.at[step - 1],
            recv_sem=recv_sem.at[step - 1],
            device_id={axis: lax.rem(me + step, count)},
            device_id_type=MESH,
        )
        copy.start()
        copies.append(copy)
    out_ref[me] = x_ref[...]
    for copy in copies:
        copy.wait()


def relay_gather(axis, me, src, out, send_sem, recv_sem):
    across = me + 1 - 2 * lax.rem(me, 2)
    over = lax.rem(me + 2, 4)
    half = src.shape[0] // 2
    low, high = pl.ds(0, half), pl.ds(half, half)

    def copy(index, src_part, block, part, device):
        return pltpu.make_async_remote_copy(
            src_ref=src_part,
            dst_ref=out.at[block, part],
            send_sem=send_sem.at[index],
            recv_sem=recv_sem.at[index],
            device_id={axis: device},
            device_id_type=MESH,
        )

    first_a = copy(0, src.at[low], me, low, across)
    first_b = copy(1, src.at[high], me, high, over)
    second_a = copy(2, src.at[high], me, high, across)
    second_b = copy(3, src.at[low], me, low, over)
    for one in (first_a, first_b, second_a, second_b):
        one.start()
    first_a.wait_recv()
    pass_b = copy(4, out.at[across, low], across, low, over)
    pass_b.start()
    first_b.wait_recv()
    pass_a = copy(5, out.at[over, high], over, high, across)
    pass_a.start()
    second_a.wait_recv()
    second_b.wait_recv()
    pass_b.wait_recv()
    pass_a.wait_recv()
    for one in (first_a, first_b, second_a, second_b, pass_b, pass_a):
        one.wait_send()


def relay_body(axis, x_ref, out_ref, send_sem, recv_sem):
    me = greet(axis, 4)
    relay_gather(axis, me, x_ref, out_ref, send_sem, recv_sem)
    out_ref[me] = x_ref[...]


def gather_blocks(x, axis, count, ident):
    if count != 4:
        return gather_all(x, axis, count, ident)
    return pl.pallas_call(
        functools.partial(relay_body, axis),
        out_shape=jax.ShapeDtypeStruct((count,) + x.shape, x.dtype),
        in_specs=[vmem_spec()],
        out_specs=vmem_spec(),
        scratch_shapes=[pltpu.SemaphoreType.DMA((6,)), pltpu.SemaphoreType.DMA((6,))],
        compiler_params=pltpu.CompilerParams(collective_id=ident, has_side_effects=True),
        name="gather_blocks",
    )(x)


def gather_all(x, axis, count, ident):
    return pl.pallas_call(
        functools.partial(gather_body, axis, count),
        out_shape=jax.ShapeDtypeStruct((count,) + x.shape, x.dtype),
        in_specs=[vmem_spec()],
        out_specs=vmem_spec(),
        scratch_shapes=[
            pltpu.SemaphoreType.DMA((count - 1,)),
            pltpu.SemaphoreType.DMA((count - 1,)),
        ],
        compiler_params=pltpu.CompilerParams(collective_id=ident, has_side_effects=True),
        name="gather_all",
    )(x)


def scatter_copies(axis, count, me, x_ref, held, send_sem, recv_sem):
    copies = []
    for step in range(1, count):
        peer = lax.rem(me + step, count)
        copies.append(
            pltpu.make_async_remote_copy(
                src_ref=x_ref.at[peer],
                dst_ref=held.at[step - 1],
                send_sem=send_sem.at[step - 1],
                recv_sem=recv_sem.at[step - 1],
                device_id={axis: peer},
                device_id_type=MESH,
            )
        )
    return copies


def scatter_start(*args):
    for copy in scatter_copies(*args):
        copy.start()


def scatter_finish(axis, count, me, x_ref, held, send_sem, recv_sem, put):
    for copy in scatter_copies(axis, count, me, x_ref, held, send_sem, recv_sem):
        copy.wait()

    def body(at):
        total = x_ref[me, at].astype(F32)
        for step in range(1, count):
            total = total + held[step - 1, at].astype(F32)
        put(at, total)

    add_tiles(x_ref.shape[1], 32, body)


def add_tiles(rows, tile, body):
    def step(index, carry):
        body(pl.ds(pl.multiple_of(index * tile, tile), tile))
        return carry

    lax.fori_loop(0, rows // tile, step, 0)


class GroupSum:
    def __init__(self, x_ref, out_ref, pair, mine, far, sems):
        self.x, self.out, self.pair, self.mine, self.far = x_ref, out_ref, pair, mine, far
        self.sems = sems
        self.groups = x_ref.shape[0]
        self.chips = self.groups // 2
        self.rows = x_ref.shape[1]
        me = lax.axis_index("dp")
        self.core = lax.rem(me, 2)
        self.chip = me // 2
        self.near = self.chip * 2 + 1 - self.core

    @staticmethod
    def scratch(shape, dtype):
        groups, rows, columns = shape
        chips = groups // 2
        return [
            VMEM((chips, rows, columns), dtype),
            VMEM((chips, rows, columns), dtype),
            VMEM((chips - 1, rows, columns), dtype),
            pltpu.SemaphoreType.DMA((chips,)),
            pltpu.SemaphoreType.DMA((chips,)),
            pltpu.SemaphoreType.DMA((6 if chips == 4 else chips - 1,)),
            pltpu.SemaphoreType.DMA((6 if chips == 4 else chips - 1,)),
        ]

    def signal(self, barrier):
        pl.semaphore_signal(
            barrier, inc=1, device_id={"dp": self.near}, device_id_type=MESH
        )
        for step in range(1, self.chips):
            pl.semaphore_signal(
                barrier, inc=1, device_id={"dp": self.owner(step)}, device_id_type=MESH
            )
        return self.chips

    def owner(self, step):
        return lax.rem(self.chip + step, self.chips) * 2 + self.core

    def pair_copies(self):
        copies = []
        for chip in range(self.chips):
            copies.append(
                pltpu.make_async_remote_copy(
                    src_ref=self.x.at[chip * 2 + 1 - self.core],
                    dst_ref=self.pair.at[chip],
                    send_sem=self.sems[0].at[chip],
                    recv_sem=self.sems[1].at[chip],
                    device_id={"dp": self.near},
                    device_id_type=MESH,
                )
            )
        return copies

    def far_copies(self):
        copies = []
        for step in range(1, self.chips):
            copies.append(
                pltpu.make_async_remote_copy(
                    src_ref=self.mine.at[lax.rem(self.chip + step, self.chips)],
                    dst_ref=self.far.at[step - 1],
                    send_sem=self.sems[2].at[step - 1],
                    recv_sem=self.sems[3].at[step - 1],
                    device_id={"dp": self.owner(step)},
                    device_id_type=MESH,
                )
            )
        return copies

    def ring_copies(self):
        right, left = lax.rem(self.chip + 1, 4), lax.rem(self.chip + 3, 4)
        opposite = lax.rem(self.chip + 2, 4)
        half = self.rows // 2
        low, high = pl.ds(0, half), pl.ds(half, half)

        def copy(index, block, part, slot, chip):
            return pltpu.make_async_remote_copy(
                src_ref=self.mine.at[block, part],
                dst_ref=self.far.at[slot, part],
                send_sem=self.sems[2].at[index],
                recv_sem=self.sems[3].at[index],
                device_id={"dp": chip * 2 + self.core},
                device_id_type=MESH,
            )

        return (
            copy(0, opposite, low, 2, right),
            copy(1, opposite, high, 2, left),
            copy(2, right, high, 0, right),
            copy(3, left, low, 1, left),
            copy(4, right, low, 0, right),
            copy(5, left, high, 1, left),
        )

    def relay(self):
        if self.chips != 4:
            return
        copies = self.ring_copies()
        half = self.rows // 2
        for index, step, base in ((0, 1, 0), (1, 3, half)):
            copies[index].wait_recv()
            block = lax.rem(self.chip + step, 4)

            def body(at, block=block, base=base):
                here = pl.ds(base + at.start, at.size)
                self.mine[block, here] = (
                    self.mine[block, here].astype(F32) + self.far[2, here].astype(F32)
                ).astype(self.mine.dtype)

            add_tiles(half, 32, body)
            copies[index + 4].start()

    def start(self):
        for copy in self.pair_copies():
            copy.start()

    def middle(self):
        for copy in self.pair_copies():
            copy.wait()

        for chip in range(self.chips):

            def body(at, chip=chip):
                self.mine[chip, at] = (
                    self.x[chip * 2 + self.core, at].astype(F32)
                    + self.pair[chip, at].astype(F32)
                ).astype(self.mine.dtype)

            add_tiles(self.rows, 32, body)
        copies = self.ring_copies()[:4] if self.chips == 4 else self.far_copies()
        for copy in copies:
            copy.start()

    def finish(self):
        if self.chips == 4:
            copies = self.ring_copies()
            for copy in copies[2:]:
                copy.wait()
            for copy in copies[:2]:
                copy.wait_send()
        else:
            for copy in self.far_copies():
                copy.wait()

        def body(at):
            total = self.mine[self.chip, at].astype(F32)
            for step in range(2 if self.chips == 4 else self.chips - 1):
                total = total + self.far[step, at].astype(F32)
            self.out[at] = total

        add_tiles(self.rows, 32, body)


def scatter_and_group_body(
    count, x_ref, up_ref, small_ref, out_ref, up_out, small_out, held, send_sem, recv_sem, *rest
):
    up = GroupSum(up_ref, up_out, rest[0], rest[1], rest[2], rest[3:7])
    small_send, small_recv = rest[7:]
    groups = small_out.shape[0]
    group = lax.axis_index("dp")
    barrier = pltpu.get_barrier_semaphore()
    me = lax.axis_index("tensor")
    for step in range(1, count):
        pl.semaphore_signal(
            barrier, inc=1, device_id={"tensor": lax.rem(me + step, count)}, device_id_type=MESH
        )
    for step in range(1, groups):
        pl.semaphore_signal(
            barrier, inc=1, device_id={"dp": lax.rem(group + step, groups)}, device_id_type=MESH
        )
    pl.semaphore_wait(barrier, count + groups - 2)
    smalls = []
    for step in range(1, groups):
        smalls.append(
            pltpu.make_async_remote_copy(
                src_ref=small_ref,
                dst_ref=small_out.at[group],
                send_sem=small_send.at[step - 1],
                recv_sem=small_recv.at[step - 1],
                device_id={"dp": lax.rem(group + step, groups)},
                device_id_type=MESH,
            )
        )

    def put(at, total):
        out_ref[at] = total.astype(out_ref.dtype)

    up.start()
    scatter_start("tensor", count, me, x_ref, held, send_sem, recv_sem)
    up.middle()
    for copy in smalls:
        copy.start()
    small_out[group] = small_ref[...]
    up.relay()
    scatter_finish("tensor", count, me, x_ref, held, send_sem, recv_sem, put)
    up.finish()
    for copy in smalls:
        copy.wait()


def scatter_and_group(x, up, small, count, ident):
    return pl.pallas_call(
        functools.partial(scatter_and_group_body, count),
        out_shape=(
            jax.ShapeDtypeStruct(x.shape[1:], x.dtype),
            jax.ShapeDtypeStruct(up.shape[1:], F32),
            jax.ShapeDtypeStruct(up.shape[:1] + small.shape, F32),
        ),
        in_specs=[vmem_spec()] * 3,
        out_specs=(vmem_spec(),) * 3,
        scratch_shapes=[
            VMEM((count - 1,) + x.shape[1:], x.dtype),
            pltpu.SemaphoreType.DMA((count - 1,)),
            pltpu.SemaphoreType.DMA((count - 1,)),
        ]
        + GroupSum.scratch(up.shape, up.dtype)
        + [pltpu.SemaphoreType.DMA((up.shape[0] - 1,))] * 2,
        compiler_params=pltpu.CompilerParams(
            collective_id=ident, has_side_effects=True, vmem_limit_bytes=BIG
        ),
        name="scatter_and_group",
    )(x, up, small)


def group_sum_body(number, *refs):
    xs, outs, rest = refs[:number], refs[number : 2 * number], refs[2 * number :]
    sums = [
        GroupSum(x, out, *rest[7 * i : 7 * i + 3], rest[7 * i + 3 : 7 * i + 7])
        for i, (x, out) in enumerate(zip(xs, outs))
    ]
    barrier = pltpu.get_barrier_semaphore()
    pl.semaphore_wait(barrier, sums[0].signal(barrier))
    for one in sums:
        one.start()
    for one in sums:
        one.middle()
    for one in sums:
        one.relay()
    for one in sums:
        one.finish()


def group_sum(arrays, ident):
    number = len(arrays)
    scratch = []
    for array in arrays:
        scratch += GroupSum.scratch(array.shape, array.dtype)
    return pl.pallas_call(
        functools.partial(group_sum_body, number),
        out_shape=tuple(jax.ShapeDtypeStruct(a.shape[1:], F32) for a in arrays),
        in_specs=[vmem_spec()] * number,
        out_specs=(vmem_spec(),) * number,
        scratch_shapes=scratch,
        compiler_params=pltpu.CompilerParams(
            collective_id=ident, has_side_effects=True, vmem_limit_bytes=BIG
        ),
        name="group_sum",
    )(*arrays)


def sum_all_body(axis, count, x_ref, out_ref, held, send_sem, recv_sem, send_two, recv_two):
    me = greet(axis, count)

    def put(at, total):
        out_ref[me, at] = total.astype(out_ref.dtype)

    scatter_start(axis, count, me, x_ref, held, send_sem, recv_sem)
    scatter_finish(axis, count, me, x_ref, held, send_sem, recv_sem, put)
    if count == 4:
        relay_gather(axis, me, out_ref.at[me], out_ref, send_two, recv_two)
        return
    copies = []
    for step in range(1, count):
        copy = pltpu.make_async_remote_copy(
            src_ref=out_ref.at[me],
            dst_ref=out_ref.at[me],
            send_sem=send_two.at[step - 1],
            recv_sem=recv_two.at[step - 1],
            device_id={axis: lax.rem(me + step, count)},
            device_id_type=MESH,
        )
        copy.start()
        copies.append(copy)
    for copy in copies:
        copy.wait()


def sum_all(x, axis, count, ident):
    return pl.pallas_call(
        functools.partial(sum_all_body, axis, count),
        out_shape=jax.ShapeDtypeStruct(x.shape, x.dtype),
        in_specs=[vmem_spec()],
        out_specs=vmem_spec(),
        scratch_shapes=[VMEM((count - 1,) + x.shape[1:], x.dtype)]
        + [pltpu.SemaphoreType.DMA((count - 1,))] * 2
        + [pltpu.SemaphoreType.DMA((6 if count == 4 else count - 1,))] * 2,
        compiler_params=pltpu.CompilerParams(collective_id=ident, has_side_effects=True),
        name="sum_all",
    )(x)


def contract(left, right, dims):
    return lax.dot_general(left, right, ((dims[:1], dims[1:]), ((), ())), preferred_element_type=F32)


def masked_scores(keys, query, length):
    scores = contract(keys, query, (0, 0))
    position = lax.broadcasted_iota(jnp.int32, scores.shape, 0)
    return jnp.where(position < length, scores, -1e30)


def attend_body(chunk, length_ref, qkv_ref, out_ref, lse_ref):
    length = length_ref[0]
    keys, vals = qkv_ref[1], qkv_ref[2]
    scale = HEAD_WIDTH ** (-0.5)
    for at in range(0, qkv_ref.shape[2], chunk):
        query = (qkv_ref[0, :, at : at + chunk].astype(F32) * scale).astype(BF)
        scores = masked_scores(keys, query, length)
        top = jnp.max(scores, axis=0, keepdims=True)
        expo = jnp.exp(scores - top)
        total = jnp.sum(expo, axis=0, keepdims=True)
        mixed = contract(vals, expo.astype(BF), (1, 0))
        out_ref[:, at : at + chunk] = (mixed * (1.0 / total)).astype(BF)
        lse_ref[0, :, at : at + chunk] = top + jnp.log(total)


def attend(qkv, lengths, chunk):
    _, width, length = qkv.shape
    heads = width // HEAD_WIDTH
    return pl.pallas_call(
        functools.partial(attend_body, chunk),
        grid=(heads,),
        out_shape=(
            jax.ShapeDtypeStruct((width, length), BF),
            jax.ShapeDtypeStruct((heads, 1, length), F32),
        ),
        in_specs=[
            pl.BlockSpec(memory_space=pltpu.SMEM),
            pl.BlockSpec((3, HEAD_WIDTH, length), lambda h: (0, h, 0)),
        ],
        out_specs=(
            pl.BlockSpec((HEAD_WIDTH, length), lambda h: (h, 0)),
            pl.BlockSpec((1, 1, length), lambda h: (h, 0, 0)),
        ),
        cost_estimate=pl.CostEstimate(
            flops=4 * width * length * length,
            bytes_accessed=8 * width * length,
            transcendentals=heads * length * length,
        ),
        compiler_params=pltpu.CompilerParams(vmem_limit_bytes=BIG),
        name="attend",
    )(lengths, qkv)


def attend_back_body(
    chunk, ranks, length_ref, qkv_ref, lse_ref, grad_ref, x_ref, out_ref, x_out, held, send_sem, recv_sem
):
    me = lax.axis_index("tensor")
    args = ("tensor", ranks, me, x_ref, held, send_sem, recv_sem)

    @pl.when(pl.program_id(0) == 0)
    def _():
        greet("tensor", ranks)
        scatter_start(*args)

    attend_back_head(chunk, length_ref, qkv_ref, lse_ref, grad_ref, out_ref)

    @pl.when(pl.program_id(0) == pl.num_programs(0) - 1)
    def _():
        piece = x_out.shape[2]

        def put(at, total):
            for group in range(x_out.shape[0]):
                x_out[group, at] = total[:, group * piece : (group + 1) * piece].astype(BF)

        scatter_finish(*args, put)


def attend_back_head(chunk, length_ref, qkv_ref, lse_ref, grad_ref, out_ref):
    length = length_ref[0]
    keys, vals = qkv_ref[1], qkv_ref[2]
    scale = HEAD_WIDTH ** (-0.5)
    span = qkv_ref.shape[2]
    g_keys = jnp.zeros((HEAD_WIDTH, span), F32)
    g_vals = jnp.zeros((HEAD_WIDTH, span), F32)
    for at in range(0, span, chunk):
        here = slice(at, at + chunk)
        query = (qkv_ref[0, :, here].astype(F32) * scale).astype(BF)
        grad = grad_ref[:, here]
        probs = jnp.exp(masked_scores(keys, query, length) - lse_ref[0, :, here])
        g_probs = contract(vals, grad, (0, 0))
        weighted = probs * g_probs
        inner = jnp.sum(weighted, axis=0, keepdims=True)
        g_scores = (weighted - probs * inner).astype(BF)
        out_ref[0, :, here] = (contract(keys, g_scores, (1, 0)) * scale).astype(BF)
        g_keys += contract(query, g_scores, (1, 1))
        g_vals += contract(grad, probs.astype(BF), (1, 1))
    out_ref[1] = g_keys.astype(BF)
    out_ref[2] = g_vals.astype(BF)


def attend_back(qkv, lengths, lse, grad, x, groups, chunk, ident):
    _, width, length = qkv.shape
    heads = width // HEAD_WIDTH
    return pl.pallas_call(
        functools.partial(attend_back_body, chunk, x.shape[0]),
        grid=(heads,),
        out_shape=(
            jax.ShapeDtypeStruct(qkv.shape, BF),
            jax.ShapeDtypeStruct((groups, x.shape[1], x.shape[2] // groups), BF),
        ),
        in_specs=[
            pl.BlockSpec(memory_space=pltpu.SMEM),
            pl.BlockSpec((3, HEAD_WIDTH, length), lambda h: (0, h, 0)),
            pl.BlockSpec((1, 1, length), lambda h: (h, 0, 0)),
            pl.BlockSpec((HEAD_WIDTH, length), lambda h: (h, 0)),
            vmem_spec(),
        ],
        out_specs=(
            pl.BlockSpec((3, HEAD_WIDTH, length), lambda h: (0, h, 0)),
            vmem_spec(),
        ),
        scratch_shapes=[
            VMEM((x.shape[0] - 1,) + x.shape[1:], x.dtype),
            pltpu.SemaphoreType.DMA((x.shape[0] - 1,)),
            pltpu.SemaphoreType.DMA((x.shape[0] - 1,)),
        ],
        cost_estimate=pl.CostEstimate(
            flops=10 * width * length * length,
            bytes_accessed=14 * width * length,
            transcendentals=heads * length * length,
        ),
        compiler_params=pltpu.CompilerParams(
            collective_id=ident, has_side_effects=True, vmem_limit_bytes=BIG
        ),
        name="attend_back",
    )(lengths, qkv, lse, grad, x)


def hidden_body(length_ref, normed_ref, up_ref, slope_ref, sum_ref):
    pre = jnp.dot(normed_ref[...], up_ref[...], preferred_element_type=F32)
    live = lax.broadcasted_iota(jnp.int32, pre.shape, 0) < length_ref[0]
    square = pre * pre
    bend = jnp.tanh(0.7978845608028654 * (pre * (1.0 + 0.044715 * square)))
    half = 0.5 * (1.0 + bend)
    act = (pre * half).astype(BF).astype(F32)
    sum_ref[...] = jnp.sum(jnp.where(live, act, 0.0), axis=0, keepdims=True)
    inner = 0.7978845608028654 * (1.0 + 3 * 0.044715 * square)
    slope = half + 0.5 * pre * (1.0 - bend * bend) * inner
    slope_ref[...] = jnp.where(live, slope, 0.0).astype(BF)


def hidden(normed, up, lengths, chunk):
    length, width = normed.shape
    units = up.shape[1]
    return pl.pallas_call(
        hidden_body,
        grid=(units // chunk,),
        out_shape=(
            jax.ShapeDtypeStruct((length, units), BF),
            jax.ShapeDtypeStruct((1, units), F32),
        ),
        in_specs=[
            pl.BlockSpec(memory_space=pltpu.SMEM),
            pl.BlockSpec((length, width), lambda f: (0, 0)),
            pl.BlockSpec((width, chunk), lambda f: (0, f)),
        ],
        out_specs=(
            pl.BlockSpec((length, chunk), lambda f: (0, f)),
            pl.BlockSpec((1, chunk), lambda f: (0, f)),
        ),
        cost_estimate=pl.CostEstimate(
            flops=2 * length * width * units,
            bytes_accessed=6 * length * units,
            transcendentals=length * units,
        ),
        compiler_params=pltpu.CompilerParams(vmem_limit_bytes=BIG),
        name="hidden",
    )(lengths, normed, up)


def per_device(
    token_ids,
    lengths,
    teacher_bins,
    embed_table,
    query_key_value_matrix,
    output_matrix,
    up_matrix,
    down_matrix,
    w_head,
):
    ranks = lax.axis_size("tensor")
    groups = lax.axis_size("dp")
    rank = lax.axis_index("tensor")
    group = lax.axis_index("dp")
    assert token_ids.shape[0] == 1
    local_len = token_ids.shape[1]
    span = local_len * ranks
    vocab_local, width = embed_table.shape
    d_local, _, e_local = query_key_value_matrix.shape
    f_local = up_matrix.shape[1]
    bins = w_head.shape[1]
    exact = lax.Precision.HIGHEST

    qkv_full = lax.all_gather(
        query_key_value_matrix.reshape(d_local, 3 * e_local), "dp", axis=0, tiled=True
    )
    out_parts = lax.all_gather(output_matrix, ("tensor", "dp"), axis=0, tiled=False)
    out_full = (
        out_parts.reshape(ranks, groups, e_local, d_local)
        .transpose(0, 2, 1, 3)
        .reshape(ranks * e_local, width)
    )
    up_full = lax.all_gather(up_matrix, "dp", axis=0, tiled=True)
    low = lax.all_gather(
        jnp.concatenate([down_matrix, w_head.reshape(bins, d_local)], axis=0), "dp", axis=0, tiled=False
    )
    down_full = low[:, :f_local]
    head_wide = low[:, f_local:].reshape(width, bins).astype(F32)

    all_ids = gather_all(token_ids, "tensor", ranks, 1).reshape(ranks, local_len)
    shifted = all_ids - rank * vocab_local
    inside = (shifted >= 0) & (shifted < vocab_local)
    rows = jnp.take(embed_table, jnp.clip(shifted, 0, vocab_local - 1), axis=0)
    first = sum_all(
        jnp.where(inside[..., None], rows, jnp.zeros((), BF)), "tensor", ranks, 2
    ).reshape(span, width)
    normed_one = normalize(first.astype(F32)).astype(BF)
    qkv = (
        lax.dot_general(qkv_full, normed_one, (((0,), (1,)), ((), ())), preferred_element_type=F32)
        .astype(BF)
        .reshape(3, e_local, span)
    )
    chunk = min(256, span)
    context, lse = attend(qkv, lengths, chunk)
    context_all = gather_blocks(context, "tensor", ranks, 3).reshape(ranks * e_local, span)
    attn = lax.dot_general(
        context_all, out_full, (((0,), (0,)), ((), ())), preferred_element_type=F32
    )
    second = (first.astype(F32) + attn).astype(BF)
    normed_f, norm_back = jax.vjp(normalize, second.astype(F32))
    normed_two = normed_f.astype(BF)
    slope, hidden_sum = hidden(normed_two, up_full, lengths, min(256, f_local))

    live = (jnp.arange(span, dtype=jnp.int32) < lengths[0]).astype(F32)
    count = lengths.astype(F32)[:, None]
    ffn_part = jnp.einsum(
        "of,jfd->ojd", hidden_sum, down_full.astype(F32), precision=exact
    ).reshape(1, width)
    ffn_all = gather_all(ffn_part, "tensor", ranks, 4)
    second_sum = jnp.sum(second.astype(F32) * live[:, None], axis=0, keepdims=True)
    pooled = (second_sum + jnp.sum(ffn_all, axis=0)) / count
    final, final_back = jax.vjp(normalize, pooled)
    logits = jnp.dot(final, head_wide, precision=exact)
    top = jnp.max(logits, axis=-1, keepdims=True)
    total_exp = jnp.log(jnp.sum(jnp.exp(logits - top), axis=-1, keepdims=True)) + top
    labels = (teacher_bins[:, None] == jnp.arange(bins, dtype=jnp.int32)[None, :]).astype(F32)
    loss_here = total_exp - jnp.sum(logits * labels, axis=-1, keepdims=True)
    g_logits = (jnp.exp(logits - total_exp) - labels) / groups
    g_final = jnp.dot(g_logits, head_wide.T, precision=exact)
    per_token = final_back(g_final)[0] / count
    rounded = per_token.astype(BF).astype(F32)
    g_hidden = jnp.einsum(
        "ojd,jfd->of",
        rounded.reshape(1, groups, d_local),
        down_full.astype(F32),
        precision=exact,
    )

    packed = jnp.concatenate(
        [hidden_sum, rounded, final, g_logits, jnp.broadcast_to(loss_here, (1, 128))], axis=1
    )

    over_seqs = (((0,), (0,)), ((), ()))
    up_base = lax.dot_general(normed_two, slope, over_seqs, preferred_element_type=F32)
    up_term = (up_base * g_hidden).astype(BF).reshape(groups, d_local, f_local)
    g_pre = (slope.astype(F32) * g_hidden).astype(BF)
    g_normed = lax.dot_general(
        g_pre, up_full, (((1,), (1,)), ((), ())), preferred_element_type=F32
    )
    g_second = (
        norm_back(g_normed)[0] + live[:, None] * (per_token / ranks)
    ).astype(BF)
    spread = lax.dot_general(
        out_full, g_second, (((1,), (1,)), ((), ())), preferred_element_type=F32
    ).astype(BF)
    g_context, up_weight_gradient, every = scatter_and_group(
        spread.reshape(ranks, e_local, span), up_term, packed, ranks, 6
    )
    every = every[:, 0]
    hidden_every = every[:, :f_local]
    rounded_every = every[:, f_local : f_local + width]
    final_every = every[:, f_local + width : f_local + 2 * width]
    rest = every[:, f_local + 2 * width :]
    loss = jnp.sum(rest[:, bins]) / groups
    mine = group * d_local
    down_weight_gradient = lax.dot_general(
        hidden_every,
        lax.dynamic_slice_in_dim(rounded_every, mine, d_local, axis=1),
        over_seqs,
        precision=exact,
    )
    grad_head = lax.dot_general(
        lax.dynamic_slice_in_dim(final_every, mine, d_local, axis=1),
        rest[:, :bins],
        over_seqs,
        precision=exact,
    )

    out_term = (
        jnp.dot(context_all, g_second, preferred_element_type=F32)
        .astype(BF)
        .reshape(ranks, e_local, width)
    )
    g_qkv, out_mine = attend_back(qkv, lengths, lse, g_context, out_term, groups, chunk, 7)
    qkv_term = lax.dot_general(
        normed_one,
        g_qkv.reshape(3 * e_local, span),
        (((0,), (1,)), ((), ())),
        preferred_element_type=F32,
    )
    qkv_gradient, output_weight_gradient = group_sum(
        [qkv_term.astype(BF).reshape(groups, d_local, 3 * e_local), out_mine], 8
    )
    query_key_value_gradient = qkv_gradient.reshape(d_local, 3, e_local)
    return (
        loss,
        query_key_value_gradient,
        output_weight_gradient,
        up_weight_gradient,
        down_weight_gradient,
        grad_head,
    )


def remote(src, dst, sems, index, device):
    return pltpu.make_async_remote_copy(
        src_ref=src,
        dst_ref=dst,
        send_sem=sems[0].at[index],
        recv_sem=sems[1].at[index],
        device_id=device,
        device_id_type=MESH,
    )


class Place:
    def __init__(self):
        self.rank = lax.axis_index("tensor")
        self.across = self.rank + 1 - 2 * lax.rem(self.rank, 2)
        self.over = lax.rem(self.rank + 2, 4)
        self.diag = 3 - self.rank
        self.group = lax.axis_index("dp")
        self.core = lax.rem(self.group, 2)
        self.chip = self.group // 2
        self.near = self.chip * 2 + 1 - self.core

    def turn(self, step):
        return lax.rem(self.chip + step, 4)

    def same(self, chip):
        return chip * 2 + self.core

    def greet(self, tensor, dp, everyone=False):
        barrier = pltpu.get_barrier_semaphore()
        peers = []
        if tensor:
            peers += [{"tensor": one} for one in (self.across, self.over, self.diag)]
        if everyone:
            peers += [{"dp": lax.rem(self.group + step, 8)} for step in range(1, 8)]
        elif dp:
            peers += [
                {"dp": self.near},
                {"dp": self.same(self.turn(1))},
                {"dp": self.same(self.turn(3))},
            ]
        for peer in peers:
            pl.semaphore_signal(barrier, inc=1, device_id=peer, device_id_type=MESH)
        pl.semaphore_wait(barrier, len(peers))


class RingGather:
    def __init__(self, at, src, own, slot, sems):
        self.at, self.src, self.own, self.slot = at, src, own, slot
        self.sems, self.local = sems[:2], sems[2]

    @staticmethod
    def scratch():
        return [
            pltpu.SemaphoreType.DMA((10,)),
            pltpu.SemaphoreType.DMA((10,)),
            pltpu.SemaphoreType.DMA((1,)),
        ]

    def copies(self):
        at = self.at
        right, left, far = at.turn(1), at.turn(3), at.turn(2)
        me, to_right, to_left = at.group, {"dp": at.same(right)}, {"dp": at.same(left)}
        near = {"dp": at.near}

        def held(index, chip, half, device):
            ref = self.slot(at.same(chip), half)
            return remote(ref, ref, self.sems, index, device)

        def first(index, half, device):
            return remote(self.own(half), self.slot(me, half), self.sems, index, device)

        return (
            first(0, 0, to_right),
            first(1, 1, to_left),
            first(2, 1, to_right),
            first(3, 0, to_left),
            held(4, left, 0, to_right),
            held(5, right, 1, to_left),
            remote(self.src, self.slot(me, None), self.sems, 6, near),
            held(7, left, None, near),
            held(8, right, None, near),
            held(9, far, None, near),
        )

    def keep(self):
        return pltpu.make_async_copy(self.src, self.slot(self.at.group, None), self.local.at[0])

    def start(self):
        copies = self.copies()
        for index in (0, 1, 2, 3, 6):
            copies[index].start()
        self.keep().start()

    def relay(self):
        copies = self.copies()
        copies[0].wait_recv()
        copies[4].start()
        copies[1].wait_recv()
        copies[5].start()

    def spread(self):
        copies = self.copies()
        copies[2].wait_recv()
        copies[7].start()
        copies[3].wait_recv()
        copies[8].start()
        copies[4].wait_recv()
        copies[5].wait_recv()
        copies[9].start()

    def finish(self):
        copies = self.copies()
        for index in (6, 7, 8, 9):
            copies[index].wait_recv()
        for copy in copies:
            copy.wait_send()
        self.keep().wait()


def rows_of(ref, block, half, size, axis=0):
    lead = (slice(None),) * axis
    if half is None:
        return ref.at[lead + (pl.ds(pl.multiple_of(block * size, size), size),)]
    part = size // 2
    return ref.at[lead + (pl.ds(pl.multiple_of(block * size + half * part, part), part),)]


def half_rows(ref, half, axis=0):
    part = ref.shape[axis] // 2
    return ref.at[(slice(None),) * axis + (pl.ds(half * part, part),)]


def ids_body(ids_ref, out_ref, ids_all, out_all, send, recv):
    at = Place()
    at.greet(True, False)
    copies = []
    for index, peer in enumerate((at.across, at.over, at.diag)):
        copies.append(
            remote(ids_ref, ids_all.at[at.rank], (send, recv), index, {"tensor": peer})
        )
    for index, peer in enumerate((at.across, at.over, at.diag)):
        copies.append(
            remote(out_ref, out_all.at[at.rank], (send, recv), 3 + index, {"tensor": peer})
        )
    for copy in copies:
        copy.start()
    ids_all[at.rank] = ids_ref[...]
    out_all[at.rank] = out_ref[...]
    for copy in copies:
        copy.wait()


def share_ids(ids, out, ident):
    return pl.pallas_call(
        ids_body,
        out_shape=(
            jax.ShapeDtypeStruct((4,) + ids.shape, ids.dtype),
            jax.ShapeDtypeStruct((4,) + out.shape, out.dtype),
        ),
        in_specs=[vmem_spec()] * 2,
        out_specs=(vmem_spec(),) * 2,
        scratch_shapes=[pltpu.SemaphoreType.DMA((6,))] * 2,
        compiler_params=pltpu.CompilerParams(collective_id=ident, has_side_effects=True),
        name="share_ids",
    )(ids, out)


def any_spec():
    return pl.BlockSpec(memory_space=pl.ANY)


class Stream:
    def __init__(self, at, x_ref, acc, held, last, whole, sems, index, rows, x_first):
        self.at, self.x, self.acc, self.held, self.last, self.whole = at, x_ref, acc, held, last, whole
        self.sems, self.index, self.rows = sems, index * 6, rows
        self.one, self.two = (at.across, at.over) if x_first else (at.over, at.across)

    def copies(self):
        at, rows, base, sems = self.at, self.rows, self.index, self.sems
        one, two = {"tensor": self.one}, {"tensor": self.two}
        return (
            remote(self.x.at[at.diag, rows], self.held.at[1, rows], sems, base, one),
            remote(self.x.at[self.one, rows], self.held.at[0, rows], sems, base + 1, one),
            remote(self.acc.at[rows], self.last.at[rows], sems, base + 2, two),
            remote(self.whole.at[at.rank, rows], self.whole.at[at.rank, rows], sems, base + 3, two),
            remote(self.whole.at[at.rank, rows], self.whole.at[at.rank, rows], sems, base + 4, one),
            remote(self.whole.at[self.two, rows], self.whole.at[self.two, rows], sems, base + 5, one),
        )

    def start(self):
        copies = self.copies()
        copies[0].start()
        copies[1].start()

    def second(self):
        copies = self.copies()
        copies[0].wait_recv()

        def body(at):
            here = pl.ds(self.rows.start + at.start, at.size)
            self.acc[here] = self.x[self.two, here] + self.held[1, here]

        add_tiles(self.rows.size, 32, body)
        copies[2].start()

    def third(self):
        copies = self.copies()
        copies[1].wait_recv()
        copies[2].wait_recv()

        def body(at):
            here = pl.ds(self.rows.start + at.start, at.size)
            self.whole[self.at.rank, here] = (
                self.x[self.at.rank, here] + self.held[0, here] + self.last[here]
            )

        add_tiles(self.rows.size, 32, body)
        copies[3].start()
        copies[4].start()

    def relay(self):
        copies = self.copies()
        copies[3].wait_recv()
        copies[5].start()

    def beside(self):
        self.copies()[4].wait_recv()

    def opposite(self):
        self.copies()[5].wait_recv()

    def finish(self):
        for copy in self.copies():
            copy.wait_send()


def embed_body(
    x_ref, w_ref, up_ref, first_out, normed_out, qkv_ref, up_out,
    acc, held, last, whole, normed, w_full, w_turn, send, recv, saved, *rest,
):
    at = Place()
    at.greet(True, True)
    d_local = w_ref.shape[1]
    local = x_ref.shape[1]
    weights = RingGather(
        at, w_ref, lambda half: half_rows(w_ref, half, 1),
        lambda block, half: rows_of(w_full, block, half, d_local, 1), rest[:3],
    )
    ups = RingGather(
        at, up_ref, lambda half: half_rows(up_ref, half),
        lambda block, half: rows_of(up_out, block, half, d_local), rest[3:],
    )
    weights.start()
    part = local // 4
    streams = [
        Stream(
            at, x_ref, acc, held, last, whole, (send, recv), index,
            pl.ds((index % 2) * (local // 2) + (index // 2) * part, part), index % 2 == 0,
        )
        for index in range(4)
    ]
    for one in streams:
        one.start()
    for one in streams:
        one.second()
    weights.relay()
    ups.start()
    for one in streams:
        one.third()
    weights.spread()
    weights.finish()
    for index in range(3):
        w_turn[index] = w_full[index].T

    def project(block, slot):
        def tile(here):
            normed[block, here] = normalize(whole[block, here].astype(F32)).astype(BF)

        add_tiles(local, 32, tile)
        base = pl.multiple_of(block * local, local)

        def matrix(index, carry):
            qkv_ref[index, :, pl.ds(base, local)] = contract(
                w_turn[index], normed[block], (1, 1)
            ).astype(BF)
            return carry

        lax.fori_loop(0, 3, matrix, 0)
        pltpu.make_async_copy(whole.at[block], first_out.at[block], saved.at[slot, 0]).start()
        pltpu.make_async_copy(normed.at[block], normed_out.at[block], saved.at[slot, 1]).start()

    for one in streams[:2]:
        one.relay()
    project(at.rank, 0)
    for one in streams[2:]:
        one.relay()
    ups.relay()
    for one in streams:
        one.beside()
    project(at.across, 1)
    project(at.over, 2)
    ups.spread()
    for one in streams:
        one.opposite()
    project(at.diag, 3)
    ups.finish()
    for one in streams:
        one.finish()
    for slot, block in enumerate((at.rank, at.across, at.over, at.diag)):
        pltpu.make_async_copy(whole.at[block], first_out.at[block], saved.at[slot, 0]).wait()
        pltpu.make_async_copy(normed.at[block], normed_out.at[block], saved.at[slot, 1]).wait()


def embed(x, w, up, ident):
    ranks, local, width = x.shape
    kinds, d_local, e_local = w.shape
    f_local = up.shape[1]
    return pl.pallas_call(
        embed_body,
        out_shape=(
            jax.ShapeDtypeStruct(x.shape, BF),
            jax.ShapeDtypeStruct(x.shape, BF),
            jax.ShapeDtypeStruct((kinds, e_local, ranks * local), BF),
            jax.ShapeDtypeStruct((width, f_local), BF),
        ),
        in_specs=[vmem_spec()] * 3,
        out_specs=(any_spec(), any_spec(), vmem_spec(), any_spec()),
        scratch_shapes=[
            VMEM((local, width), BF),
            VMEM((2, local, width), BF),
            VMEM((local, width), BF),
            VMEM(x.shape, BF),
            VMEM(x.shape, BF),
            VMEM((kinds, width, e_local), BF),
            VMEM((kinds, e_local, width), BF),
            pltpu.SemaphoreType.DMA((24,)),
            pltpu.SemaphoreType.DMA((24,)),
            pltpu.SemaphoreType.DMA((4, 2)),
        ]
        + RingGather.scratch()
        + RingGather.scratch(),
        compiler_params=pltpu.CompilerParams(
            collective_id=ident, has_side_effects=True, vmem_limit_bytes=BIG
        ),
        name="embed",
    )(x, w, up)


def attend_send_body(
    chunk, length_ref, qkv_ref, col_ref, ctx_out, lse_ref, out_full, ctx_ref, saved, send, recv, *rest
):
    at = Place()
    head = pl.program_id(0)
    last = pl.num_programs(0) - 1
    size = HEAD_WIDTH // 2
    d_local = col_ref.shape[1]
    e_rows = col_ref.shape[0]

    def columns(block, half):
        lanes = pl.ds(pl.multiple_of(block * d_local, d_local), d_local)
        if half is None:
            return out_full.at[:, lanes]
        return out_full.at[pl.ds(half * (e_rows // 2), e_rows // 2), lanes]

    outs = RingGather(at, col_ref, lambda half: half_rows(col_ref, half), columns, rest)

    def copies(one):
        def copy(index, block, half, peer):
            ref = ctx_ref.at[block, pl.ds(pl.multiple_of(one * HEAD_WIDTH + half * size, size), size)]
            return pltpu.make_async_remote_copy(
                src_ref=ref,
                dst_ref=ref,
                send_sem=send.at[one, index],
                recv_sem=recv.at[one, index],
                device_id={"tensor": peer},
                device_id_type=MESH,
            )

        return (
            copy(0, at.rank, 0, at.across),
            copy(1, at.rank, 1, at.over),
            copy(2, at.rank, 1, at.across),
            copy(3, at.rank, 0, at.over),
            copy(4, at.across, 0, at.over),
            copy(5, at.over, 1, at.across),
        )

    def relay(one):
        group = copies(one)
        group[0].wait_recv()
        group[4].start()
        group[1].wait_recv()
        group[5].start()

    @pl.when(head == 0)
    def _():
        at.greet(True, True)
        outs.start()

    length = length_ref[0]
    keys, vals = qkv_ref[1], qkv_ref[2]
    scale = HEAD_WIDTH ** (-0.5)
    for start in range(0, qkv_ref.shape[2], chunk):
        here = slice(start, start + chunk)
        query = (qkv_ref[0, :, here].astype(F32) * scale).astype(BF)
        scores = masked_scores(keys, query, length)
        top = jnp.max(scores, axis=0, keepdims=True)
        expo = jnp.exp(scores - top)
        total = jnp.sum(expo, axis=0, keepdims=True)
        mixed = contract(vals, expo.astype(BF), (1, 0))
        ctx_ref[at.rank, pl.ds(pl.multiple_of(head * HEAD_WIDTH, HEAD_WIDTH), HEAD_WIDTH), here] = (
            mixed * (1.0 / total)
        ).astype(BF)
        lse_ref[0, :, here] = top + jnp.log(total)

    @pl.when(head > 0)
    def _():
        relay(head - 1)

    for copy in copies(head)[:4]:
        copy.start()

    @pl.when(head == 1)
    def _():
        outs.relay()

    @pl.when(head == last)
    def _():
        relay(last)
        outs.spread()

        def save(one):
            here = pl.ds(pl.multiple_of(one * HEAD_WIDTH, HEAD_WIDTH), HEAD_WIDTH)
            return pltpu.make_async_copy(ctx_ref.at[:, here], ctx_out.at[:, here], saved.at[one])

        def drain(one, carry):
            group = copies(one)
            for copy in group[2:]:
                copy.wait_recv()
            for copy in group:
                copy.wait_send()
            save(one).start()
            return carry

        lax.fori_loop(0, last + 1, drain, 0)
        outs.finish()

        def store(one, carry):
            save(one).wait()
            return carry

        lax.fori_loop(0, last + 1, store, 0)


def attend_send(qkv, lengths, column, chunk, ident):
    _, width, length = qkv.shape
    heads = width // HEAD_WIDTH
    assert heads > 1
    return pl.pallas_call(
        functools.partial(attend_send_body, chunk),
        grid=(heads,),
        out_shape=(
            jax.ShapeDtypeStruct((4, width, length), BF),
            jax.ShapeDtypeStruct((heads, 1, length), F32),
            jax.ShapeDtypeStruct((column.shape[0], 8 * column.shape[1]), BF),
        ),
        in_specs=[
            pl.BlockSpec(memory_space=pltpu.SMEM),
            pl.BlockSpec((3, HEAD_WIDTH, length), lambda h: (0, h, 0)),
            vmem_spec(),
        ],
        out_specs=(
            any_spec(),
            pl.BlockSpec((1, 1, length), lambda h: (h, 0, 0)),
            any_spec(),
        ),
        scratch_shapes=[VMEM((4, width, length), BF), pltpu.SemaphoreType.DMA((heads,))]
        + [pltpu.SemaphoreType.DMA((heads, 6))] * 2
        + RingGather.scratch(),
        compiler_params=pltpu.CompilerParams(
            collective_id=ident, has_side_effects=True, vmem_limit_bytes=BIG
        ),
        name="attend_send",
    )(lengths, qkv, column)


def exact_dot(row, matrix, dims):
    high = row.astype(BF).astype(F32)
    middle = (row - high).astype(BF).astype(F32)
    low = row - high - middle
    shape = (8, row.shape[1])
    index = lax.broadcasted_iota(jnp.int32, shape, 0)
    stacked = jnp.where(
        index == 0, jnp.broadcast_to(high, shape),
        jnp.where(
            index == 1, jnp.broadcast_to(middle, shape),
            jnp.where(index == 2, jnp.broadcast_to(low, shape), 0.0),
        ),
    ).astype(BF)
    return jnp.sum(contract(stacked, matrix, dims), axis=0, keepdims=True)


def classify_body(
    length_ref, bin_ref, normed_ref, up_ref, base_ref, down_ref, head_ref,
    slope_ref, small_ref, hidden_ref, token_ref,
    sums, down_full, head_full, parts, send, recv, *rest,
):
    at = Place()
    step = pl.program_id(0)
    last = pl.num_programs(0) - 1
    units, width = down_full.shape
    chunk = up_ref.shape[1]
    d_local = down_ref.shape[1]
    bins = head_ref.shape[1]

    def columns(block, half):
        lanes = pl.ds(pl.multiple_of(block * d_local, d_local), d_local)
        if half is None:
            return down_full.at[:, lanes]
        return down_full.at[pl.ds(half * (units // 2), units // 2), lanes]

    downs = RingGather(at, down_ref, lambda half: half_rows(down_ref, half), columns, rest[:3])
    heads = RingGather(
        at, head_ref, lambda half: half_rows(head_ref, half),
        lambda block, half: rows_of(head_full, block, half, d_local), rest[3:],
    )

    @pl.when(step == 0)
    def _():
        at.greet(True, True)
        downs.start()
        heads.start()

    pre = jnp.dot(normed_ref[...], up_ref[...], preferred_element_type=F32)
    live = lax.broadcasted_iota(jnp.int32, pre.shape, 0) < length_ref[0]
    square = pre * pre
    bend = jnp.tanh(0.7978845608028654 * (pre * (1.0 + 0.044715 * square)))
    half = 0.5 * (1.0 + bend)
    act = (pre * half).astype(BF).astype(F32)
    sums[:, pl.ds(pl.multiple_of(step * chunk, chunk), chunk)] = jnp.sum(
        jnp.where(live, act, 0.0), axis=0, keepdims=True
    )
    inner = 0.7978845608028654 * (1.0 + 3 * 0.044715 * square)
    slope = half + 0.5 * pre * (1.0 - bend * bend) * inner
    slope_ref[...] = jnp.where(live, slope, 0.0).astype(BF)

    @pl.when(step == last)
    def _():
        downs.relay()
        heads.relay()
        downs.spread()
        heads.spread()
        downs.finish()
        heads.finish()
        hidden_sum = sums[...]
        parts[at.rank] = exact_dot(hidden_sum, down_full[...], (1, 0))
        copies = [
            remote(parts.at[at.rank], parts.at[at.rank], (send, recv), index, {"tensor": peer})
            for index, peer in enumerate((at.across, at.over, at.diag))
        ]
        for copy in copies:
            copy.start()
        for copy in copies:
            copy.wait()
        count = jnp.full((1, 1), length_ref[0], jnp.int32).astype(F32)
        total = base_ref[...]
        for index in range(4):
            total = total + parts[index]
        pooled = total / count
        mean = jnp.mean(pooled, axis=-1, keepdims=True)
        centered = pooled - mean
        scale = lax.rsqrt(jnp.mean(centered * centered, axis=-1, keepdims=True) + EPS)
        final = centered * scale
        logits = exact_dot(final, head_full[...], (1, 0))
        top = jnp.max(logits, axis=-1, keepdims=True)
        total_exp = jnp.log(jnp.sum(jnp.exp(logits - top), axis=-1, keepdims=True)) + top
        labels = (lax.broadcasted_iota(jnp.int32, logits.shape, 1) == bin_ref[0]).astype(F32)
        loss = total_exp - jnp.sum(logits * labels, axis=-1, keepdims=True)
        g_logits = (jnp.exp(logits - total_exp) - labels) / 8.0
        g_final = exact_dot(g_logits, head_full[...], (1, 1))
        g_pooled = scale * (
            g_final
            - jnp.mean(g_final, axis=-1, keepdims=True)
            - final * jnp.mean(g_final * final, axis=-1, keepdims=True)
        )
        per_token = g_pooled / count
        rounded = per_token.astype(BF)
        token_ref[...] = per_token
        hidden_ref[...] = contract(
            jnp.broadcast_to(rounded.astype(F32), (8, width)).astype(BF), down_full[...], (1, 1)
        )[:1]
        small_ref[:, :units] = hidden_sum
        small_ref[:, units : units + width] = rounded.astype(F32)
        small_ref[:, units + width : units + 2 * width] = final
        small_ref[:, units + 2 * width : units + 2 * width + bins] = g_logits
        small_ref[:, units + 2 * width + bins :] = jnp.broadcast_to(loss, (1, 128))


def classify(normed, up, base, down, head, lengths, bins_at, chunk, ident):
    length, width = normed.shape
    units = up.shape[1]
    bins = head.shape[1]
    return pl.pallas_call(
        classify_body,
        grid=(units // chunk,),
        out_shape=(
            jax.ShapeDtypeStruct((length, units), BF),
            jax.ShapeDtypeStruct((1, units + 2 * width + bins + 128), F32),
            jax.ShapeDtypeStruct((1, units), F32),
            jax.ShapeDtypeStruct((1, width), F32),
        ),
        in_specs=[
            pl.BlockSpec(memory_space=pltpu.SMEM),
            pl.BlockSpec(memory_space=pltpu.SMEM),
            vmem_spec(),
            pl.BlockSpec((width, chunk), lambda f: (0, f)),
            vmem_spec(),
            vmem_spec(),
            vmem_spec(),
        ],
        out_specs=(
            pl.BlockSpec((length, chunk), lambda f: (0, f)),
            vmem_spec(),
            vmem_spec(),
            vmem_spec(),
        ),
        scratch_shapes=[
            VMEM((1, units), F32),
            VMEM((units, width), BF),
            VMEM((width, bins), BF),
            VMEM((4, 1, width), F32),
            pltpu.SemaphoreType.DMA((3,)),
            pltpu.SemaphoreType.DMA((3,)),
        ]
        + RingGather.scratch()
        + RingGather.scratch(),
        compiler_params=pltpu.CompilerParams(
            collective_id=ident, has_side_effects=True, vmem_limit_bytes=BIG
        ),
        name="classify",
    )(lengths, bins_at, normed, up, base, down, head)


class Fold:
    def __init__(self, at, src, held, acc, last, sems, base, rows, x_first):
        self.at, self.src, self.held, self.acc, self.last = at, src, held, acc, last
        self.sems, self.base, self.rows = sems, base, rows
        self.one, self.two = (at.across, at.over) if x_first else (at.over, at.across)

    def copies(self):
        rows, base, sems = self.rows, self.base, self.sems
        one, two = {"tensor": self.one}, {"tensor": self.two}
        return (
            remote(self.src.at[self.at.diag, rows], self.held.at[1, rows], sems, base, one),
            remote(self.src.at[self.one, rows], self.held.at[0, rows], sems, base + 1, one),
            remote(self.acc.at[rows], self.last.at[rows], sems, base + 2, two),
        )

    def start(self):
        copies = self.copies()
        copies[0].start()
        copies[1].start()

    def tiles(self, body):
        def step(at):
            body(pl.ds(pl.multiple_of(self.rows.start + at.start, 32), at.size))

        add_tiles(self.rows.size, 32, step)

    def second(self):
        copies = self.copies()
        copies[0].wait_recv()

        def body(here):
            self.acc[here] = (
                self.src[self.two, here].astype(F32) + self.held[1, here].astype(F32)
            ).astype(BF)

        self.tiles(body)
        copies[2].start()

    def third(self, put):
        copies = self.copies()
        copies[1].wait_recv()
        copies[2].wait_recv()

        def body(here):
            put(
                here,
                self.src[self.at.rank, here].astype(F32)
                + self.held[0, here].astype(F32)
                + self.last[here].astype(F32),
            )

        self.tiles(body)

    def finish(self):
        for copy in self.copies():
            copy.wait_send()


class DirectSum(GroupSum):
    def __init__(self, x_ref, pair, mine, far, sems, tile):
        super().__init__(x_ref, None, pair, mine, far, sems)
        self.tile = tile

    def middle(self):
        for copy in self.pair_copies():
            copy.wait()
        for chip in range(self.chips):

            def body(at, chip=chip):
                self.mine[chip, at] = (
                    self.x[chip * 2 + self.core, at].astype(F32)
                    + self.pair[chip, at].astype(F32)
                ).astype(BF)

            add_tiles(self.rows, self.tile, body)
        for copy in self.far_copies():
            copy.start()

    def finish(self, put):
        for copy in self.far_copies():
            copy.wait()

        def body(at):
            total = self.mine[self.chip, at].astype(F32)
            for step in range(self.chips - 1):
                total = total + self.far[step, at].astype(F32)
            put(at, total)

        add_tiles(self.rows, self.tile, body)


def backward_body(
    chunk, length_ref, qkv_ref, lse_ref, small_ref, g_second_in, out_in, up_in, ctx_in, normed_in,
    qkv_out, out_out, up_out, small_out,
    g_second, outs, up_term, ctx, normed, loads,
    spread, g_ctx, s_held, s_acc, s_last, s_send, s_recv,
    out_term, o_held, o_acc, o_last, o_send, o_recv,
    out_mine, o_pair, o_own, o_far, o_sem0, o_sem1, o_sem2, o_sem3,
    u_pair, u_own, u_far, u_sem0, u_sem1, u_sem2, u_sem3,
    g_qkv, q_term, q_pair, q_own, q_far, q_sem0, q_sem1, q_sem2, q_sem3,
    smalls, m_send, m_recv,
):
    at = Place()
    head = pl.program_id(0)
    heads = lse_ref.shape[0] * q_term.shape[0]
    end = heads - 1
    e_local = g_ctx.shape[0]
    d_local = q_term.shape[3]
    groups = q_term.shape[1]
    half = HEAD_WIDTH // 2
    length = length_ref[0]
    scale = HEAD_WIDTH ** (-0.5)
    span = qkv_ref.shape[2]

    def load(index):
        pairs = (
            (g_second_in, g_second), (out_in, outs), (up_in, up_term), (ctx_in, ctx), (normed_in, normed)
        )
        return pltpu.make_async_copy(*pairs[index], loads.at[index])

    def folds(one):
        return [
            Fold(
                at, spread, s_held, s_acc, s_last, (s_send, s_recv), one * 6 + part * 3,
                pl.ds(pl.multiple_of(one * HEAD_WIDTH + part * half, half), half), part == 0,
            )
            for part in range(2)
        ]

    out_folds = [
        Fold(
            at, out_term, o_held, o_acc, o_last, (o_send, o_recv), part * 3,
            pl.ds(part * (e_local // 2), e_local // 2), part == 0,
        )
        for part in range(2)
    ]
    up_sum = GroupSum(up_term, up_out, u_pair, u_own, u_far, (u_sem0, u_sem1, u_sem2, u_sem3))
    out_sum = DirectSum(out_mine, o_pair, o_own, o_far, (o_sem0, o_sem1, o_sem2, o_sem3), 64)

    def qkv_sum(one):
        return DirectSum(
            q_term.at[one], q_pair.at[one], q_own.at[one], q_far.at[one],
            (q_sem0.at[one], q_sem1.at[one], q_sem2.at[one], q_sem3.at[one]), q_term.shape[2],
        )

    def small_copies():
        return [
            remote(
                small_ref, smalls.at[at.group], (m_send, m_recv), step - 1,
                {"dp": lax.rem(at.group + step, groups)},
            )
            for step in range(1, groups)
        ]

    def put_context(here, total):
        g_ctx[here] = total.astype(BF)

    def put_out(here, total):
        for group in range(groups):
            out_mine[group, here] = total[:, group * d_local : (group + 1) * d_local].astype(BF)

    @pl.when(head == 0)
    def _():
        for index in range(5):
            load(index).start()
        at.greet(True, True, True)
        load(2).wait()
        up_sum.start()
        for copy in small_copies():
            copy.start()
        smalls[at.group] = small_ref[...]
        load(0).wait()
        load(1).wait()

        def spread_head(one, carry):
            left = jnp.concatenate(
                [
                    outs[pl.ds(pl.multiple_of(part * e_local + one * HEAD_WIDTH, HEAD_WIDTH), HEAD_WIDTH)]
                    for part in range(4)
                ],
                axis=0,
            )
            result = contract(left, g_second[...], (1, 1)).astype(BF)
            for part in range(4):
                spread[part, pl.ds(pl.multiple_of(one * HEAD_WIDTH, HEAD_WIDTH), HEAD_WIDTH)] = result[
                    part * HEAD_WIDTH : (part + 1) * HEAD_WIDTH
                ]
            for fold in folds(one):
                fold.start()
            return carry

        lax.fori_loop(0, 2, spread_head, 0)
        up_sum.middle()
        for fold in folds(0):
            fold.second()
        lax.fori_loop(2, heads, spread_head, 0)
        for fold in folds(1):
            fold.second()
        load(3).wait()

        def out_block(one, carry):
            rows = pl.ds(pl.multiple_of(one * e_local, e_local), e_local)
            out_term[one] = jnp.dot(
                ctx[rows], g_second[...], preferred_element_type=F32
            ).astype(BF)
            return carry

        lax.fori_loop(0, 4, out_block, 0)
        load(4).wait()

    for fold in folds(head):
        fold.third(put_context)

    keys, vals = qkv_ref[1], qkv_ref[2]
    g_keys = jnp.zeros((HEAD_WIDTH, span), F32)
    g_vals = jnp.zeros((HEAD_WIDTH, span), F32)
    mine = pl.ds(pl.multiple_of(head * HEAD_WIDTH, HEAD_WIDTH), HEAD_WIDTH)
    for index, start in enumerate(range(0, span, chunk)):
        here = slice(start, start + chunk)
        query = (qkv_ref[0, :, here].astype(F32) * scale).astype(BF)
        grad = g_ctx[mine, here]
        probs = jnp.exp(masked_scores(keys, query, length) - lse_ref[0, :, here])
        g_probs = contract(vals, grad, (0, 0))
        weighted = probs * g_probs
        inner = jnp.sum(weighted, axis=0, keepdims=True)
        g_scores = (weighted - probs * inner).astype(BF)
        g_qkv[:HEAD_WIDTH, here] = (contract(keys, g_scores, (1, 0)) * scale).astype(BF)
        g_keys += contract(query, g_scores, (1, 1))
        g_vals += contract(grad, probs.astype(BF), (1, 1))
        if index == 1:

            @pl.when((head > 0) & (head < end))
            def _():
                qkv_sum(head - 1).middle()

            @pl.when(head == end)
            def _():
                for fold in out_folds:
                    fold.third(put_out)
                out_sum.start()
                qkv_sum(head - 1).middle()

            @pl.when(head == end - 1)
            def _():
                for fold in out_folds:
                    fold.second()

    g_qkv[HEAD_WIDTH : 2 * HEAD_WIDTH] = g_keys.astype(BF)
    g_qkv[2 * HEAD_WIDTH :] = g_vals.astype(BF)
    result = jnp.dot(g_qkv[...], normed[...], preferred_element_type=F32)
    for group in range(groups):
        q_term[head, group] = result[:, group * d_local : (group + 1) * d_local].astype(BF)
    qkv_sum(head).start()

    @pl.when(head == 0)
    def _():
        def second(one, carry):
            for fold in folds(one):
                fold.second()
            return carry

        lax.fori_loop(2, heads, second, 0)
        for fold in out_folds:
            fold.start()
        up_sum.relay()

    @pl.when(head == end)
    def _():
        out_sum.middle()
        qkv_sum(head).middle()
        up_sum.finish()
        for copy in small_copies():
            copy.wait()
        small_out[...] = smalls[...]

        def drain(one, carry):
            for fold in folds(one):
                fold.finish()
            return carry

        lax.fori_loop(0, heads, drain, 0)
        for fold in out_folds:
            fold.finish()

        def put_final(here, total):
            out_out[here] = total

        out_sum.finish(put_final)

        def store(one, carry):
            def put(here, total):
                for kind in range(3):
                    qkv_out[kind, pl.ds(pl.multiple_of(one * HEAD_WIDTH, HEAD_WIDTH), HEAD_WIDTH)] = total[
                        kind * HEAD_WIDTH : (kind + 1) * HEAD_WIDTH
                    ]

            qkv_sum(one).finish(put)
            return carry

        lax.fori_loop(0, heads, store, 0)


def backward(qkv, lengths, lse, small, g_second, out_full, up_term, context, normed, chunk, ident):
    _, width, length = qkv.shape
    heads = width // HEAD_WIDTH
    groups, d_local, f_local = up_term.shape
    full = out_full.shape[1]
    rows = 3 * HEAD_WIDTH
    dma = pltpu.SemaphoreType.DMA
    return pl.pallas_call(
        functools.partial(backward_body, chunk),
        grid=(heads,),
        out_shape=(
            jax.ShapeDtypeStruct((3, width, d_local), F32),
            jax.ShapeDtypeStruct((width, d_local), F32),
            jax.ShapeDtypeStruct((d_local, f_local), F32),
            jax.ShapeDtypeStruct((groups,) + small.shape, F32),
        ),
        in_specs=[
            pl.BlockSpec(memory_space=pltpu.SMEM),
            pl.BlockSpec((3, HEAD_WIDTH, length), lambda h: (0, h, 0)),
            pl.BlockSpec((1, 1, length), lambda h: (h, 0, 0)),
            vmem_spec(),
        ]
        + [any_spec()] * 5,
        out_specs=(vmem_spec(),) * 4,
        scratch_shapes=[
            VMEM(g_second.shape, BF),
            VMEM(out_full.shape, BF),
            VMEM(up_term.shape, BF),
            VMEM(context.shape, BF),
            VMEM(normed.shape, BF),
            dma((5,)),
            VMEM((4, width, length), BF),
            VMEM((width, length), BF),
            VMEM((2, width, length), BF),
            VMEM((width, length), BF),
            VMEM((width, length), BF),
            dma((heads * 6,)),
            dma((heads * 6,)),
            VMEM((4, width, full), BF),
            VMEM((2, width, full), BF),
            VMEM((width, full), BF),
            VMEM((width, full), BF),
            dma((6,)),
            dma((6,)),
            VMEM((groups, width, d_local), BF),
            VMEM((4, width, d_local), BF),
            VMEM((4, width, d_local), BF),
            VMEM((3, width, d_local), BF),
            dma((4,)),
            dma((4,)),
            dma((3,)),
            dma((3,)),
        ]
        + GroupSum.scratch(up_term.shape, BF)
        + [
            VMEM((rows, length), BF),
            VMEM((heads, groups, rows, d_local), BF),
            VMEM((heads, 4, rows, d_local), BF),
            VMEM((heads, 4, rows, d_local), BF),
            VMEM((heads, 3, rows, d_local), BF),
            dma((heads, 4)),
            dma((heads, 4)),
            dma((heads, 3)),
            dma((heads, 3)),
            VMEM((groups,) + small.shape, F32),
            dma((groups - 1,)),
            dma((groups - 1,)),
        ],
        compiler_params=pltpu.CompilerParams(
            collective_id=ident, has_side_effects=True, vmem_limit_bytes=BIG
        ),
        name="backward",
    )(lengths, qkv, lse, small, g_second, out_full, up_term, context, normed)


def per_device_block(
    token_ids,
    lengths,
    teacher_bins,
    embed_table,
    query_key_value_matrix,
    output_matrix,
    up_matrix,
    down_matrix,
    w_head,
):
    ranks = lax.axis_size("tensor")
    groups = lax.axis_size("dp")
    rank = lax.axis_index("tensor")
    group = lax.axis_index("dp")
    assert token_ids.shape[0] == 1
    local_len = token_ids.shape[1]
    span = local_len * ranks
    vocab_local, width = embed_table.shape
    d_local, _, e_local = query_key_value_matrix.shape
    f_local = up_matrix.shape[1]
    bins = w_head.shape[1]
    exact = lax.Precision.HIGHEST

    all_ids, out_columns = share_ids(token_ids, output_matrix, 11)
    all_ids = all_ids.reshape(ranks, local_len)
    shifted = all_ids - rank * vocab_local
    inside = (shifted >= 0) & (shifted < vocab_local)
    rows = jnp.take(embed_table, jnp.clip(shifted, 0, vocab_local - 1), axis=0)
    first, normed_one, qkv, up_full = embed(
        jnp.where(inside[..., None], rows, jnp.zeros((), BF)),
        query_key_value_matrix.transpose(1, 0, 2),
        up_matrix,
        12,
    )
    first = first.reshape(span, width)
    normed_one = normed_one.reshape(span, width)
    chunk = min(256, span)
    context, lse, out_full = attend_send(
        qkv, lengths, out_columns.reshape(ranks * e_local, d_local), chunk, 13
    )
    context_all = context.reshape(ranks * e_local, span)
    attn = lax.dot_general(
        context_all, out_full, (((0,), (0,)), ((), ())), preferred_element_type=F32
    )
    second = (first.astype(F32) + attn).astype(BF)
    normed_f, norm_back = jax.vjp(normalize, second.astype(F32))
    normed_two = normed_f.astype(BF)
    live = (jnp.arange(span, dtype=jnp.int32) < lengths[0]).astype(F32)
    second_sum = jnp.sum(second.astype(F32) * live[:, None], axis=0, keepdims=True)
    slope, packed, g_hidden, per_token = classify(
        normed_two, up_full, second_sum, down_matrix, w_head, lengths, teacher_bins,
        min(256, f_local), 14,
    )

    over_seqs = (((0,), (0,)), ((), ()))
    up_base = lax.dot_general(normed_two, slope, over_seqs, preferred_element_type=F32)
    up_term = (up_base * g_hidden).astype(BF).reshape(groups, d_local, f_local)
    g_pre = (slope.astype(F32) * g_hidden).astype(BF)
    g_normed = lax.dot_general(
        g_pre, up_full, (((1,), (1,)), ((), ())), preferred_element_type=F32
    )
    g_second = (
        norm_back(g_normed)[0] + live[:, None] * (per_token / ranks)
    ).astype(BF)
    qkv_gradient, output_weight_gradient, up_weight_gradient, every = backward(
        qkv, lengths, lse, packed, g_second, out_full, up_term, context_all, normed_one, chunk, 15
    )
    every = every[:, 0]
    hidden_every = every[:, :f_local]
    rounded_every = every[:, f_local : f_local + width]
    final_every = every[:, f_local + width : f_local + 2 * width]
    rest = every[:, f_local + 2 * width :]
    loss = jnp.sum(rest[:, bins]) / groups
    mine = group * d_local
    down_weight_gradient = lax.dot_general(
        hidden_every,
        lax.dynamic_slice_in_dim(rounded_every, mine, d_local, axis=1),
        over_seqs,
        precision=exact,
    )
    grad_head = lax.dot_general(
        lax.dynamic_slice_in_dim(final_every, mine, d_local, axis=1),
        rest[:, :bins],
        over_seqs,
        precision=exact,
    )

    query_key_value_gradient = qkv_gradient.transpose(2, 0, 1)
    return (
        loss,
        query_key_value_gradient,
        output_weight_gradient,
        up_weight_gradient,
        down_weight_gradient,
        grad_head,
    )


def solution(mesh):
    placed = (
        P("dp", "tensor"),
        P("dp"),
        P("dp"),
        P("tensor", None),
        P("dp", None, "tensor"),
        P("tensor", "dp"),
        P("dp", "tensor"),
        P("tensor", "dp"),
        P("dp", None),
    )
    return jax.shard_map(
        per_device_block if (mesh.shape["tensor"], mesh.shape["dp"]) == (4, 8) else per_device,
        mesh=mesh,
        in_specs=placed,
        out_specs=(
            P(),
            P("dp", None, "tensor"),
            P("tensor", "dp"),
            P("dp", "tensor"),
            P("tensor", "dp"),
            P("dp", None),
        ),
        check_vma=False,
    )
```

```python
import functools

import jax
import jax.numpy as jnp
from jax import lax
from jax.experimental import pallas as pl
from jax.experimental.pallas import tpu as pltpu
from jax.sharding import PartitionSpec as P

HEAD_WIDTH = 64
EPS = 1e-05
BF = jnp.bfloat16
F32 = jnp.float32
MESH = pl.DeviceIdType.MESH
VMEM = pltpu.VMEM
BIG = 60 * 1024 * 1024


def normalize(values):
    mean = jnp.mean(values, axis=-1, keepdims=True)
    centered = values - mean
    return centered * lax.rsqrt(jnp.mean(centered * centered, axis=-1, keepdims=True) + EPS)


def vmem_spec():
    return pl.BlockSpec(memory_space=pltpu.VMEM)


def greet(axis, count):
    me = lax.axis_index(axis)
    barrier = pltpu.get_barrier_semaphore()
    for step in range(1, count):
        pl.semaphore_signal(
            barrier, inc=1, device_id={axis: lax.rem(me + step, count)}, device_id_type=MESH
        )
    pl.semaphore_wait(barrier, count - 1)
    return me


def gather_body(axis, count, x_ref, out_ref, send_sem, recv_sem):
    me = greet(axis, count)
    copies = []
    for step in range(1, count):
        copy = pltpu.make_async_remote_copy(
            src_ref=x_ref,
            dst_ref=out_ref.at[me],
            send_sem=send_sem.at[step - 1],
            recv_sem=recv_sem.at[step - 1],
            device_id={axis: lax.rem(me + step, count)},
            device_id_type=MESH,
        )
        copy.start()
        copies.append(copy)
    out_ref[me] = x_ref[...]
    for copy in copies:
        copy.wait()


def relay_gather(axis, me, src, out, send_sem, recv_sem):
    across = me + 1 - 2 * lax.rem(me, 2)
    over = lax.rem(me + 2, 4)
    half = src.shape[0] // 2
    low, high = pl.ds(0, half), pl.ds(half, half)

    def copy(index, src_part, block, part, device):
        return pltpu.make_async_remote_copy(
            src_ref=src_part,
            dst_ref=out.at[block, part],
            send_sem=send_sem.at[index],
            recv_sem=recv_sem.at[index],
            device_id={axis: device},
            device_id_type=MESH,
        )

    first_a = copy(0, src.at[low], me, low, across)
    first_b = copy(1, src.at[high], me, high, over)
    second_a = copy(2, src.at[high], me, high, across)
    second_b = copy(3, src.at[low], me, low, over)
    for one in (first_a, first_b, second_a, second_b):
        one.start()
    first_a.wait_recv()
    pass_b = copy(4, out.at[across, low], across, low, over)
    pass_b.start()
    first_b.wait_recv()
    pass_a = copy(5, out.at[over, high], over, high, across)
    pass_a.start()
    second_a.wait_recv()
    second_b.wait_recv()
    pass_b.wait_recv()
    pass_a.wait_recv()
    for one in (first_a, first_b, second_a, second_b, pass_b, pass_a):
        one.wait_send()


def relay_body(axis, x_ref, out_ref, send_sem, recv_sem):
    me = greet(axis, 4)
    relay_gather(axis, me, x_ref, out_ref, send_sem, recv_sem)
    out_ref[me] = x_ref[...]


def gather_blocks(x, axis, count, ident):
    if count != 4:
        return gather_all(x, axis, count, ident)
    return pl.pallas_call(
        functools.partial(relay_body, axis),
        out_shape=jax.ShapeDtypeStruct((count,) + x.shape, x.dtype),
        in_specs=[vmem_spec()],
        out_specs=vmem_spec(),
        scratch_shapes=[pltpu.SemaphoreType.DMA((6,)), pltpu.SemaphoreType.DMA((6,))],
        compiler_params=pltpu.CompilerParams(collective_id=ident, has_side_effects=True),
        name="gather_blocks",
    )(x)


def gather_all(x, axis, count, ident):
    return pl.pallas_call(
        functools.partial(gather_body, axis, count),
        out_shape=jax.ShapeDtypeStruct((count,) + x.shape, x.dtype),
        in_specs=[vmem_spec()],
        out_specs=vmem_spec(),
        scratch_shapes=[
            pltpu.SemaphoreType.DMA((count - 1,)),
            pltpu.SemaphoreType.DMA((count - 1,)),
        ],
        compiler_params=pltpu.CompilerParams(collective_id=ident, has_side_effects=True),
        name="gather_all",
    )(x)


def scatter_copies(axis, count, me, x_ref, held, send_sem, recv_sem):
    copies = []
    for step in range(1, count):
        peer = lax.rem(me + step, count)
        copies.append(
            pltpu.make_async_remote_copy(
                src_ref=x_ref.at[peer],
                dst_ref=held.at[step - 1],
                send_sem=send_sem.at[step - 1],
                recv_sem=recv_sem.at[step - 1],
                device_id={axis: peer},
                device_id_type=MESH,
            )
        )
    return copies


def scatter_start(*args):
    for copy in scatter_copies(*args):
        copy.start()


def scatter_finish(axis, count, me, x_ref, held, send_sem, recv_sem, put):
    for copy in scatter_copies(axis, count, me, x_ref, held, send_sem, recv_sem):
        copy.wait()

    def body(at):
        total = x_ref[me, at].astype(F32)
        for step in range(1, count):
            total = total + held[step - 1, at].astype(F32)
        put(at, total)

    add_tiles(x_ref.shape[1], 32, body)


def add_tiles(rows, tile, body):
    def step(index, carry):
        body(pl.ds(pl.multiple_of(index * tile, tile), tile))
        return carry

    lax.fori_loop(0, rows // tile, step, 0)


class GroupSum:
    def __init__(self, x_ref, out_ref, pair, mine, far, sems):
        self.x, self.out, self.pair, self.mine, self.far = x_ref, out_ref, pair, mine, far
        self.sems = sems
        self.groups = x_ref.shape[0]
        self.chips = self.groups // 2
        self.rows = x_ref.shape[1]
        me = lax.axis_index("dp")
        self.core = lax.rem(me, 2)
        self.chip = me // 2
        self.near = self.chip * 2 + 1 - self.core

    @staticmethod
    def scratch(shape, dtype):
        groups, rows, columns = shape
        chips = groups // 2
        return [
            VMEM((chips, rows, columns), dtype),
            VMEM((chips, rows, columns), dtype),
            VMEM((chips - 1, rows, columns), dtype),
            pltpu.SemaphoreType.DMA((chips,)),
            pltpu.SemaphoreType.DMA((chips,)),
            pltpu.SemaphoreType.DMA((6 if chips == 4 else chips - 1,)),
            pltpu.SemaphoreType.DMA((6 if chips == 4 else chips - 1,)),
        ]

    def signal(self, barrier):
        pl.semaphore_signal(
            barrier, inc=1, device_id={"dp": self.near}, device_id_type=MESH
        )
        for step in range(1, self.chips):
            pl.semaphore_signal(
                barrier, inc=1, device_id={"dp": self.owner(step)}, device_id_type=MESH
            )
        return self.chips

    def owner(self, step):
        return lax.rem(self.chip + step, self.chips) * 2 + self.core

    def pair_copies(self):
        copies = []
        for chip in range(self.chips):
            copies.append(
                pltpu.make_async_remote_copy(
                    src_ref=self.x.at[chip * 2 + 1 - self.core],
                    dst_ref=self.pair.at[chip],
                    send_sem=self.sems[0].at[chip],
                    recv_sem=self.sems[1].at[chip],
                    device_id={"dp": self.near},
                    device_id_type=MESH,
                )
            )
        return copies

    def far_copies(self):
        copies = []
        for step in range(1, self.chips):
            copies.append(
                pltpu.make_async_remote_copy(
                    src_ref=self.mine.at[lax.rem(self.chip + step, self.chips)],
                    dst_ref=self.far.at[step - 1],
                    send_sem=self.sems[2].at[step - 1],
                    recv_sem=self.sems[3].at[step - 1],
                    device_id={"dp": self.owner(step)},
                    device_id_type=MESH,
                )
            )
        return copies

    def ring_copies(self):
        right, left = lax.rem(self.chip + 1, 4), lax.rem(self.chip + 3, 4)
        opposite = lax.rem(self.chip + 2, 4)
        half = self.rows // 2
        low, high = pl.ds(0, half), pl.ds(half, half)

        def copy(index, block, part, slot, chip):
            return pltpu.make_async_remote_copy(
                src_ref=self.mine.at[block, part],
                dst_ref=self.far.at[slot, part],
                send_sem=self.sems[2].at[index],
                recv_sem=self.sems[3].at[index],
                device_id={"dp": chip * 2 + self.core},
                device_id_type=MESH,
            )

        return (
            copy(0, opposite, low, 2, right),
            copy(1, opposite, high, 2, left),
            copy(2, right, high, 0, right),
            copy(3, left, low, 1, left),
            copy(4, right, low, 0, right),
            copy(5, left, high, 1, left),
        )

    def relay(self):
        if self.chips != 4:
            return
        copies = self.ring_copies()
        half = self.rows // 2
        for index, step, base in ((0, 1, 0), (1, 3, half)):
            copies[index].wait_recv()
            block = lax.rem(self.chip + step, 4)

            def body(at, block=block, base=base):
                here = pl.ds(base + at.start, at.size)
                self.mine[block, here] = (
                    self.mine[block, here].astype(F32) + self.far[2, here].astype(F32)
                ).astype(self.mine.dtype)

            add_tiles(half, 32, body)
            copies[index + 4].start()

    def start(self):
        for copy in self.pair_copies():
            copy.start()

    def middle(self):
        for copy in self.pair_copies():
            copy.wait()

        for chip in range(self.chips):

            def body(at, chip=chip):
                self.mine[chip, at] = (
                    self.x[chip * 2 + self.core, at].astype(F32)
                    + self.pair[chip, at].astype(F32)
                ).astype(self.mine.dtype)

            add_tiles(self.rows, 32, body)
        copies = self.ring_copies()[:4] if self.chips == 4 else self.far_copies()
        for copy in copies:
            copy.start()

    def finish(self):
        if self.chips == 4:
            copies = self.ring_copies()
            for copy in copies[2:]:
                copy.wait()
            for copy in copies[:2]:
                copy.wait_send()
        else:
            for copy in self.far_copies():
                copy.wait()

        def body(at):
            total = self.mine[self.chip, at].astype(F32)
            for step in range(2 if self.chips == 4 else self.chips - 1):
                total = total + self.far[step, at].astype(F32)
            self.out[at] = total

        add_tiles(self.rows, 32, body)


def scatter_and_group_body(
    count, x_ref, up_ref, small_ref, out_ref, up_out, small_out, held, send_sem, recv_sem, *rest
):
    up = GroupSum(up_ref, up_out, rest[0], rest[1], rest[2], rest[3:7])
    small_send, small_recv = rest[7:]
    groups = small_out.shape[0]
    group = lax.axis_index("dp")
    barrier = pltpu.get_barrier_semaphore()
    me = lax.axis_index("tensor")
    for step in range(1, count):
        pl.semaphore_signal(
            barrier, inc=1, device_id={"tensor": lax.rem(me + step, count)}, device_id_type=MESH
        )
    for step in range(1, groups):
        pl.semaphore_signal(
            barrier, inc=1, device_id={"dp": lax.rem(group + step, groups)}, device_id_type=MESH
        )
    pl.semaphore_wait(barrier, count + groups - 2)
    smalls = []
    for step in range(1, groups):
        smalls.append(
            pltpu.make_async_remote_copy(
                src_ref=small_ref,
                dst_ref=small_out.at[group],
                send_sem=small_send.at[step - 1],
                recv_sem=small_recv.at[step - 1],
                device_id={"dp": lax.rem(group + step, groups)},
                device_id_type=MESH,
            )
        )

    def put(at, total):
        out_ref[at] = total.astype(out_ref.dtype)

    up.start()
    scatter_start("tensor", count, me, x_ref, held, send_sem, recv_sem)
    up.middle()
    for copy in smalls:
        copy.start()
    small_out[group] = small_ref[...]
    up.relay()
    scatter_finish("tensor", count, me, x_ref, held, send_sem, recv_sem, put)
    up.finish()
    for copy in smalls:
        copy.wait()


def scatter_and_group(x, up, small, count, ident):
    return pl.pallas_call(
        functools.partial(scatter_and_group_body, count),
        out_shape=(
            jax.ShapeDtypeStruct(x.shape[1:], x.dtype),
            jax.ShapeDtypeStruct(up.shape[1:], F32),
            jax.ShapeDtypeStruct(up.shape[:1] + small.shape, F32),
        ),
        in_specs=[vmem_spec()] * 3,
        out_specs=(vmem_spec(),) * 3,
        scratch_shapes=[
            VMEM((count - 1,) + x.shape[1:], x.dtype),
            pltpu.SemaphoreType.DMA((count - 1,)),
            pltpu.SemaphoreType.DMA((count - 1,)),
        ]
        + GroupSum.scratch(up.shape, up.dtype)
        + [pltpu.SemaphoreType.DMA((up.shape[0] - 1,))] * 2,
        compiler_params=pltpu.CompilerParams(
            collective_id=ident, has_side_effects=True, vmem_limit_bytes=BIG
        ),
        name="scatter_and_group",
    )(x, up, small)


def group_sum_body(number, *refs):
    xs, outs, rest = refs[:number], refs[number : 2 * number], refs[2 * number :]
    sums = [
        GroupSum(x, out, *rest[7 * i : 7 * i + 3], rest[7 * i + 3 : 7 * i + 7])
        for i, (x, out) in enumerate(zip(xs, outs))
    ]
    barrier = pltpu.get_barrier_semaphore()
    pl.semaphore_wait(barrier, sums[0].signal(barrier))
    for one in sums:
        one.start()
    for one in sums:
        one.middle()
    for one in sums:
        one.relay()
    for one in sums:
        one.finish()


def group_sum(arrays, ident):
    number = len(arrays)
    scratch = []
    for array in arrays:
        scratch += GroupSum.scratch(array.shape, array.dtype)
    return pl.pallas_call(
        functools.partial(group_sum_body, number),
        out_shape=tuple(jax.ShapeDtypeStruct(a.shape[1:], F32) for a in arrays),
        in_specs=[vmem_spec()] * number,
        out_specs=(vmem_spec(),) * number,
        scratch_shapes=scratch,
        compiler_params=pltpu.CompilerParams(
            collective_id=ident, has_side_effects=True, vmem_limit_bytes=BIG
        ),
        name="group_sum",
    )(*arrays)


def sum_all_body(axis, count, x_ref, out_ref, held, send_sem, recv_sem, send_two, recv_two):
    me = greet(axis, count)

    def put(at, total):
        out_ref[me, at] = total.astype(out_ref.dtype)

    scatter_start(axis, count, me, x_ref, held, send_sem, recv_sem)
    scatter_finish(axis, count, me, x_ref, held, send_sem, recv_sem, put)
    if count == 4:
        relay_gather(axis, me, out_ref.at[me], out_ref, send_two, recv_two)
        return
    copies = []
    for step in range(1, count):
        copy = pltpu.make_async_remote_copy(
            src_ref=out_ref.at[me],
            dst_ref=out_ref.at[me],
            send_sem=send_two.at[step - 1],
            recv_sem=recv_two.at[step - 1],
            device_id={axis: lax.rem(me + step, count)},
            device_id_type=MESH,
        )
        copy.start()
        copies.append(copy)
    for copy in copies:
        copy.wait()


def sum_all(x, axis, count, ident):
    return pl.pallas_call(
        functools.partial(sum_all_body, axis, count),
        out_shape=jax.ShapeDtypeStruct(x.shape, x.dtype),
        in_specs=[vmem_spec()],
        out_specs=vmem_spec(),
        scratch_shapes=[VMEM((count - 1,) + x.shape[1:], x.dtype)]
        + [pltpu.SemaphoreType.DMA((count - 1,))] * 2
        + [pltpu.SemaphoreType.DMA((6 if count == 4 else count - 1,))] * 2,
        compiler_params=pltpu.CompilerParams(collective_id=ident, has_side_effects=True),
        name="sum_all",
    )(x)


def contract(left, right, dims):
    return lax.dot_general(left, right, ((dims[:1], dims[1:]), ((), ())), preferred_element_type=F32)


def masked_scores(keys, query, length):
    scores = contract(keys, query, (0, 0))
    position = lax.broadcasted_iota(jnp.int32, scores.shape, 0)
    return jnp.where(position < length, scores, -1e30)


def attend_body(chunk, length_ref, qkv_ref, out_ref, lse_ref):
    length = length_ref[0]
    keys, vals = qkv_ref[1], qkv_ref[2]
    scale = HEAD_WIDTH ** (-0.5)
    for at in range(0, qkv_ref.shape[2], chunk):
        query = (qkv_ref[0, :, at : at + chunk].astype(F32) * scale).astype(BF)
        scores = masked_scores(keys, query, length)
        top = jnp.max(scores, axis=0, keepdims=True)
        expo = jnp.exp(scores - top)
        total = jnp.sum(expo, axis=0, keepdims=True)
        mixed = contract(vals, expo.astype(BF), (1, 0))
        out_ref[:, at : at + chunk] = (mixed * (1.0 / total)).astype(BF)
        lse_ref[0, :, at : at + chunk] = top + jnp.log(total)


def attend(qkv, lengths, chunk):
    _, width, length = qkv.shape
    heads = width // HEAD_WIDTH
    return pl.pallas_call(
        functools.partial(attend_body, chunk),
        grid=(heads,),
        out_shape=(
            jax.ShapeDtypeStruct((width, length), BF),
            jax.ShapeDtypeStruct((heads, 1, length), F32),
        ),
        in_specs=[
            pl.BlockSpec(memory_space=pltpu.SMEM),
            pl.BlockSpec((3, HEAD_WIDTH, length), lambda h: (0, h, 0)),
        ],
        out_specs=(
            pl.BlockSpec((HEAD_WIDTH, length), lambda h: (h, 0)),
            pl.BlockSpec((1, 1, length), lambda h: (h, 0, 0)),
        ),
        cost_estimate=pl.CostEstimate(
            flops=4 * width * length * length,
            bytes_accessed=8 * width * length,
            transcendentals=heads * length * length,
        ),
        compiler_params=pltpu.CompilerParams(vmem_limit_bytes=BIG),
        name="attend",
    )(lengths, qkv)


def attend_back_body(
    chunk, ranks, length_ref, qkv_ref, lse_ref, grad_ref, x_ref, out_ref, x_out, held, send_sem, recv_sem
):
    me = lax.axis_index("tensor")
    args = ("tensor", ranks, me, x_ref, held, send_sem, recv_sem)

    @pl.when(pl.program_id(0) == 0)
    def _():
        greet("tensor", ranks)
        scatter_start(*args)

    attend_back_head(chunk, length_ref, qkv_ref, lse_ref, grad_ref, out_ref)

    @pl.when(pl.program_id(0) == pl.num_programs(0) - 1)
    def _():
        piece = x_out.shape[2]

        def put(at, total):
            for group in range(x_out.shape[0]):
                x_out[group, at] = total[:, group * piece : (group + 1) * piece].astype(BF)

        scatter_finish(*args, put)


def attend_back_head(chunk, length_ref, qkv_ref, lse_ref, grad_ref, out_ref):
    length = length_ref[0]
    keys, vals = qkv_ref[1], qkv_ref[2]
    scale = HEAD_WIDTH ** (-0.5)
    span = qkv_ref.shape[2]
    g_keys = jnp.zeros((HEAD_WIDTH, span), F32)
    g_vals = jnp.zeros((HEAD_WIDTH, span), F32)
    for at in range(0, span, chunk):
        here = slice(at, at + chunk)
        query = (qkv_ref[0, :, here].astype(F32) * scale).astype(BF)
        grad = grad_ref[:, here]
        probs = jnp.exp(masked_scores(keys, query, length) - lse_ref[0, :, here])
        g_probs = contract(vals, grad, (0, 0))
        weighted = probs * g_probs
        inner = jnp.sum(weighted, axis=0, keepdims=True)
        g_scores = (weighted - probs * inner).astype(BF)
        out_ref[0, :, here] = (contract(keys, g_scores, (1, 0)) * scale).astype(BF)
        g_keys += contract(query, g_scores, (1, 1))
        g_vals += contract(grad, probs.astype(BF), (1, 1))
    out_ref[1] = g_keys.astype(BF)
    out_ref[2] = g_vals.astype(BF)


def attend_back(qkv, lengths, lse, grad, x, groups, chunk, ident):
    _, width, length = qkv.shape
    heads = width // HEAD_WIDTH
    return pl.pallas_call(
        functools.partial(attend_back_body, chunk, x.shape[0]),
        grid=(heads,),
        out_shape=(
            jax.ShapeDtypeStruct(qkv.shape, BF),
            jax.ShapeDtypeStruct((groups, x.shape[1], x.shape[2] // groups), BF),
        ),
        in_specs=[
            pl.BlockSpec(memory_space=pltpu.SMEM),
            pl.BlockSpec((3, HEAD_WIDTH, length), lambda h: (0, h, 0)),
            pl.BlockSpec((1, 1, length), lambda h: (h, 0, 0)),
            pl.BlockSpec((HEAD_WIDTH, length), lambda h: (h, 0)),
            vmem_spec(),
        ],
        out_specs=(
            pl.BlockSpec((3, HEAD_WIDTH, length), lambda h: (0, h, 0)),
            vmem_spec(),
        ),
        scratch_shapes=[
            VMEM((x.shape[0] - 1,) + x.shape[1:], x.dtype),
            pltpu.SemaphoreType.DMA((x.shape[0] - 1,)),
            pltpu.SemaphoreType.DMA((x.shape[0] - 1,)),
        ],
        cost_estimate=pl.CostEstimate(
            flops=10 * width * length * length,
            bytes_accessed=14 * width * length,
            transcendentals=heads * length * length,
        ),
        compiler_params=pltpu.CompilerParams(
            collective_id=ident, has_side_effects=True, vmem_limit_bytes=BIG
        ),
        name="attend_back",
    )(lengths, qkv, lse, grad, x)


def hidden_body(length_ref, normed_ref, up_ref, slope_ref, sum_ref):
    pre = jnp.dot(normed_ref[...], up_ref[...], preferred_element_type=F32)
    live = lax.broadcasted_iota(jnp.int32, pre.shape, 0) < length_ref[0]
    square = pre * pre
    bend = jnp.tanh(0.7978845608028654 * (pre * (1.0 + 0.044715 * square)))
    half = 0.5 * (1.0 + bend)
    act = (pre * half).astype(BF).astype(F32)
    sum_ref[...] = jnp.sum(jnp.where(live, act, 0.0), axis=0, keepdims=True)
    inner = 0.7978845608028654 * (1.0 + 3 * 0.044715 * square)
    slope = half + 0.5 * pre * (1.0 - bend * bend) * inner
    slope_ref[...] = jnp.where(live, slope, 0.0).astype(BF)


def hidden(normed, up, lengths, chunk):
    length, width = normed.shape
    units = up.shape[1]
    return pl.pallas_call(
        hidden_body,
        grid=(units // chunk,),
        out_shape=(
            jax.ShapeDtypeStruct((length, units), BF),
            jax.ShapeDtypeStruct((1, units), F32),
        ),
        in_specs=[
            pl.BlockSpec(memory_space=pltpu.SMEM),
            pl.BlockSpec((length, width), lambda f: (0, 0)),
            pl.BlockSpec((width, chunk), lambda f: (0, f)),
        ],
        out_specs=(
            pl.BlockSpec((length, chunk), lambda f: (0, f)),
            pl.BlockSpec((1, chunk), lambda f: (0, f)),
        ),
        cost_estimate=pl.CostEstimate(
            flops=2 * length * width * units,
            bytes_accessed=6 * length * units,
            transcendentals=length * units,
        ),
        compiler_params=pltpu.CompilerParams(vmem_limit_bytes=BIG),
        name="hidden",
    )(lengths, normed, up)


def per_device(
    token_ids,
    lengths,
    teacher_bins,
    embed_table,
    query_key_value_matrix,
    output_matrix,
    up_matrix,
    down_matrix,
    w_head,
):
    ranks = lax.axis_size("tensor")
    groups = lax.axis_size("dp")
    rank = lax.axis_index("tensor")
    group = lax.axis_index("dp")
    assert token_ids.shape[0] == 1
    local_len = token_ids.shape[1]
    span = local_len * ranks
    vocab_local, width = embed_table.shape
    d_local, _, e_local = query_key_value_matrix.shape
    f_local = up_matrix.shape[1]
    bins = w_head.shape[1]
    exact = lax.Precision.HIGHEST

    qkv_full = lax.all_gather(
        query_key_value_matrix.reshape(d_local, 3 * e_local), "dp", axis=0, tiled=True
    )
    out_parts = lax.all_gather(output_matrix, ("tensor", "dp"), axis=0, tiled=False)
    out_full = (
        out_parts.reshape(ranks, groups, e_local, d_local)
        .transpose(0, 2, 1, 3)
        .reshape(ranks * e_local, width)
    )
    up_full = lax.all_gather(up_matrix, "dp", axis=0, tiled=True)
    low = lax.all_gather(
        jnp.concatenate([down_matrix, w_head.reshape(bins, d_local)], axis=0), "dp", axis=0, tiled=False
    )
    down_full = low[:, :f_local]
    head_wide = low[:, f_local:].reshape(width, bins).astype(F32)

    all_ids = gather_all(token_ids, "tensor", ranks, 1).reshape(ranks, local_len)
    shifted = all_ids - rank * vocab_local
    inside = (shifted >= 0) & (shifted < vocab_local)
    rows = jnp.take(embed_table, jnp.clip(shifted, 0, vocab_local - 1), axis=0)
    first = sum_all(
        jnp.where(inside[..., None], rows, jnp.zeros((), BF)), "tensor", ranks, 2
    ).reshape(span, width)
    normed_one = normalize(first.astype(F32)).astype(BF)
    qkv = (
        lax.dot_general(qkv_full, normed_one, (((0,), (1,)), ((), ())), preferred_element_type=F32)
        .astype(BF)
        .reshape(3, e_local, span)
    )
    chunk = min(256, span)
    context, lse = attend(qkv, lengths, chunk)
    context_all = gather_blocks(context, "tensor", ranks, 3).reshape(ranks * e_local, span)
    attn = lax.dot_general(
        context_all, out_full, (((0,), (0,)), ((), ())), preferred_element_type=F32
    )
    second = (first.astype(F32) + attn).astype(BF)
    normed_f, norm_back = jax.vjp(normalize, second.astype(F32))
    normed_two = normed_f.astype(BF)
    slope, hidden_sum = hidden(normed_two, up_full, lengths, min(256, f_local))

    live = (jnp.arange(span, dtype=jnp.int32) < lengths[0]).astype(F32)
    count = lengths.astype(F32)[:, None]
    ffn_part = jnp.einsum(
        "of,jfd->ojd", hidden_sum, down_full.astype(F32), precision=exact
    ).reshape(1, width)
    ffn_all = gather_all(ffn_part, "tensor", ranks, 4)
    second_sum = jnp.sum(second.astype(F32) * live[:, None], axis=0, keepdims=True)
    pooled = (second_sum + jnp.sum(ffn_all, axis=0)) / count
    final, final_back = jax.vjp(normalize, pooled)
    logits = jnp.dot(final, head_wide, precision=exact)
    top = jnp.max(logits, axis=-1, keepdims=True)
    total_exp = jnp.log(jnp.sum(jnp.exp(logits - top), axis=-1, keepdims=True)) + top
    labels = (teacher_bins[:, None] == jnp.arange(bins, dtype=jnp.int32)[None, :]).astype(F32)
    loss_here = total_exp - jnp.sum(logits * labels, axis=-1, keepdims=True)
    g_logits = (jnp.exp(logits - total_exp) - labels) / groups
    g_final = jnp.dot(g_logits, head_wide.T, precision=exact)
    per_token = final_back(g_final)[0] / count
    rounded = per_token.astype(BF).astype(F32)
    g_hidden = jnp.einsum(
        "ojd,jfd->of",
        rounded.reshape(1, groups, d_local),
        down_full.astype(F32),
        precision=exact,
    )

    packed = jnp.concatenate(
        [hidden_sum, rounded, final, g_logits, jnp.broadcast_to(loss_here, (1, 128))], axis=1
    )

    over_seqs = (((0,), (0,)), ((), ()))
    up_base = lax.dot_general(normed_two, slope, over_seqs, preferred_element_type=F32)
    up_term = (up_base * g_hidden).astype(BF).reshape(groups, d_local, f_local)
    g_pre = (slope.astype(F32) * g_hidden).astype(BF)
    g_normed = lax.dot_general(
        g_pre, up_full, (((1,), (1,)), ((), ())), preferred_element_type=F32
    )
    g_second = (
        norm_back(g_normed)[0] + live[:, None] * (per_token / ranks)
    ).astype(BF)
    spread = lax.dot_general(
        out_full, g_second, (((1,), (1,)), ((), ())), preferred_element_type=F32
    ).astype(BF)
    g_context, up_weight_gradient, every = scatter_and_group(
        spread.reshape(ranks, e_local, span), up_term, packed, ranks, 6
    )
    every = every[:, 0]
    hidden_every = every[:, :f_local]
    rounded_every = every[:, f_local : f_local + width]
    final_every = every[:, f_local + width : f_local + 2 * width]
    rest = every[:, f_local + 2 * width :]
    loss = jnp.sum(rest[:, bins]) / groups
    mine = group * d_local
    down_weight_gradient = lax.dot_general(
        hidden_every,
        lax.dynamic_slice_in_dim(rounded_every, mine, d_local, axis=1),
        over_seqs,
        precision=exact,
    )
    grad_head = lax.dot_general(
        lax.dynamic_slice_in_dim(final_every, mine, d_local, axis=1),
        rest[:, :bins],
        over_seqs,
        precision=exact,
    )

    out_term = (
        jnp.dot(context_all, g_second, preferred_element_type=F32)
        .astype(BF)
        .reshape(ranks, e_local, width)
    )
    g_qkv, out_mine = attend_back(qkv, lengths, lse, g_context, out_term, groups, chunk, 7)
    qkv_term = lax.dot_general(
        normed_one,
        g_qkv.reshape(3 * e_local, span),
        (((0,), (1,)), ((), ())),
        preferred_element_type=F32,
    )
    qkv_gradient, output_weight_gradient = group_sum(
        [qkv_term.astype(BF).reshape(groups, d_local, 3 * e_local), out_mine], 8
    )
    query_key_value_gradient = qkv_gradient.reshape(d_local, 3, e_local)
    return (
        loss,
        query_key_value_gradient,
        output_weight_gradient,
        up_weight_gradient,
        down_weight_gradient,
        grad_head,
    )


def remote(src, dst, sems, index, device):
    return pltpu.make_async_remote_copy(
        src_ref=src,
        dst_ref=dst,
        send_sem=sems[0].at[index],
        recv_sem=sems[1].at[index],
        device_id=device,
        device_id_type=MESH,
    )


class Place:
    def __init__(self):
        self.rank = lax.axis_index("tensor")
        self.across = self.rank + 1 - 2 * lax.rem(self.rank, 2)
        self.over = lax.rem(self.rank + 2, 4)
        self.diag = 3 - self.rank
        self.group = lax.axis_index("dp")
        self.core = lax.rem(self.group, 2)
        self.chip = self.group // 2
        self.near = self.chip * 2 + 1 - self.core

    def turn(self, step):
        return lax.rem(self.chip + step, 4)

    def same(self, chip):
        return chip * 2 + self.core

    def peers(self, everyone=False):
        peers = [{"tensor": one} for one in (self.across, self.over, self.diag)]
        if everyone:
            return peers + [{"dp": lax.rem(self.group + step, 8)} for step in range(1, 8)]
        return peers + [
            {"dp": self.near},
            {"dp": self.same(self.turn(1))},
            {"dp": self.same(self.turn(3))},
        ]

    def signal(self, peers):
        barrier = pltpu.get_barrier_semaphore()
        for peer in peers:
            pl.semaphore_signal(barrier, inc=1, device_id=peer, device_id_type=MESH)

    def ready(self, peers):
        pl.semaphore_wait(pltpu.get_barrier_semaphore(), len(peers))


class RingGather:
    def __init__(self, at, src, own, slot, sems):
        self.at, self.src, self.own, self.slot = at, src, own, slot
        self.sems, self.local = sems[:2], sems[2]

    @staticmethod
    def scratch():
        return [
            pltpu.SemaphoreType.DMA((10,)),
            pltpu.SemaphoreType.DMA((10,)),
            pltpu.SemaphoreType.DMA((1,)),
        ]

    def copies(self):
        at = self.at
        right, left, far = at.turn(1), at.turn(3), at.turn(2)
        me, to_right, to_left = at.group, {"dp": at.same(right)}, {"dp": at.same(left)}
        near = {"dp": at.near}

        def held(index, chip, half, device):
            ref = self.slot(at.same(chip), half)
            return remote(ref, ref, self.sems, index, device)

        def first(index, half, device):
            return remote(self.own(half), self.slot(me, half), self.sems, index, device)

        return (
            first(0, 0, to_right),
            first(1, 1, to_left),
            first(2, 1, to_right),
            first(3, 0, to_left),
            held(4, left, 0, to_right),
            held(5, right, 1, to_left),
            remote(self.src, self.slot(me, None), self.sems, 6, near),
            held(7, left, None, near),
            held(8, right, None, near),
            held(9, far, None, near),
        )

    def keep(self):
        return pltpu.make_async_copy(self.src, self.slot(self.at.group, None), self.local.at[0])

    def start(self):
        copies = self.copies()
        for index in (0, 1, 2, 3, 6):
            copies[index].start()
        self.keep().start()

    def relay(self):
        copies = self.copies()
        copies[0].wait_recv()
        copies[4].start()
        copies[1].wait_recv()
        copies[5].start()

    def spread(self):
        copies = self.copies()
        copies[2].wait_recv()
        copies[7].start()
        copies[3].wait_recv()
        copies[8].start()
        copies[4].wait_recv()
        copies[5].wait_recv()
        copies[9].start()

    def finish(self):
        copies = self.copies()
        for index in (6, 7, 8, 9):
            copies[index].wait_recv()
        for copy in copies:
            copy.wait_send()
        self.keep().wait()

    def near(self):
        copies = self.copies()
        for index in (0, 2):
            copies[index].wait_recv()
        copies[7].start()
        for index in (1, 3):
            copies[index].wait_recv()
        copies[8].start()

    def close_near(self):
        copies = self.copies()
        for index in (6, 7, 8):
            copies[index].wait_recv()
        for index in (0, 1, 2, 3, 6, 7, 8):
            copies[index].wait_send()
        self.keep().wait()

    def pass_on(self):
        copies = self.copies()
        copies[4].start()
        copies[5].start()

    def far(self):
        copies = self.copies()
        copies[4].wait_recv()
        copies[5].wait_recv()
        copies[9].start()

    def close_far(self):
        copies = self.copies()
        copies[9].wait_recv()
        for index in (4, 5, 9):
            copies[index].wait_send()


def columns_of(ref, size):
    rows = ref.shape[0]

    def slot(block, half):
        lanes = pl.ds(pl.multiple_of(block * size, size), size)
        if half is None:
            return ref.at[:, lanes]
        return ref.at[pl.ds(half * (rows // 2), rows // 2), lanes]

    return slot


def rows_of(ref, block, half, size, axis=0):
    lead = (slice(None),) * axis
    if half is None:
        return ref.at[lead + (pl.ds(pl.multiple_of(block * size, size), size),)]
    part = size // 2
    return ref.at[lead + (pl.ds(pl.multiple_of(block * size + half * part, part), part),)]


def half_rows(ref, half, axis=0):
    part = ref.shape[axis] // 2
    return ref.at[(slice(None),) * axis + (pl.ds(half * part, part),)]


def ids_body(ids_ref, ids_all, send, recv):
    at = Place()
    peers = at.peers()[:3]
    at.signal(peers)
    ids_all[at.rank] = ids_ref[...]
    at.ready(peers)
    copies = [
        remote(ids_ref, ids_all.at[at.rank], (send, recv), index, peer)
        for index, peer in enumerate(peers)
    ]
    for copy in copies:
        copy.start()
    for copy in copies:
        copy.wait()


def share_ids(ids, ident):
    return pl.pallas_call(
        ids_body,
        out_shape=jax.ShapeDtypeStruct((4,) + ids.shape, ids.dtype),
        in_specs=[vmem_spec()],
        out_specs=vmem_spec(),
        scratch_shapes=[pltpu.SemaphoreType.DMA((3,))] * 2,
        compiler_params=pltpu.CompilerParams(collective_id=ident, has_side_effects=True),
        name="share_ids",
    )(ids)


def any_spec():
    return pl.BlockSpec(memory_space=pl.ANY)


class Stream:
    def __init__(self, at, x_ref, acc, held, last, whole, sems, index, rows, x_first):
        self.at, self.x, self.acc, self.held, self.last, self.whole = at, x_ref, acc, held, last, whole
        self.sems, self.index, self.rows = sems, index * 6, rows
        self.one, self.two = (at.across, at.over) if x_first else (at.over, at.across)

    def copies(self):
        at, rows, base, sems = self.at, self.rows, self.index, self.sems
        one, two = {"tensor": self.one}, {"tensor": self.two}
        return (
            remote(self.x.at[at.diag, rows], self.held.at[1, rows], sems, base, one),
            remote(self.x.at[self.one, rows], self.held.at[0, rows], sems, base + 1, one),
            remote(self.acc.at[rows], self.last.at[rows], sems, base + 2, two),
            remote(self.whole.at[at.rank, rows], self.whole.at[at.rank, rows], sems, base + 3, two),
            remote(self.whole.at[at.rank, rows], self.whole.at[at.rank, rows], sems, base + 4, one),
            remote(self.whole.at[self.two, rows], self.whole.at[self.two, rows], sems, base + 5, one),
        )

    def start(self):
        copies = self.copies()
        copies[0].start()
        copies[1].start()

    def second(self):
        copies = self.copies()
        copies[0].wait_recv()

        def body(at):
            here = pl.ds(self.rows.start + at.start, at.size)
            self.acc[here] = self.x[self.two, here] + self.held[1, here]

        add_tiles(self.rows.size, 32, body)
        copies[2].start()

    def third(self):
        copies = self.copies()
        copies[1].wait_recv()
        copies[2].wait_recv()

        def body(at):
            here = pl.ds(self.rows.start + at.start, at.size)
            self.whole[self.at.rank, here] = (
                self.x[self.at.rank, here] + self.held[0, here] + self.last[here]
            )

        add_tiles(self.rows.size, 32, body)
        copies[3].start()
        copies[4].start()

    def relay(self):
        copies = self.copies()
        copies[3].wait_recv()
        copies[5].start()

    def beside(self):
        self.copies()[4].wait_recv()

    def opposite(self):
        self.copies()[5].wait_recv()

    def finish(self):
        for copy in self.copies():
            copy.wait_send()


def front_body(
    chunk, length_ref, x_in, w_ref, up_ref, down_ref, head_ref, out_ref,
    first_out, normed_out, qkv_out, ctx_out, lse_ref, up_out, out_full, down_out, head_out,
    x_ref, acc, held, last, whole, normed, qkv_ref, w_full, w_turn, ctx_ref, cols,
    load, saved, send, recv, col_send, col_recv, ctx_send, ctx_recv, ctx_saved, *rest,
):
    at = Place()
    peers = at.peers()
    at.signal(peers)
    entry = pltpu.make_async_copy(x_in, x_ref, load.at[0])
    entry.start()
    d_local = w_ref.shape[1]
    local = x_ref.shape[1]
    e_local = w_ref.shape[2]
    span = qkv_ref.shape[2]
    heads = lse_ref.shape[0]
    size = HEAD_WIDTH // 2
    weights = RingGather(
        at, w_ref, lambda half: half_rows(w_ref, half, 1),
        lambda block, half: rows_of(w_full, block, half, d_local, 1), rest[:3],
    )
    ups = RingGather(
        at, up_ref, lambda half: half_rows(up_ref, half),
        lambda block, half: rows_of(up_out, block, half, d_local), rest[3:6],
    )
    tops = RingGather(
        at, head_ref, lambda half: half_rows(head_ref, half),
        lambda block, half: rows_of(head_out, block, half, d_local), rest[6:9],
    )
    downs = RingGather(
        at, down_ref, lambda half: half_rows(down_ref, half), columns_of(down_out, d_local), rest[9:12]
    )
    outs = RingGather(
        at, cols, lambda half: half_rows(cols, half), columns_of(out_full, d_local), rest[12:15]
    )
    mine = pl.ds(pl.multiple_of(at.rank * e_local, e_local), e_local)
    own_columns = pltpu.make_async_copy(out_ref, cols.at[mine], load.at[1])
    own_columns.start()
    column_copies = [
        remote(out_ref, cols.at[mine], (col_send, col_recv), index, peer)
        for index, peer in enumerate(peers[:3])
    ]

    at.ready(peers)
    weights.start()
    entry.wait()
    part = local // 4
    streams = [
        Stream(
            at, x_ref, acc, held, last, whole, (send, recv), index,
            pl.ds((index % 2) * (local // 2) + (index // 2) * part, part), index % 2 == 0,
        )
        for index in range(4)
    ]
    for one in streams:
        one.start()
    for one in streams:
        one.second()
    weights.relay()
    ups.start()
    tops.start()
    for one in streams:
        one.third()
    for copy in column_copies:
        copy.start()
    weights.spread()
    weights.finish()
    for index in range(3):
        w_turn[index] = w_full[index].T

    def saves(slot, block):
        base = pl.multiple_of(block * local, local)
        return (
            pltpu.make_async_copy(whole.at[block], first_out.at[block], saved.at[slot, 0]),
            pltpu.make_async_copy(normed.at[block], normed_out.at[block], saved.at[slot, 1]),
            pltpu.make_async_copy(
                qkv_ref.at[:, :, pl.ds(base, local)], qkv_out.at[:, :, pl.ds(base, local)], saved.at[slot, 2]
            ),
        )

    def project(block, slot):
        def tile(here):
            normed[block, here] = normalize(whole[block, here].astype(F32)).astype(BF)

        add_tiles(local, 32, tile)
        base = pl.multiple_of(block * local, local)

        def matrix(index, carry):
            qkv_ref[index, :, pl.ds(base, local)] = contract(
                w_turn[index], normed[block], (1, 1)
            ).astype(BF)
            return carry

        lax.fori_loop(0, 3, matrix, 0)
        for copy in saves(slot, block):
            copy.start()

    for one in streams[:2]:
        one.relay()
    project(at.rank, 0)
    for one in streams[2:]:
        one.relay()
    ups.relay()
    tops.relay()
    downs.start()
    for one in streams:
        one.beside()
    project(at.across, 1)
    project(at.over, 2)
    for one in streams:
        one.opposite()
    project(at.diag, 3)
    own_columns.wait()
    for copy in column_copies:
        copy.wait()
    outs.start()

    def copies(one):
        def copy(index, block, half, peer):
            ref = ctx_ref.at[block, pl.ds(pl.multiple_of(one * HEAD_WIDTH + half * size, size), size)]
            return pltpu.make_async_remote_copy(
                src_ref=ref,
                dst_ref=ref,
                send_sem=ctx_send.at[one, index],
                recv_sem=ctx_recv.at[one, index],
                device_id={"tensor": peer},
                device_id_type=MESH,
            )

        return (
            copy(0, at.rank, 0, at.across),
            copy(1, at.rank, 1, at.over),
            copy(2, at.rank, 1, at.across),
            copy(3, at.rank, 0, at.over),
            copy(4, at.across, 0, at.over),
            copy(5, at.over, 1, at.across),
        )

    def relay(one):
        group = copies(one)
        group[0].wait_recv()
        group[4].start()
        group[1].wait_recv()
        group[5].start()

    def save(one):
        here = pl.ds(pl.multiple_of(one * HEAD_WIDTH, HEAD_WIDTH), HEAD_WIDTH)
        return pltpu.make_async_copy(ctx_ref.at[:, here], ctx_out.at[:, here], ctx_saved.at[one])

    length = length_ref[0]
    scale = HEAD_WIDTH ** (-0.5)

    def attend_head(head, carry):
        lines = pl.ds(pl.multiple_of(head * HEAD_WIDTH, HEAD_WIDTH), HEAD_WIDTH)
        keys, vals = qkv_ref[1, lines], qkv_ref[2, lines]
        for start in range(0, span, chunk):
            here = slice(start, start + chunk)
            query = (qkv_ref[0, lines, here].astype(F32) * scale).astype(BF)
            scores = masked_scores(keys, query, length)
            top = jnp.max(scores, axis=0, keepdims=True)
            expo = jnp.exp(scores - top)
            total = jnp.sum(expo, axis=0, keepdims=True)
            mixed = contract(vals, expo.astype(BF), (1, 0))
            ctx_ref[at.rank, lines, here] = (mixed * (1.0 / total)).astype(BF)
            lse_ref[head, :, here] = top + jnp.log(total)

        for copy in copies(head)[:4]:
            copy.start()

        @pl.when(head > 0)
        def _():
            relay(head - 1)

        @pl.when(head == 0)
        def _():
            ups.spread()
            tops.spread()

        @pl.when(head == 1)
        def _():
            downs.near()

        return carry

    lax.fori_loop(0, heads, attend_head, 0)
    outs.relay()
    relay(heads - 1)
    ups.finish()
    tops.finish()
    downs.close_near()
    for one in streams:
        one.finish()

    def drain(one, carry):
        group = copies(one)
        for copy in group[2:]:
            copy.wait_recv()
        save(one).start()
        for copy in group:
            copy.wait_send()
        return carry

    lax.fori_loop(0, heads, drain, 0)
    outs.spread()
    for slot, block in enumerate((at.rank, at.across, at.over, at.diag)):
        for copy in saves(slot, block):
            copy.wait()

    def store(one, carry):
        save(one).wait()
        return carry

    lax.fori_loop(0, heads, store, 0)
    outs.finish()


def front(x, w, up, down, top, out, lengths, chunk, ident):
    ranks, local, width = x.shape
    kinds, d_local, e_local = w.shape
    f_local = up.shape[1]
    heads = e_local // HEAD_WIDTH
    span = ranks * local
    assert heads > 1
    dma = pltpu.SemaphoreType.DMA
    return pl.pallas_call(
        functools.partial(front_body, chunk),
        out_shape=(
            jax.ShapeDtypeStruct(x.shape, BF),
            jax.ShapeDtypeStruct(x.shape, BF),
            jax.ShapeDtypeStruct((kinds, e_local, span), BF),
            jax.ShapeDtypeStruct((ranks, e_local, span), BF),
            jax.ShapeDtypeStruct((heads, 1, span), F32),
            jax.ShapeDtypeStruct((width, f_local), BF),
            jax.ShapeDtypeStruct((ranks * e_local, width), BF),
            jax.ShapeDtypeStruct((f_local, width), BF),
            jax.ShapeDtypeStruct((width, top.shape[1]), BF),
        ),
        in_specs=[pl.BlockSpec(memory_space=pltpu.SMEM), any_spec()] + [vmem_spec()] * 5,
        out_specs=(any_spec(),) * 4 + (vmem_spec(),) + (any_spec(),) * 4,
        scratch_shapes=[
            VMEM(x.shape, BF),
            VMEM((local, width), BF),
            VMEM((2, local, width), BF),
            VMEM((local, width), BF),
            VMEM(x.shape, BF),
            VMEM(x.shape, BF),
            VMEM((kinds, e_local, span), BF),
            VMEM((kinds, width, e_local), BF),
            VMEM((kinds, e_local, width), BF),
            VMEM((ranks, e_local, span), BF),
            VMEM((ranks * e_local, d_local), BF),
            dma((2,)),
            dma((4, 3)),
            dma((24,)),
            dma((24,)),
            dma((3,)),
            dma((3,)),
            dma((heads, 6)),
            dma((heads, 6)),
            dma((heads,)),
        ]
        + RingGather.scratch() * 5,
        compiler_params=pltpu.CompilerParams(
            collective_id=ident, has_side_effects=True, vmem_limit_bytes=BIG
        ),
        name="front",
    )(lengths, x, w, up, down, top, out)


def exact_dot(row, matrix, dims):
    high = row.astype(BF).astype(F32)
    middle = (row - high).astype(BF).astype(F32)
    low = row - high - middle
    shape = (8, row.shape[1])
    index = lax.broadcasted_iota(jnp.int32, shape, 0)
    stacked = jnp.where(
        index == 0, jnp.broadcast_to(high, shape),
        jnp.where(
            index == 1, jnp.broadcast_to(middle, shape),
            jnp.where(index == 2, jnp.broadcast_to(low, shape), 0.0),
        ),
    ).astype(BF)
    return jnp.sum(contract(stacked, matrix, dims), axis=0, keepdims=True)


def classify_body(
    length_ref, bin_ref, normed_ref, up_ref, base_ref, down_in, head_full,
    slope_ref, small_ref, hidden_ref, token_ref,
    sums, down_full, parts, loads, send, recv, *rest,
):
    at = Place()
    step = pl.program_id(0)
    last = pl.num_programs(0) - 1
    units, width = down_full.shape
    chunk = up_ref.shape[1]
    d_local = width // 8
    bins = head_full.shape[1]
    slot = columns_of(down_full, d_local)
    source = columns_of(down_in, d_local)
    downs = RingGather(at, slot(at.group, None), lambda half: slot(at.group, half), slot, rest)

    def load(index):
        block = (at.same(at.turn(1)), at.same(at.turn(3)), at.group)[index % 3]
        if index > 2:
            block = block + 1 - 2 * at.core
        return pltpu.make_async_copy(source(block, None), slot(block, None), loads.at[index])

    @pl.when(step == 0)
    def _():
        at.signal(at.peers())
        for index in range(6):
            load(index).start()

    pre = jnp.dot(normed_ref[...], up_ref[...], preferred_element_type=F32)
    live = lax.broadcasted_iota(jnp.int32, pre.shape, 0) < length_ref[0]
    square = pre * pre
    bend = jnp.tanh(0.7978845608028654 * (pre * (1.0 + 0.044715 * square)))
    half = 0.5 * (1.0 + bend)
    act = (pre * half).astype(BF).astype(F32)
    sums[:, pl.ds(pl.multiple_of(step * chunk, chunk), chunk)] = jnp.sum(
        jnp.where(live, act, 0.0), axis=0, keepdims=True
    )
    inner = 0.7978845608028654 * (1.0 + 3 * 0.044715 * square)
    slope = half + 0.5 * pre * (1.0 - bend * bend) * inner
    slope_ref[...] = jnp.where(live, slope, 0.0).astype(BF)

    @pl.when(step == 0)
    def _():
        at.ready(at.peers())
        load(0).wait()
        load(1).wait()
        downs.pass_on()

    @pl.when(step == last)
    def _():
        downs.far()
        for index in range(2, 6):
            load(index).wait()
        downs.close_far()
        hidden_sum = sums[...]
        parts[at.rank] = exact_dot(hidden_sum, down_full[...], (1, 0))
        copies = [
            remote(parts.at[at.rank], parts.at[at.rank], (send, recv), index, {"tensor": peer})
            for index, peer in enumerate((at.across, at.over, at.diag))
        ]
        for copy in copies:
            copy.start()
        for copy in copies:
            copy.wait()
        count = jnp.full((1, 1), length_ref[0], jnp.int32).astype(F32)
        total = base_ref[...]
        for index in range(4):
            total = total + parts[index]
        pooled = total / count
        mean = jnp.mean(pooled, axis=-1, keepdims=True)
        centered = pooled - mean
        scale = lax.rsqrt(jnp.mean(centered * centered, axis=-1, keepdims=True) + EPS)
        final = centered * scale
        logits = exact_dot(final, head_full[...], (1, 0))
        top = jnp.max(logits, axis=-1, keepdims=True)
        total_exp = jnp.log(jnp.sum(jnp.exp(logits - top), axis=-1, keepdims=True)) + top
        labels = (lax.broadcasted_iota(jnp.int32, logits.shape, 1) == bin_ref[0]).astype(F32)
        loss = total_exp - jnp.sum(logits * labels, axis=-1, keepdims=True)
        g_logits = (jnp.exp(logits - total_exp) - labels) / 8.0
        g_final = exact_dot(g_logits, head_full[...], (1, 1))
        g_pooled = scale * (
            g_final
            - jnp.mean(g_final, axis=-1, keepdims=True)
            - final * jnp.mean(g_final * final, axis=-1, keepdims=True)
        )
        per_token = g_pooled / count
        rounded = per_token.astype(BF)
        token_ref[...] = per_token
        hidden_ref[...] = contract(
            jnp.broadcast_to(rounded.astype(F32), (8, width)).astype(BF), down_full[...], (1, 1)
        )[:1]
        small_ref[:, :units] = hidden_sum
        small_ref[:, units : units + width] = rounded.astype(F32)
        small_ref[:, units + width : units + 2 * width] = final
        small_ref[:, units + 2 * width : units + 2 * width + bins] = g_logits
        small_ref[:, units + 2 * width + bins :] = jnp.broadcast_to(loss, (1, 128))


def classify(normed, up, base, down, head, lengths, bins_at, chunk, ident):
    length, width = normed.shape
    units = up.shape[1]
    bins = head.shape[1]
    return pl.pallas_call(
        classify_body,
        grid=(units // chunk,),
        out_shape=(
            jax.ShapeDtypeStruct((length, units), BF),
            jax.ShapeDtypeStruct((1, units + 2 * width + bins + 128), F32),
            jax.ShapeDtypeStruct((1, units), F32),
            jax.ShapeDtypeStruct((1, width), F32),
        ),
        in_specs=[
            pl.BlockSpec(memory_space=pltpu.SMEM),
            pl.BlockSpec(memory_space=pltpu.SMEM),
            vmem_spec(),
            pl.BlockSpec((width, chunk), lambda f: (0, f)),
            vmem_spec(),
            any_spec(),
            vmem_spec(),
        ],
        out_specs=(
            pl.BlockSpec((length, chunk), lambda f: (0, f)),
            vmem_spec(),
            vmem_spec(),
            vmem_spec(),
        ),
        scratch_shapes=[
            VMEM((1, units), F32),
            VMEM((units, width), BF),
            VMEM((4, 1, width), F32),
            pltpu.SemaphoreType.DMA((6,)),
            pltpu.SemaphoreType.DMA((3,)),
            pltpu.SemaphoreType.DMA((3,)),
        ]
        + RingGather.scratch(),
        compiler_params=pltpu.CompilerParams(
            collective_id=ident, has_side_effects=True, vmem_limit_bytes=BIG
        ),
        name="classify",
    )(lengths, bins_at, normed, up, base, down, head)


class Fold:
    def __init__(self, at, src, held, acc, last, sems, base, rows, x_first):
        self.at, self.src, self.held, self.acc, self.last = at, src, held, acc, last
        self.sems, self.base, self.rows = sems, base, rows
        self.one, self.two = (at.across, at.over) if x_first else (at.over, at.across)

    def copies(self):
        rows, base, sems = self.rows, self.base, self.sems
        one, two = {"tensor": self.one}, {"tensor": self.two}
        return (
            remote(self.src.at[self.at.diag, rows], self.held.at[1, rows], sems, base, one),
            remote(self.src.at[self.one, rows], self.held.at[0, rows], sems, base + 1, one),
            remote(self.acc.at[rows], self.last.at[rows], sems, base + 2, two),
        )

    def start(self):
        copies = self.copies()
        copies[0].start()
        copies[1].start()

    def tiles(self, body):
        def step(at):
            body(pl.ds(pl.multiple_of(self.rows.start + at.start, 32), at.size))

        add_tiles(self.rows.size, 32, step)

    def second(self):
        copies = self.copies()
        copies[0].wait_recv()

        def body(here):
            self.acc[here] = (
                self.src[self.two, here].astype(F32) + self.held[1, here].astype(F32)
            ).astype(BF)

        self.tiles(body)
        copies[2].start()

    def third(self, put):
        copies = self.copies()
        copies[1].wait_recv()
        copies[2].wait_recv()

        def body(here):
            put(
                here,
                self.src[self.at.rank, here].astype(F32)
                + self.held[0, here].astype(F32)
                + self.last[here].astype(F32),
            )

        self.tiles(body)

    def finish(self):
        for copy in self.copies():
            copy.wait_send()


class DirectSum(GroupSum):
    def __init__(self, x_ref, pair, mine, far, sems, tile):
        super().__init__(x_ref, None, pair, mine, far, sems)
        self.tile = tile

    def middle(self):
        for copy in self.pair_copies():
            copy.wait()
        for chip in range(self.chips):

            def body(at, chip=chip):
                self.mine[chip, at] = (
                    self.x[chip * 2 + self.core, at].astype(F32)
                    + self.pair[chip, at].astype(F32)
                ).astype(BF)

            add_tiles(self.rows, self.tile, body)
        for copy in self.far_copies():
            copy.start()

    def finish(self, put):
        for copy in self.far_copies():
            copy.wait()

        def body(at):
            total = self.mine[self.chip, at].astype(F32)
            for step in range(self.chips - 1):
                total = total + self.far[step, at].astype(F32)
            put(at, total)

        add_tiles(self.far.shape[1], self.tile, body)


def backward_body(
    chunk, length_ref, qkv_ref, lse_ref, small_ref, g_second_in, out_in, up_in, ctx_in, normed_in,
    qkv_out, out_out, up_out, small_out,
    g_second, outs, up_term, ctx, normed, loads,
    spread, g_ctx, s_held, s_acc, s_last, s_send, s_recv,
    out_term, o_pair, out_sum, o_held, o_acc, o_last, o_send, o_recv,
    o_own, o_far, o_sem0, o_sem1, o_sem2, o_sem3,
    u_pair, u_own, u_far, u_sem0, u_sem1, u_sem2, u_sem3,
    g_qkv, q_term, q_pair, q_own, q_far, q_sem0, q_sem1, q_sem2, q_sem3,
    smalls, m_send, m_recv,
):
    at = Place()
    head = pl.program_id(0)
    heads = lse_ref.shape[0] * q_term.shape[0]
    end = heads - 1
    e_local = g_ctx.shape[0]
    d_local = q_term.shape[3]
    groups = q_term.shape[1]
    half = HEAD_WIDTH // 2
    length = length_ref[0]
    scale = HEAD_WIDTH ** (-0.5)
    span = qkv_ref.shape[2]

    def load(index):
        pairs = (
            (g_second_in, g_second), (out_in, outs), (up_in, up_term), (ctx_in, ctx), (normed_in, normed)
        )
        return pltpu.make_async_copy(*pairs[index], loads.at[index])

    def folds(one):
        return [
            Fold(
                at, spread, s_held, s_acc, s_last, (s_send, s_recv), one * 6 + part * 3,
                pl.ds(pl.multiple_of(one * HEAD_WIDTH + part * half, half), half), part == 0,
            )
            for part in range(2)
        ]

    out_folds = [
        Fold(
            at, out_sum, o_held, o_acc, o_last, (o_send, o_recv), part * 3,
            pl.ds(part * (e_local // 2), e_local // 2), part == 0,
        )
        for part in range(2)
    ]
    up_sum = GroupSum(up_term, up_out, u_pair, u_own, u_far, (u_sem0, u_sem1, u_sem2, u_sem3))
    out_group = DirectSum(out_term, o_pair, o_own, o_far, (o_sem0, o_sem1, o_sem2, o_sem3), 64)

    def qkv_sum(one):
        return DirectSum(
            q_term.at[one], q_pair.at[one], q_own.at[one], q_far.at[one],
            (q_sem0.at[one], q_sem1.at[one], q_sem2.at[one], q_sem3.at[one]), q_term.shape[2],
        )

    def small_copies():
        return [
            remote(
                small_ref, smalls.at[at.group], (m_send, m_recv), step - 1,
                {"dp": lax.rem(at.group + step, groups)},
            )
            for step in range(1, groups)
        ]

    def put_context(here, total):
        g_ctx[here] = total.astype(BF)

    def put_out(here, total):
        for chip in range(4):
            o_own[chip, here] = total[:, chip * d_local : (chip + 1) * d_local].astype(BF)

    def pair_out():
        for copy in out_group.pair_copies():
            copy.wait()

        def block(one, carry):
            for chip in range(4):

                def body(rows):
                    here = pl.ds(pl.multiple_of(one * e_local + rows.start, 64), rows.size)
                    out_sum[one, rows, chip * d_local : (chip + 1) * d_local] = (
                        out_term[chip * 2 + at.core, here].astype(F32)
                        + o_pair[chip, here].astype(F32)
                    ).astype(BF)

                add_tiles(e_local, 64, body)
            return carry

        lax.fori_loop(0, 4, block, 0)

    @pl.when(head == 0)
    def _():
        at.signal(at.peers(True))
        for index in range(5):
            load(index).start()
        load(2).wait()
        at.ready(at.peers(True))
        up_sum.start()
        for copy in small_copies():
            copy.start()
        smalls[at.group] = small_ref[...]
        load(0).wait()
        load(1).wait()

        def spread_head(one, carry):
            left = jnp.concatenate(
                [
                    outs[pl.ds(pl.multiple_of(part * e_local + one * HEAD_WIDTH, HEAD_WIDTH), HEAD_WIDTH)]
                    for part in range(4)
                ],
                axis=0,
            )
            result = contract(left, g_second[...], (1, 1)).astype(BF)
            for part in range(4):
                spread[part, pl.ds(pl.multiple_of(one * HEAD_WIDTH, HEAD_WIDTH), HEAD_WIDTH)] = result[
                    part * HEAD_WIDTH : (part + 1) * HEAD_WIDTH
                ]
            for fold in folds(one):
                fold.start()
            return carry

        lax.fori_loop(0, 2, spread_head, 0)
        up_sum.middle()
        for fold in folds(0):
            fold.second()
        lax.fori_loop(2, heads, spread_head, 0)
        for fold in folds(1):
            fold.second()
        load(3).wait()

        def out_block(one, carry):
            rows = pl.ds(pl.multiple_of(one * e_local, e_local), e_local)
            result = jnp.dot(ctx[rows], g_second[...], preferred_element_type=F32)
            for group in range(groups):
                out_term[group, rows] = result[:, group * d_local : (group + 1) * d_local].astype(BF)
            return carry

        lax.fori_loop(0, 4, out_block, 0)
        out_group.start()
        load(4).wait()

    for fold in folds(head):
        fold.third(put_context)

    keys, vals = qkv_ref[1], qkv_ref[2]
    g_keys = jnp.zeros((HEAD_WIDTH, span), F32)
    g_vals = jnp.zeros((HEAD_WIDTH, span), F32)
    mine = pl.ds(pl.multiple_of(head * HEAD_WIDTH, HEAD_WIDTH), HEAD_WIDTH)
    for index, start in enumerate(range(0, span, chunk)):
        here = slice(start, start + chunk)
        query = (qkv_ref[0, :, here].astype(F32) * scale).astype(BF)
        grad = g_ctx[mine, here]
        probs = jnp.exp(masked_scores(keys, query, length) - lse_ref[0, :, here])
        g_probs = contract(vals, grad, (0, 0))
        weighted = probs * g_probs
        inner = jnp.sum(weighted, axis=0, keepdims=True)
        g_scores = (weighted - probs * inner).astype(BF)
        g_qkv[:HEAD_WIDTH, here] = (contract(keys, g_scores, (1, 0)) * scale).astype(BF)
        g_keys += contract(query, g_scores, (1, 1))
        g_vals += contract(grad, probs.astype(BF), (1, 1))
        if index == 1:

            @pl.when(head > 0)
            def _():
                qkv_sum(head - 1).middle()

            @pl.when(head == 1)
            def _():
                for fold in out_folds:
                    fold.second()

            @pl.when(head == 2)
            def _():
                for fold in out_folds:
                    fold.third(put_out)
                for copy in out_group.far_copies():
                    copy.start()

    g_qkv[HEAD_WIDTH : 2 * HEAD_WIDTH] = g_keys.astype(BF)
    g_qkv[2 * HEAD_WIDTH :] = g_vals.astype(BF)
    result = jnp.dot(g_qkv[...], normed[...], preferred_element_type=F32)
    for group in range(groups):
        q_term[head, group] = result[:, group * d_local : (group + 1) * d_local].astype(BF)
    qkv_sum(head).start()

    @pl.when(head == 0)
    def _():
        def second(one, carry):
            for fold in folds(one):
                fold.second()
            return carry

        lax.fori_loop(2, heads, second, 0)
        pair_out()
        for fold in out_folds:
            fold.start()
        up_sum.relay()

    @pl.when(head == end)
    def _():
        qkv_sum(head).middle()
        up_sum.finish()
        for copy in small_copies():
            copy.wait()
        small_out[...] = smalls[...]

        def drain(one, carry):
            for fold in folds(one):
                fold.finish()
            return carry

        lax.fori_loop(0, heads, drain, 0)
        for fold in out_folds:
            fold.finish()

        def put_final(here, total):
            out_out[here] = total

        out_group.finish(put_final)

        def store(one, carry):
            def put(here, total):
                for kind in range(3):
                    qkv_out[kind, pl.ds(pl.multiple_of(one * HEAD_WIDTH, HEAD_WIDTH), HEAD_WIDTH)] = total[
                        kind * HEAD_WIDTH : (kind + 1) * HEAD_WIDTH
                    ]

            qkv_sum(one).finish(put)
            return carry

        lax.fori_loop(0, heads, store, 0)


def backward(qkv, lengths, lse, small, g_second, out_full, up_term, context, normed, chunk, ident):
    _, width, length = qkv.shape
    heads = width // HEAD_WIDTH
    groups, d_local, f_local = up_term.shape
    full = out_full.shape[1]
    rows = 3 * HEAD_WIDTH
    dma = pltpu.SemaphoreType.DMA
    return pl.pallas_call(
        functools.partial(backward_body, chunk),
        grid=(heads,),
        out_shape=(
            jax.ShapeDtypeStruct((3, width, d_local), F32),
            jax.ShapeDtypeStruct((width, d_local), F32),
            jax.ShapeDtypeStruct((d_local, f_local), F32),
            jax.ShapeDtypeStruct((groups,) + small.shape, F32),
        ),
        in_specs=[
            pl.BlockSpec(memory_space=pltpu.SMEM),
            pl.BlockSpec((3, HEAD_WIDTH, length), lambda h: (0, h, 0)),
            pl.BlockSpec((1, 1, length), lambda h: (h, 0, 0)),
            vmem_spec(),
        ]
        + [any_spec()] * 5,
        out_specs=(vmem_spec(),) * 4,
        scratch_shapes=[
            VMEM(g_second.shape, BF),
            VMEM(out_full.shape, BF),
            VMEM(up_term.shape, BF),
            VMEM(context.shape, BF),
            VMEM(normed.shape, BF),
            dma((5,)),
            VMEM((4, width, length), BF),
            VMEM((width, length), BF),
            VMEM((2, width, length), BF),
            VMEM((width, length), BF),
            VMEM((width, length), BF),
            dma((heads * 6,)),
            dma((heads * 6,)),
            VMEM((groups, 4 * width, d_local), BF),
            VMEM((4, 4 * width, d_local), BF),
            VMEM((4, width, full // 2), BF),
            VMEM((2, width, full // 2), BF),
            VMEM((width, full // 2), BF),
            VMEM((width, full // 2), BF),
            dma((6,)),
            dma((6,)),
            VMEM((4, width, d_local), BF),
            VMEM((3, width, d_local), BF),
            dma((4,)),
            dma((4,)),
            dma((3,)),
            dma((3,)),
        ]
        + GroupSum.scratch(up_term.shape, BF)
        + [
            VMEM((rows, length), BF),
            VMEM((heads, groups, rows, d_local), BF),
            VMEM((heads, 4, rows, d_local), BF),
            VMEM((heads, 4, rows, d_local), BF),
            VMEM((heads, 3, rows, d_local), BF),
            dma((heads, 4)),
            dma((heads, 4)),
            dma((heads, 3)),
            dma((heads, 3)),
            VMEM((groups,) + small.shape, F32),
            dma((groups - 1,)),
            dma((groups - 1,)),
        ],
        compiler_params=pltpu.CompilerParams(
            collective_id=ident, has_side_effects=True, vmem_limit_bytes=BIG
        ),
        name="backward",
    )(lengths, qkv, lse, small, g_second, out_full, up_term, context, normed)


def per_device_block(
    token_ids,
    lengths,
    teacher_bins,
    embed_table,
    query_key_value_matrix,
    output_matrix,
    up_matrix,
    down_matrix,
    w_head,
):
    ranks = lax.axis_size("tensor")
    groups = lax.axis_size("dp")
    rank = lax.axis_index("tensor")
    group = lax.axis_index("dp")
    assert token_ids.shape[0] == 1
    local_len = token_ids.shape[1]
    span = local_len * ranks
    vocab_local, width = embed_table.shape
    d_local, _, e_local = query_key_value_matrix.shape
    f_local = up_matrix.shape[1]
    bins = w_head.shape[1]
    exact = lax.Precision.HIGHEST

    all_ids = share_ids(token_ids, 11)
    all_ids = all_ids.reshape(ranks, local_len)
    shifted = all_ids - rank * vocab_local
    inside = (shifted >= 0) & (shifted < vocab_local)
    rows = jnp.take(embed_table, jnp.clip(shifted, 0, vocab_local - 1), axis=0)
    chunk = min(256, span)
    first, normed_one, qkv, context, lse, up_full, out_full, down_part, head_full = front(
        jnp.where(inside[..., None], rows, jnp.zeros((), BF)),
        query_key_value_matrix.transpose(1, 0, 2),
        up_matrix,
        down_matrix,
        w_head,
        output_matrix,
        lengths,
        chunk,
        12,
    )
    first = first.reshape(span, width)
    normed_one = normed_one.reshape(span, width)
    context_all = context.reshape(ranks * e_local, span)
    attn = lax.dot_general(
        context_all, out_full, (((0,), (0,)), ((), ())), preferred_element_type=F32
    )
    second = (first.astype(F32) + attn).astype(BF)
    normed_f, norm_back = jax.vjp(normalize, second.astype(F32))
    normed_two = normed_f.astype(BF)
    live = (jnp.arange(span, dtype=jnp.int32) < lengths[0]).astype(F32)
    second_sum = jnp.sum(second.astype(F32) * live[:, None], axis=0, keepdims=True)
    slope, packed, g_hidden, per_token = classify(
        normed_two, up_full, second_sum, down_part, head_full, lengths, teacher_bins,
        min(256, f_local), 14,
    )

    over_seqs = (((0,), (0,)), ((), ()))
    up_base = lax.dot_general(normed_two, slope, over_seqs, preferred_element_type=F32)
    up_term = (up_base * g_hidden).astype(BF).reshape(groups, d_local, f_local)
    g_pre = (slope.astype(F32) * g_hidden).astype(BF)
    g_normed = lax.dot_general(
        g_pre, up_full, (((1,), (1,)), ((), ())), preferred_element_type=F32
    )
    g_second = (
        norm_back(g_normed)[0] + live[:, None] * (per_token / ranks)
    ).astype(BF)
    qkv_gradient, output_weight_gradient, up_weight_gradient, every = backward(
        qkv, lengths, lse, packed, g_second, out_full, up_term, context_all, normed_one, chunk, 15
    )
    every = every[:, 0]
    hidden_every = every[:, :f_local]
    rounded_every = every[:, f_local : f_local + width]
    final_every = every[:, f_local + width : f_local + 2 * width]
    rest = every[:, f_local + 2 * width :]
    loss = jnp.sum(rest[:, bins]) / groups
    mine = group * d_local
    down_weight_gradient = lax.dot_general(
        hidden_every,
        lax.dynamic_slice_in_dim(rounded_every, mine, d_local, axis=1),
        over_seqs,
        precision=exact,
    )
    grad_head = lax.dot_general(
        lax.dynamic_slice_in_dim(final_every, mine, d_local, axis=1),
        rest[:, :bins],
        over_seqs,
        precision=exact,
    )

    query_key_value_gradient = qkv_gradient.transpose(2, 0, 1)
    return (
        loss,
        query_key_value_gradient,
        output_weight_gradient,
        up_weight_gradient,
        down_weight_gradient,
        grad_head,
    )


def solution(mesh):
    placed = (
        P("dp", "tensor"),
        P("dp"),
        P("dp"),
        P("tensor", None),
        P("dp", None, "tensor"),
        P("tensor", "dp"),
        P("dp", "tensor"),
        P("tensor", "dp"),
        P("dp", None),
    )
    return jax.shard_map(
        per_device_block if (mesh.shape["tensor"], mesh.shape["dp"]) == (4, 8) else per_device,
        mesh=mesh,
        in_specs=placed,
        out_specs=(
            P(),
            P("dp", None, "tensor"),
            P("tensor", "dp"),
            P("dp", "tensor"),
            P("tensor", "dp"),
            P("dp", None),
        ),
        check_vma=False,
    )
```

```python
import functools

import jax
import jax.numpy as jnp
from jax import lax
from jax.experimental import pallas as pl
from jax.experimental.pallas import tpu as pltpu
from jax.sharding import PartitionSpec as P

HEAD_WIDTH = 64
EPS = 1e-05
BF = jnp.bfloat16
F32 = jnp.float32
MESH = pl.DeviceIdType.MESH
VMEM = pltpu.VMEM
BIG = 60 * 1024 * 1024


def normalize(values):
    mean = jnp.mean(values, axis=-1, keepdims=True)
    centered = values - mean
    return centered * lax.rsqrt(jnp.mean(centered * centered, axis=-1, keepdims=True) + EPS)


def vmem_spec():
    return pl.BlockSpec(memory_space=pltpu.VMEM)


def greet(axis, count):
    me = lax.axis_index(axis)
    barrier = pltpu.get_barrier_semaphore()
    for step in range(1, count):
        pl.semaphore_signal(
            barrier, inc=1, device_id={axis: lax.rem(me + step, count)}, device_id_type=MESH
        )
    pl.semaphore_wait(barrier, count - 1)
    return me


def gather_body(axis, count, x_ref, out_ref, send_sem, recv_sem):
    me = greet(axis, count)
    copies = []
    for step in range(1, count):
        copy = pltpu.make_async_remote_copy(
            src_ref=x_ref,
            dst_ref=out_ref.at[me],
            send_sem=send_sem.at[step - 1],
            recv_sem=recv_sem.at[step - 1],
            device_id={axis: lax.rem(me + step, count)},
            device_id_type=MESH,
        )
        copy.start()
        copies.append(copy)
    out_ref[me] = x_ref[...]
    for copy in copies:
        copy.wait()


def relay_gather(axis, me, src, out, send_sem, recv_sem):
    across = me + 1 - 2 * lax.rem(me, 2)
    over = lax.rem(me + 2, 4)
    half = src.shape[0] // 2
    low, high = pl.ds(0, half), pl.ds(half, half)

    def copy(index, src_part, block, part, device):
        return pltpu.make_async_remote_copy(
            src_ref=src_part,
            dst_ref=out.at[block, part],
            send_sem=send_sem.at[index],
            recv_sem=recv_sem.at[index],
            device_id={axis: device},
            device_id_type=MESH,
        )

    first_a = copy(0, src.at[low], me, low, across)
    first_b = copy(1, src.at[high], me, high, over)
    second_a = copy(2, src.at[high], me, high, across)
    second_b = copy(3, src.at[low], me, low, over)
    for one in (first_a, first_b, second_a, second_b):
        one.start()
    first_a.wait_recv()
    pass_b = copy(4, out.at[across, low], across, low, over)
    pass_b.start()
    first_b.wait_recv()
    pass_a = copy(5, out.at[over, high], over, high, across)
    pass_a.start()
    second_a.wait_recv()
    second_b.wait_recv()
    pass_b.wait_recv()
    pass_a.wait_recv()
    for one in (first_a, first_b, second_a, second_b, pass_b, pass_a):
        one.wait_send()


def relay_body(axis, x_ref, out_ref, send_sem, recv_sem):
    me = greet(axis, 4)
    relay_gather(axis, me, x_ref, out_ref, send_sem, recv_sem)
    out_ref[me] = x_ref[...]


def gather_blocks(x, axis, count, ident):
    if count != 4:
        return gather_all(x, axis, count, ident)
    return pl.pallas_call(
        functools.partial(relay_body, axis),
        out_shape=jax.ShapeDtypeStruct((count,) + x.shape, x.dtype),
        in_specs=[vmem_spec()],
        out_specs=vmem_spec(),
        scratch_shapes=[pltpu.SemaphoreType.DMA((6,)), pltpu.SemaphoreType.DMA((6,))],
        compiler_params=pltpu.CompilerParams(collective_id=ident, has_side_effects=True),
        name="gather_blocks",
    )(x)


def gather_all(x, axis, count, ident):
    return pl.pallas_call(
        functools.partial(gather_body, axis, count),
        out_shape=jax.ShapeDtypeStruct((count,) + x.shape, x.dtype),
        in_specs=[vmem_spec()],
        out_specs=vmem_spec(),
        scratch_shapes=[
            pltpu.SemaphoreType.DMA((count - 1,)),
            pltpu.SemaphoreType.DMA((count - 1,)),
        ],
        compiler_params=pltpu.CompilerParams(collective_id=ident, has_side_effects=True),
        name="gather_all",
    )(x)


def scatter_copies(axis, count, me, x_ref, held, send_sem, recv_sem):
    copies = []
    for step in range(1, count):
        peer = lax.rem(me + step, count)
        copies.append(
            pltpu.make_async_remote_copy(
                src_ref=x_ref.at[peer],
                dst_ref=held.at[step - 1],
                send_sem=send_sem.at[step - 1],
                recv_sem=recv_sem.at[step - 1],
                device_id={axis: peer},
                device_id_type=MESH,
            )
        )
    return copies


def scatter_start(*args):
    for copy in scatter_copies(*args):
        copy.start()


def scatter_finish(axis, count, me, x_ref, held, send_sem, recv_sem, put):
    for copy in scatter_copies(axis, count, me, x_ref, held, send_sem, recv_sem):
        copy.wait()

    def body(at):
        total = x_ref[me, at].astype(F32)
        for step in range(1, count):
            total = total + held[step - 1, at].astype(F32)
        put(at, total)

    add_tiles(x_ref.shape[1], 32, body)


def add_tiles(rows, tile, body):
    def step(index, carry):
        body(pl.ds(pl.multiple_of(index * tile, tile), tile))
        return carry

    lax.fori_loop(0, rows // tile, step, 0)


class GroupSum:
    def __init__(self, x_ref, out_ref, pair, mine, far, sems):
        self.x, self.out, self.pair, self.mine, self.far = x_ref, out_ref, pair, mine, far
        self.sems = sems
        self.groups = x_ref.shape[0]
        self.chips = self.groups // 2
        self.rows = x_ref.shape[1]
        me = lax.axis_index("dp")
        self.core = lax.rem(me, 2)
        self.chip = me // 2
        self.near = self.chip * 2 + 1 - self.core

    @staticmethod
    def scratch(shape, dtype):
        groups, rows, columns = shape
        chips = groups // 2
        return [
            VMEM((chips, rows, columns), dtype),
            VMEM((chips, rows, columns), dtype),
            VMEM((chips - 1, rows, columns), dtype),
            pltpu.SemaphoreType.DMA((chips,)),
            pltpu.SemaphoreType.DMA((chips,)),
            pltpu.SemaphoreType.DMA((6 if chips == 4 else chips - 1,)),
            pltpu.SemaphoreType.DMA((6 if chips == 4 else chips - 1,)),
        ]

    def signal(self, barrier):
        pl.semaphore_signal(
            barrier, inc=1, device_id={"dp": self.near}, device_id_type=MESH
        )
        for step in range(1, self.chips):
            pl.semaphore_signal(
                barrier, inc=1, device_id={"dp": self.owner(step)}, device_id_type=MESH
            )
        return self.chips

    def owner(self, step):
        return lax.rem(self.chip + step, self.chips) * 2 + self.core

    def pair_copies(self):
        copies = []
        for chip in range(self.chips):
            copies.append(
                pltpu.make_async_remote_copy(
                    src_ref=self.x.at[chip * 2 + 1 - self.core],
                    dst_ref=self.pair.at[chip],
                    send_sem=self.sems[0].at[chip],
                    recv_sem=self.sems[1].at[chip],
                    device_id={"dp": self.near},
                    device_id_type=MESH,
                )
            )
        return copies

    def far_copies(self):
        copies = []
        for step in range(1, self.chips):
            copies.append(
                pltpu.make_async_remote_copy(
                    src_ref=self.mine.at[lax.rem(self.chip + step, self.chips)],
                    dst_ref=self.far.at[step - 1],
                    send_sem=self.sems[2].at[step - 1],
                    recv_sem=self.sems[3].at[step - 1],
                    device_id={"dp": self.owner(step)},
                    device_id_type=MESH,
                )
            )
        return copies

    def ring_copies(self):
        right, left = lax.rem(self.chip + 1, 4), lax.rem(self.chip + 3, 4)
        opposite = lax.rem(self.chip + 2, 4)
        half = self.rows // 2
        low, high = pl.ds(0, half), pl.ds(half, half)

        def copy(index, block, part, slot, chip):
            return pltpu.make_async_remote_copy(
                src_ref=self.mine.at[block, part],
                dst_ref=self.far.at[slot, part],
                send_sem=self.sems[2].at[index],
                recv_sem=self.sems[3].at[index],
                device_id={"dp": chip * 2 + self.core},
                device_id_type=MESH,
            )

        return (
            copy(0, opposite, low, 2, right),
            copy(1, opposite, high, 2, left),
            copy(2, right, high, 0, right),
            copy(3, left, low, 1, left),
            copy(4, right, low, 0, right),
            copy(5, left, high, 1, left),
        )

    def relay(self):
        if self.chips != 4:
            return
        copies = self.ring_copies()
        half = self.rows // 2
        for index, step, base in ((0, 1, 0), (1, 3, half)):
            copies[index].wait_recv()
            block = lax.rem(self.chip + step, 4)

            def body(at, block=block, base=base):
                here = pl.ds(base + at.start, at.size)
                self.mine[block, here] = (
                    self.mine[block, here].astype(F32) + self.far[2, here].astype(F32)
                ).astype(self.mine.dtype)

            add_tiles(half, 32, body)
            copies[index + 4].start()

    def start(self):
        for copy in self.pair_copies():
            copy.start()

    def middle(self):
        for copy in self.pair_copies():
            copy.wait()

        for chip in range(self.chips):

            def body(at, chip=chip):
                self.mine[chip, at] = (
                    self.x[chip * 2 + self.core, at].astype(F32)
                    + self.pair[chip, at].astype(F32)
                ).astype(self.mine.dtype)

            add_tiles(self.rows, 32, body)
        copies = self.ring_copies()[:4] if self.chips == 4 else self.far_copies()
        for copy in copies:
            copy.start()

    def finish(self):
        if self.chips == 4:
            copies = self.ring_copies()
            for copy in copies[2:]:
                copy.wait()
            for copy in copies[:2]:
                copy.wait_send()
        else:
            for copy in self.far_copies():
                copy.wait()

        def body(at):
            total = self.mine[self.chip, at].astype(F32)
            for step in range(2 if self.chips == 4 else self.chips - 1):
                total = total + self.far[step, at].astype(F32)
            self.out[at] = total

        add_tiles(self.rows, 32, body)


def scatter_and_group_body(
    count, x_ref, up_ref, small_ref, out_ref, up_out, small_out, held, send_sem, recv_sem, *rest
):
    up = GroupSum(up_ref, up_out, rest[0], rest[1], rest[2], rest[3:7])
    small_send, small_recv = rest[7:]
    groups = small_out.shape[0]
    group = lax.axis_index("dp")
    barrier = pltpu.get_barrier_semaphore()
    me = lax.axis_index("tensor")
    for step in range(1, count):
        pl.semaphore_signal(
            barrier, inc=1, device_id={"tensor": lax.rem(me + step, count)}, device_id_type=MESH
        )
    for step in range(1, groups):
        pl.semaphore_signal(
            barrier, inc=1, device_id={"dp": lax.rem(group + step, groups)}, device_id_type=MESH
        )
    pl.semaphore_wait(barrier, count + groups - 2)
    smalls = []
    for step in range(1, groups):
        smalls.append(
            pltpu.make_async_remote_copy(
                src_ref=small_ref,
                dst_ref=small_out.at[group],
                send_sem=small_send.at[step - 1],
                recv_sem=small_recv.at[step - 1],
                device_id={"dp": lax.rem(group + step, groups)},
                device_id_type=MESH,
            )
        )

    def put(at, total):
        out_ref[at] = total.astype(out_ref.dtype)

    up.start()
    scatter_start("tensor", count, me, x_ref, held, send_sem, recv_sem)
    up.middle()
    for copy in smalls:
        copy.start()
    small_out[group] = small_ref[...]
    up.relay()
    scatter_finish("tensor", count, me, x_ref, held, send_sem, recv_sem, put)
    up.finish()
    for copy in smalls:
        copy.wait()


def scatter_and_group(x, up, small, count, ident):
    return pl.pallas_call(
        functools.partial(scatter_and_group_body, count),
        out_shape=(
            jax.ShapeDtypeStruct(x.shape[1:], x.dtype),
            jax.ShapeDtypeStruct(up.shape[1:], F32),
            jax.ShapeDtypeStruct(up.shape[:1] + small.shape, F32),
        ),
        in_specs=[vmem_spec()] * 3,
        out_specs=(vmem_spec(),) * 3,
        scratch_shapes=[
            VMEM((count - 1,) + x.shape[1:], x.dtype),
            pltpu.SemaphoreType.DMA((count - 1,)),
            pltpu.SemaphoreType.DMA((count - 1,)),
        ]
        + GroupSum.scratch(up.shape, up.dtype)
        + [pltpu.SemaphoreType.DMA((up.shape[0] - 1,))] * 2,
        compiler_params=pltpu.CompilerParams(
            collective_id=ident, has_side_effects=True, vmem_limit_bytes=BIG
        ),
        name="scatter_and_group",
    )(x, up, small)


def group_sum_body(number, *refs):
    xs, outs, rest = refs[:number], refs[number : 2 * number], refs[2 * number :]
    sums = [
        GroupSum(x, out, *rest[7 * i : 7 * i + 3], rest[7 * i + 3 : 7 * i + 7])
        for i, (x, out) in enumerate(zip(xs, outs))
    ]
    barrier = pltpu.get_barrier_semaphore()
    pl.semaphore_wait(barrier, sums[0].signal(barrier))
    for one in sums:
        one.start()
    for one in sums:
        one.middle()
    for one in sums:
        one.relay()
    for one in sums:
        one.finish()


def group_sum(arrays, ident):
    number = len(arrays)
    scratch = []
    for array in arrays:
        scratch += GroupSum.scratch(array.shape, array.dtype)
    return pl.pallas_call(
        functools.partial(group_sum_body, number),
        out_shape=tuple(jax.ShapeDtypeStruct(a.shape[1:], F32) for a in arrays),
        in_specs=[vmem_spec()] * number,
        out_specs=(vmem_spec(),) * number,
        scratch_shapes=scratch,
        compiler_params=pltpu.CompilerParams(
            collective_id=ident, has_side_effects=True, vmem_limit_bytes=BIG
        ),
        name="group_sum",
    )(*arrays)


def sum_all_body(axis, count, x_ref, out_ref, held, send_sem, recv_sem, send_two, recv_two):
    me = greet(axis, count)

    def put(at, total):
        out_ref[me, at] = total.astype(out_ref.dtype)

    scatter_start(axis, count, me, x_ref, held, send_sem, recv_sem)
    scatter_finish(axis, count, me, x_ref, held, send_sem, recv_sem, put)
    if count == 4:
        relay_gather(axis, me, out_ref.at[me], out_ref, send_two, recv_two)
        return
    copies = []
    for step in range(1, count):
        copy = pltpu.make_async_remote_copy(
            src_ref=out_ref.at[me],
            dst_ref=out_ref.at[me],
            send_sem=send_two.at[step - 1],
            recv_sem=recv_two.at[step - 1],
            device_id={axis: lax.rem(me + step, count)},
            device_id_type=MESH,
        )
        copy.start()
        copies.append(copy)
    for copy in copies:
        copy.wait()


def sum_all(x, axis, count, ident):
    return pl.pallas_call(
        functools.partial(sum_all_body, axis, count),
        out_shape=jax.ShapeDtypeStruct(x.shape, x.dtype),
        in_specs=[vmem_spec()],
        out_specs=vmem_spec(),
        scratch_shapes=[VMEM((count - 1,) + x.shape[1:], x.dtype)]
        + [pltpu.SemaphoreType.DMA((count - 1,))] * 2
        + [pltpu.SemaphoreType.DMA((6 if count == 4 else count - 1,))] * 2,
        compiler_params=pltpu.CompilerParams(collective_id=ident, has_side_effects=True),
        name="sum_all",
    )(x)


def contract(left, right, dims):
    return lax.dot_general(left, right, ((dims[:1], dims[1:]), ((), ())), preferred_element_type=F32)


def masked_scores(keys, query, length):
    scores = contract(keys, query, (0, 0))
    position = lax.broadcasted_iota(jnp.int32, scores.shape, 0)
    return jnp.where(position < length, scores, -1e30)


def attend_body(chunk, length_ref, qkv_ref, out_ref, lse_ref):
    length = length_ref[0]
    keys, vals = qkv_ref[1], qkv_ref[2]
    scale = HEAD_WIDTH ** (-0.5)
    for at in range(0, qkv_ref.shape[2], chunk):
        query = (qkv_ref[0, :, at : at + chunk].astype(F32) * scale).astype(BF)
        scores = masked_scores(keys, query, length)
        top = jnp.max(scores, axis=0, keepdims=True)
        expo = jnp.exp(scores - top)
        total = jnp.sum(expo, axis=0, keepdims=True)
        mixed = contract(vals, expo.astype(BF), (1, 0))
        out_ref[:, at : at + chunk] = (mixed * (1.0 / total)).astype(BF)
        lse_ref[0, :, at : at + chunk] = top + jnp.log(total)


def attend(qkv, lengths, chunk):
    _, width, length = qkv.shape
    heads = width // HEAD_WIDTH
    return pl.pallas_call(
        functools.partial(attend_body, chunk),
        grid=(heads,),
        out_shape=(
            jax.ShapeDtypeStruct((width, length), BF),
            jax.ShapeDtypeStruct((heads, 1, length), F32),
        ),
        in_specs=[
            pl.BlockSpec(memory_space=pltpu.SMEM),
            pl.BlockSpec((3, HEAD_WIDTH, length), lambda h: (0, h, 0)),
        ],
        out_specs=(
            pl.BlockSpec((HEAD_WIDTH, length), lambda h: (h, 0)),
            pl.BlockSpec((1, 1, length), lambda h: (h, 0, 0)),
        ),
        cost_estimate=pl.CostEstimate(
            flops=4 * width * length * length,
            bytes_accessed=8 * width * length,
            transcendentals=heads * length * length,
        ),
        compiler_params=pltpu.CompilerParams(vmem_limit_bytes=BIG),
        name="attend",
    )(lengths, qkv)


def attend_back_body(
    chunk, ranks, length_ref, qkv_ref, lse_ref, grad_ref, x_ref, out_ref, x_out, held, send_sem, recv_sem
):
    me = lax.axis_index("tensor")
    args = ("tensor", ranks, me, x_ref, held, send_sem, recv_sem)

    @pl.when(pl.program_id(0) == 0)
    def _():
        greet("tensor", ranks)
        scatter_start(*args)

    attend_back_head(chunk, length_ref, qkv_ref, lse_ref, grad_ref, out_ref)

    @pl.when(pl.program_id(0) == pl.num_programs(0) - 1)
    def _():
        piece = x_out.shape[2]

        def put(at, total):
            for group in range(x_out.shape[0]):
                x_out[group, at] = total[:, group * piece : (group + 1) * piece].astype(BF)

        scatter_finish(*args, put)


def attend_back_head(chunk, length_ref, qkv_ref, lse_ref, grad_ref, out_ref):
    length = length_ref[0]
    keys, vals = qkv_ref[1], qkv_ref[2]
    scale = HEAD_WIDTH ** (-0.5)
    span = qkv_ref.shape[2]
    g_keys = jnp.zeros((HEAD_WIDTH, span), F32)
    g_vals = jnp.zeros((HEAD_WIDTH, span), F32)
    for at in range(0, span, chunk):
        here = slice(at, at + chunk)
        query = (qkv_ref[0, :, here].astype(F32) * scale).astype(BF)
        grad = grad_ref[:, here]
        probs = jnp.exp(masked_scores(keys, query, length) - lse_ref[0, :, here])
        g_probs = contract(vals, grad, (0, 0))
        weighted = probs * g_probs
        inner = jnp.sum(weighted, axis=0, keepdims=True)
        g_scores = (weighted - probs * inner).astype(BF)
        out_ref[0, :, here] = (contract(keys, g_scores, (1, 0)) * scale).astype(BF)
        g_keys += contract(query, g_scores, (1, 1))
        g_vals += contract(grad, probs.astype(BF), (1, 1))
    out_ref[1] = g_keys.astype(BF)
    out_ref[2] = g_vals.astype(BF)


def attend_back(qkv, lengths, lse, grad, x, groups, chunk, ident):
    _, width, length = qkv.shape
    heads = width // HEAD_WIDTH
    return pl.pallas_call(
        functools.partial(attend_back_body, chunk, x.shape[0]),
        grid=(heads,),
        out_shape=(
            jax.ShapeDtypeStruct(qkv.shape, BF),
            jax.ShapeDtypeStruct((groups, x.shape[1], x.shape[2] // groups), BF),
        ),
        in_specs=[
            pl.BlockSpec(memory_space=pltpu.SMEM),
            pl.BlockSpec((3, HEAD_WIDTH, length), lambda h: (0, h, 0)),
            pl.BlockSpec((1, 1, length), lambda h: (h, 0, 0)),
            pl.BlockSpec((HEAD_WIDTH, length), lambda h: (h, 0)),
            vmem_spec(),
        ],
        out_specs=(
            pl.BlockSpec((3, HEAD_WIDTH, length), lambda h: (0, h, 0)),
            vmem_spec(),
        ),
        scratch_shapes=[
            VMEM((x.shape[0] - 1,) + x.shape[1:], x.dtype),
            pltpu.SemaphoreType.DMA((x.shape[0] - 1,)),
            pltpu.SemaphoreType.DMA((x.shape[0] - 1,)),
        ],
        cost_estimate=pl.CostEstimate(
            flops=10 * width * length * length,
            bytes_accessed=14 * width * length,
            transcendentals=heads * length * length,
        ),
        compiler_params=pltpu.CompilerParams(
            collective_id=ident, has_side_effects=True, vmem_limit_bytes=BIG
        ),
        name="attend_back",
    )(lengths, qkv, lse, grad, x)


def hidden_body(length_ref, normed_ref, up_ref, slope_ref, sum_ref):
    pre = jnp.dot(normed_ref[...], up_ref[...], preferred_element_type=F32)
    live = lax.broadcasted_iota(jnp.int32, pre.shape, 0) < length_ref[0]
    square = pre * pre
    bend = jnp.tanh(0.7978845608028654 * (pre * (1.0 + 0.044715 * square)))
    half = 0.5 * (1.0 + bend)
    act = (pre * half).astype(BF).astype(F32)
    sum_ref[...] = jnp.sum(jnp.where(live, act, 0.0), axis=0, keepdims=True)
    inner = 0.7978845608028654 * (1.0 + 3 * 0.044715 * square)
    slope = half + 0.5 * pre * (1.0 - bend * bend) * inner
    slope_ref[...] = jnp.where(live, slope, 0.0).astype(BF)


def hidden(normed, up, lengths, chunk):
    length, width = normed.shape
    units = up.shape[1]
    return pl.pallas_call(
        hidden_body,
        grid=(units // chunk,),
        out_shape=(
            jax.ShapeDtypeStruct((length, units), BF),
            jax.ShapeDtypeStruct((1, units), F32),
        ),
        in_specs=[
            pl.BlockSpec(memory_space=pltpu.SMEM),
            pl.BlockSpec((length, width), lambda f: (0, 0)),
            pl.BlockSpec((width, chunk), lambda f: (0, f)),
        ],
        out_specs=(
            pl.BlockSpec((length, chunk), lambda f: (0, f)),
            pl.BlockSpec((1, chunk), lambda f: (0, f)),
        ),
        cost_estimate=pl.CostEstimate(
            flops=2 * length * width * units,
            bytes_accessed=6 * length * units,
            transcendentals=length * units,
        ),
        compiler_params=pltpu.CompilerParams(vmem_limit_bytes=BIG),
        name="hidden",
    )(lengths, normed, up)


def per_device(
    token_ids,
    lengths,
    teacher_bins,
    embed_table,
    query_key_value_matrix,
    output_matrix,
    up_matrix,
    down_matrix,
    w_head,
):
    ranks = lax.axis_size("tensor")
    groups = lax.axis_size("dp")
    rank = lax.axis_index("tensor")
    group = lax.axis_index("dp")
    assert token_ids.shape[0] == 1
    local_len = token_ids.shape[1]
    span = local_len * ranks
    vocab_local, width = embed_table.shape
    d_local, _, e_local = query_key_value_matrix.shape
    f_local = up_matrix.shape[1]
    bins = w_head.shape[1]
    exact = lax.Precision.HIGHEST

    qkv_full = lax.all_gather(
        query_key_value_matrix.reshape(d_local, 3 * e_local), "dp", axis=0, tiled=True
    )
    out_parts = lax.all_gather(output_matrix, ("tensor", "dp"), axis=0, tiled=False)
    out_full = (
        out_parts.reshape(ranks, groups, e_local, d_local)
        .transpose(0, 2, 1, 3)
        .reshape(ranks * e_local, width)
    )
    up_full = lax.all_gather(up_matrix, "dp", axis=0, tiled=True)
    low = lax.all_gather(
        jnp.concatenate([down_matrix, w_head.reshape(bins, d_local)], axis=0), "dp", axis=0, tiled=False
    )
    down_full = low[:, :f_local]
    head_wide = low[:, f_local:].reshape(width, bins).astype(F32)

    all_ids = gather_all(token_ids, "tensor", ranks, 1).reshape(ranks, local_len)
    shifted = all_ids - rank * vocab_local
    inside = (shifted >= 0) & (shifted < vocab_local)
    rows = jnp.take(embed_table, jnp.clip(shifted, 0, vocab_local - 1), axis=0)
    first = sum_all(
        jnp.where(inside[..., None], rows, jnp.zeros((), BF)), "tensor", ranks, 2
    ).reshape(span, width)
    normed_one = normalize(first.astype(F32)).astype(BF)
    qkv = (
        lax.dot_general(qkv_full, normed_one, (((0,), (1,)), ((), ())), preferred_element_type=F32)
        .astype(BF)
        .reshape(3, e_local, span)
    )
    chunk = min(256, span)
    context, lse = attend(qkv, lengths, chunk)
    context_all = gather_blocks(context, "tensor", ranks, 3).reshape(ranks * e_local, span)
    attn = lax.dot_general(
        context_all, out_full, (((0,), (0,)), ((), ())), preferred_element_type=F32
    )
    second = (first.astype(F32) + attn).astype(BF)
    normed_f, norm_back = jax.vjp(normalize, second.astype(F32))
    normed_two = normed_f.astype(BF)
    slope, hidden_sum = hidden(normed_two, up_full, lengths, min(256, f_local))

    live = (jnp.arange(span, dtype=jnp.int32) < lengths[0]).astype(F32)
    count = lengths.astype(F32)[:, None]
    ffn_part = jnp.einsum(
        "of,jfd->ojd", hidden_sum, down_full.astype(F32), precision=exact
    ).reshape(1, width)
    ffn_all = gather_all(ffn_part, "tensor", ranks, 4)
    second_sum = jnp.sum(second.astype(F32) * live[:, None], axis=0, keepdims=True)
    pooled = (second_sum + jnp.sum(ffn_all, axis=0)) / count
    final, final_back = jax.vjp(normalize, pooled)
    logits = jnp.dot(final, head_wide, precision=exact)
    top = jnp.max(logits, axis=-1, keepdims=True)
    total_exp = jnp.log(jnp.sum(jnp.exp(logits - top), axis=-1, keepdims=True)) + top
    labels = (teacher_bins[:, None] == jnp.arange(bins, dtype=jnp.int32)[None, :]).astype(F32)
    loss_here = total_exp - jnp.sum(logits * labels, axis=-1, keepdims=True)
    g_logits = (jnp.exp(logits - total_exp) - labels) / groups
    g_final = jnp.dot(g_logits, head_wide.T, precision=exact)
    per_token = final_back(g_final)[0] / count
    rounded = per_token.astype(BF).astype(F32)
    g_hidden = jnp.einsum(
        "ojd,jfd->of",
        rounded.reshape(1, groups, d_local),
        down_full.astype(F32),
        precision=exact,
    )

    packed = jnp.concatenate(
        [hidden_sum, rounded, final, g_logits, jnp.broadcast_to(loss_here, (1, 128))], axis=1
    )

    over_seqs = (((0,), (0,)), ((), ()))
    up_base = lax.dot_general(normed_two, slope, over_seqs, preferred_element_type=F32)
    up_term = (up_base * g_hidden).astype(BF).reshape(groups, d_local, f_local)
    g_pre = (slope.astype(F32) * g_hidden).astype(BF)
    g_normed = lax.dot_general(
        g_pre, up_full, (((1,), (1,)), ((), ())), preferred_element_type=F32
    )
    g_second = (
        norm_back(g_normed)[0] + live[:, None] * (per_token / ranks)
    ).astype(BF)
    spread = lax.dot_general(
        out_full, g_second, (((1,), (1,)), ((), ())), preferred_element_type=F32
    ).astype(BF)
    g_context, up_weight_gradient, every = scatter_and_group(
        spread.reshape(ranks, e_local, span), up_term, packed, ranks, 6
    )
    every = every[:, 0]
    hidden_every = every[:, :f_local]
    rounded_every = every[:, f_local : f_local + width]
    final_every = every[:, f_local + width : f_local + 2 * width]
    rest = every[:, f_local + 2 * width :]
    loss = jnp.sum(rest[:, bins]) / groups
    mine = group * d_local
    down_weight_gradient = lax.dot_general(
        hidden_every,
        lax.dynamic_slice_in_dim(rounded_every, mine, d_local, axis=1),
        over_seqs,
        precision=exact,
    )
    grad_head = lax.dot_general(
        lax.dynamic_slice_in_dim(final_every, mine, d_local, axis=1),
        rest[:, :bins],
        over_seqs,
        precision=exact,
    )

    out_term = (
        jnp.dot(context_all, g_second, preferred_element_type=F32)
        .astype(BF)
        .reshape(ranks, e_local, width)
    )
    g_qkv, out_mine = attend_back(qkv, lengths, lse, g_context, out_term, groups, chunk, 7)
    qkv_term = lax.dot_general(
        normed_one,
        g_qkv.reshape(3 * e_local, span),
        (((0,), (1,)), ((), ())),
        preferred_element_type=F32,
    )
    qkv_gradient, output_weight_gradient = group_sum(
        [qkv_term.astype(BF).reshape(groups, d_local, 3 * e_local), out_mine], 8
    )
    query_key_value_gradient = qkv_gradient.reshape(d_local, 3, e_local)
    return (
        loss,
        query_key_value_gradient,
        output_weight_gradient,
        up_weight_gradient,
        down_weight_gradient,
        grad_head,
    )


def remote(src, dst, sems, index, device):
    return pltpu.make_async_remote_copy(
        src_ref=src,
        dst_ref=dst,
        send_sem=sems[0].at[index],
        recv_sem=sems[1].at[index],
        device_id=device,
        device_id_type=MESH,
    )


class Place:
    def __init__(self):
        self.rank = lax.axis_index("tensor")
        self.across = self.rank + 1 - 2 * lax.rem(self.rank, 2)
        self.over = lax.rem(self.rank + 2, 4)
        self.diag = 3 - self.rank
        self.group = lax.axis_index("dp")
        self.core = lax.rem(self.group, 2)
        self.chip = self.group // 2
        self.near = self.chip * 2 + 1 - self.core

    def turn(self, step):
        return lax.rem(self.chip + step, 4)

    def same(self, chip):
        return chip * 2 + self.core

    def peers(self, everyone=False):
        peers = [{"tensor": one} for one in (self.across, self.over, self.diag)]
        if everyone:
            return peers + [{"dp": lax.rem(self.group + step, 8)} for step in range(1, 8)]
        return peers + [
            {"dp": self.near},
            {"dp": self.same(self.turn(1))},
            {"dp": self.same(self.turn(3))},
        ]

    def signal(self, peers):
        barrier = pltpu.get_barrier_semaphore()
        for peer in peers:
            pl.semaphore_signal(barrier, inc=1, device_id=peer, device_id_type=MESH)

    def ready(self, peers):
        pl.semaphore_wait(pltpu.get_barrier_semaphore(), len(peers))


class RingGather:
    def __init__(self, at, src, own, slot, sems):
        self.at, self.src, self.own, self.slot = at, src, own, slot
        self.sems, self.local = sems[:2], sems[2]

    @staticmethod
    def scratch():
        return [
            pltpu.SemaphoreType.DMA((10,)),
            pltpu.SemaphoreType.DMA((10,)),
            pltpu.SemaphoreType.DMA((1,)),
        ]

    def copies(self):
        at = self.at
        right, left, far = at.turn(1), at.turn(3), at.turn(2)
        me, to_right, to_left = at.group, {"dp": at.same(right)}, {"dp": at.same(left)}
        near = {"dp": at.near}

        def held(index, chip, half, device):
            ref = self.slot(at.same(chip), half)
            return remote(ref, ref, self.sems, index, device)

        def first(index, half, device):
            return remote(self.own(half), self.slot(me, half), self.sems, index, device)

        return (
            first(0, 0, to_right),
            first(1, 1, to_left),
            first(2, 1, to_right),
            first(3, 0, to_left),
            held(4, left, 0, to_right),
            held(5, right, 1, to_left),
            remote(self.src, self.slot(me, None), self.sems, 6, near),
            held(7, left, None, near),
            held(8, right, None, near),
            held(9, far, None, near),
        )

    def keep(self):
        return pltpu.make_async_copy(self.src, self.slot(self.at.group, None), self.local.at[0])

    def start(self):
        copies = self.copies()
        for index in (0, 1, 2, 3, 6):
            copies[index].start()
        self.keep().start()

    def relay(self):
        copies = self.copies()
        copies[0].wait_recv()
        copies[4].start()
        copies[1].wait_recv()
        copies[5].start()

    def spread(self):
        copies = self.copies()
        copies[2].wait_recv()
        copies[7].start()
        copies[3].wait_recv()
        copies[8].start()
        copies[4].wait_recv()
        copies[5].wait_recv()
        copies[9].start()

    def finish(self):
        copies = self.copies()
        for index in (6, 7, 8, 9):
            copies[index].wait_recv()
        for copy in copies:
            copy.wait_send()
        self.keep().wait()

    def near(self):
        copies = self.copies()
        for index in (0, 2):
            copies[index].wait_recv()
        copies[7].start()
        for index in (1, 3):
            copies[index].wait_recv()
        copies[8].start()

    def close_near(self):
        copies = self.copies()
        for index in (6, 7, 8):
            copies[index].wait_recv()
        for index in (0, 1, 2, 3, 6, 7, 8):
            copies[index].wait_send()
        self.keep().wait()

    def pass_on(self):
        copies = self.copies()
        copies[4].start()
        copies[5].start()

    def far(self):
        copies = self.copies()
        copies[4].wait_recv()
        copies[5].wait_recv()
        copies[9].start()

    def close_far(self):
        copies = self.copies()
        copies[9].wait_recv()
        for index in (4, 5, 9):
            copies[index].wait_send()


def columns_of(ref, size):
    rows = ref.shape[0]

    def slot(block, half):
        lanes = pl.ds(pl.multiple_of(block * size, size), size)
        if half is None:
            return ref.at[:, lanes]
        return ref.at[pl.ds(half * (rows // 2), rows // 2), lanes]

    return slot


def rows_of(ref, block, half, size, axis=0):
    lead = (slice(None),) * axis
    if half is None:
        return ref.at[lead + (pl.ds(pl.multiple_of(block * size, size), size),)]
    part = size // 2
    return ref.at[lead + (pl.ds(pl.multiple_of(block * size + half * part, part), part),)]


def half_rows(ref, half, axis=0):
    part = ref.shape[axis] // 2
    return ref.at[(slice(None),) * axis + (pl.ds(half * part, part),)]


def ids_body(ids_ref, ids_all, send, recv):
    at = Place()
    peers = at.peers()[:3]
    at.signal(peers)
    ids_all[at.rank] = ids_ref[...]
    at.ready(peers)
    copies = [
        remote(ids_ref, ids_all.at[at.rank], (send, recv), index, peer)
        for index, peer in enumerate(peers)
    ]
    for copy in copies:
        copy.start()
    for copy in copies:
        copy.wait()


def share_ids(ids, ident):
    return pl.pallas_call(
        ids_body,
        out_shape=jax.ShapeDtypeStruct((4,) + ids.shape, ids.dtype),
        in_specs=[vmem_spec()],
        out_specs=vmem_spec(),
        scratch_shapes=[pltpu.SemaphoreType.DMA((3,))] * 2,
        compiler_params=pltpu.CompilerParams(collective_id=ident, has_side_effects=True),
        name="share_ids",
    )(ids)


def any_spec():
    return pl.BlockSpec(memory_space=pl.ANY)


class Stream:
    def __init__(self, at, x_ref, acc, held, last, whole, sems, index, rows, x_first):
        self.at, self.x, self.acc, self.held, self.last, self.whole = at, x_ref, acc, held, last, whole
        self.sems, self.index, self.rows = sems, index * 6, rows
        self.one, self.two = (at.across, at.over) if x_first else (at.over, at.across)

    def copies(self):
        at, rows, base, sems = self.at, self.rows, self.index, self.sems
        one, two = {"tensor": self.one}, {"tensor": self.two}
        return (
            remote(self.x.at[at.diag, rows], self.held.at[1, rows], sems, base, one),
            remote(self.x.at[self.one, rows], self.held.at[0, rows], sems, base + 1, one),
            remote(self.acc.at[rows], self.last.at[rows], sems, base + 2, two),
            remote(self.whole.at[at.rank, rows], self.whole.at[at.rank, rows], sems, base + 3, two),
            remote(self.whole.at[at.rank, rows], self.whole.at[at.rank, rows], sems, base + 4, one),
            remote(self.whole.at[self.two, rows], self.whole.at[self.two, rows], sems, base + 5, one),
        )

    def start(self):
        copies = self.copies()
        copies[0].start()
        copies[1].start()

    def second(self):
        copies = self.copies()
        copies[0].wait_recv()

        def body(at):
            here = pl.ds(self.rows.start + at.start, at.size)
            self.acc[here] = self.x[self.two, here] + self.held[1, here]

        add_tiles(self.rows.size, 32, body)
        copies[2].start()

    def third(self):
        copies = self.copies()
        copies[1].wait_recv()
        copies[2].wait_recv()

        def body(at):
            here = pl.ds(self.rows.start + at.start, at.size)
            self.whole[self.at.rank, here] = (
                self.x[self.at.rank, here] + self.held[0, here] + self.last[here]
            )

        add_tiles(self.rows.size, 32, body)
        copies[3].start()
        copies[4].start()

    def relay(self):
        copies = self.copies()
        copies[3].wait_recv()
        copies[5].start()

    def beside(self):
        self.copies()[4].wait_recv()

    def opposite(self):
        self.copies()[5].wait_recv()

    def finish(self):
        for copy in self.copies():
            copy.wait_send()


def front_body(
    chunk, length_ref, x_in, w_ref, up_ref, down_ref, head_ref, out_ref,
    first_out, normed_out, qkv_out, ctx_out, lse_ref, up_out, out_full, down_out, head_out,
    x_ref, acc, held, last, whole, normed, qkv_ref, w_full, w_turn, ctx_ref, cols,
    load, saved, send, recv, col_send, col_recv, ctx_send, ctx_recv, ctx_saved, *rest,
):
    at = Place()
    peers = at.peers()
    at.signal(peers)
    entry = pltpu.make_async_copy(x_in, x_ref, load.at[0])
    entry.start()
    d_local = w_ref.shape[1]
    local = x_ref.shape[1]
    e_local = w_ref.shape[2]
    span = qkv_ref.shape[2]
    heads = lse_ref.shape[0]
    size = HEAD_WIDTH // 2
    weights = RingGather(
        at, w_ref, lambda half: half_rows(w_ref, half, 1),
        lambda block, half: rows_of(w_full, block, half, d_local, 1), rest[:3],
    )
    ups = RingGather(
        at, up_ref, lambda half: half_rows(up_ref, half),
        lambda block, half: rows_of(up_out, block, half, d_local), rest[3:6],
    )
    tops = RingGather(
        at, head_ref, lambda half: half_rows(head_ref, half),
        lambda block, half: rows_of(head_out, block, half, d_local), rest[6:9],
    )
    downs = RingGather(
        at, down_ref, lambda half: half_rows(down_ref, half), columns_of(down_out, d_local), rest[9:12]
    )
    outs = RingGather(
        at, cols, lambda half: half_rows(cols, half), columns_of(out_full, d_local), rest[12:15]
    )
    mine = pl.ds(pl.multiple_of(at.rank * e_local, e_local), e_local)
    own_columns = pltpu.make_async_copy(out_ref, cols.at[mine], load.at[1])
    own_columns.start()
    column_copies = [
        remote(out_ref, cols.at[mine], (col_send, col_recv), index, peer)
        for index, peer in enumerate(peers[:3])
    ]

    at.ready(peers)
    weights.start()
    entry.wait()
    part = local // 4
    streams = [
        Stream(
            at, x_ref, acc, held, last, whole, (send, recv), index,
            pl.ds((index % 2) * (local // 2) + (index // 2) * part, part), index % 2 == 0,
        )
        for index in range(4)
    ]
    for one in streams:
        one.start()
    for one in streams:
        one.second()
    weights.relay()
    ups.start()
    tops.start()
    for one in streams:
        one.third()
    for copy in column_copies:
        copy.start()
    weights.spread()
    weights.finish()
    for index in range(3):
        w_turn[index] = w_full[index].T

    def saves(slot, block):
        base = pl.multiple_of(block * local, local)
        return (
            pltpu.make_async_copy(whole.at[block], first_out.at[block], saved.at[slot, 0]),
            pltpu.make_async_copy(normed.at[block], normed_out.at[block], saved.at[slot, 1]),
            pltpu.make_async_copy(
                qkv_ref.at[:, :, pl.ds(base, local)], qkv_out.at[:, :, pl.ds(base, local)], saved.at[slot, 2]
            ),
        )

    def project(block, slot):
        def tile(here):
            normed[block, here] = normalize(whole[block, here].astype(F32)).astype(BF)

        add_tiles(local, 32, tile)
        base = pl.multiple_of(block * local, local)

        def matrix(index, carry):
            qkv_ref[index, :, pl.ds(base, local)] = contract(
                w_turn[index], normed[block], (1, 1)
            ).astype(BF)
            return carry

        lax.fori_loop(0, 3, matrix, 0)
        for copy in saves(slot, block):
            copy.start()

    for one in streams[:2]:
        one.relay()
    project(at.rank, 0)
    for one in streams[2:]:
        one.relay()
    ups.relay()
    tops.relay()
    downs.start()
    for one in streams:
        one.beside()
    project(at.across, 1)
    project(at.over, 2)
    for one in streams:
        one.opposite()
    project(at.diag, 3)
    own_columns.wait()
    for copy in column_copies:
        copy.wait()
    outs.start()

    def copies(one):
        def copy(index, block, half, peer):
            ref = ctx_ref.at[block, pl.ds(pl.multiple_of(one * HEAD_WIDTH + half * size, size), size)]
            return pltpu.make_async_remote_copy(
                src_ref=ref,
                dst_ref=ref,
                send_sem=ctx_send.at[one, index],
                recv_sem=ctx_recv.at[one, index],
                device_id={"tensor": peer},
                device_id_type=MESH,
            )

        return (
            copy(0, at.rank, 0, at.across),
            copy(1, at.rank, 1, at.over),
            copy(2, at.rank, 1, at.across),
            copy(3, at.rank, 0, at.over),
            copy(4, at.across, 0, at.over),
            copy(5, at.over, 1, at.across),
        )

    def relay(one):
        group = copies(one)
        group[0].wait_recv()
        group[4].start()
        group[1].wait_recv()
        group[5].start()

    def save(one):
        here = pl.ds(pl.multiple_of(one * HEAD_WIDTH, HEAD_WIDTH), HEAD_WIDTH)
        return pltpu.make_async_copy(ctx_ref.at[:, here], ctx_out.at[:, here], ctx_saved.at[one])

    length = length_ref[0]
    scale = HEAD_WIDTH ** (-0.5)

    def attend_head(head, carry):
        lines = pl.ds(pl.multiple_of(head * HEAD_WIDTH, HEAD_WIDTH), HEAD_WIDTH)
        keys, vals = qkv_ref[1, lines], qkv_ref[2, lines]
        for start in range(0, span, chunk):
            here = slice(start, start + chunk)
            query = (qkv_ref[0, lines, here].astype(F32) * scale).astype(BF)
            scores = masked_scores(keys, query, length)
            top = jnp.max(scores, axis=0, keepdims=True)
            expo = jnp.exp(scores - top)
            total = jnp.sum(expo, axis=0, keepdims=True)
            mixed = contract(vals, expo.astype(BF), (1, 0))
            ctx_ref[at.rank, lines, here] = (mixed * (1.0 / total)).astype(BF)
            lse_ref[head, :, here] = top + jnp.log(total)

        for copy in copies(head)[:4]:
            copy.start()

        @pl.when(head > 0)
        def _():
            relay(head - 1)

        @pl.when(head == 0)
        def _():
            ups.spread()
            tops.spread()

        @pl.when(head == 1)
        def _():
            downs.near()

        return carry

    lax.fori_loop(0, heads, attend_head, 0)
    outs.relay()
    relay(heads - 1)
    ups.finish()
    tops.finish()
    downs.close_near()
    for one in streams:
        one.finish()

    def drain(one, carry):
        group = copies(one)
        for copy in group[2:]:
            copy.wait_recv()
        save(one).start()
        for copy in group:
            copy.wait_send()
        return carry

    lax.fori_loop(0, heads, drain, 0)
    outs.spread()
    for slot, block in enumerate((at.rank, at.across, at.over, at.diag)):
        for copy in saves(slot, block):
            copy.wait()

    def store(one, carry):
        save(one).wait()
        return carry

    lax.fori_loop(0, heads, store, 0)
    outs.finish()


def front(x, w, up, down, top, out, lengths, chunk, ident):
    ranks, local, width = x.shape
    kinds, d_local, e_local = w.shape
    f_local = up.shape[1]
    heads = e_local // HEAD_WIDTH
    span = ranks * local
    assert heads > 1
    dma = pltpu.SemaphoreType.DMA
    return pl.pallas_call(
        functools.partial(front_body, chunk),
        out_shape=(
            jax.ShapeDtypeStruct(x.shape, BF),
            jax.ShapeDtypeStruct(x.shape, BF),
            jax.ShapeDtypeStruct((kinds, e_local, span), BF),
            jax.ShapeDtypeStruct((ranks, e_local, span), BF),
            jax.ShapeDtypeStruct((heads, 1, span), F32),
            jax.ShapeDtypeStruct((width, f_local), BF),
            jax.ShapeDtypeStruct((ranks * e_local, width), BF),
            jax.ShapeDtypeStruct((f_local, width), BF),
            jax.ShapeDtypeStruct((width, top.shape[1]), BF),
        ),
        in_specs=[pl.BlockSpec(memory_space=pltpu.SMEM), any_spec()] + [vmem_spec()] * 5,
        out_specs=(any_spec(),) * 4 + (vmem_spec(),) + (any_spec(),) * 4,
        scratch_shapes=[
            VMEM(x.shape, BF),
            VMEM((local, width), BF),
            VMEM((2, local, width), BF),
            VMEM((local, width), BF),
            VMEM(x.shape, BF),
            VMEM(x.shape, BF),
            VMEM((kinds, e_local, span), BF),
            VMEM((kinds, width, e_local), BF),
            VMEM((kinds, e_local, width), BF),
            VMEM((ranks, e_local, span), BF),
            VMEM((ranks * e_local, d_local), BF),
            dma((2,)),
            dma((4, 3)),
            dma((24,)),
            dma((24,)),
            dma((3,)),
            dma((3,)),
            dma((heads, 6)),
            dma((heads, 6)),
            dma((heads,)),
        ]
        + RingGather.scratch() * 5,
        compiler_params=pltpu.CompilerParams(
            collective_id=ident, has_side_effects=True, vmem_limit_bytes=BIG
        ),
        name="front",
    )(lengths, x, w, up, down, top, out)


def exact_dot(row, matrix, dims):
    high = row.astype(BF).astype(F32)
    middle = (row - high).astype(BF).astype(F32)
    low = row - high - middle
    shape = (8, row.shape[1])
    index = lax.broadcasted_iota(jnp.int32, shape, 0)
    stacked = jnp.where(
        index == 0, jnp.broadcast_to(high, shape),
        jnp.where(
            index == 1, jnp.broadcast_to(middle, shape),
            jnp.where(index == 2, jnp.broadcast_to(low, shape), 0.0),
        ),
    ).astype(BF)
    return jnp.sum(contract(stacked, matrix, dims), axis=0, keepdims=True)


class Fold:
    def __init__(self, at, src, held, acc, last, sems, base, rows, x_first):
        self.at, self.src, self.held, self.acc, self.last = at, src, held, acc, last
        self.sems, self.base, self.rows = sems, base, rows
        self.one, self.two = (at.across, at.over) if x_first else (at.over, at.across)

    def copies(self):
        rows, base, sems = self.rows, self.base, self.sems
        one, two = {"tensor": self.one}, {"tensor": self.two}
        return (
            remote(self.src.at[self.at.diag, rows], self.held.at[1, rows], sems, base, one),
            remote(self.src.at[self.one, rows], self.held.at[0, rows], sems, base + 1, one),
            remote(self.acc.at[rows], self.last.at[rows], sems, base + 2, two),
        )

    def start(self):
        copies = self.copies()
        copies[0].start()
        copies[1].start()

    def tiles(self, body):
        def step(at):
            body(pl.ds(pl.multiple_of(self.rows.start + at.start, 32), at.size))

        add_tiles(self.rows.size, 32, step)

    def second(self):
        copies = self.copies()
        copies[0].wait_recv()

        def body(here):
            self.acc[here] = (
                self.src[self.two, here].astype(F32) + self.held[1, here].astype(F32)
            ).astype(BF)

        self.tiles(body)
        copies[2].start()

    def third(self, put):
        copies = self.copies()
        copies[1].wait_recv()
        copies[2].wait_recv()

        def body(here):
            put(
                here,
                self.src[self.at.rank, here].astype(F32)
                + self.held[0, here].astype(F32)
                + self.last[here].astype(F32),
            )

        self.tiles(body)

    def finish(self):
        for copy in self.copies():
            copy.wait_send()


class DirectSum(GroupSum):
    def __init__(self, x_ref, pair, mine, far, sems, tile):
        super().__init__(x_ref, None, pair, mine, far, sems)
        self.tile = tile

    def middle(self):
        for copy in self.pair_copies():
            copy.wait()
        for chip in range(self.chips):

            def body(at, chip=chip):
                self.mine[chip, at] = (
                    self.x[chip * 2 + self.core, at].astype(F32)
                    + self.pair[chip, at].astype(F32)
                ).astype(BF)

            add_tiles(self.rows, self.tile, body)
        for copy in self.far_copies():
            copy.start()

    def finish(self, put):
        for copy in self.far_copies():
            copy.wait()

        def body(at):
            total = self.mine[self.chip, at].astype(F32)
            for step in range(self.chips - 1):
                total = total + self.far[step, at].astype(F32)
            put(at, total)

        add_tiles(self.far.shape[1], self.tile, body)


def stack_rows(rows):
    rows = list(rows)
    zero = jnp.zeros(rows[0].shape, F32)
    while len(rows) * rows[0].shape[0] % 16:
        rows.append(zero)
    return jnp.concatenate(rows, axis=0).astype(BF)


def split_three(values):
    high = values.astype(BF).astype(F32)
    middle = (values - high).astype(BF).astype(F32)
    return high, middle, values - high - middle


def finish_body(
    chunk, length_ref, bin_ref, top_ref, lse_ref,
    first_in, ctx_in, out_in, up_in, down_in, qkv_in, normed_in,
    qkv_out, out_out, up_out, down_out, top_out, loss_out,
    first, ctx, outs, up_full, down_full, qkv_ref, normed, loads, down_loads,
    work, second, normed_two, turned, slope, sums, base, up_base, parts, p_send, p_recv, token, small_ref,
    d_send, d_recv, d_local_sem,
    g_second, up_term,
    spread, g_ctx, s_held, s_acc, s_last, s_send, s_recv,
    out_term, o_pair, out_sum, o_held, o_acc, o_last, o_send, o_recv,
    o_own, o_far, o_sem0, o_sem1, o_sem2, o_sem3,
    u_pair, u_own, u_far, u_sem0, u_sem1, u_sem2, u_sem3,
    g_qkv, q_term, q_pair, q_own, q_far, q_sem0, q_sem1, q_sem2, q_sem3,
    smalls, m_send, m_recv,
):
    at = Place()
    peers = at.peers(True)
    at.signal(peers)
    heads = lse_ref.shape[0]
    end = heads - 1
    e_local = g_ctx.shape[0]
    d_local = q_term.shape[3]
    groups = q_term.shape[1]
    span, width = first.shape
    units = slope.shape[1]
    bins = top_ref.shape[1]
    half = HEAD_WIDTH // 2
    length = length_ref[0]
    scale = HEAD_WIDTH ** (-0.5)
    local = span // 4

    pairs = (
        (ctx_in, ctx), (out_in, outs), (first_in, first), (up_in, up_full), (qkv_in, qkv_ref), (normed_in, normed)
    )

    def load(index):
        return pltpu.make_async_copy(*pairs[index], loads.at[index])

    slot = columns_of(down_full, d_local)
    source = columns_of(down_in, d_local)
    downs = RingGather(
        at, slot(at.group, None), lambda part: slot(at.group, part), slot, (d_send, d_recv, d_local_sem)
    )

    def load_down(index):
        block = (at.same(at.turn(1)), at.same(at.turn(3)), at.group)[index % 3]
        if index > 2:
            block = block + 1 - 2 * at.core
        return pltpu.make_async_copy(source(block, None), slot(block, None), down_loads.at[index])

    load(0).start()
    load(1).start()
    for index in range(2):
        load_down(index).start()
    load(2).start()
    load(3).start()
    for index in range(2, 6):
        load_down(index).start()
    load(4).start()
    load(5).start()
    base[...] = jnp.zeros(base.shape, F32)
    load(0).wait()
    load(1).wait()
    load(2).wait()

    def project_tile(tile, carry):
        start = pl.multiple_of(tile * local, local)
        work[...] = contract(ctx[:, pl.ds(start, local)], outs[...], (0, 0))

        def body(rows):
            here = pl.ds(pl.multiple_of(start + rows.start, 32), rows.size)
            value = (first[here].astype(F32) + work[rows]).astype(BF)
            second[here] = value
            value = value.astype(F32)
            normed_two[here] = normalize(value).astype(BF)
            live = lax.broadcasted_iota(jnp.int32, value.shape, 0) + here.start < length
            base[...] += jnp.sum(jnp.where(live, value, 0.0), axis=0, keepdims=True)

        add_tiles(local, 32, body)
        turned[:, pl.ds(start, local)] = normed_two[pl.ds(start, local)].T
        return carry

    lax.fori_loop(0, 1, project_tile, 0)
    load_down(0).wait()
    load_down(1).wait()
    at.ready(peers)
    downs.pass_on()
    lax.fori_loop(1, 4, project_tile, 0)
    load(3).wait()

    def hidden_chunk(step, carry):
        lanes = pl.ds(pl.multiple_of(step * chunk, chunk), chunk)
        pre = jnp.dot(normed_two[...], up_full[:, lanes], preferred_element_type=F32)
        live = lax.broadcasted_iota(jnp.int32, pre.shape, 0) < length
        square = pre * pre
        bend = jnp.tanh(0.7978845608028654 * (pre * (1.0 + 0.044715 * square)))
        part = 0.5 * (1.0 + bend)
        act = (pre * part).astype(BF).astype(F32)
        sums[:, lanes] = jnp.sum(jnp.where(live, act, 0.0), axis=0, keepdims=True)
        inner = 0.7978845608028654 * (1.0 + 3 * 0.044715 * square)
        value = part + 0.5 * pre * (1.0 - bend * bend) * inner
        slope[:, lanes] = jnp.where(live, value, 0.0).astype(BF)
        return carry

    lax.fori_loop(0, units // chunk, hidden_chunk, 0)
    downs.far()
    for index in range(2, 6):
        load_down(index).wait()
    downs.close_far()
    hidden_sum = sums[...]
    parts[at.rank] = exact_dot(hidden_sum, down_full[...], (1, 0))
    part_copies = [
        remote(parts.at[at.rank], parts.at[at.rank], (p_send, p_recv), index, peer)
        for index, peer in enumerate(peers[:3])
    ]
    for copy in part_copies:
        copy.start()

    def base_chunk(step, carry):
        lanes = pl.ds(pl.multiple_of(step * chunk, chunk), chunk)
        up_base[:, lanes] = jnp.dot(turned[...], slope[:, lanes], preferred_element_type=F32)
        return carry

    lax.fori_loop(0, units // chunk, base_chunk, 0)
    for copy in part_copies:
        copy.wait()
    count = jnp.full((1, 1), length, jnp.int32).astype(F32)
    total = base[...]
    for index in range(4):
        total = total + parts[index]
    pooled = total / count
    mean = jnp.mean(pooled, axis=-1, keepdims=True)
    centered = pooled - mean
    norm_scale = lax.rsqrt(jnp.mean(centered * centered, axis=-1, keepdims=True) + EPS)
    final = centered * norm_scale
    logits = exact_dot(final, top_ref[...], (1, 0))
    highest = jnp.max(logits, axis=-1, keepdims=True)
    total_exp = jnp.log(jnp.sum(jnp.exp(logits - highest), axis=-1, keepdims=True)) + highest
    labels = (lax.broadcasted_iota(jnp.int32, logits.shape, 1) == bin_ref[0]).astype(F32)
    loss = total_exp - jnp.sum(logits * labels, axis=-1, keepdims=True)
    g_logits = (jnp.exp(logits - total_exp) - labels) / 8.0
    g_final = exact_dot(g_logits, top_ref[...], (1, 1))
    g_pooled = norm_scale * (
        g_final
        - jnp.mean(g_final, axis=-1, keepdims=True)
        - final * jnp.mean(g_final * final, axis=-1, keepdims=True)
    )
    per_token = g_pooled / count
    rounded = per_token.astype(BF).astype(F32)
    token[...] = per_token / 4.0
    sums[...] = contract(
        jnp.broadcast_to(rounded, (8, width)).astype(BF), down_full[...], (1, 1)
    )[:1]
    small_ref[:, :units] = hidden_sum
    small_ref[:, units : units + width] = rounded
    small_ref[:, units + width : units + 2 * width] = final
    small_ref[:, units + 2 * width : units + 2 * width + bins] = g_logits
    small_ref[:, units + 2 * width + bins :] = jnp.broadcast_to(loss, (1, 128))

    def scale_group(group, carry):
        def body(rows):
            here = pl.ds(pl.multiple_of(group * d_local + rows.start, 32), rows.size)
            up_term[group, rows] = (up_base[here] * sums[...]).astype(BF)

        add_tiles(d_local, 32, body)
        return carry

    lax.fori_loop(0, groups, scale_group, 0)
    up_sum = GroupSum(up_term, up_out, u_pair, u_own, u_far, (u_sem0, u_sem1, u_sem2, u_sem3))
    up_sum.start()

    def small_copies():
        return [
            remote(
                small_ref, smalls.at[at.group], (m_send, m_recv), step - 1,
                {"dp": lax.rem(at.group + step, groups)},
            )
            for step in range(1, groups)
        ]

    for copy in small_copies():
        copy.start()
    smalls[at.group] = small_ref[...]

    def back_tile(tile, carry):
        start = pl.multiple_of(tile * local, local)

        def pre(rows):
            here = pl.ds(pl.multiple_of(start + rows.start, 32), rows.size)
            slope[here] = (slope[here].astype(F32) * sums[...]).astype(BF)

        add_tiles(local, 32, pre)
        work[...] = contract(slope[pl.ds(start, local)], up_full[...], (1, 1))

        def body(rows):
            here = pl.ds(pl.multiple_of(start + rows.start, 32), rows.size)
            value = second[here].astype(F32)
            grad = work[rows]
            away = value - jnp.mean(value, axis=-1, keepdims=True)
            inverse = lax.rsqrt(jnp.mean(away * away, axis=-1, keepdims=True) + EPS)
            unit = away * inverse
            back = inverse * (
                grad
                - jnp.mean(grad, axis=-1, keepdims=True)
                - unit * jnp.mean(grad * unit, axis=-1, keepdims=True)
            )
            live = lax.broadcasted_iota(jnp.int32, value.shape, 0) + here.start < length
            g_second[here] = (back + jnp.where(live, token[...], 0.0)).astype(BF)

        add_tiles(local, 32, body)
        return carry

    lax.fori_loop(0, 4, back_tile, 0)
    up_sum.middle()

    def folds(one):
        return [
            Fold(
                at, spread, s_held, s_acc, s_last, (s_send, s_recv), one * 6 + part * 3,
                pl.ds(pl.multiple_of(one * HEAD_WIDTH + part * half, half), half), part == 0,
            )
            for part in range(2)
        ]

    out_folds = [
        Fold(
            at, out_sum, o_held, o_acc, o_last, (o_send, o_recv), part * 3,
            pl.ds(part * (e_local // 2), e_local // 2), part == 0,
        )
        for part in range(2)
    ]
    out_group = DirectSum(out_term, o_pair, o_own, o_far, (o_sem0, o_sem1, o_sem2, o_sem3), 64)

    def qkv_sum(one):
        return DirectSum(
            q_term.at[one], q_pair.at[one], q_own.at[one], q_far.at[one],
            (q_sem0.at[one], q_sem1.at[one], q_sem2.at[one], q_sem3.at[one]), q_term.shape[2],
        )

    def put_context(here, total):
        g_ctx[here] = total.astype(BF)

    def put_out(here, total):
        for chip in range(4):
            o_own[chip, here] = total[:, chip * d_local : (chip + 1) * d_local].astype(BF)

    def pair_out():
        for copy in out_group.pair_copies():
            copy.wait()

        def block(one, carry):
            for chip in range(4):

                def body(rows):
                    here = pl.ds(pl.multiple_of(one * e_local + rows.start, 64), rows.size)
                    out_sum[one, rows, chip * d_local : (chip + 1) * d_local] = (
                        out_term[chip * 2 + at.core, here].astype(F32)
                        + o_pair[chip, here].astype(F32)
                    ).astype(BF)

                add_tiles(e_local, 64, body)
            return carry

        lax.fori_loop(0, 4, block, 0)

    def spread_head(one, carry):
        left = jnp.concatenate(
            [
                outs[pl.ds(pl.multiple_of(part * e_local + one * HEAD_WIDTH, HEAD_WIDTH), HEAD_WIDTH)]
                for part in range(4)
            ],
            axis=0,
        )
        result = contract(left, g_second[...], (1, 1)).astype(BF)
        for part in range(4):
            spread[part, pl.ds(pl.multiple_of(one * HEAD_WIDTH, HEAD_WIDTH), HEAD_WIDTH)] = result[
                part * HEAD_WIDTH : (part + 1) * HEAD_WIDTH
            ]
        for fold in folds(one):
            fold.start()
        return carry

    lax.fori_loop(0, 2, spread_head, 0)
    for fold in folds(0):
        fold.second()
    lax.fori_loop(2, heads, spread_head, 0)
    for fold in folds(1):
        fold.second()

    def out_block(one, carry):
        rows = pl.ds(pl.multiple_of(one * e_local, e_local), e_local)
        result = jnp.dot(ctx[rows], g_second[...], preferred_element_type=F32)
        for group in range(groups):
            out_term[group, rows] = result[:, group * d_local : (group + 1) * d_local].astype(BF)
        return carry

    lax.fori_loop(0, 4, out_block, 0)
    out_group.start()
    load(4).wait()
    load(5).wait()

    def back_head(head, carry):
        for fold in folds(head):
            fold.third(put_context)

        mine = pl.ds(pl.multiple_of(head * HEAD_WIDTH, HEAD_WIDTH), HEAD_WIDTH)
        keys, vals = qkv_ref[1, mine], qkv_ref[2, mine]
        g_keys = jnp.zeros((HEAD_WIDTH, span), F32)
        g_vals = jnp.zeros((HEAD_WIDTH, span), F32)
        for index, start in enumerate(range(0, span, local)):
            here = slice(start, start + local)
            query = (qkv_ref[0, mine, here].astype(F32) * scale).astype(BF)
            grad = g_ctx[mine, here]
            probs = jnp.exp(masked_scores(keys, query, length) - lse_ref[head, :, here])
            g_probs = contract(vals, grad, (0, 0))
            weighted = probs * g_probs
            inner = jnp.sum(weighted, axis=0, keepdims=True)
            g_scores = (weighted - probs * inner).astype(BF)
            g_qkv[:HEAD_WIDTH, here] = (contract(keys, g_scores, (1, 0)) * scale).astype(BF)
            g_keys += contract(query, g_scores, (1, 1))
            g_vals += contract(grad, probs.astype(BF), (1, 1))
            if index == 1:

                @pl.when(head > 0)
                def _():
                    qkv_sum(head - 1).middle()

                @pl.when(head == 1)
                def _():
                    for fold in out_folds:
                        fold.second()

                @pl.when(head == 2)
                def _():
                    for fold in out_folds:
                        fold.third(put_out)
                    for copy in out_group.far_copies():
                        copy.start()

        g_qkv[HEAD_WIDTH : 2 * HEAD_WIDTH] = g_keys.astype(BF)
        g_qkv[2 * HEAD_WIDTH :] = g_vals.astype(BF)
        result = jnp.dot(g_qkv[...], normed[...], preferred_element_type=F32)
        for group in range(groups):
            q_term[head, group] = result[:, group * d_local : (group + 1) * d_local].astype(BF)
        qkv_sum(head).start()

        @pl.when(head == 0)
        def _():
            def second(one, carry):
                for fold in folds(one):
                    fold.second()
                return carry

            lax.fori_loop(2, heads, second, 0)
            pair_out()
            for fold in out_folds:
                fold.start()
            up_sum.relay()
        return carry

    lax.fori_loop(0, heads, back_head, 0)
    qkv_sum(end).middle()
    up_sum.finish()
    for copy in small_copies():
        copy.wait()

    def lines(start, size):
        return [smalls[group, :, pl.ds(start, size)] for group in range(groups)]

    mine_d = pl.multiple_of(at.group * d_local, d_local)
    units_all = split_three(jnp.concatenate(lines(0, units), axis=0))
    tokens_all = jnp.concatenate(lines(units + mine_d, d_local), axis=0)
    down_out[...] = contract(stack_rows(units_all), stack_rows([tokens_all] * 3), (0, 0))
    finals = split_three(jnp.concatenate(lines(units + width + mine_d, d_local), axis=0))
    errors = split_three(jnp.concatenate(lines(units + 2 * width, bins), axis=0))
    order = [(i, j) for i in range(3) for j in range(3) if i + j < 4]
    top_out[...] = contract(
        stack_rows([finals[i] for i, _ in order]), stack_rows([errors[j] for _, j in order]), (0, 0)
    )
    losses = jnp.concatenate(lines(units + 2 * width + bins, 128), axis=0)
    loss_out[...] = jnp.sum(losses, axis=0, keepdims=True) / 8.0

    def drain(one, carry):
        for fold in folds(one):
            fold.finish()
        return carry

    lax.fori_loop(0, heads, drain, 0)
    for fold in out_folds:
        fold.finish()

    def put_final(here, total):
        out_out[here] = total

    out_group.finish(put_final)

    def store(one, carry):
        def put(here, total):
            for kind in range(3):
                qkv_out[kind, pl.ds(pl.multiple_of(one * HEAD_WIDTH, HEAD_WIDTH), HEAD_WIDTH)] = total[
                    kind * HEAD_WIDTH : (kind + 1) * HEAD_WIDTH
                ]

        qkv_sum(one).finish(put)
        return carry

    lax.fori_loop(0, heads, store, 0)


def finish(lengths, bins_at, top, lse, first, context, out_full, up, down, qkv, normed, chunk, ident):
    _, width, length = qkv.shape
    full, units = up.shape
    heads = width // HEAD_WIDTH
    groups = lax.axis_size("dp")
    d_local = full // groups
    bins = top.shape[1]
    rows = 3 * HEAD_WIDTH
    small = units + 2 * full + bins + 128
    dma = pltpu.SemaphoreType.DMA
    smem = pl.BlockSpec(memory_space=pltpu.SMEM)
    return pl.pallas_call(
        functools.partial(finish_body, chunk),
        out_shape=(
            jax.ShapeDtypeStruct((3, width, d_local), F32),
            jax.ShapeDtypeStruct((width, d_local), F32),
            jax.ShapeDtypeStruct((d_local, units), F32),
            jax.ShapeDtypeStruct((units, d_local), F32),
            jax.ShapeDtypeStruct((d_local, bins), F32),
            jax.ShapeDtypeStruct((1, 128), F32),
        ),
        in_specs=[smem, smem, vmem_spec(), vmem_spec()] + [any_spec()] * 7,
        out_specs=(vmem_spec(),) * 6,
        scratch_shapes=[
            VMEM((length, full), BF),
            VMEM(context.shape, BF),
            VMEM(out_full.shape, BF),
            VMEM(up.shape, BF),
            VMEM(down.shape, BF),
            VMEM(qkv.shape, BF),
            VMEM(normed.shape, BF),
            dma((6,)),
            dma((6,)),
            VMEM((length // 4, full), F32),
            VMEM((length, full), BF),
            VMEM((length, full), BF),
            VMEM((full, length), BF),
            VMEM((length, units), BF),
            VMEM((1, units), F32),
            VMEM((1, full), F32),
            VMEM((full, units), F32),
            VMEM((4, 1, full), F32),
            dma((3,)),
            dma((3,)),
            VMEM((1, full), F32),
            VMEM((1, small), F32),
        ]
        + RingGather.scratch()
        + [
            VMEM((length, full), BF),
            VMEM((groups, d_local, units), BF),
            VMEM((4, width, length), BF),
            VMEM((width, length), BF),
            VMEM((2, width, length), BF),
            VMEM((width, length), BF),
            VMEM((width, length), BF),
            dma((heads * 6,)),
            dma((heads * 6,)),
            VMEM((groups, 4 * width, d_local), BF),
            VMEM((4, 4 * width, d_local), BF),
            VMEM((4, width, full // 2), BF),
            VMEM((2, width, full // 2), BF),
            VMEM((width, full // 2), BF),
            VMEM((width, full // 2), BF),
            dma((6,)),
            dma((6,)),
            VMEM((4, width, d_local), BF),
            VMEM((3, width, d_local), BF),
            dma((4,)),
            dma((4,)),
            dma((3,)),
            dma((3,)),
        ]
        + GroupSum.scratch((groups, d_local, units), BF)
        + [
            VMEM((rows, length), BF),
            VMEM((heads, groups, rows, d_local), BF),
            VMEM((heads, 4, rows, d_local), BF),
            VMEM((heads, 4, rows, d_local), BF),
            VMEM((heads, 3, rows, d_local), BF),
            dma((heads, 4)),
            dma((heads, 4)),
            dma((heads, 3)),
            dma((heads, 3)),
            VMEM((groups, 1, small), F32),
            dma((groups - 1,)),
            dma((groups - 1,)),
        ],
        compiler_params=pltpu.CompilerParams(
            collective_id=ident, has_side_effects=True, vmem_limit_bytes=BIG
        ),
        name="finish",
    )(lengths, bins_at, top, lse, first, context, out_full, up, down, qkv, normed)


def per_device_block(
    token_ids,
    lengths,
    teacher_bins,
    embed_table,
    query_key_value_matrix,
    output_matrix,
    up_matrix,
    down_matrix,
    w_head,
):
    ranks = lax.axis_size("tensor")
    rank = lax.axis_index("tensor")
    assert token_ids.shape[0] == 1
    local_len = token_ids.shape[1]
    span = local_len * ranks
    vocab_local, width = embed_table.shape
    _, _, e_local = query_key_value_matrix.shape
    f_local = up_matrix.shape[1]

    all_ids = share_ids(token_ids, 11)
    all_ids = all_ids.reshape(ranks, local_len)
    shifted = all_ids - rank * vocab_local
    inside = (shifted >= 0) & (shifted < vocab_local)
    rows = jnp.take(embed_table, jnp.clip(shifted, 0, vocab_local - 1), axis=0)
    chunk = min(256, span)
    first, normed_one, qkv, context, lse, up_full, out_full, down_part, head_full = front(
        jnp.where(inside[..., None], rows, jnp.zeros((), BF)),
        query_key_value_matrix.transpose(1, 0, 2),
        up_matrix,
        down_matrix,
        w_head,
        output_matrix,
        lengths,
        chunk,
        12,
    )
    first = first.reshape(span, width)
    normed_one = normed_one.reshape(span, width)
    context_all = context.reshape(ranks * e_local, span)
    (
        qkv_gradient,
        output_weight_gradient,
        up_weight_gradient,
        down_weight_gradient,
        grad_head,
        losses,
    ) = finish(
        lengths, teacher_bins, head_full, lse, first, context_all, out_full, up_full, down_part,
        qkv, normed_one, min(256, f_local), 15,
    )
    loss = losses[0, 0]
    query_key_value_gradient = qkv_gradient.transpose(2, 0, 1)
    return (
        loss,
        query_key_value_gradient,
        output_weight_gradient,
        up_weight_gradient,
        down_weight_gradient,
        grad_head,
    )


def solution(mesh):
    placed = (
        P("dp", "tensor"),
        P("dp"),
        P("dp"),
        P("tensor", None),
        P("dp", None, "tensor"),
        P("tensor", "dp"),
        P("dp", "tensor"),
        P("tensor", "dp"),
        P("dp", None),
    )
    return jax.shard_map(
        per_device_block if (mesh.shape["tensor"], mesh.shape["dp"]) == (4, 8) else per_device,
        mesh=mesh,
        in_specs=placed,
        out_specs=(
            P(),
            P("dp", None, "tensor"),
            P("tensor", "dp"),
            P("dp", "tensor"),
            P("tensor", "dp"),
            P("dp", None),
        ),
        check_vma=False,
    )
```

```python
import functools

import jax
import jax.numpy as jnp
from jax import lax
from jax.experimental import pallas as pl
from jax.experimental.pallas import tpu as pltpu
from jax.sharding import PartitionSpec as P

HEAD_WIDTH = 64
EPS = 1e-05
BF = jnp.bfloat16
F32 = jnp.float32
MESH = pl.DeviceIdType.MESH
VMEM = pltpu.VMEM
BIG = 60 * 1024 * 1024


def normalize(values):
    mean = jnp.mean(values, axis=-1, keepdims=True)
    centered = values - mean
    return centered * lax.rsqrt(jnp.mean(centered * centered, axis=-1, keepdims=True) + EPS)


def vmem_spec():
    return pl.BlockSpec(memory_space=pltpu.VMEM)


def greet(axis, count):
    me = lax.axis_index(axis)
    barrier = pltpu.get_barrier_semaphore()
    for step in range(1, count):
        pl.semaphore_signal(
            barrier, inc=1, device_id={axis: lax.rem(me + step, count)}, device_id_type=MESH
        )
    pl.semaphore_wait(barrier, count - 1)
    return me


def gather_body(axis, count, x_ref, out_ref, send_sem, recv_sem):
    me = greet(axis, count)
    copies = []
    for step in range(1, count):
        copy = pltpu.make_async_remote_copy(
            src_ref=x_ref,
            dst_ref=out_ref.at[me],
            send_sem=send_sem.at[step - 1],
            recv_sem=recv_sem.at[step - 1],
            device_id={axis: lax.rem(me + step, count)},
            device_id_type=MESH,
        )
        copy.start()
        copies.append(copy)
    out_ref[me] = x_ref[...]
    for copy in copies:
        copy.wait()


def relay_gather(axis, me, src, out, send_sem, recv_sem):
    across = me + 1 - 2 * lax.rem(me, 2)
    over = lax.rem(me + 2, 4)
    half = src.shape[0] // 2
    low, high = pl.ds(0, half), pl.ds(half, half)

    def copy(index, src_part, block, part, device):
        return pltpu.make_async_remote_copy(
            src_ref=src_part,
            dst_ref=out.at[block, part],
            send_sem=send_sem.at[index],
            recv_sem=recv_sem.at[index],
            device_id={axis: device},
            device_id_type=MESH,
        )

    first_a = copy(0, src.at[low], me, low, across)
    first_b = copy(1, src.at[high], me, high, over)
    second_a = copy(2, src.at[high], me, high, across)
    second_b = copy(3, src.at[low], me, low, over)
    for one in (first_a, first_b, second_a, second_b):
        one.start()
    first_a.wait_recv()
    pass_b = copy(4, out.at[across, low], across, low, over)
    pass_b.start()
    first_b.wait_recv()
    pass_a = copy(5, out.at[over, high], over, high, across)
    pass_a.start()
    second_a.wait_recv()
    second_b.wait_recv()
    pass_b.wait_recv()
    pass_a.wait_recv()
    for one in (first_a, first_b, second_a, second_b, pass_b, pass_a):
        one.wait_send()


def relay_body(axis, x_ref, out_ref, send_sem, recv_sem):
    me = greet(axis, 4)
    relay_gather(axis, me, x_ref, out_ref, send_sem, recv_sem)
    out_ref[me] = x_ref[...]


def gather_blocks(x, axis, count, ident):
    if count != 4:
        return gather_all(x, axis, count, ident)
    return pl.pallas_call(
        functools.partial(relay_body, axis),
        out_shape=jax.ShapeDtypeStruct((count,) + x.shape, x.dtype),
        in_specs=[vmem_spec()],
        out_specs=vmem_spec(),
        scratch_shapes=[pltpu.SemaphoreType.DMA((6,)), pltpu.SemaphoreType.DMA((6,))],
        compiler_params=pltpu.CompilerParams(collective_id=ident, has_side_effects=True),
        name="gather_blocks",
    )(x)


def gather_all(x, axis, count, ident):
    return pl.pallas_call(
        functools.partial(gather_body, axis, count),
        out_shape=jax.ShapeDtypeStruct((count,) + x.shape, x.dtype),
        in_specs=[vmem_spec()],
        out_specs=vmem_spec(),
        scratch_shapes=[
            pltpu.SemaphoreType.DMA((count - 1,)),
            pltpu.SemaphoreType.DMA((count - 1,)),
        ],
        compiler_params=pltpu.CompilerParams(collective_id=ident, has_side_effects=True),
        name="gather_all",
    )(x)


def scatter_copies(axis, count, me, x_ref, held, send_sem, recv_sem):
    copies = []
    for step in range(1, count):
        peer = lax.rem(me + step, count)
        copies.append(
            pltpu.make_async_remote_copy(
                src_ref=x_ref.at[peer],
                dst_ref=held.at[step - 1],
                send_sem=send_sem.at[step - 1],
                recv_sem=recv_sem.at[step - 1],
                device_id={axis: peer},
                device_id_type=MESH,
            )
        )
    return copies


def scatter_start(*args):
    for copy in scatter_copies(*args):
        copy.start()


def scatter_finish(axis, count, me, x_ref, held, send_sem, recv_sem, put):
    for copy in scatter_copies(axis, count, me, x_ref, held, send_sem, recv_sem):
        copy.wait()

    def body(at):
        total = x_ref[me, at].astype(F32)
        for step in range(1, count):
            total = total + held[step - 1, at].astype(F32)
        put(at, total)

    add_tiles(x_ref.shape[1], 32, body)


def add_tiles(rows, tile, body):
    def step(index, carry):
        body(pl.ds(pl.multiple_of(index * tile, tile), tile))
        return carry

    lax.fori_loop(0, rows // tile, step, 0)


class GroupSum:
    def __init__(self, x_ref, out_ref, pair, mine, far, sems):
        self.x, self.out, self.pair, self.mine, self.far = x_ref, out_ref, pair, mine, far
        self.sems = sems
        self.groups = x_ref.shape[0]
        self.chips = self.groups // 2
        self.rows = x_ref.shape[1]
        me = lax.axis_index("dp")
        self.core = lax.rem(me, 2)
        self.chip = me // 2
        self.near = self.chip * 2 + 1 - self.core

    @staticmethod
    def scratch(shape, dtype):
        groups, rows, columns = shape
        chips = groups // 2
        return [
            VMEM((chips, rows, columns), dtype),
            VMEM((chips, rows, columns), dtype),
            VMEM((chips - 1, rows, columns), dtype),
            pltpu.SemaphoreType.DMA((chips,)),
            pltpu.SemaphoreType.DMA((chips,)),
            pltpu.SemaphoreType.DMA((6 if chips == 4 else chips - 1,)),
            pltpu.SemaphoreType.DMA((6 if chips == 4 else chips - 1,)),
        ]

    def signal(self, barrier):
        pl.semaphore_signal(
            barrier, inc=1, device_id={"dp": self.near}, device_id_type=MESH
        )
        for step in range(1, self.chips):
            pl.semaphore_signal(
                barrier, inc=1, device_id={"dp": self.owner(step)}, device_id_type=MESH
            )
        return self.chips

    def owner(self, step):
        return lax.rem(self.chip + step, self.chips) * 2 + self.core

    def pair_copies(self):
        copies = []
        for chip in range(self.chips):
            copies.append(
                pltpu.make_async_remote_copy(
                    src_ref=self.x.at[chip * 2 + 1 - self.core],
                    dst_ref=self.pair.at[chip],
                    send_sem=self.sems[0].at[chip],
                    recv_sem=self.sems[1].at[chip],
                    device_id={"dp": self.near},
                    device_id_type=MESH,
                )
            )
        return copies

    def far_copies(self):
        copies = []
        for step in range(1, self.chips):
            copies.append(
                pltpu.make_async_remote_copy(
                    src_ref=self.mine.at[lax.rem(self.chip + step, self.chips)],
                    dst_ref=self.far.at[step - 1],
                    send_sem=self.sems[2].at[step - 1],
                    recv_sem=self.sems[3].at[step - 1],
                    device_id={"dp": self.owner(step)},
                    device_id_type=MESH,
                )
            )
        return copies

    def ring_copies(self):
        right, left = lax.rem(self.chip + 1, 4), lax.rem(self.chip + 3, 4)
        opposite = lax.rem(self.chip + 2, 4)
        half = self.rows // 2
        low, high = pl.ds(0, half), pl.ds(half, half)

        def copy(index, block, part, slot, chip):
            return pltpu.make_async_remote_copy(
                src_ref=self.mine.at[block, part],
                dst_ref=self.far.at[slot, part],
                send_sem=self.sems[2].at[index],
                recv_sem=self.sems[3].at[index],
                device_id={"dp": chip * 2 + self.core},
                device_id_type=MESH,
            )

        return (
            copy(0, opposite, low, 2, right),
            copy(1, opposite, high, 2, left),
            copy(2, right, high, 0, right),
            copy(3, left, low, 1, left),
            copy(4, right, low, 0, right),
            copy(5, left, high, 1, left),
        )

    def relay(self):
        if self.chips != 4:
            return
        copies = self.ring_copies()
        half = self.rows // 2
        for index, step, base in ((0, 1, 0), (1, 3, half)):
            copies[index].wait_recv()
            block = lax.rem(self.chip + step, 4)

            def body(at, block=block, base=base):
                here = pl.ds(base + at.start, at.size)
                self.mine[block, here] = (
                    self.mine[block, here].astype(F32) + self.far[2, here].astype(F32)
                ).astype(self.mine.dtype)

            add_tiles(half, 32, body)
            copies[index + 4].start()

    def start(self):
        for copy in self.pair_copies():
            copy.start()

    def middle(self):
        for copy in self.pair_copies():
            copy.wait()

        for chip in range(self.chips):

            def body(at, chip=chip):
                self.mine[chip, at] = (
                    self.x[chip * 2 + self.core, at].astype(F32)
                    + self.pair[chip, at].astype(F32)
                ).astype(self.mine.dtype)

            add_tiles(self.rows, 32, body)
        copies = self.ring_copies()[:4] if self.chips == 4 else self.far_copies()
        for copy in copies:
            copy.start()

    def finish(self):
        if self.chips == 4:
            copies = self.ring_copies()
            for copy in copies[2:]:
                copy.wait()
            for copy in copies[:2]:
                copy.wait_send()
        else:
            for copy in self.far_copies():
                copy.wait()

        def body(at):
            total = self.mine[self.chip, at].astype(F32)
            for step in range(2 if self.chips == 4 else self.chips - 1):
                total = total + self.far[step, at].astype(F32)
            self.out[at] = total

        add_tiles(self.rows, 32, body)


def scatter_and_group_body(
    count, x_ref, up_ref, small_ref, out_ref, up_out, small_out, held, send_sem, recv_sem, *rest
):
    up = GroupSum(up_ref, up_out, rest[0], rest[1], rest[2], rest[3:7])
    small_send, small_recv = rest[7:]
    groups = small_out.shape[0]
    group = lax.axis_index("dp")
    barrier = pltpu.get_barrier_semaphore()
    me = lax.axis_index("tensor")
    for step in range(1, count):
        pl.semaphore_signal(
            barrier, inc=1, device_id={"tensor": lax.rem(me + step, count)}, device_id_type=MESH
        )
    for step in range(1, groups):
        pl.semaphore_signal(
            barrier, inc=1, device_id={"dp": lax.rem(group + step, groups)}, device_id_type=MESH
        )
    pl.semaphore_wait(barrier, count + groups - 2)
    smalls = []
    for step in range(1, groups):
        smalls.append(
            pltpu.make_async_remote_copy(
                src_ref=small_ref,
                dst_ref=small_out.at[group],
                send_sem=small_send.at[step - 1],
                recv_sem=small_recv.at[step - 1],
                device_id={"dp": lax.rem(group + step, groups)},
                device_id_type=MESH,
            )
        )

    def put(at, total):
        out_ref[at] = total.astype(out_ref.dtype)

    up.start()
    scatter_start("tensor", count, me, x_ref, held, send_sem, recv_sem)
    up.middle()
    for copy in smalls:
        copy.start()
    small_out[group] = small_ref[...]
    up.relay()
    scatter_finish("tensor", count, me, x_ref, held, send_sem, recv_sem, put)
    up.finish()
    for copy in smalls:
        copy.wait()


def scatter_and_group(x, up, small, count, ident):
    return pl.pallas_call(
        functools.partial(scatter_and_group_body, count),
        out_shape=(
            jax.ShapeDtypeStruct(x.shape[1:], x.dtype),
            jax.ShapeDtypeStruct(up.shape[1:], F32),
            jax.ShapeDtypeStruct(up.shape[:1] + small.shape, F32),
        ),
        in_specs=[vmem_spec()] * 3,
        out_specs=(vmem_spec(),) * 3,
        scratch_shapes=[
            VMEM((count - 1,) + x.shape[1:], x.dtype),
            pltpu.SemaphoreType.DMA((count - 1,)),
            pltpu.SemaphoreType.DMA((count - 1,)),
        ]
        + GroupSum.scratch(up.shape, up.dtype)
        + [pltpu.SemaphoreType.DMA((up.shape[0] - 1,))] * 2,
        compiler_params=pltpu.CompilerParams(
            collective_id=ident, has_side_effects=True, vmem_limit_bytes=BIG
        ),
        name="scatter_and_group",
    )(x, up, small)


def group_sum_body(number, *refs):
    xs, outs, rest = refs[:number], refs[number : 2 * number], refs[2 * number :]
    sums = [
        GroupSum(x, out, *rest[7 * i : 7 * i + 3], rest[7 * i + 3 : 7 * i + 7])
        for i, (x, out) in enumerate(zip(xs, outs))
    ]
    barrier = pltpu.get_barrier_semaphore()
    pl.semaphore_wait(barrier, sums[0].signal(barrier))
    for one in sums:
        one.start()
    for one in sums:
        one.middle()
    for one in sums:
        one.relay()
    for one in sums:
        one.finish()


def group_sum(arrays, ident):
    number = len(arrays)
    scratch = []
    for array in arrays:
        scratch += GroupSum.scratch(array.shape, array.dtype)
    return pl.pallas_call(
        functools.partial(group_sum_body, number),
        out_shape=tuple(jax.ShapeDtypeStruct(a.shape[1:], F32) for a in arrays),
        in_specs=[vmem_spec()] * number,
        out_specs=(vmem_spec(),) * number,
        scratch_shapes=scratch,
        compiler_params=pltpu.CompilerParams(
            collective_id=ident, has_side_effects=True, vmem_limit_bytes=BIG
        ),
        name="group_sum",
    )(*arrays)


def sum_all_body(axis, count, x_ref, out_ref, held, send_sem, recv_sem, send_two, recv_two):
    me = greet(axis, count)

    def put(at, total):
        out_ref[me, at] = total.astype(out_ref.dtype)

    scatter_start(axis, count, me, x_ref, held, send_sem, recv_sem)
    scatter_finish(axis, count, me, x_ref, held, send_sem, recv_sem, put)
    if count == 4:
        relay_gather(axis, me, out_ref.at[me], out_ref, send_two, recv_two)
        return
    copies = []
    for step in range(1, count):
        copy = pltpu.make_async_remote_copy(
            src_ref=out_ref.at[me],
            dst_ref=out_ref.at[me],
            send_sem=send_two.at[step - 1],
            recv_sem=recv_two.at[step - 1],
            device_id={axis: lax.rem(me + step, count)},
            device_id_type=MESH,
        )
        copy.start()
        copies.append(copy)
    for copy in copies:
        copy.wait()


def sum_all(x, axis, count, ident):
    return pl.pallas_call(
        functools.partial(sum_all_body, axis, count),
        out_shape=jax.ShapeDtypeStruct(x.shape, x.dtype),
        in_specs=[vmem_spec()],
        out_specs=vmem_spec(),
        scratch_shapes=[VMEM((count - 1,) + x.shape[1:], x.dtype)]
        + [pltpu.SemaphoreType.DMA((count - 1,))] * 2
        + [pltpu.SemaphoreType.DMA((6 if count == 4 else count - 1,))] * 2,
        compiler_params=pltpu.CompilerParams(collective_id=ident, has_side_effects=True),
        name="sum_all",
    )(x)


def contract(left, right, dims):
    return lax.dot_general(left, right, ((dims[:1], dims[1:]), ((), ())), preferred_element_type=F32)


def masked_scores(keys, query, length):
    scores = contract(keys, query, (0, 0))
    position = lax.broadcasted_iota(jnp.int32, scores.shape, 0)
    return jnp.where(position < length, scores, -1e30)


def attend_body(chunk, length_ref, qkv_ref, out_ref, lse_ref):
    length = length_ref[0]
    keys, vals = qkv_ref[1], qkv_ref[2]
    scale = HEAD_WIDTH ** (-0.5)
    for at in range(0, qkv_ref.shape[2], chunk):
        query = (qkv_ref[0, :, at : at + chunk].astype(F32) * scale).astype(BF)
        scores = masked_scores(keys, query, length)
        top = jnp.max(scores, axis=0, keepdims=True)
        expo = jnp.exp(scores - top)
        total = jnp.sum(expo, axis=0, keepdims=True)
        mixed = contract(vals, expo.astype(BF), (1, 0))
        out_ref[:, at : at + chunk] = (mixed * (1.0 / total)).astype(BF)
        lse_ref[0, :, at : at + chunk] = top + jnp.log(total)


def attend(qkv, lengths, chunk):
    _, width, length = qkv.shape
    heads = width // HEAD_WIDTH
    return pl.pallas_call(
        functools.partial(attend_body, chunk),
        grid=(heads,),
        out_shape=(
            jax.ShapeDtypeStruct((width, length), BF),
            jax.ShapeDtypeStruct((heads, 1, length), F32),
        ),
        in_specs=[
            pl.BlockSpec(memory_space=pltpu.SMEM),
            pl.BlockSpec((3, HEAD_WIDTH, length), lambda h: (0, h, 0)),
        ],
        out_specs=(
            pl.BlockSpec((HEAD_WIDTH, length), lambda h: (h, 0)),
            pl.BlockSpec((1, 1, length), lambda h: (h, 0, 0)),
        ),
        cost_estimate=pl.CostEstimate(
            flops=4 * width * length * length,
            bytes_accessed=8 * width * length,
            transcendentals=heads * length * length,
        ),
        compiler_params=pltpu.CompilerParams(vmem_limit_bytes=BIG),
        name="attend",
    )(lengths, qkv)


def attend_back_body(
    chunk, ranks, length_ref, qkv_ref, lse_ref, grad_ref, x_ref, out_ref, x_out, held, send_sem, recv_sem
):
    me = lax.axis_index("tensor")
    args = ("tensor", ranks, me, x_ref, held, send_sem, recv_sem)

    @pl.when(pl.program_id(0) == 0)
    def _():
        greet("tensor", ranks)
        scatter_start(*args)

    attend_back_head(chunk, length_ref, qkv_ref, lse_ref, grad_ref, out_ref)

    @pl.when(pl.program_id(0) == pl.num_programs(0) - 1)
    def _():
        piece = x_out.shape[2]

        def put(at, total):
            for group in range(x_out.shape[0]):
                x_out[group, at] = total[:, group * piece : (group + 1) * piece].astype(BF)

        scatter_finish(*args, put)


def attend_back_head(chunk, length_ref, qkv_ref, lse_ref, grad_ref, out_ref):
    length = length_ref[0]
    keys, vals = qkv_ref[1], qkv_ref[2]
    scale = HEAD_WIDTH ** (-0.5)
    span = qkv_ref.shape[2]
    g_keys = jnp.zeros((HEAD_WIDTH, span), F32)
    g_vals = jnp.zeros((HEAD_WIDTH, span), F32)
    for at in range(0, span, chunk):
        here = slice(at, at + chunk)
        query = (qkv_ref[0, :, here].astype(F32) * scale).astype(BF)
        grad = grad_ref[:, here]
        probs = jnp.exp(masked_scores(keys, query, length) - lse_ref[0, :, here])
        g_probs = contract(vals, grad, (0, 0))
        weighted = probs * g_probs
        inner = jnp.sum(weighted, axis=0, keepdims=True)
        g_scores = (weighted - probs * inner).astype(BF)
        out_ref[0, :, here] = (contract(keys, g_scores, (1, 0)) * scale).astype(BF)
        g_keys += contract(query, g_scores, (1, 1))
        g_vals += contract(grad, probs.astype(BF), (1, 1))
    out_ref[1] = g_keys.astype(BF)
    out_ref[2] = g_vals.astype(BF)


def attend_back(qkv, lengths, lse, grad, x, groups, chunk, ident):
    _, width, length = qkv.shape
    heads = width // HEAD_WIDTH
    return pl.pallas_call(
        functools.partial(attend_back_body, chunk, x.shape[0]),
        grid=(heads,),
        out_shape=(
            jax.ShapeDtypeStruct(qkv.shape, BF),
            jax.ShapeDtypeStruct((groups, x.shape[1], x.shape[2] // groups), BF),
        ),
        in_specs=[
            pl.BlockSpec(memory_space=pltpu.SMEM),
            pl.BlockSpec((3, HEAD_WIDTH, length), lambda h: (0, h, 0)),
            pl.BlockSpec((1, 1, length), lambda h: (h, 0, 0)),
            pl.BlockSpec((HEAD_WIDTH, length), lambda h: (h, 0)),
            vmem_spec(),
        ],
        out_specs=(
            pl.BlockSpec((3, HEAD_WIDTH, length), lambda h: (0, h, 0)),
            vmem_spec(),
        ),
        scratch_shapes=[
            VMEM((x.shape[0] - 1,) + x.shape[1:], x.dtype),
            pltpu.SemaphoreType.DMA((x.shape[0] - 1,)),
            pltpu.SemaphoreType.DMA((x.shape[0] - 1,)),
        ],
        cost_estimate=pl.CostEstimate(
            flops=10 * width * length * length,
            bytes_accessed=14 * width * length,
            transcendentals=heads * length * length,
        ),
        compiler_params=pltpu.CompilerParams(
            collective_id=ident, has_side_effects=True, vmem_limit_bytes=BIG
        ),
        name="attend_back",
    )(lengths, qkv, lse, grad, x)


def hidden_body(length_ref, normed_ref, up_ref, slope_ref, sum_ref):
    pre = jnp.dot(normed_ref[...], up_ref[...], preferred_element_type=F32)
    live = lax.broadcasted_iota(jnp.int32, pre.shape, 0) < length_ref[0]
    square = pre * pre
    bend = jnp.tanh(0.7978845608028654 * (pre * (1.0 + 0.044715 * square)))
    half = 0.5 * (1.0 + bend)
    act = (pre * half).astype(BF).astype(F32)
    sum_ref[...] = jnp.sum(jnp.where(live, act, 0.0), axis=0, keepdims=True)
    inner = 0.7978845608028654 * (1.0 + 3 * 0.044715 * square)
    slope = half + 0.5 * pre * (1.0 - bend * bend) * inner
    slope_ref[...] = jnp.where(live, slope, 0.0).astype(BF)


def hidden(normed, up, lengths, chunk):
    length, width = normed.shape
    units = up.shape[1]
    return pl.pallas_call(
        hidden_body,
        grid=(units // chunk,),
        out_shape=(
            jax.ShapeDtypeStruct((length, units), BF),
            jax.ShapeDtypeStruct((1, units), F32),
        ),
        in_specs=[
            pl.BlockSpec(memory_space=pltpu.SMEM),
            pl.BlockSpec((length, width), lambda f: (0, 0)),
            pl.BlockSpec((width, chunk), lambda f: (0, f)),
        ],
        out_specs=(
            pl.BlockSpec((length, chunk), lambda f: (0, f)),
            pl.BlockSpec((1, chunk), lambda f: (0, f)),
        ),
        cost_estimate=pl.CostEstimate(
            flops=2 * length * width * units,
            bytes_accessed=6 * length * units,
            transcendentals=length * units,
        ),
        compiler_params=pltpu.CompilerParams(vmem_limit_bytes=BIG),
        name="hidden",
    )(lengths, normed, up)


def per_device(
    token_ids,
    lengths,
    teacher_bins,
    embed_table,
    query_key_value_matrix,
    output_matrix,
    up_matrix,
    down_matrix,
    w_head,
):
    ranks = lax.axis_size("tensor")
    groups = lax.axis_size("dp")
    rank = lax.axis_index("tensor")
    group = lax.axis_index("dp")
    assert token_ids.shape[0] == 1
    local_len = token_ids.shape[1]
    span = local_len * ranks
    vocab_local, width = embed_table.shape
    d_local, _, e_local = query_key_value_matrix.shape
    f_local = up_matrix.shape[1]
    bins = w_head.shape[1]
    exact = lax.Precision.HIGHEST

    qkv_full = lax.all_gather(
        query_key_value_matrix.reshape(d_local, 3 * e_local), "dp", axis=0, tiled=True
    )
    out_parts = lax.all_gather(output_matrix, ("tensor", "dp"), axis=0, tiled=False)
    out_full = (
        out_parts.reshape(ranks, groups, e_local, d_local)
        .transpose(0, 2, 1, 3)
        .reshape(ranks * e_local, width)
    )
    up_full = lax.all_gather(up_matrix, "dp", axis=0, tiled=True)
    low = lax.all_gather(
        jnp.concatenate([down_matrix, w_head.reshape(bins, d_local)], axis=0), "dp", axis=0, tiled=False
    )
    down_full = low[:, :f_local]
    head_wide = low[:, f_local:].reshape(width, bins).astype(F32)

    all_ids = gather_all(token_ids, "tensor", ranks, 1).reshape(ranks, local_len)
    shifted = all_ids - rank * vocab_local
    inside = (shifted >= 0) & (shifted < vocab_local)
    rows = jnp.take(embed_table, jnp.clip(shifted, 0, vocab_local - 1), axis=0)
    first = sum_all(
        jnp.where(inside[..., None], rows, jnp.zeros((), BF)), "tensor", ranks, 2
    ).reshape(span, width)
    normed_one = normalize(first.astype(F32)).astype(BF)
    qkv = (
        lax.dot_general(qkv_full, normed_one, (((0,), (1,)), ((), ())), preferred_element_type=F32)
        .astype(BF)
        .reshape(3, e_local, span)
    )
    chunk = min(256, span)
    context, lse = attend(qkv, lengths, chunk)
    context_all = gather_blocks(context, "tensor", ranks, 3).reshape(ranks * e_local, span)
    attn = lax.dot_general(
        context_all, out_full, (((0,), (0,)), ((), ())), preferred_element_type=F32
    )
    second = (first.astype(F32) + attn).astype(BF)
    normed_f, norm_back = jax.vjp(normalize, second.astype(F32))
    normed_two = normed_f.astype(BF)
    slope, hidden_sum = hidden(normed_two, up_full, lengths, min(256, f_local))

    live = (jnp.arange(span, dtype=jnp.int32) < lengths[0]).astype(F32)
    count = lengths.astype(F32)[:, None]
    ffn_part = jnp.einsum(
        "of,jfd->ojd", hidden_sum, down_full.astype(F32), precision=exact
    ).reshape(1, width)
    ffn_all = gather_all(ffn_part, "tensor", ranks, 4)
    second_sum = jnp.sum(second.astype(F32) * live[:, None], axis=0, keepdims=True)
    pooled = (second_sum + jnp.sum(ffn_all, axis=0)) / count
    final, final_back = jax.vjp(normalize, pooled)
    logits = jnp.dot(final, head_wide, precision=exact)
    top = jnp.max(logits, axis=-1, keepdims=True)
    total_exp = jnp.log(jnp.sum(jnp.exp(logits - top), axis=-1, keepdims=True)) + top
    labels = (teacher_bins[:, None] == jnp.arange(bins, dtype=jnp.int32)[None, :]).astype(F32)
    loss_here = total_exp - jnp.sum(logits * labels, axis=-1, keepdims=True)
    g_logits = (jnp.exp(logits - total_exp) - labels) / groups
    g_final = jnp.dot(g_logits, head_wide.T, precision=exact)
    per_token = final_back(g_final)[0] / count
    rounded = per_token.astype(BF).astype(F32)
    g_hidden = jnp.einsum(
        "ojd,jfd->of",
        rounded.reshape(1, groups, d_local),
        down_full.astype(F32),
        precision=exact,
    )

    packed = jnp.concatenate(
        [hidden_sum, rounded, final, g_logits, jnp.broadcast_to(loss_here, (1, 128))], axis=1
    )

    over_seqs = (((0,), (0,)), ((), ()))
    up_base = lax.dot_general(normed_two, slope, over_seqs, preferred_element_type=F32)
    up_term = (up_base * g_hidden).astype(BF).reshape(groups, d_local, f_local)
    g_pre = (slope.astype(F32) * g_hidden).astype(BF)
    g_normed = lax.dot_general(
        g_pre, up_full, (((1,), (1,)), ((), ())), preferred_element_type=F32
    )
    g_second = (
        norm_back(g_normed)[0] + live[:, None] * (per_token / ranks)
    ).astype(BF)
    spread = lax.dot_general(
        out_full, g_second, (((1,), (1,)), ((), ())), preferred_element_type=F32
    ).astype(BF)
    g_context, up_weight_gradient, every = scatter_and_group(
        spread.reshape(ranks, e_local, span), up_term, packed, ranks, 6
    )
    every = every[:, 0]
    hidden_every = every[:, :f_local]
    rounded_every = every[:, f_local : f_local + width]
    final_every = every[:, f_local + width : f_local + 2 * width]
    rest = every[:, f_local + 2 * width :]
    loss = jnp.sum(rest[:, bins]) / groups
    mine = group * d_local
    down_weight_gradient = lax.dot_general(
        hidden_every,
        lax.dynamic_slice_in_dim(rounded_every, mine, d_local, axis=1),
        over_seqs,
        precision=exact,
    )
    grad_head = lax.dot_general(
        lax.dynamic_slice_in_dim(final_every, mine, d_local, axis=1),
        rest[:, :bins],
        over_seqs,
        precision=exact,
    )

    out_term = (
        jnp.dot(context_all, g_second, preferred_element_type=F32)
        .astype(BF)
        .reshape(ranks, e_local, width)
    )
    g_qkv, out_mine = attend_back(qkv, lengths, lse, g_context, out_term, groups, chunk, 7)
    qkv_term = lax.dot_general(
        normed_one,
        g_qkv.reshape(3 * e_local, span),
        (((0,), (1,)), ((), ())),
        preferred_element_type=F32,
    )
    qkv_gradient, output_weight_gradient = group_sum(
        [qkv_term.astype(BF).reshape(groups, d_local, 3 * e_local), out_mine], 8
    )
    query_key_value_gradient = qkv_gradient.reshape(d_local, 3, e_local)
    return (
        loss,
        query_key_value_gradient,
        output_weight_gradient,
        up_weight_gradient,
        down_weight_gradient,
        grad_head,
    )


def remote(src, dst, sems, index, device):
    return pltpu.make_async_remote_copy(
        src_ref=src,
        dst_ref=dst,
        send_sem=sems[0].at[index],
        recv_sem=sems[1].at[index],
        device_id=device,
        device_id_type=MESH,
    )


class Place:
    def __init__(self):
        self.rank = lax.axis_index("tensor")
        self.across = self.rank + 1 - 2 * lax.rem(self.rank, 2)
        self.over = lax.rem(self.rank + 2, 4)
        self.diag = 3 - self.rank
        self.group = lax.axis_index("dp")
        self.core = lax.rem(self.group, 2)
        self.chip = self.group // 2
        self.near = self.chip * 2 + 1 - self.core

    def turn(self, step):
        return lax.rem(self.chip + step, 4)

    def same(self, chip):
        return chip * 2 + self.core

    def peers(self, everyone=False):
        peers = [{"tensor": one} for one in (self.across, self.over, self.diag)]
        if everyone:
            return peers + [{"dp": lax.rem(self.group + step, 8)} for step in range(1, 8)]
        return peers + [
            {"dp": self.near},
            {"dp": self.same(self.turn(1))},
            {"dp": self.same(self.turn(3))},
        ]

    def signal(self, peers):
        barrier = pltpu.get_barrier_semaphore()
        for peer in peers:
            pl.semaphore_signal(barrier, inc=1, device_id=peer, device_id_type=MESH)

    def ready(self, peers):
        pl.semaphore_wait(pltpu.get_barrier_semaphore(), len(peers))


class RingGather:
    def __init__(self, at, src, own, slot, sems):
        self.at, self.src, self.own, self.slot = at, src, own, slot
        self.sems, self.local = sems[:2], sems[2]

    @staticmethod
    def scratch():
        return [
            pltpu.SemaphoreType.DMA((10,)),
            pltpu.SemaphoreType.DMA((10,)),
            pltpu.SemaphoreType.DMA((1,)),
        ]

    def copies(self):
        at = self.at
        right, left, far = at.turn(1), at.turn(3), at.turn(2)
        me, to_right, to_left = at.group, {"dp": at.same(right)}, {"dp": at.same(left)}
        near = {"dp": at.near}

        def held(index, chip, half, device):
            ref = self.slot(at.same(chip), half)
            return remote(ref, ref, self.sems, index, device)

        def first(index, half, device):
            return remote(self.own(half), self.slot(me, half), self.sems, index, device)

        return (
            first(0, 0, to_right),
            first(1, 1, to_left),
            first(2, 1, to_right),
            first(3, 0, to_left),
            held(4, left, 0, to_right),
            held(5, right, 1, to_left),
            remote(self.src, self.slot(me, None), self.sems, 6, near),
            held(7, left, None, near),
            held(8, right, None, near),
            held(9, far, None, near),
        )

    def keep(self):
        return pltpu.make_async_copy(self.src, self.slot(self.at.group, None), self.local.at[0])

    def start(self):
        copies = self.copies()
        for index in (0, 1, 2, 3, 6):
            copies[index].start()
        self.keep().start()

    def relay(self):
        copies = self.copies()
        copies[0].wait_recv()
        copies[4].start()
        copies[1].wait_recv()
        copies[5].start()

    def spread(self):
        copies = self.copies()
        copies[2].wait_recv()
        copies[7].start()
        copies[3].wait_recv()
        copies[8].start()
        copies[4].wait_recv()
        copies[5].wait_recv()
        copies[9].start()

    def finish(self):
        copies = self.copies()
        for index in (6, 7, 8, 9):
            copies[index].wait_recv()
        for copy in copies:
            copy.wait_send()
        self.keep().wait()

    def start_half(self):
        copies = self.copies()
        for index in (0, 1, 6):
            copies[index].start()
        self.keep().start()

    def close_half(self):
        copies = self.copies()
        for index in (0, 1, 6):
            copies[index].wait()
        self.keep().wait()

    def start_rest(self):
        copies = self.copies()
        for index in (2, 3, 4, 5):
            copies[index].start()

    def near(self):
        copies = self.copies()
        copies[2].wait_recv()
        copies[7].start()
        copies[3].wait_recv()
        copies[8].start()

    def far(self):
        copies = self.copies()
        copies[4].wait_recv()
        copies[5].wait_recv()
        copies[9].start()

    def close_rest(self):
        copies = self.copies()
        for index in (7, 8, 9):
            copies[index].wait_recv()
        for index in (2, 3, 4, 5, 7, 8, 9):
            copies[index].wait_send()


def columns_of(ref, size):
    rows = ref.shape[0]

    def slot(block, half):
        lanes = pl.ds(pl.multiple_of(block * size, size), size)
        if half is None:
            return ref.at[:, lanes]
        return ref.at[pl.ds(half * (rows // 2), rows // 2), lanes]

    return slot


def rows_of(ref, block, half, size, axis=0):
    lead = (slice(None),) * axis
    if half is None:
        return ref.at[lead + (pl.ds(pl.multiple_of(block * size, size), size),)]
    part = size // 2
    return ref.at[lead + (pl.ds(pl.multiple_of(block * size + half * part, part), part),)]


def half_rows(ref, half, axis=0):
    part = ref.shape[axis] // 2
    return ref.at[(slice(None),) * axis + (pl.ds(half * part, part),)]


def ids_body(ids_ref, ids_all, send, recv):
    at = Place()
    peers = at.peers()[:3]
    at.signal(peers)
    ids_all[at.rank] = ids_ref[...]
    at.ready(peers)
    copies = [
        remote(ids_ref, ids_all.at[at.rank], (send, recv), index, peer)
        for index, peer in enumerate(peers)
    ]
    for copy in copies:
        copy.start()
    for copy in copies:
        copy.wait()


def share_ids(ids, ident):
    return pl.pallas_call(
        ids_body,
        out_shape=jax.ShapeDtypeStruct((4,) + ids.shape, ids.dtype),
        in_specs=[vmem_spec()],
        out_specs=vmem_spec(),
        scratch_shapes=[pltpu.SemaphoreType.DMA((3,))] * 2,
        compiler_params=pltpu.CompilerParams(collective_id=ident, has_side_effects=True),
        name="share_ids",
    )(ids)


def any_spec():
    return pl.BlockSpec(memory_space=pl.ANY)


class Stream:
    def __init__(self, at, x_ref, acc, held, last, whole, sems, index, rows, x_first):
        self.at, self.x, self.acc, self.held, self.last, self.whole = at, x_ref, acc, held, last, whole
        self.sems, self.index, self.rows = sems, index * 6, rows
        self.one, self.two = (at.across, at.over) if x_first else (at.over, at.across)

    def copies(self):
        at, rows, base, sems = self.at, self.rows, self.index, self.sems
        one, two = {"tensor": self.one}, {"tensor": self.two}
        return (
            remote(self.x.at[at.diag, rows], self.held.at[1, rows], sems, base, one),
            remote(self.x.at[self.one, rows], self.held.at[0, rows], sems, base + 1, one),
            remote(self.acc.at[rows], self.last.at[rows], sems, base + 2, two),
            remote(self.whole.at[at.rank, rows], self.whole.at[at.rank, rows], sems, base + 3, two),
            remote(self.whole.at[at.rank, rows], self.whole.at[at.rank, rows], sems, base + 4, one),
            remote(self.whole.at[self.two, rows], self.whole.at[self.two, rows], sems, base + 5, one),
        )

    def start(self):
        copies = self.copies()
        copies[0].start()
        copies[1].start()

    def second(self):
        copies = self.copies()
        copies[0].wait_recv()

        def body(at):
            here = pl.ds(self.rows.start + at.start, at.size)
            self.acc[here] = self.x[self.two, here] + self.held[1, here]

        add_tiles(self.rows.size, 32, body)
        copies[2].start()

    def third(self):
        copies = self.copies()
        copies[1].wait_recv()
        copies[2].wait_recv()

        def body(at):
            here = pl.ds(self.rows.start + at.start, at.size)
            self.whole[self.at.rank, here] = (
                self.x[self.at.rank, here] + self.held[0, here] + self.last[here]
            )

        add_tiles(self.rows.size, 32, body)
        copies[3].start()
        copies[4].start()

    def relay(self):
        copies = self.copies()
        copies[3].wait_recv()
        copies[5].start()

    def beside(self):
        self.copies()[4].wait_recv()

    def opposite(self):
        self.copies()[5].wait_recv()

    def finish(self):
        for copy in self.copies():
            copy.wait_send()


def front_body(
    chunk, length_ref, x_in, w_ref, up_ref, down_ref, head_ref, out_ref,
    first_out, normed_out, qkv_out, ctx_out, lse_ref, up_out, out_full, down_out, head_out,
    x_ref, acc, held, last, whole, normed, qkv_ref, w_full, w_turn, ctx_ref, cols,
    load, saved, send, recv, col_send, col_recv, ctx_send, ctx_recv, ctx_saved, *rest,
):
    at = Place()
    peers = at.peers()
    at.signal(peers)
    entry = pltpu.make_async_copy(x_in, x_ref, load.at[0])
    entry.start()
    d_local = w_ref.shape[1]
    local = x_ref.shape[1]
    e_local = w_ref.shape[2]
    span = qkv_ref.shape[2]
    heads = lse_ref.shape[0]
    size = HEAD_WIDTH // 2
    weights = RingGather(
        at, w_ref, lambda half: half_rows(w_ref, half, 1),
        lambda block, half: rows_of(w_full, block, half, d_local, 1), rest[:3],
    )
    ups = RingGather(
        at, up_ref, lambda half: half_rows(up_ref, half),
        lambda block, half: rows_of(up_out, block, half, d_local), rest[3:6],
    )
    tops = RingGather(
        at, head_ref, lambda half: half_rows(head_ref, half),
        lambda block, half: rows_of(head_out, block, half, d_local), rest[6:9],
    )
    downs = RingGather(
        at, down_ref, lambda half: half_rows(down_ref, half), columns_of(down_out, d_local), rest[9:12]
    )
    outs = RingGather(
        at, cols, lambda half: half_rows(cols, half), columns_of(out_full, d_local), rest[12:15]
    )
    mine = pl.ds(pl.multiple_of(at.rank * e_local, e_local), e_local)
    own_columns = pltpu.make_async_copy(out_ref, cols.at[mine], load.at[1])
    own_columns.start()
    column_copies = [
        remote(out_ref, cols.at[mine], (col_send, col_recv), index, peer)
        for index, peer in enumerate(peers[:3])
    ]

    at.ready(peers)
    weights.start()
    entry.wait()
    part = local // 4
    streams = [
        Stream(
            at, x_ref, acc, held, last, whole, (send, recv), index,
            pl.ds((index % 2) * (local // 2) + (index // 2) * part, part), index % 2 == 0,
        )
        for index in range(4)
    ]
    for one in streams:
        one.start()
    for one in streams:
        one.second()
    weights.relay()
    ups.start()
    tops.start()
    for one in streams:
        one.third()
    for copy in column_copies:
        copy.start()
    weights.spread()
    weights.finish()
    for index in range(3):
        w_turn[index] = w_full[index].T

    def saves(slot, block):
        base = pl.multiple_of(block * local, local)
        return (
            pltpu.make_async_copy(whole.at[block], first_out.at[block], saved.at[slot, 0]),
            pltpu.make_async_copy(normed.at[block], normed_out.at[block], saved.at[slot, 1]),
            pltpu.make_async_copy(
                qkv_ref.at[:, :, pl.ds(base, local)], qkv_out.at[:, :, pl.ds(base, local)], saved.at[slot, 2]
            ),
        )

    def project(block, slot):
        def tile(here):
            normed[block, here] = normalize(whole[block, here].astype(F32)).astype(BF)

        add_tiles(local, 32, tile)
        base = pl.multiple_of(block * local, local)

        def matrix(index, carry):
            qkv_ref[index, :, pl.ds(base, local)] = contract(
                w_turn[index], normed[block], (1, 1)
            ).astype(BF)
            return carry

        lax.fori_loop(0, 3, matrix, 0)
        for copy in saves(slot, block):
            copy.start()

    for one in streams[:2]:
        one.relay()
    project(at.rank, 0)
    for one in streams[2:]:
        one.relay()
    ups.relay()
    tops.relay()
    for one in streams:
        one.beside()
    own_columns.wait()
    for copy in column_copies:
        copy.wait()
    outs.start()
    downs.start_half()
    project(at.across, 1)
    project(at.over, 2)
    for one in streams:
        one.opposite()
    project(at.diag, 3)

    def copies(one):
        def copy(index, block, half, peer):
            ref = ctx_ref.at[block, pl.ds(pl.multiple_of(one * HEAD_WIDTH + half * size, size), size)]
            return pltpu.make_async_remote_copy(
                src_ref=ref,
                dst_ref=ref,
                send_sem=ctx_send.at[one, index],
                recv_sem=ctx_recv.at[one, index],
                device_id={"tensor": peer},
                device_id_type=MESH,
            )

        return (
            copy(0, at.rank, 0, at.across),
            copy(1, at.rank, 1, at.over),
            copy(2, at.rank, 1, at.across),
            copy(3, at.rank, 0, at.over),
            copy(4, at.across, 0, at.over),
            copy(5, at.over, 1, at.across),
        )

    def relay(one):
        group = copies(one)
        group[0].wait_recv()
        group[4].start()
        group[1].wait_recv()
        group[5].start()

    def save(one):
        here = pl.ds(pl.multiple_of(one * HEAD_WIDTH, HEAD_WIDTH), HEAD_WIDTH)
        return pltpu.make_async_copy(ctx_ref.at[:, here], ctx_out.at[:, here], ctx_saved.at[one])

    length = length_ref[0]
    scale = HEAD_WIDTH ** (-0.5)

    def attend_head(head, carry):
        lines = pl.ds(pl.multiple_of(head * HEAD_WIDTH, HEAD_WIDTH), HEAD_WIDTH)
        keys, vals = qkv_ref[1, lines], qkv_ref[2, lines]
        for start in range(0, span, chunk):
            here = slice(start, start + chunk)
            query = (qkv_ref[0, lines, here].astype(F32) * scale).astype(BF)
            scores = masked_scores(keys, query, length)
            top = jnp.max(scores, axis=0, keepdims=True)
            expo = jnp.exp(scores - top)
            total = jnp.sum(expo, axis=0, keepdims=True)
            mixed = contract(vals, expo.astype(BF), (1, 0))
            ctx_ref[at.rank, lines, here] = (mixed * (1.0 / total)).astype(BF)
            lse_ref[head, :, here] = top + jnp.log(total)

        for copy in copies(head)[:4]:
            copy.start()

        @pl.when(head > 0)
        def _():
            relay(head - 1)

        @pl.when(head == 0)
        def _():
            ups.spread()
            tops.spread()

        @pl.when(head == 2)
        def _():
            outs.relay()

        return carry

    lax.fori_loop(0, heads, attend_head, 0)
    relay(heads - 1)
    outs.spread()
    ups.finish()
    tops.finish()
    downs.close_half()
    for one in streams:
        one.finish()

    def drain(one, carry):
        group = copies(one)
        for copy in group[2:]:
            copy.wait_recv()
        save(one).start()
        for copy in group:
            copy.wait_send()
        return carry

    lax.fori_loop(0, heads, drain, 0)
    for slot, block in enumerate((at.rank, at.across, at.over, at.diag)):
        for copy in saves(slot, block):
            copy.wait()

    def store(one, carry):
        save(one).wait()
        return carry

    lax.fori_loop(0, heads, store, 0)
    outs.finish()


def front(x, w, up, down, top, out, lengths, chunk, ident):
    ranks, local, width = x.shape
    kinds, d_local, e_local = w.shape
    f_local = up.shape[1]
    heads = e_local // HEAD_WIDTH
    span = ranks * local
    assert heads > 2
    dma = pltpu.SemaphoreType.DMA
    return pl.pallas_call(
        functools.partial(front_body, chunk),
        out_shape=(
            jax.ShapeDtypeStruct(x.shape, BF),
            jax.ShapeDtypeStruct(x.shape, BF),
            jax.ShapeDtypeStruct((kinds, e_local, span), BF),
            jax.ShapeDtypeStruct((ranks, e_local, span), BF),
            jax.ShapeDtypeStruct((heads, 1, span), F32),
            jax.ShapeDtypeStruct((width, f_local), BF),
            jax.ShapeDtypeStruct((ranks * e_local, width), BF),
            jax.ShapeDtypeStruct((f_local, width), BF),
            jax.ShapeDtypeStruct((width, top.shape[1]), BF),
        ),
        in_specs=[pl.BlockSpec(memory_space=pltpu.SMEM), any_spec()] + [vmem_spec()] * 5,
        out_specs=(any_spec(),) * 4 + (vmem_spec(),) + (any_spec(),) * 4,
        scratch_shapes=[
            VMEM(x.shape, BF),
            VMEM((local, width), BF),
            VMEM((2, local, width), BF),
            VMEM((local, width), BF),
            VMEM(x.shape, BF),
            VMEM(x.shape, BF),
            VMEM((kinds, e_local, span), BF),
            VMEM((kinds, width, e_local), BF),
            VMEM((kinds, e_local, width), BF),
            VMEM((ranks, e_local, span), BF),
            VMEM((ranks * e_local, d_local), BF),
            dma((2,)),
            dma((4, 3)),
            dma((24,)),
            dma((24,)),
            dma((3,)),
            dma((3,)),
            dma((heads, 6)),
            dma((heads, 6)),
            dma((heads,)),
        ]
        + RingGather.scratch() * 5,
        compiler_params=pltpu.CompilerParams(
            collective_id=ident, has_side_effects=True, vmem_limit_bytes=BIG
        ),
        name="front",
    )(lengths, x, w, up, down, top, out)


def exact_dot(row, matrix, dims):
    high = row.astype(BF).astype(F32)
    middle = (row - high).astype(BF).astype(F32)
    low = row - high - middle
    shape = (8, row.shape[1])
    index = lax.broadcasted_iota(jnp.int32, shape, 0)
    stacked = jnp.where(
        index == 0, jnp.broadcast_to(high, shape),
        jnp.where(
            index == 1, jnp.broadcast_to(middle, shape),
            jnp.where(index == 2, jnp.broadcast_to(low, shape), 0.0),
        ),
    ).astype(BF)
    return jnp.sum(contract(stacked, matrix, dims), axis=0, keepdims=True)


class Fold:
    def __init__(self, at, src, held, acc, last, sems, base, rows, x_first):
        self.at, self.src, self.held, self.acc, self.last = at, src, held, acc, last
        self.sems, self.base, self.rows = sems, base, rows
        self.one, self.two = (at.across, at.over) if x_first else (at.over, at.across)

    def copies(self):
        rows, base, sems = self.rows, self.base, self.sems
        one, two = {"tensor": self.one}, {"tensor": self.two}
        return (
            remote(self.src.at[self.at.diag, rows], self.held.at[1, rows], sems, base, one),
            remote(self.src.at[self.one, rows], self.held.at[0, rows], sems, base + 1, one),
            remote(self.acc.at[rows], self.last.at[rows], sems, base + 2, two),
        )

    def start(self):
        copies = self.copies()
        copies[0].start()
        copies[1].start()

    def tiles(self, body):
        def step(at):
            body(pl.ds(pl.multiple_of(self.rows.start + at.start, 32), at.size))

        add_tiles(self.rows.size, 32, step)

    def second(self):
        copies = self.copies()
        copies[0].wait_recv()

        def body(here):
            self.acc[here] = (
                self.src[self.two, here].astype(F32) + self.held[1, here].astype(F32)
            ).astype(BF)

        self.tiles(body)
        copies[2].start()

    def third(self, put):
        copies = self.copies()
        copies[1].wait_recv()
        copies[2].wait_recv()

        def body(here):
            put(
                here,
                self.src[self.at.rank, here].astype(F32)
                + self.held[0, here].astype(F32)
                + self.last[here].astype(F32),
            )

        self.tiles(body)

    def finish(self):
        for copy in self.copies():
            copy.wait_send()


class DirectSum(GroupSum):
    def __init__(self, x_ref, pair, mine, far, sems, tile):
        super().__init__(x_ref, None, pair, mine, far, sems)
        self.tile = tile

    def middle(self):
        for copy in self.pair_copies():
            copy.wait()
        for chip in range(self.chips):

            def body(at, chip=chip):
                self.mine[chip, at] = (
                    self.x[chip * 2 + self.core, at].astype(F32)
                    + self.pair[chip, at].astype(F32)
                ).astype(BF)

            add_tiles(self.rows, self.tile, body)
        for copy in self.far_copies():
            copy.start()

    def finish(self, put):
        for copy in self.far_copies():
            copy.wait()

        def body(at):
            total = self.mine[self.chip, at].astype(F32)
            for step in range(self.chips - 1):
                total = total + self.far[step, at].astype(F32)
            put(at, total)

        add_tiles(self.far.shape[1], self.tile, body)


def stack_rows(rows):
    rows = list(rows)
    zero = jnp.zeros(rows[0].shape, F32)
    while len(rows) * rows[0].shape[0] % 16:
        rows.append(zero)
    return jnp.concatenate(rows, axis=0).astype(BF)


def split_three(values):
    high = values.astype(BF).astype(F32)
    middle = (values - high).astype(BF).astype(F32)
    return high, middle, values - high - middle


def finish_body(
    chunk, length_ref, bin_ref, top_ref, lse_ref,
    first_in, ctx_in, out_in, up_in, down_in, qkv_in, normed_in,
    qkv_out, out_out, up_out, down_out, top_out, loss_out,
    first, ctx, outs, up_full, down_full, qkv_ref, normed, loads, tile_loads, down_loads, stats,
    work, second, normed_two, turned, slope, sums, base, up_base, parts, p_send, p_recv, token, small_ref,
    d_send, d_recv, d_local_sem,
    g_second, up_term,
    spread, g_ctx, s_held, s_acc, s_last, s_send, s_recv,
    out_term, o_pair, out_sum, o_held, o_acc, o_last, o_send, o_recv,
    o_own, o_far, o_sem0, o_sem1, o_sem2, o_sem3,
    u_pair, u_own, u_far, u_sem0, u_sem1, u_sem2, u_sem3,
    g_qkv, q_term, q_pair, q_own, q_far, q_sem0, q_sem1, q_sem2, q_sem3,
    smalls, m_send, m_recv, q_all,
):
    at = Place()
    peers = at.peers(True)
    at.signal(peers)
    heads = lse_ref.shape[0]
    end = heads - 1
    e_local = g_ctx.shape[0]
    d_local = q_term.shape[3]
    groups = q_term.shape[1]
    span, width = first.shape
    units = slope.shape[1]
    bins = top_ref.shape[1]
    half = HEAD_WIDTH // 2
    length = length_ref[0]
    scale = HEAD_WIDTH ** (-0.5)
    local = span // 4

    pairs = ((out_in, outs), (up_in, up_full), (qkv_in, qkv_ref), (normed_in, normed))

    def load(index):
        return pltpu.make_async_copy(*pairs[index], loads.at[index])

    def load_tile(tile):
        here = pl.ds(pl.multiple_of(tile * local, local), local)
        return (
            pltpu.make_async_copy(ctx_in.at[:, here], ctx.at[:, here], tile_loads.at[tile, 0]),
            pltpu.make_async_copy(first_in.at[here], first.at[here], tile_loads.at[tile, 1]),
        )

    slot = columns_of(down_full, d_local)
    source = columns_of(down_in, d_local)
    downs = RingGather(
        at, slot(at.group, None), lambda part: slot(at.group, part), slot, (d_send, d_recv, d_local_sem)
    )

    def load_down(index):
        other = at.group + 1 - 2 * at.core
        ends = ((at.same(at.turn(3)), 0), (at.same(at.turn(1)), 1), (at.group, None), (other, None))
        return pltpu.make_async_copy(
            source(*ends[index]), slot(*ends[index]), down_loads.at[index]
        )

    load(0).start()
    for copy in load_tile(0):
        copy.start()
    for index in range(3):
        load_down(index).start()
    for tile in range(1, 4):
        for copy in load_tile(tile):
            copy.start()
    load(1).start()
    load_down(3).start()
    load(2).start()
    load(3).start()
    base[...] = jnp.zeros(base.shape, F32)
    load(0).wait()

    def project_tile(tile, carry):
        for copy in load_tile(tile):
            copy.wait()
        start = pl.multiple_of(tile * local, local)
        work[...] = contract(ctx[:, pl.ds(start, local)], outs[...], (0, 0))

        def body(rows):
            here = pl.ds(pl.multiple_of(start + rows.start, 64), rows.size)
            value = (first[here].astype(F32) + work[rows]).astype(BF)
            second[here] = value
            value = value.astype(F32)
            mean = jnp.mean(value, axis=-1, keepdims=True)
            away = value - mean
            inverse = lax.rsqrt(jnp.mean(away * away, axis=-1, keepdims=True) + EPS)
            normed_two[here] = (away * inverse).astype(BF)
            stats[0, here] = jnp.broadcast_to(mean, (rows.size, 128))
            stats[1, here] = jnp.broadcast_to(inverse, (rows.size, 128))
            live = lax.broadcasted_iota(jnp.int32, value.shape, 0) + here.start < length
            base[...] += jnp.sum(
                jnp.where(live, value, 0.0).reshape(rows.size // 8, 8, width), axis=0
            )

        add_tiles(local, 64, body)
        turned[:, pl.ds(start, local)] = normed_two[pl.ds(start, local)].T
        return carry

    lax.fori_loop(0, 1, project_tile, 0)
    for index in range(3):
        load_down(index).wait()
    at.ready(peers)
    downs.start_rest()
    lax.fori_loop(1, 4, project_tile, 0)
    load(1).wait()

    def hidden_chunk(step, carry):
        lanes = pl.ds(pl.multiple_of(step * chunk, chunk), chunk)
        pre = jnp.dot(normed_two[...], up_full[:, lanes], preferred_element_type=F32)
        live = lax.broadcasted_iota(jnp.int32, pre.shape, 0) < length
        square = pre * pre
        bend = jnp.tanh(0.7978845608028654 * (pre * (1.0 + 0.044715 * square)))
        part = 0.5 * (1.0 + bend)
        act = (pre * part).astype(BF).astype(F32)
        sums[:, lanes] = jnp.sum(jnp.where(live, act, 0.0), axis=0, keepdims=True)
        inner = 0.7978845608028654 * (1.0 + 3 * 0.044715 * square)
        value = part + 0.5 * pre * (1.0 - bend * bend) * inner
        slope[:, lanes] = jnp.where(live, value, 0.0).astype(BF)
        return carry

    lax.fori_loop(0, units // chunk, hidden_chunk, 0)
    load_down(3).wait()
    downs.near()
    downs.far()
    downs.close_rest()
    hidden_sum = sums[...]
    parts[at.rank] = exact_dot(hidden_sum, down_full[...], (1, 0))
    part_copies = [
        remote(parts.at[at.rank], parts.at[at.rank], (p_send, p_recv), index, peer)
        for index, peer in enumerate(peers[:3])
    ]
    for copy in part_copies:
        copy.start()

    def base_chunk(step, carry):
        lanes = pl.ds(pl.multiple_of(step * chunk, chunk), chunk)
        up_base[:, lanes] = jnp.dot(turned[...], slope[:, lanes], preferred_element_type=F32)
        return carry

    lax.fori_loop(0, units // chunk, base_chunk, 0)
    for copy in part_copies:
        copy.wait()
    count = jnp.full((1, 1), length, jnp.int32).astype(F32)
    total = jnp.sum(base[...], axis=0, keepdims=True)
    for index in range(4):
        total = total + parts[index]
    pooled = total / count
    mean = jnp.mean(pooled, axis=-1, keepdims=True)
    centered = pooled - mean
    norm_scale = lax.rsqrt(jnp.mean(centered * centered, axis=-1, keepdims=True) + EPS)
    final = centered * norm_scale
    logits = exact_dot(final, top_ref[...], (1, 0))
    highest = jnp.max(logits, axis=-1, keepdims=True)
    total_exp = jnp.log(jnp.sum(jnp.exp(logits - highest), axis=-1, keepdims=True)) + highest
    labels = (lax.broadcasted_iota(jnp.int32, logits.shape, 1) == bin_ref[0]).astype(F32)
    loss = total_exp - jnp.sum(logits * labels, axis=-1, keepdims=True)
    g_logits = (jnp.exp(logits - total_exp) - labels) / 8.0
    g_final = exact_dot(g_logits, top_ref[...], (1, 1))
    g_pooled = norm_scale * (
        g_final
        - jnp.mean(g_final, axis=-1, keepdims=True)
        - final * jnp.mean(g_final * final, axis=-1, keepdims=True)
    )
    per_token = g_pooled / count
    rounded = per_token.astype(BF).astype(F32)
    token[...] = per_token / 4.0
    sums[...] = contract(
        jnp.broadcast_to(rounded, (8, width)).astype(BF), down_full[...], (1, 1)
    )[:1]
    small_ref[:, :units] = hidden_sum
    small_ref[:, units : units + width] = rounded
    small_ref[:, units + width : units + 2 * width] = final
    small_ref[:, units + 2 * width : units + 2 * width + bins] = g_logits
    small_ref[:, units + 2 * width + bins :] = jnp.broadcast_to(loss, (1, 128))

    def scale_group(group, carry):
        def body(rows):
            here = pl.ds(pl.multiple_of(group * d_local + rows.start, 32), rows.size)
            up_term[group, rows] = (up_base[here] * sums[...]).astype(BF)

        add_tiles(d_local, 32, body)
        return carry

    lax.fori_loop(0, groups, scale_group, 0)
    up_sum = GroupSum(up_term, up_out, u_pair, u_own, u_far, (u_sem0, u_sem1, u_sem2, u_sem3))
    up_sum.start()

    def small_copies():
        return [
            remote(
                small_ref, smalls.at[at.group], (m_send, m_recv), step - 1,
                {"dp": lax.rem(at.group + step, groups)},
            )
            for step in range(1, groups)
        ]

    for copy in small_copies():
        copy.start()
    smalls[at.group] = small_ref[...]

    def back_tile(tile, carry):
        start = pl.multiple_of(tile * local, local)

        def pre(rows):
            here = pl.ds(pl.multiple_of(start + rows.start, 64), rows.size)
            slope[here] = (slope[here].astype(F32) * sums[...]).astype(BF)

        add_tiles(local, 64, pre)
        work[...] = contract(slope[pl.ds(start, local)], up_full[...], (1, 1))

        def body(rows):
            here = pl.ds(pl.multiple_of(start + rows.start, 64), rows.size)
            grad = work[rows]
            inverse = stats[1, here, :1]
            unit = (second[here].astype(F32) - stats[0, here, :1]) * inverse
            back = inverse * (
                grad
                - jnp.mean(grad, axis=-1, keepdims=True)
                - unit * jnp.mean(grad * unit, axis=-1, keepdims=True)
            )
            live = lax.broadcasted_iota(jnp.int32, grad.shape, 0) + here.start < length
            g_second[here] = (back + jnp.where(live, token[...], 0.0)).astype(BF)

        add_tiles(local, 64, body)
        return carry

    lax.fori_loop(0, 1, back_tile, 0)
    up_sum.middle()
    lax.fori_loop(1, 4, back_tile, 0)

    def folds(one):
        return [
            Fold(
                at, spread, s_held, s_acc, s_last, (s_send, s_recv), one * 6 + part * 3,
                pl.ds(pl.multiple_of(one * HEAD_WIDTH + part * half, half), half), part == 0,
            )
            for part in range(2)
        ]

    out_folds = [
        Fold(
            at, out_sum, o_held, o_acc, o_last, (o_send, o_recv), part * 3,
            pl.ds(part * (e_local // 2), e_local // 2), part == 0,
        )
        for part in range(2)
    ]
    out_group = DirectSum(out_term, o_pair, o_own, o_far, (o_sem0, o_sem1, o_sem2, o_sem3), 64)

    def qkv_sum(one):
        return DirectSum(
            q_term.at[one], q_pair.at[one], q_own.at[one], q_far.at[one],
            (q_sem0.at[one], q_sem1.at[one], q_sem2.at[one], q_sem3.at[one]), q_term.shape[2],
        )

    def put_context(here, total):
        g_ctx[here] = total.astype(BF)

    def put_out(here, total):
        for chip in range(4):
            o_own[chip, here] = total[:, chip * d_local : (chip + 1) * d_local].astype(BF)

    def pair_out():
        for copy in out_group.pair_copies():
            copy.wait()

        def block(one, carry):
            for chip in range(4):

                def body(rows):
                    here = pl.ds(pl.multiple_of(one * e_local + rows.start, 64), rows.size)
                    out_sum[one, rows, chip * d_local : (chip + 1) * d_local] = (
                        out_term[chip * 2 + at.core, here].astype(F32)
                        + o_pair[chip, here].astype(F32)
                    ).astype(BF)

                add_tiles(e_local, 64, body)
            return carry

        lax.fori_loop(0, 4, block, 0)

    def spread_head(one, carry):
        left = jnp.concatenate(
            [
                outs[pl.ds(pl.multiple_of(part * e_local + one * HEAD_WIDTH, HEAD_WIDTH), HEAD_WIDTH)]
                for part in range(4)
            ],
            axis=0,
        )
        result = contract(left, g_second[...], (1, 1)).astype(BF)
        for part in range(4):
            spread[part, pl.ds(pl.multiple_of(one * HEAD_WIDTH, HEAD_WIDTH), HEAD_WIDTH)] = result[
                part * HEAD_WIDTH : (part + 1) * HEAD_WIDTH
            ]
        for fold in folds(one):
            fold.start()
        return carry

    def out_block(one, carry):
        rows = pl.ds(pl.multiple_of(one * e_local, e_local), e_local)
        result = jnp.dot(ctx[rows], g_second[...], preferred_element_type=F32)
        for group in range(groups):
            out_term[group, rows] = result[:, group * d_local : (group + 1) * d_local].astype(BF)
        return carry

    lax.fori_loop(0, 2, spread_head, 0)
    lax.fori_loop(0, 2, out_block, 0)
    for fold in folds(0):
        fold.second()
    lax.fori_loop(2, heads, spread_head, 0)
    for fold in folds(1):
        fold.second()
    lax.fori_loop(2, 4, out_block, 0)
    out_group.start()
    up_sum.relay()
    load(2).wait()
    load(3).wait()

    def back_head(head, carry):
        for fold in folds(head):
            fold.third(put_context)

        mine = pl.ds(pl.multiple_of(head * HEAD_WIDTH, HEAD_WIDTH), HEAD_WIDTH)
        keys, vals = qkv_ref[1, mine], qkv_ref[2, mine]
        g_keys = jnp.zeros((HEAD_WIDTH, span), F32)
        g_vals = jnp.zeros((HEAD_WIDTH, span), F32)
        for index, start in enumerate(range(0, span, local)):
            here = slice(start, start + local)
            query = (qkv_ref[0, mine, here].astype(F32) * scale).astype(BF)
            grad = g_ctx[mine, here]
            probs = jnp.exp(masked_scores(keys, query, length) - lse_ref[head, :, here])
            g_probs = contract(vals, grad, (0, 0))
            weighted = probs * g_probs
            inner = jnp.sum(weighted, axis=0, keepdims=True)
            g_scores = (weighted - probs * inner).astype(BF)
            g_qkv[:HEAD_WIDTH, here] = (contract(keys, g_scores, (1, 0)) * scale).astype(BF)
            g_keys += contract(query, g_scores, (1, 1))
            g_vals += contract(grad, probs.astype(BF), (1, 1))
            if index == 1:

                @pl.when(head > 0)
                def _():
                    qkv_sum(head - 1).middle()

            if index == 3:

                @pl.when(head == 1)
                def _():
                    for fold in out_folds:
                        fold.second()

                @pl.when(head == 2)
                def _():
                    for fold in out_folds:
                        fold.third(put_out)
                    for copy in out_group.far_copies():
                        copy.start()

        g_qkv[HEAD_WIDTH : 2 * HEAD_WIDTH] = g_keys.astype(BF)
        g_qkv[2 * HEAD_WIDTH :] = g_vals.astype(BF)
        result = jnp.dot(g_qkv[...], normed[...], preferred_element_type=F32)
        for group in range(groups):
            q_term[head, group] = result[:, group * d_local : (group + 1) * d_local].astype(BF)
        qkv_sum(head).start()

        @pl.when(head == 0)
        def _():
            def second(one, carry):
                for fold in folds(one):
                    fold.second()
                return carry

            lax.fori_loop(2, heads, second, 0)
            pair_out()
            for fold in out_folds:
                fold.start()
        return carry

    lax.fori_loop(0, heads, back_head, 0)
    qkv_sum(end).middle()
    up_sum.finish()
    for copy in small_copies():
        copy.wait()

    def lines(start, size):
        return [smalls[group, :, pl.ds(start, size)] for group in range(groups)]

    mine_d = pl.multiple_of(at.group * d_local, d_local)
    units_all = split_three(jnp.concatenate(lines(0, units), axis=0))
    tokens_all = jnp.concatenate(lines(units + mine_d, d_local), axis=0)
    down_out[...] = contract(stack_rows(units_all), stack_rows([tokens_all] * 3), (0, 0))
    finals = split_three(jnp.concatenate(lines(units + width + mine_d, d_local), axis=0))
    errors = split_three(jnp.concatenate(lines(units + 2 * width, bins), axis=0))
    order = [(i, j) for i in range(3) for j in range(3) if i + j < 4]
    top_out[...] = contract(
        stack_rows([finals[i] for i, _ in order]), stack_rows([errors[j] for _, j in order]), (0, 0)
    )
    losses = jnp.concatenate(lines(units + 2 * width + bins, 128), axis=0)
    loss_out[...] = jnp.sum(losses, axis=0, keepdims=True) / 8.0

    def drain(one, carry):
        for fold in folds(one):
            fold.finish()
        return carry

    lax.fori_loop(0, heads, drain, 0)
    for fold in out_folds:
        fold.finish()

    def put_final(here, total):
        out_out[here] = total

    out_group.finish(put_final)

    def store(one, carry):
        def put(here, total):
            for kind in range(3):
                q_all[kind, pl.ds(pl.multiple_of(one * HEAD_WIDTH, HEAD_WIDTH), HEAD_WIDTH)] = total[
                    kind * HEAD_WIDTH : (kind + 1) * HEAD_WIDTH
                ]

        qkv_sum(one).finish(put)
        return carry

    lax.fori_loop(0, heads, store, 0)
    for kind in range(3):
        qkv_out[kind] = q_all[kind].T


def finish(lengths, bins_at, top, lse, first, context, out_full, up, down, qkv, normed, chunk, ident):
    _, width, length = qkv.shape
    full, units = up.shape
    heads = width // HEAD_WIDTH
    groups = lax.axis_size("dp")
    d_local = full // groups
    bins = top.shape[1]
    rows = 3 * HEAD_WIDTH
    small = units + 2 * full + bins + 128
    dma = pltpu.SemaphoreType.DMA
    smem = pl.BlockSpec(memory_space=pltpu.SMEM)
    return pl.pallas_call(
        functools.partial(finish_body, chunk),
        out_shape=(
            jax.ShapeDtypeStruct((3, d_local, width), F32),
            jax.ShapeDtypeStruct((width, d_local), F32),
            jax.ShapeDtypeStruct((d_local, units), F32),
            jax.ShapeDtypeStruct((units, d_local), F32),
            jax.ShapeDtypeStruct((d_local, bins), F32),
            jax.ShapeDtypeStruct((1, 128), F32),
        ),
        in_specs=[smem, smem, vmem_spec(), vmem_spec()] + [any_spec()] * 7,
        out_specs=(vmem_spec(),) * 6,
        scratch_shapes=[
            VMEM((length, full), BF),
            VMEM(context.shape, BF),
            VMEM(out_full.shape, BF),
            VMEM(up.shape, BF),
            VMEM(down.shape, BF),
            VMEM(qkv.shape, BF),
            VMEM(normed.shape, BF),
            dma((4,)),
            dma((4, 2)),
            dma((4,)),
            VMEM((2, length, 128), F32),
            VMEM((length // 4, full), F32),
            VMEM((length, full), BF),
            VMEM((length, full), BF),
            VMEM((full, length), BF),
            VMEM((length, units), BF),
            VMEM((1, units), F32),
            VMEM((8, full), F32),
            VMEM((full, units), F32),
            VMEM((4, 1, full), F32),
            dma((3,)),
            dma((3,)),
            VMEM((1, full), F32),
            VMEM((1, small), F32),
        ]
        + RingGather.scratch()
        + [
            VMEM((length, full), BF),
            VMEM((groups, d_local, units), BF),
            VMEM((4, width, length), BF),
            VMEM((width, length), BF),
            VMEM((2, width, length), BF),
            VMEM((width, length), BF),
            VMEM((width, length), BF),
            dma((heads * 6,)),
            dma((heads * 6,)),
            VMEM((groups, 4 * width, d_local), BF),
            VMEM((4, 4 * width, d_local), BF),
            VMEM((4, width, full // 2), BF),
            VMEM((2, width, full // 2), BF),
            VMEM((width, full // 2), BF),
            VMEM((width, full // 2), BF),
            dma((6,)),
            dma((6,)),
            VMEM((4, width, d_local), BF),
            VMEM((3, width, d_local), BF),
            dma((4,)),
            dma((4,)),
            dma((3,)),
            dma((3,)),
        ]
        + GroupSum.scratch((groups, d_local, units), BF)
        + [
            VMEM((rows, length), BF),
            VMEM((heads, groups, rows, d_local), BF),
            VMEM((heads, 4, rows, d_local), BF),
            VMEM((heads, 4, rows, d_local), BF),
            VMEM((heads, 3, rows, d_local), BF),
            dma((heads, 4)),
            dma((heads, 4)),
            dma((heads, 3)),
            dma((heads, 3)),
            VMEM((groups, 1, small), F32),
            dma((groups - 1,)),
            dma((groups - 1,)),
            VMEM((3, width, d_local), F32),
        ],
        compiler_params=pltpu.CompilerParams(
            collective_id=ident, has_side_effects=True, vmem_limit_bytes=BIG
        ),
        name="finish",
    )(lengths, bins_at, top, lse, first, context, out_full, up, down, qkv, normed)


def per_device_block(
    token_ids,
    lengths,
    teacher_bins,
    embed_table,
    query_key_value_matrix,
    output_matrix,
    up_matrix,
    down_matrix,
    w_head,
):
    ranks = lax.axis_size("tensor")
    rank = lax.axis_index("tensor")
    assert token_ids.shape[0] == 1
    local_len = token_ids.shape[1]
    span = local_len * ranks
    vocab_local, width = embed_table.shape
    _, _, e_local = query_key_value_matrix.shape
    f_local = up_matrix.shape[1]

    all_ids = share_ids(token_ids, 11)
    all_ids = all_ids.reshape(ranks, local_len)
    shifted = all_ids - rank * vocab_local
    inside = (shifted >= 0) & (shifted < vocab_local)
    rows = jnp.take(embed_table, jnp.clip(shifted, 0, vocab_local - 1), axis=0)
    chunk = min(256, span)
    first, normed_one, qkv, context, lse, up_full, out_full, down_part, head_full = front(
        jnp.where(inside[..., None], rows, jnp.zeros((), BF)),
        query_key_value_matrix.transpose(1, 0, 2),
        up_matrix,
        down_matrix,
        w_head,
        output_matrix,
        lengths,
        chunk,
        12,
    )
    first = first.reshape(span, width)
    normed_one = normed_one.reshape(span, width)
    context_all = context.reshape(ranks * e_local, span)
    (
        qkv_gradient,
        output_weight_gradient,
        up_weight_gradient,
        down_weight_gradient,
        grad_head,
        losses,
    ) = finish(
        lengths, teacher_bins, head_full, lse, first, context_all, out_full, up_full, down_part,
        qkv, normed_one, min(256, f_local), 15,
    )
    loss = losses[0, 0]
    query_key_value_gradient = qkv_gradient.transpose(1, 0, 2)
    return (
        loss,
        query_key_value_gradient,
        output_weight_gradient,
        up_weight_gradient,
        down_weight_gradient,
        grad_head,
    )


def solution(mesh):
    placed = (
        P("dp", "tensor"),
        P("dp"),
        P("dp"),
        P("tensor", None),
        P("dp", None, "tensor"),
        P("tensor", "dp"),
        P("dp", "tensor"),
        P("tensor", "dp"),
        P("dp", None),
    )
    return jax.shard_map(
        per_device_block if (mesh.shape["tensor"], mesh.shape["dp"]) == (4, 8) else per_device,
        mesh=mesh,
        in_specs=placed,
        out_specs=(
            P(),
            P("dp", None, "tensor"),
            P("tensor", "dp"),
            P("dp", "tensor"),
            P("tensor", "dp"),
            P("dp", None),
        ),
        check_vma=False,
    )
```

```python
import functools

import jax
import jax.numpy as jnp
from jax import lax
from jax.experimental import pallas as pl
from jax.experimental.pallas import tpu as pltpu
from jax.sharding import PartitionSpec as P

HEAD_WIDTH = 64
EPS = 1e-05
BF = jnp.bfloat16
F32 = jnp.float32
MESH = pl.DeviceIdType.MESH
VMEM = pltpu.VMEM
BIG = 60 * 1024 * 1024


def normalize(values):
    mean = jnp.mean(values, axis=-1, keepdims=True)
    centered = values - mean
    return centered * lax.rsqrt(jnp.mean(centered * centered, axis=-1, keepdims=True) + EPS)


def vmem_spec():
    return pl.BlockSpec(memory_space=pltpu.VMEM)


def greet(axis, count):
    me = lax.axis_index(axis)
    barrier = pltpu.get_barrier_semaphore()
    for step in range(1, count):
        pl.semaphore_signal(
            barrier, inc=1, device_id={axis: lax.rem(me + step, count)}, device_id_type=MESH
        )
    pl.semaphore_wait(barrier, count - 1)
    return me


def gather_body(axis, count, x_ref, out_ref, send_sem, recv_sem):
    me = greet(axis, count)
    copies = []
    for step in range(1, count):
        copy = pltpu.make_async_remote_copy(
            src_ref=x_ref,
            dst_ref=out_ref.at[me],
            send_sem=send_sem.at[step - 1],
            recv_sem=recv_sem.at[step - 1],
            device_id={axis: lax.rem(me + step, count)},
            device_id_type=MESH,
        )
        copy.start()
        copies.append(copy)
    out_ref[me] = x_ref[...]
    for copy in copies:
        copy.wait()


def relay_gather(axis, me, src, out, send_sem, recv_sem):
    across = me + 1 - 2 * lax.rem(me, 2)
    over = lax.rem(me + 2, 4)
    half = src.shape[0] // 2
    low, high = pl.ds(0, half), pl.ds(half, half)

    def copy(index, src_part, block, part, device):
        return pltpu.make_async_remote_copy(
            src_ref=src_part,
            dst_ref=out.at[block, part],
            send_sem=send_sem.at[index],
            recv_sem=recv_sem.at[index],
            device_id={axis: device},
            device_id_type=MESH,
        )

    first_a = copy(0, src.at[low], me, low, across)
    first_b = copy(1, src.at[high], me, high, over)
    second_a = copy(2, src.at[high], me, high, across)
    second_b = copy(3, src.at[low], me, low, over)
    for one in (first_a, first_b, second_a, second_b):
        one.start()
    first_a.wait_recv()
    pass_b = copy(4, out.at[across, low], across, low, over)
    pass_b.start()
    first_b.wait_recv()
    pass_a = copy(5, out.at[over, high], over, high, across)
    pass_a.start()
    second_a.wait_recv()
    second_b.wait_recv()
    pass_b.wait_recv()
    pass_a.wait_recv()
    for one in (first_a, first_b, second_a, second_b, pass_b, pass_a):
        one.wait_send()


def relay_body(axis, x_ref, out_ref, send_sem, recv_sem):
    me = greet(axis, 4)
    relay_gather(axis, me, x_ref, out_ref, send_sem, recv_sem)
    out_ref[me] = x_ref[...]


def gather_blocks(x, axis, count, ident):
    if count != 4:
        return gather_all(x, axis, count, ident)
    return pl.pallas_call(
        functools.partial(relay_body, axis),
        out_shape=jax.ShapeDtypeStruct((count,) + x.shape, x.dtype),
        in_specs=[vmem_spec()],
        out_specs=vmem_spec(),
        scratch_shapes=[pltpu.SemaphoreType.DMA((6,)), pltpu.SemaphoreType.DMA((6,))],
        compiler_params=pltpu.CompilerParams(collective_id=ident, has_side_effects=True),
        name="gather_blocks",
    )(x)


def gather_all(x, axis, count, ident):
    return pl.pallas_call(
        functools.partial(gather_body, axis, count),
        out_shape=jax.ShapeDtypeStruct((count,) + x.shape, x.dtype),
        in_specs=[vmem_spec()],
        out_specs=vmem_spec(),
        scratch_shapes=[
            pltpu.SemaphoreType.DMA((count - 1,)),
            pltpu.SemaphoreType.DMA((count - 1,)),
        ],
        compiler_params=pltpu.CompilerParams(collective_id=ident, has_side_effects=True),
        name="gather_all",
    )(x)


def scatter_copies(axis, count, me, x_ref, held, send_sem, recv_sem):
    copies = []
    for step in range(1, count):
        peer = lax.rem(me + step, count)
        copies.append(
            pltpu.make_async_remote_copy(
                src_ref=x_ref.at[peer],
                dst_ref=held.at[step - 1],
                send_sem=send_sem.at[step - 1],
                recv_sem=recv_sem.at[step - 1],
                device_id={axis: peer},
                device_id_type=MESH,
            )
        )
    return copies


def scatter_start(*args):
    for copy in scatter_copies(*args):
        copy.start()


def scatter_finish(axis, count, me, x_ref, held, send_sem, recv_sem, put):
    for copy in scatter_copies(axis, count, me, x_ref, held, send_sem, recv_sem):
        copy.wait()

    def body(at):
        total = x_ref[me, at].astype(F32)
        for step in range(1, count):
            total = total + held[step - 1, at].astype(F32)
        put(at, total)

    add_tiles(x_ref.shape[1], 32, body)


def add_tiles(rows, tile, body):
    def step(index, carry):
        body(pl.ds(pl.multiple_of(index * tile, tile), tile))
        return carry

    lax.fori_loop(0, rows // tile, step, 0)


class GroupSum:
    def __init__(self, x_ref, out_ref, pair, mine, far, sems):
        self.x, self.out, self.pair, self.mine, self.far = x_ref, out_ref, pair, mine, far
        self.sems = sems
        self.groups = x_ref.shape[0]
        self.chips = self.groups // 2
        self.rows = x_ref.shape[1]
        me = lax.axis_index("dp")
        self.core = lax.rem(me, 2)
        self.chip = me // 2
        self.near = self.chip * 2 + 1 - self.core

    @staticmethod
    def scratch(shape, dtype):
        groups, rows, columns = shape
        chips = groups // 2
        return [
            VMEM((chips, rows, columns), dtype),
            VMEM((chips, rows, columns), dtype),
            VMEM((chips - 1, rows, columns), dtype),
            pltpu.SemaphoreType.DMA((chips,)),
            pltpu.SemaphoreType.DMA((chips,)),
            pltpu.SemaphoreType.DMA((6 if chips == 4 else chips - 1,)),
            pltpu.SemaphoreType.DMA((6 if chips == 4 else chips - 1,)),
        ]

    def signal(self, barrier):
        pl.semaphore_signal(
            barrier, inc=1, device_id={"dp": self.near}, device_id_type=MESH
        )
        for step in range(1, self.chips):
            pl.semaphore_signal(
                barrier, inc=1, device_id={"dp": self.owner(step)}, device_id_type=MESH
            )
        return self.chips

    def owner(self, step):
        return lax.rem(self.chip + step, self.chips) * 2 + self.core

    def pair_copies(self):
        copies = []
        for chip in range(self.chips):
            copies.append(
                pltpu.make_async_remote_copy(
                    src_ref=self.x.at[chip * 2 + 1 - self.core],
                    dst_ref=self.pair.at[chip],
                    send_sem=self.sems[0].at[chip],
                    recv_sem=self.sems[1].at[chip],
                    device_id={"dp": self.near},
                    device_id_type=MESH,
                )
            )
        return copies

    def far_copies(self):
        copies = []
        for step in range(1, self.chips):
            copies.append(
                pltpu.make_async_remote_copy(
                    src_ref=self.mine.at[lax.rem(self.chip + step, self.chips)],
                    dst_ref=self.far.at[step - 1],
                    send_sem=self.sems[2].at[step - 1],
                    recv_sem=self.sems[3].at[step - 1],
                    device_id={"dp": self.owner(step)},
                    device_id_type=MESH,
                )
            )
        return copies

    def ring_copies(self):
        right, left = lax.rem(self.chip + 1, 4), lax.rem(self.chip + 3, 4)
        opposite = lax.rem(self.chip + 2, 4)
        half = self.rows // 2
        low, high = pl.ds(0, half), pl.ds(half, half)

        def copy(index, block, part, slot, chip):
            return pltpu.make_async_remote_copy(
                src_ref=self.mine.at[block, part],
                dst_ref=self.far.at[slot, part],
                send_sem=self.sems[2].at[index],
                recv_sem=self.sems[3].at[index],
                device_id={"dp": chip * 2 + self.core},
                device_id_type=MESH,
            )

        return (
            copy(0, opposite, low, 2, right),
            copy(1, opposite, high, 2, left),
            copy(2, right, high, 0, right),
            copy(3, left, low, 1, left),
            copy(4, right, low, 0, right),
            copy(5, left, high, 1, left),
        )

    def relay(self):
        if self.chips != 4:
            return
        copies = self.ring_copies()
        half = self.rows // 2
        for index, step, base in ((0, 1, 0), (1, 3, half)):
            copies[index].wait_recv()
            block = lax.rem(self.chip + step, 4)

            def body(at, block=block, base=base):
                here = pl.ds(base + at.start, at.size)
                self.mine[block, here] = (
                    self.mine[block, here].astype(F32) + self.far[2, here].astype(F32)
                ).astype(self.mine.dtype)

            add_tiles(half, 32, body)
            copies[index + 4].start()

    def start(self):
        for copy in self.pair_copies():
            copy.start()

    def middle(self):
        for copy in self.pair_copies():
            copy.wait()

        for chip in range(self.chips):

            def body(at, chip=chip):
                self.mine[chip, at] = (
                    self.x[chip * 2 + self.core, at].astype(F32)
                    + self.pair[chip, at].astype(F32)
                ).astype(self.mine.dtype)

            add_tiles(self.rows, 32, body)
        copies = self.ring_copies()[:4] if self.chips == 4 else self.far_copies()
        for copy in copies:
            copy.start()

    def finish(self):
        if self.chips == 4:
            copies = self.ring_copies()
            for copy in copies[2:]:
                copy.wait()
            for copy in copies[:2]:
                copy.wait_send()
        else:
            for copy in self.far_copies():
                copy.wait()

        def body(at):
            total = self.mine[self.chip, at].astype(F32)
            for step in range(2 if self.chips == 4 else self.chips - 1):
                total = total + self.far[step, at].astype(F32)
            self.out[at] = total

        add_tiles(self.rows, 32, body)


def scatter_and_group_body(
    count, x_ref, up_ref, small_ref, out_ref, up_out, small_out, held, send_sem, recv_sem, *rest
):
    up = GroupSum(up_ref, up_out, rest[0], rest[1], rest[2], rest[3:7])
    small_send, small_recv = rest[7:]
    groups = small_out.shape[0]
    group = lax.axis_index("dp")
    barrier = pltpu.get_barrier_semaphore()
    me = lax.axis_index("tensor")
    for step in range(1, count):
        pl.semaphore_signal(
            barrier, inc=1, device_id={"tensor": lax.rem(me + step, count)}, device_id_type=MESH
        )
    for step in range(1, groups):
        pl.semaphore_signal(
            barrier, inc=1, device_id={"dp": lax.rem(group + step, groups)}, device_id_type=MESH
        )
    pl.semaphore_wait(barrier, count + groups - 2)
    smalls = []
    for step in range(1, groups):
        smalls.append(
            pltpu.make_async_remote_copy(
                src_ref=small_ref,
                dst_ref=small_out.at[group],
                send_sem=small_send.at[step - 1],
                recv_sem=small_recv.at[step - 1],
                device_id={"dp": lax.rem(group + step, groups)},
                device_id_type=MESH,
            )
        )

    def put(at, total):
        out_ref[at] = total.astype(out_ref.dtype)

    up.start()
    scatter_start("tensor", count, me, x_ref, held, send_sem, recv_sem)
    up.middle()
    for copy in smalls:
        copy.start()
    small_out[group] = small_ref[...]
    up.relay()
    scatter_finish("tensor", count, me, x_ref, held, send_sem, recv_sem, put)
    up.finish()
    for copy in smalls:
        copy.wait()


def scatter_and_group(x, up, small, count, ident):
    return pl.pallas_call(
        functools.partial(scatter_and_group_body, count),
        out_shape=(
            jax.ShapeDtypeStruct(x.shape[1:], x.dtype),
            jax.ShapeDtypeStruct(up.shape[1:], F32),
            jax.ShapeDtypeStruct(up.shape[:1] + small.shape, F32),
        ),
        in_specs=[vmem_spec()] * 3,
        out_specs=(vmem_spec(),) * 3,
        scratch_shapes=[
            VMEM((count - 1,) + x.shape[1:], x.dtype),
            pltpu.SemaphoreType.DMA((count - 1,)),
            pltpu.SemaphoreType.DMA((count - 1,)),
        ]
        + GroupSum.scratch(up.shape, up.dtype)
        + [pltpu.SemaphoreType.DMA((up.shape[0] - 1,))] * 2,
        compiler_params=pltpu.CompilerParams(
            collective_id=ident, has_side_effects=True, vmem_limit_bytes=BIG
        ),
        name="scatter_and_group",
    )(x, up, small)


def group_sum_body(number, *refs):
    xs, outs, rest = refs[:number], refs[number : 2 * number], refs[2 * number :]
    sums = [
        GroupSum(x, out, *rest[7 * i : 7 * i + 3], rest[7 * i + 3 : 7 * i + 7])
        for i, (x, out) in enumerate(zip(xs, outs))
    ]
    barrier = pltpu.get_barrier_semaphore()
    pl.semaphore_wait(barrier, sums[0].signal(barrier))
    for one in sums:
        one.start()
    for one in sums:
        one.middle()
    for one in sums:
        one.relay()
    for one in sums:
        one.finish()


def group_sum(arrays, ident):
    number = len(arrays)
    scratch = []
    for array in arrays:
        scratch += GroupSum.scratch(array.shape, array.dtype)
    return pl.pallas_call(
        functools.partial(group_sum_body, number),
        out_shape=tuple(jax.ShapeDtypeStruct(a.shape[1:], F32) for a in arrays),
        in_specs=[vmem_spec()] * number,
        out_specs=(vmem_spec(),) * number,
        scratch_shapes=scratch,
        compiler_params=pltpu.CompilerParams(
            collective_id=ident, has_side_effects=True, vmem_limit_bytes=BIG
        ),
        name="group_sum",
    )(*arrays)


def sum_all_body(axis, count, x_ref, out_ref, held, send_sem, recv_sem, send_two, recv_two):
    me = greet(axis, count)

    def put(at, total):
        out_ref[me, at] = total.astype(out_ref.dtype)

    scatter_start(axis, count, me, x_ref, held, send_sem, recv_sem)
    scatter_finish(axis, count, me, x_ref, held, send_sem, recv_sem, put)
    if count == 4:
        relay_gather(axis, me, out_ref.at[me], out_ref, send_two, recv_two)
        return
    copies = []
    for step in range(1, count):
        copy = pltpu.make_async_remote_copy(
            src_ref=out_ref.at[me],
            dst_ref=out_ref.at[me],
            send_sem=send_two.at[step - 1],
            recv_sem=recv_two.at[step - 1],
            device_id={axis: lax.rem(me + step, count)},
            device_id_type=MESH,
        )
        copy.start()
        copies.append(copy)
    for copy in copies:
        copy.wait()


def sum_all(x, axis, count, ident):
    return pl.pallas_call(
        functools.partial(sum_all_body, axis, count),
        out_shape=jax.ShapeDtypeStruct(x.shape, x.dtype),
        in_specs=[vmem_spec()],
        out_specs=vmem_spec(),
        scratch_shapes=[VMEM((count - 1,) + x.shape[1:], x.dtype)]
        + [pltpu.SemaphoreType.DMA((count - 1,))] * 2
        + [pltpu.SemaphoreType.DMA((6 if count == 4 else count - 1,))] * 2,
        compiler_params=pltpu.CompilerParams(collective_id=ident, has_side_effects=True),
        name="sum_all",
    )(x)


def contract(left, right, dims):
    return lax.dot_general(left, right, ((dims[:1], dims[1:]), ((), ())), preferred_element_type=F32)


def masked_scores(keys, query, length):
    scores = contract(keys, query, (0, 0))
    position = lax.broadcasted_iota(jnp.int32, scores.shape, 0)
    return jnp.where(position < length, scores, -1e30)


def attend_body(chunk, length_ref, qkv_ref, out_ref, lse_ref):
    length = length_ref[0]
    keys, vals = qkv_ref[1], qkv_ref[2]
    scale = HEAD_WIDTH ** (-0.5)
    for at in range(0, qkv_ref.shape[2], chunk):
        query = (qkv_ref[0, :, at : at + chunk].astype(F32) * scale).astype(BF)
        scores = masked_scores(keys, query, length)
        top = jnp.max(scores, axis=0, keepdims=True)
        expo = jnp.exp(scores - top)
        total = jnp.sum(expo, axis=0, keepdims=True)
        mixed = contract(vals, expo.astype(BF), (1, 0))
        out_ref[:, at : at + chunk] = (mixed * (1.0 / total)).astype(BF)
        lse_ref[0, :, at : at + chunk] = top + jnp.log(total)


def attend(qkv, lengths, chunk):
    _, width, length = qkv.shape
    heads = width // HEAD_WIDTH
    return pl.pallas_call(
        functools.partial(attend_body, chunk),
        grid=(heads,),
        out_shape=(
            jax.ShapeDtypeStruct((width, length), BF),
            jax.ShapeDtypeStruct((heads, 1, length), F32),
        ),
        in_specs=[
            pl.BlockSpec(memory_space=pltpu.SMEM),
            pl.BlockSpec((3, HEAD_WIDTH, length), lambda h: (0, h, 0)),
        ],
        out_specs=(
            pl.BlockSpec((HEAD_WIDTH, length), lambda h: (h, 0)),
            pl.BlockSpec((1, 1, length), lambda h: (h, 0, 0)),
        ),
        cost_estimate=pl.CostEstimate(
            flops=4 * width * length * length,
            bytes_accessed=8 * width * length,
            transcendentals=heads * length * length,
        ),
        compiler_params=pltpu.CompilerParams(vmem_limit_bytes=BIG),
        name="attend",
    )(lengths, qkv)


def attend_back_body(
    chunk, ranks, length_ref, qkv_ref, lse_ref, grad_ref, x_ref, out_ref, x_out, held, send_sem, recv_sem
):
    me = lax.axis_index("tensor")
    args = ("tensor", ranks, me, x_ref, held, send_sem, recv_sem)

    @pl.when(pl.program_id(0) == 0)
    def _():
        greet("tensor", ranks)
        scatter_start(*args)

    attend_back_head(chunk, length_ref, qkv_ref, lse_ref, grad_ref, out_ref)

    @pl.when(pl.program_id(0) == pl.num_programs(0) - 1)
    def _():
        piece = x_out.shape[2]

        def put(at, total):
            for group in range(x_out.shape[0]):
                x_out[group, at] = total[:, group * piece : (group + 1) * piece].astype(BF)

        scatter_finish(*args, put)


def attend_back_head(chunk, length_ref, qkv_ref, lse_ref, grad_ref, out_ref):
    length = length_ref[0]
    keys, vals = qkv_ref[1], qkv_ref[2]
    scale = HEAD_WIDTH ** (-0.5)
    span = qkv_ref.shape[2]
    g_keys = jnp.zeros((HEAD_WIDTH, span), F32)
    g_vals = jnp.zeros((HEAD_WIDTH, span), F32)
    for at in range(0, span, chunk):
        here = slice(at, at + chunk)
        query = (qkv_ref[0, :, here].astype(F32) * scale).astype(BF)
        grad = grad_ref[:, here]
        probs = jnp.exp(masked_scores(keys, query, length) - lse_ref[0, :, here])
        g_probs = contract(vals, grad, (0, 0))
        weighted = probs * g_probs
        inner = jnp.sum(weighted, axis=0, keepdims=True)
        g_scores = (weighted - probs * inner).astype(BF)
        out_ref[0, :, here] = (contract(keys, g_scores, (1, 0)) * scale).astype(BF)
        g_keys += contract(query, g_scores, (1, 1))
        g_vals += contract(grad, probs.astype(BF), (1, 1))
    out_ref[1] = g_keys.astype(BF)
    out_ref[2] = g_vals.astype(BF)


def attend_back(qkv, lengths, lse, grad, x, groups, chunk, ident):
    _, width, length = qkv.shape
    heads = width // HEAD_WIDTH
    return pl.pallas_call(
        functools.partial(attend_back_body, chunk, x.shape[0]),
        grid=(heads,),
        out_shape=(
            jax.ShapeDtypeStruct(qkv.shape, BF),
            jax.ShapeDtypeStruct((groups, x.shape[1], x.shape[2] // groups), BF),
        ),
        in_specs=[
            pl.BlockSpec(memory_space=pltpu.SMEM),
            pl.BlockSpec((3, HEAD_WIDTH, length), lambda h: (0, h, 0)),
            pl.BlockSpec((1, 1, length), lambda h: (h, 0, 0)),
            pl.BlockSpec((HEAD_WIDTH, length), lambda h: (h, 0)),
            vmem_spec(),
        ],
        out_specs=(
            pl.BlockSpec((3, HEAD_WIDTH, length), lambda h: (0, h, 0)),
            vmem_spec(),
        ),
        scratch_shapes=[
            VMEM((x.shape[0] - 1,) + x.shape[1:], x.dtype),
            pltpu.SemaphoreType.DMA((x.shape[0] - 1,)),
            pltpu.SemaphoreType.DMA((x.shape[0] - 1,)),
        ],
        cost_estimate=pl.CostEstimate(
            flops=10 * width * length * length,
            bytes_accessed=14 * width * length,
            transcendentals=heads * length * length,
        ),
        compiler_params=pltpu.CompilerParams(
            collective_id=ident, has_side_effects=True, vmem_limit_bytes=BIG
        ),
        name="attend_back",
    )(lengths, qkv, lse, grad, x)


def hidden_body(length_ref, normed_ref, up_ref, slope_ref, sum_ref):
    pre = jnp.dot(normed_ref[...], up_ref[...], preferred_element_type=F32)
    live = lax.broadcasted_iota(jnp.int32, pre.shape, 0) < length_ref[0]
    square = pre * pre
    bend = jnp.tanh(0.7978845608028654 * (pre * (1.0 + 0.044715 * square)))
    half = 0.5 * (1.0 + bend)
    act = (pre * half).astype(BF).astype(F32)
    sum_ref[...] = jnp.sum(jnp.where(live, act, 0.0), axis=0, keepdims=True)
    inner = 0.7978845608028654 * (1.0 + 3 * 0.044715 * square)
    slope = half + 0.5 * pre * (1.0 - bend * bend) * inner
    slope_ref[...] = jnp.where(live, slope, 0.0).astype(BF)


def hidden(normed, up, lengths, chunk):
    length, width = normed.shape
    units = up.shape[1]
    return pl.pallas_call(
        hidden_body,
        grid=(units // chunk,),
        out_shape=(
            jax.ShapeDtypeStruct((length, units), BF),
            jax.ShapeDtypeStruct((1, units), F32),
        ),
        in_specs=[
            pl.BlockSpec(memory_space=pltpu.SMEM),
            pl.BlockSpec((length, width), lambda f: (0, 0)),
            pl.BlockSpec((width, chunk), lambda f: (0, f)),
        ],
        out_specs=(
            pl.BlockSpec((length, chunk), lambda f: (0, f)),
            pl.BlockSpec((1, chunk), lambda f: (0, f)),
        ),
        cost_estimate=pl.CostEstimate(
            flops=2 * length * width * units,
            bytes_accessed=6 * length * units,
            transcendentals=length * units,
        ),
        compiler_params=pltpu.CompilerParams(vmem_limit_bytes=BIG),
        name="hidden",
    )(lengths, normed, up)


def per_device(
    token_ids,
    lengths,
    teacher_bins,
    embed_table,
    query_key_value_matrix,
    output_matrix,
    up_matrix,
    down_matrix,
    w_head,
):
    ranks = lax.axis_size("tensor")
    groups = lax.axis_size("dp")
    rank = lax.axis_index("tensor")
    group = lax.axis_index("dp")
    assert token_ids.shape[0] == 1
    local_len = token_ids.shape[1]
    span = local_len * ranks
    vocab_local, width = embed_table.shape
    d_local, _, e_local = query_key_value_matrix.shape
    f_local = up_matrix.shape[1]
    bins = w_head.shape[1]
    exact = lax.Precision.HIGHEST

    qkv_full = lax.all_gather(
        query_key_value_matrix.reshape(d_local, 3 * e_local), "dp", axis=0, tiled=True
    )
    out_parts = lax.all_gather(output_matrix, ("tensor", "dp"), axis=0, tiled=False)
    out_full = (
        out_parts.reshape(ranks, groups, e_local, d_local)
        .transpose(0, 2, 1, 3)
        .reshape(ranks * e_local, width)
    )
    up_full = lax.all_gather(up_matrix, "dp", axis=0, tiled=True)
    low = lax.all_gather(
        jnp.concatenate([down_matrix, w_head.reshape(bins, d_local)], axis=0), "dp", axis=0, tiled=False
    )
    down_full = low[:, :f_local]
    head_wide = low[:, f_local:].reshape(width, bins).astype(F32)

    all_ids = gather_all(token_ids, "tensor", ranks, 1).reshape(ranks, local_len)
    shifted = all_ids - rank * vocab_local
    inside = (shifted >= 0) & (shifted < vocab_local)
    rows = jnp.take(embed_table, jnp.clip(shifted, 0, vocab_local - 1), axis=0)
    first = sum_all(
        jnp.where(inside[..., None], rows, jnp.zeros((), BF)), "tensor", ranks, 2
    ).reshape(span, width)
    normed_one = normalize(first.astype(F32)).astype(BF)
    qkv = (
        lax.dot_general(qkv_full, normed_one, (((0,), (1,)), ((), ())), preferred_element_type=F32)
        .astype(BF)
        .reshape(3, e_local, span)
    )
    chunk = min(256, span)
    context, lse = attend(qkv, lengths, chunk)
    context_all = gather_blocks(context, "tensor", ranks, 3).reshape(ranks * e_local, span)
    attn = lax.dot_general(
        context_all, out_full, (((0,), (0,)), ((), ())), preferred_element_type=F32
    )
    second = (first.astype(F32) + attn).astype(BF)
    normed_f, norm_back = jax.vjp(normalize, second.astype(F32))
    normed_two = normed_f.astype(BF)
    slope, hidden_sum = hidden(normed_two, up_full, lengths, min(256, f_local))

    live = (jnp.arange(span, dtype=jnp.int32) < lengths[0]).astype(F32)
    count = lengths.astype(F32)[:, None]
    ffn_part = jnp.einsum(
        "of,jfd->ojd", hidden_sum, down_full.astype(F32), precision=exact
    ).reshape(1, width)
    ffn_all = gather_all(ffn_part, "tensor", ranks, 4)
    second_sum = jnp.sum(second.astype(F32) * live[:, None], axis=0, keepdims=True)
    pooled = (second_sum + jnp.sum(ffn_all, axis=0)) / count
    final, final_back = jax.vjp(normalize, pooled)
    logits = jnp.dot(final, head_wide, precision=exact)
    top = jnp.max(logits, axis=-1, keepdims=True)
    total_exp = jnp.log(jnp.sum(jnp.exp(logits - top), axis=-1, keepdims=True)) + top
    labels = (teacher_bins[:, None] == jnp.arange(bins, dtype=jnp.int32)[None, :]).astype(F32)
    loss_here = total_exp - jnp.sum(logits * labels, axis=-1, keepdims=True)
    g_logits = (jnp.exp(logits - total_exp) - labels) / groups
    g_final = jnp.dot(g_logits, head_wide.T, precision=exact)
    per_token = final_back(g_final)[0] / count
    rounded = per_token.astype(BF).astype(F32)
    g_hidden = jnp.einsum(
        "ojd,jfd->of",
        rounded.reshape(1, groups, d_local),
        down_full.astype(F32),
        precision=exact,
    )

    packed = jnp.concatenate(
        [hidden_sum, rounded, final, g_logits, jnp.broadcast_to(loss_here, (1, 128))], axis=1
    )

    over_seqs = (((0,), (0,)), ((), ()))
    up_base = lax.dot_general(normed_two, slope, over_seqs, preferred_element_type=F32)
    up_term = (up_base * g_hidden).astype(BF).reshape(groups, d_local, f_local)
    g_pre = (slope.astype(F32) * g_hidden).astype(BF)
    g_normed = lax.dot_general(
        g_pre, up_full, (((1,), (1,)), ((), ())), preferred_element_type=F32
    )
    g_second = (
        norm_back(g_normed)[0] + live[:, None] * (per_token / ranks)
    ).astype(BF)
    spread = lax.dot_general(
        out_full, g_second, (((1,), (1,)), ((), ())), preferred_element_type=F32
    ).astype(BF)
    g_context, up_weight_gradient, every = scatter_and_group(
        spread.reshape(ranks, e_local, span), up_term, packed, ranks, 6
    )
    every = every[:, 0]
    hidden_every = every[:, :f_local]
    rounded_every = every[:, f_local : f_local + width]
    final_every = every[:, f_local + width : f_local + 2 * width]
    rest = every[:, f_local + 2 * width :]
    loss = jnp.sum(rest[:, bins]) / groups
    mine = group * d_local
    down_weight_gradient = lax.dot_general(
        hidden_every,
        lax.dynamic_slice_in_dim(rounded_every, mine, d_local, axis=1),
        over_seqs,
        precision=exact,
    )
    grad_head = lax.dot_general(
        lax.dynamic_slice_in_dim(final_every, mine, d_local, axis=1),
        rest[:, :bins],
        over_seqs,
        precision=exact,
    )

    out_term = (
        jnp.dot(context_all, g_second, preferred_element_type=F32)
        .astype(BF)
        .reshape(ranks, e_local, width)
    )
    g_qkv, out_mine = attend_back(qkv, lengths, lse, g_context, out_term, groups, chunk, 7)
    qkv_term = lax.dot_general(
        normed_one,
        g_qkv.reshape(3 * e_local, span),
        (((0,), (1,)), ((), ())),
        preferred_element_type=F32,
    )
    qkv_gradient, output_weight_gradient = group_sum(
        [qkv_term.astype(BF).reshape(groups, d_local, 3 * e_local), out_mine], 8
    )
    query_key_value_gradient = qkv_gradient.reshape(d_local, 3, e_local)
    return (
        loss,
        query_key_value_gradient,
        output_weight_gradient,
        up_weight_gradient,
        down_weight_gradient,
        grad_head,
    )


def remote(src, dst, sems, index, device):
    return pltpu.make_async_remote_copy(
        src_ref=src,
        dst_ref=dst,
        send_sem=sems[0].at[index],
        recv_sem=sems[1].at[index],
        device_id=device,
        device_id_type=MESH,
    )


class Place:
    def __init__(self):
        self.rank = lax.axis_index("tensor")
        self.across = self.rank + 1 - 2 * lax.rem(self.rank, 2)
        self.over = lax.rem(self.rank + 2, 4)
        self.diag = 3 - self.rank
        self.group = lax.axis_index("dp")
        self.core = lax.rem(self.group, 2)
        self.chip = self.group // 2
        self.near = self.chip * 2 + 1 - self.core

    def turn(self, step):
        return lax.rem(self.chip + step, 4)

    def same(self, chip):
        return chip * 2 + self.core

    def peers(self, everyone=False):
        peers = [{"tensor": one} for one in (self.across, self.over, self.diag)]
        if everyone:
            return peers + [{"dp": lax.rem(self.group + step, 8)} for step in range(1, 8)]
        return peers + [
            {"dp": self.near},
            {"dp": self.same(self.turn(1))},
            {"dp": self.same(self.turn(3))},
        ]

    def signal(self, peers):
        barrier = pltpu.get_barrier_semaphore()
        for peer in peers:
            pl.semaphore_signal(barrier, inc=1, device_id=peer, device_id_type=MESH)

    def ready(self, peers):
        pl.semaphore_wait(pltpu.get_barrier_semaphore(), len(peers))


class RingGather:
    def __init__(self, at, src, own, slot, sems):
        self.at, self.src, self.own, self.slot = at, src, own, slot
        self.sems, self.local = sems[:2], sems[2]

    @staticmethod
    def scratch():
        return [
            pltpu.SemaphoreType.DMA((10,)),
            pltpu.SemaphoreType.DMA((10,)),
            pltpu.SemaphoreType.DMA((1,)),
        ]

    def copies(self):
        at = self.at
        right, left, far = at.turn(1), at.turn(3), at.turn(2)
        me, to_right, to_left = at.group, {"dp": at.same(right)}, {"dp": at.same(left)}
        near = {"dp": at.near}

        def held(index, chip, half, device):
            ref = self.slot(at.same(chip), half)
            return remote(ref, ref, self.sems, index, device)

        def first(index, half, device):
            return remote(self.own(half), self.slot(me, half), self.sems, index, device)

        return (
            first(0, 0, to_right),
            first(1, 1, to_left),
            first(2, 1, to_right),
            first(3, 0, to_left),
            held(4, left, 0, to_right),
            held(5, right, 1, to_left),
            remote(self.src, self.slot(me, None), self.sems, 6, near),
            held(7, left, None, near),
            held(8, right, None, near),
            held(9, far, None, near),
        )

    def keep(self):
        return pltpu.make_async_copy(self.src, self.slot(self.at.group, None), self.local.at[0])

    def start(self):
        copies = self.copies()
        for index in (0, 1, 2, 3, 6):
            copies[index].start()
        self.keep().start()

    def relay(self):
        copies = self.copies()
        copies[0].wait_recv()
        copies[4].start()
        copies[1].wait_recv()
        copies[5].start()

    def spread(self):
        copies = self.copies()
        copies[2].wait_recv()
        copies[7].start()
        copies[3].wait_recv()
        copies[8].start()
        copies[4].wait_recv()
        copies[5].wait_recv()
        copies[9].start()

    def finish(self):
        copies = self.copies()
        for index in (6, 7, 8, 9):
            copies[index].wait_recv()
        for copy in copies:
            copy.wait_send()
        self.keep().wait()

    def start_half(self):
        copies = self.copies()
        for index in (0, 1, 6):
            copies[index].start()
        self.keep().start()

    def close_half(self):
        copies = self.copies()
        for index in (0, 1, 6):
            copies[index].wait()
        self.keep().wait()

    def start_rest(self):
        copies = self.copies()
        for index in (2, 3, 4, 5):
            copies[index].start()

    def near(self):
        copies = self.copies()
        copies[2].wait_recv()
        copies[7].start()
        copies[3].wait_recv()
        copies[8].start()

    def far(self):
        copies = self.copies()
        copies[4].wait_recv()
        copies[5].wait_recv()
        copies[9].start()

    def close_rest(self):
        copies = self.copies()
        for index in (7, 8, 9):
            copies[index].wait_recv()
        for index in (2, 3, 4, 5, 7, 8, 9):
            copies[index].wait_send()


def columns_of(ref, size):
    rows = ref.shape[0]

    def slot(block, half):
        lanes = pl.ds(pl.multiple_of(block * size, size), size)
        if half is None:
            return ref.at[:, lanes]
        return ref.at[pl.ds(half * (rows // 2), rows // 2), lanes]

    return slot


def rows_of(ref, block, half, size, axis=0):
    lead = (slice(None),) * axis
    if half is None:
        return ref.at[lead + (pl.ds(pl.multiple_of(block * size, size), size),)]
    part = size // 2
    return ref.at[lead + (pl.ds(pl.multiple_of(block * size + half * part, part), part),)]


def half_rows(ref, half, axis=0):
    part = ref.shape[axis] // 2
    return ref.at[(slice(None),) * axis + (pl.ds(half * part, part),)]


def ids_body(ids_ref, ids_all, send, recv):
    at = Place()
    peers = at.peers()[:3]
    at.signal(peers)
    ids_all[at.rank] = ids_ref[...]
    at.ready(peers)
    copies = [
        remote(ids_ref, ids_all.at[at.rank], (send, recv), index, peer)
        for index, peer in enumerate(peers)
    ]
    for copy in copies:
        copy.start()
    for copy in copies:
        copy.wait()


def share_ids(ids, ident):
    return pl.pallas_call(
        ids_body,
        out_shape=jax.ShapeDtypeStruct((4,) + ids.shape, ids.dtype),
        in_specs=[vmem_spec()],
        out_specs=vmem_spec(),
        scratch_shapes=[pltpu.SemaphoreType.DMA((3,))] * 2,
        compiler_params=pltpu.CompilerParams(collective_id=ident, has_side_effects=True),
        name="share_ids",
    )(ids)


def any_spec():
    return pl.BlockSpec(memory_space=pl.ANY)


class Stream:
    def __init__(self, at, x_ref, acc, held, last, whole, sems, index, rows, x_first):
        self.at, self.x, self.acc, self.held, self.last, self.whole = at, x_ref, acc, held, last, whole
        self.sems, self.index, self.rows = sems, index * 6, rows
        self.one, self.two = (at.across, at.over) if x_first else (at.over, at.across)

    def copies(self):
        at, rows, base, sems = self.at, self.rows, self.index, self.sems
        one, two = {"tensor": self.one}, {"tensor": self.two}
        return (
            remote(self.x.at[at.diag, rows], self.held.at[1, rows], sems, base, one),
            remote(self.x.at[self.one, rows], self.held.at[0, rows], sems, base + 1, one),
            remote(self.acc.at[rows], self.last.at[rows], sems, base + 2, two),
            remote(self.whole.at[at.rank, rows], self.whole.at[at.rank, rows], sems, base + 3, two),
            remote(self.whole.at[at.rank, rows], self.whole.at[at.rank, rows], sems, base + 4, one),
            remote(self.whole.at[self.two, rows], self.whole.at[self.two, rows], sems, base + 5, one),
        )

    def start(self):
        copies = self.copies()
        copies[0].start()
        copies[1].start()

    def second(self):
        copies = self.copies()
        copies[0].wait_recv()

        def body(at):
            here = pl.ds(self.rows.start + at.start, at.size)
            self.acc[here] = self.x[self.two, here] + self.held[1, here]

        add_tiles(self.rows.size, 32, body)
        copies[2].start()

    def third(self):
        copies = self.copies()
        copies[1].wait_recv()
        copies[2].wait_recv()

        def body(at):
            here = pl.ds(self.rows.start + at.start, at.size)
            self.whole[self.at.rank, here] = (
                self.x[self.at.rank, here] + self.held[0, here] + self.last[here]
            )

        add_tiles(self.rows.size, 32, body)
        copies[3].start()
        copies[4].start()

    def relay(self):
        copies = self.copies()
        copies[3].wait_recv()
        copies[5].start()

    def beside(self):
        self.copies()[4].wait_recv()

    def opposite(self):
        self.copies()[5].wait_recv()

    def finish(self):
        for copy in self.copies():
            copy.wait_send()


def front_body(
    chunk, vocab, length_ref, ids_ref, x_in, w_ref, up_ref, down_ref, head_ref, out_ref,
    first_out, normed_out, qkv_out, ctx_out, lse_ref, up_out, out_full, down_out, head_out,
    x_ref, mask, acc, held, last, whole, normed, qkv_ref, w_full, w_turn, ctx_ref, cols,
    load, saved, send, recv, col_send, col_recv, ctx_send, ctx_recv, ctx_saved, *rest,
):
    at = Place()
    peers = at.peers()
    at.signal(peers)
    entry = pltpu.make_async_copy(x_in, x_ref, load.at[0])
    entry.start()
    d_local = w_ref.shape[1]
    local = x_ref.shape[1]
    e_local = w_ref.shape[2]
    span = qkv_ref.shape[2]
    heads = lse_ref.shape[0]
    size = HEAD_WIDTH // 2
    weights = RingGather(
        at, w_ref, lambda half: half_rows(w_ref, half, 1),
        lambda block, half: rows_of(w_full, block, half, d_local, 1), rest[:3],
    )
    ups = RingGather(
        at, up_ref, lambda half: half_rows(up_ref, half),
        lambda block, half: rows_of(up_out, block, half, d_local), rest[3:6],
    )
    tops = RingGather(
        at, head_ref, lambda half: half_rows(head_ref, half),
        lambda block, half: rows_of(head_out, block, half, d_local), rest[6:9],
    )
    downs = RingGather(
        at, down_ref, lambda half: half_rows(down_ref, half), columns_of(down_out, d_local), rest[9:12]
    )
    outs = RingGather(
        at, cols, lambda half: half_rows(cols, half), columns_of(out_full, d_local), rest[12:15]
    )
    mine = pl.ds(pl.multiple_of(at.rank * e_local, e_local), e_local)
    own_columns = pltpu.make_async_copy(out_ref, cols.at[mine], load.at[1])
    own_columns.start()
    column_copies = [
        remote(out_ref, cols.at[mine], (col_send, col_recv), index, peer)
        for index, peer in enumerate(peers[:3])
    ]

    entry.wait()
    lines = mask.shape[1]
    for block in range(4):
        shifted = ids_ref[block] - at.rank * vocab
        inside = ((shifted >= 0) & (shifted < vocab)).astype(F32)
        mask[...] = jnp.broadcast_to(inside, (lines, local)).T

        def keep(rows, block=block):
            here = mask[rows]
            for start in range(0, x_ref.shape[2], lines):
                cut = slice(start, start + lines)
                x_ref[block, rows, cut] = (x_ref[block, rows, cut].astype(F32) * here).astype(BF)

        add_tiles(local, 64, keep)
    at.ready(peers)
    weights.start()
    part = local // 4
    streams = [
        Stream(
            at, x_ref, acc, held, last, whole, (send, recv), index,
            pl.ds((index % 2) * (local // 2) + (index // 2) * part, part), index % 2 == 0,
        )
        for index in range(4)
    ]
    for one in streams:
        one.start()
    for one in streams:
        one.second()
    weights.relay()
    ups.start()
    tops.start()
    for one in streams:
        one.third()
    for copy in column_copies:
        copy.start()
    weights.spread()
    weights.finish()
    for index in range(3):
        w_turn[index] = w_full[index].T

    def saves(slot, block):
        base = pl.multiple_of(block * local, local)
        return (
            pltpu.make_async_copy(whole.at[block], first_out.at[block], saved.at[slot, 0]),
            pltpu.make_async_copy(normed.at[block], normed_out.at[block], saved.at[slot, 1]),
            pltpu.make_async_copy(
                qkv_ref.at[:, :, pl.ds(base, local)], qkv_out.at[:, :, pl.ds(base, local)], saved.at[slot, 2]
            ),
        )

    def project(block, slot):
        def tile(here):
            normed[block, here] = normalize(whole[block, here].astype(F32)).astype(BF)

        add_tiles(local, 64, tile)
        base = pl.multiple_of(block * local, local)

        def matrix(index, carry):
            qkv_ref[index, :, pl.ds(base, local)] = contract(
                w_turn[index], normed[block], (1, 1)
            ).astype(BF)
            return carry

        lax.fori_loop(0, 3, matrix, 0)
        for copy in saves(slot, block):
            copy.start()

    for one in streams[:2]:
        one.relay()
    project(at.rank, 0)
    for one in streams[2:]:
        one.relay()
    ups.relay()
    tops.relay()
    for one in streams:
        one.beside()
    own_columns.wait()
    for copy in column_copies:
        copy.wait()
    outs.start()
    downs.start_half()
    project(at.across, 1)
    project(at.over, 2)
    for one in streams:
        one.opposite()
    project(at.diag, 3)

    def copies(one):
        def copy(index, block, half, peer):
            ref = ctx_ref.at[block, pl.ds(pl.multiple_of(one * HEAD_WIDTH + half * size, size), size)]
            return pltpu.make_async_remote_copy(
                src_ref=ref,
                dst_ref=ref,
                send_sem=ctx_send.at[one, index],
                recv_sem=ctx_recv.at[one, index],
                device_id={"tensor": peer},
                device_id_type=MESH,
            )

        return (
            copy(0, at.rank, 0, at.across),
            copy(1, at.rank, 1, at.over),
            copy(2, at.rank, 1, at.across),
            copy(3, at.rank, 0, at.over),
            copy(4, at.across, 0, at.over),
            copy(5, at.over, 1, at.across),
        )

    def relay(one):
        group = copies(one)
        group[0].wait_recv()
        group[4].start()
        group[1].wait_recv()
        group[5].start()

    def save(one):
        here = pl.ds(pl.multiple_of(one * HEAD_WIDTH, HEAD_WIDTH), HEAD_WIDTH)
        return pltpu.make_async_copy(ctx_ref.at[:, here], ctx_out.at[:, here], ctx_saved.at[one])

    length = length_ref[0]
    scale = HEAD_WIDTH ** (-0.5)

    def attend_head(head, carry):
        lines = pl.ds(pl.multiple_of(head * HEAD_WIDTH, HEAD_WIDTH), HEAD_WIDTH)
        keys, vals = qkv_ref[1, lines], qkv_ref[2, lines]
        for start in range(0, span, chunk):
            here = slice(start, start + chunk)
            query = (qkv_ref[0, lines, here].astype(F32) * scale).astype(BF)
            scores = masked_scores(keys, query, length)
            top = jnp.max(scores, axis=0, keepdims=True)
            expo = jnp.exp(scores - top)
            total = jnp.sum(expo, axis=0, keepdims=True)
            mixed = contract(vals, expo.astype(BF), (1, 0))
            ctx_ref[at.rank, lines, here] = (mixed * (1.0 / total)).astype(BF)
            lse_ref[head, :, here] = top + jnp.log(total)

        for copy in copies(head)[:4]:
            copy.start()

        @pl.when(head > 0)
        def _():
            relay(head - 1)

        @pl.when(head == 0)
        def _():
            ups.spread()
            tops.spread()

        @pl.when(head == 2)
        def _():
            outs.relay()

        return carry

    lax.fori_loop(0, heads, attend_head, 0)
    relay(heads - 1)
    outs.spread()
    ups.finish()
    tops.finish()
    downs.close_half()
    for one in streams:
        one.finish()

    def drain(one, carry):
        group = copies(one)
        for copy in group[2:]:
            copy.wait_recv()
        save(one).start()
        for copy in group:
            copy.wait_send()
        return carry

    lax.fori_loop(0, heads, drain, 0)
    for slot, block in enumerate((at.rank, at.across, at.over, at.diag)):
        for copy in saves(slot, block):
            copy.wait()

    def store(one, carry):
        save(one).wait()
        return carry

    lax.fori_loop(0, heads, store, 0)
    outs.finish()


def front(ids, x, w, up, down, top, out, lengths, vocab, chunk, ident):
    ranks, local, width = x.shape
    kinds, d_local, e_local = w.shape
    f_local = up.shape[1]
    heads = e_local // HEAD_WIDTH
    span = ranks * local
    assert heads > 2
    dma = pltpu.SemaphoreType.DMA
    return pl.pallas_call(
        functools.partial(front_body, chunk, vocab),
        out_shape=(
            jax.ShapeDtypeStruct(x.shape, BF),
            jax.ShapeDtypeStruct(x.shape, BF),
            jax.ShapeDtypeStruct((kinds, e_local, span), BF),
            jax.ShapeDtypeStruct((ranks, e_local, span), BF),
            jax.ShapeDtypeStruct((heads, 1, span), F32),
            jax.ShapeDtypeStruct((width, f_local), BF),
            jax.ShapeDtypeStruct((ranks * e_local, width), BF),
            jax.ShapeDtypeStruct((f_local, width), BF),
            jax.ShapeDtypeStruct((width, top.shape[1]), BF),
        ),
        in_specs=[pl.BlockSpec(memory_space=pltpu.SMEM), vmem_spec(), any_spec()] + [vmem_spec()] * 5,
        out_specs=(any_spec(),) * 4 + (vmem_spec(),) + (any_spec(),) * 4,
        scratch_shapes=[
            VMEM(x.shape, BF),
            VMEM((local, 128), F32),
            VMEM((local, width), BF),
            VMEM((2, local, width), BF),
            VMEM((local, width), BF),
            VMEM(x.shape, BF),
            VMEM(x.shape, BF),
            VMEM((kinds, e_local, span), BF),
            VMEM((kinds, width, e_local), BF),
            VMEM((kinds, e_local, width), BF),
            VMEM((ranks, e_local, span), BF),
            VMEM((ranks * e_local, d_local), BF),
            dma((2,)),
            dma((4, 3)),
            dma((24,)),
            dma((24,)),
            dma((3,)),
            dma((3,)),
            dma((heads, 6)),
            dma((heads, 6)),
            dma((heads,)),
        ]
        + RingGather.scratch() * 5,
        compiler_params=pltpu.CompilerParams(
            collective_id=ident, has_side_effects=True, vmem_limit_bytes=BIG
        ),
        name="front",
    )(lengths, ids, x, w, up, down, top, out)


def exact_dot(row, matrix, dims):
    high = row.astype(BF).astype(F32)
    middle = (row - high).astype(BF).astype(F32)
    low = row - high - middle
    shape = (8, row.shape[1])
    index = lax.broadcasted_iota(jnp.int32, shape, 0)
    stacked = jnp.where(
        index == 0, jnp.broadcast_to(high, shape),
        jnp.where(
            index == 1, jnp.broadcast_to(middle, shape),
            jnp.where(index == 2, jnp.broadcast_to(low, shape), 0.0),
        ),
    ).astype(BF)
    return jnp.sum(contract(stacked, matrix, dims), axis=0, keepdims=True)


class Fold:
    def __init__(self, at, src, held, acc, last, sems, base, rows, x_first):
        self.at, self.src, self.held, self.acc, self.last = at, src, held, acc, last
        self.sems, self.base, self.rows = sems, base, rows
        self.one, self.two = (at.across, at.over) if x_first else (at.over, at.across)

    def copies(self):
        rows, base, sems = self.rows, self.base, self.sems
        one, two = {"tensor": self.one}, {"tensor": self.two}
        return (
            remote(self.src.at[self.at.diag, rows], self.held.at[1, rows], sems, base, one),
            remote(self.src.at[self.one, rows], self.held.at[0, rows], sems, base + 1, one),
            remote(self.acc.at[rows], self.last.at[rows], sems, base + 2, two),
        )

    def start(self):
        copies = self.copies()
        copies[0].start()
        copies[1].start()

    def tiles(self, body):
        def step(at):
            body(pl.ds(pl.multiple_of(self.rows.start + at.start, 32), at.size))

        add_tiles(self.rows.size, 32, step)

    def second(self):
        copies = self.copies()
        copies[0].wait_recv()

        def body(here):
            self.acc[here] = (
                self.src[self.two, here].astype(F32) + self.held[1, here].astype(F32)
            ).astype(BF)

        self.tiles(body)
        copies[2].start()

    def third(self, put):
        copies = self.copies()
        copies[1].wait_recv()
        copies[2].wait_recv()

        def body(here):
            put(
                here,
                self.src[self.at.rank, here].astype(F32)
                + self.held[0, here].astype(F32)
                + self.last[here].astype(F32),
            )

        self.tiles(body)

    def finish(self):
        for copy in self.copies():
            copy.wait_send()


class DirectSum(GroupSum):
    def __init__(self, x_ref, pair, mine, far, sems, tile):
        super().__init__(x_ref, None, pair, mine, far, sems)
        self.tile = tile

    def middle(self):
        for copy in self.pair_copies():
            copy.wait()
        for chip in range(self.chips):

            def body(at, chip=chip):
                self.mine[chip, at] = (
                    self.x[chip * 2 + self.core, at].astype(F32)
                    + self.pair[chip, at].astype(F32)
                ).astype(BF)

            add_tiles(self.rows, self.tile, body)
        self.send()

    def send(self):
        for copy in self.far_copies():
            copy.start()

    def settle(self):
        for copy in self.far_copies():
            copy.wait()
        return self.chips - 1

    def finish(self, put):
        steps = self.settle()

        def body(at):
            total = self.mine[self.chip, at].astype(F32)
            for step in range(steps):
                total = total + self.far[step, at].astype(F32)
            put(at, total)

        add_tiles(self.far.shape[1], self.tile, body)


class RelaySum(DirectSum):
    def __init__(self, *args):
        super().__init__(*args)
        self.rows = self.far.shape[1]

    def send(self):
        for copy in self.ring_copies()[:4]:
            copy.start()

    def settle(self):
        copies = self.ring_copies()
        for copy in copies[2:]:
            copy.wait()
        for copy in copies[:2]:
            copy.wait_send()
        return 2


def stack_rows(rows):
    rows = list(rows)
    zero = jnp.zeros(rows[0].shape, F32)
    while len(rows) * rows[0].shape[0] % 16:
        rows.append(zero)
    return jnp.concatenate(rows, axis=0).astype(BF)


def split_three(values):
    high = values.astype(BF).astype(F32)
    middle = (values - high).astype(BF).astype(F32)
    return high, middle, values - high - middle


def finish_body(
    chunk, length_ref, bin_ref, top_ref, lse_ref,
    first_in, ctx_in, out_in, up_in, down_in, qkv_in, normed_in,
    qkv_out, out_out, up_out, down_out, top_out, loss_out,
    first, ctx, outs, up_full, down_full, qkv_ref, normed, loads, tile_loads, down_loads, stats,
    work, second, normed_two, turned, slope, sums, base, up_base, parts, p_send, p_recv, token, small_ref,
    d_send, d_recv, d_local_sem,
    g_second, up_term,
    spread, g_ctx, s_held, s_acc, s_last, s_send, s_recv,
    out_term, o_pair, out_sum, o_held, o_acc, o_last, o_send, o_recv,
    o_own, o_far, o_sem0, o_sem1, o_sem2, o_sem3,
    u_pair, u_own, u_far, u_sem0, u_sem1, u_sem2, u_sem3,
    g_qkv, q_term, q_pair, q_own, q_far, q_sem0, q_sem1, q_sem2, q_sem3,
    smalls, m_send, m_recv, q_all,
):
    at = Place()
    peers = at.peers(True)
    at.signal(peers)
    heads = lse_ref.shape[0]
    end = heads - 1
    e_local = g_ctx.shape[0]
    d_local = q_term.shape[3]
    groups = q_term.shape[1]
    span, width = first.shape
    units = slope.shape[1]
    bins = top_ref.shape[1]
    half = HEAD_WIDTH // 2
    length = length_ref[0]
    scale = HEAD_WIDTH ** (-0.5)
    local = span // 4

    pairs = ((out_in, outs), (up_in, up_full), (qkv_in, qkv_ref), (normed_in, normed))

    def load(index):
        return pltpu.make_async_copy(*pairs[index], loads.at[index])

    def load_tile(tile):
        here = pl.ds(pl.multiple_of(tile * local, local), local)
        return (
            pltpu.make_async_copy(ctx_in.at[:, here], ctx.at[:, here], tile_loads.at[tile, 0]),
            pltpu.make_async_copy(first_in.at[here], first.at[here], tile_loads.at[tile, 1]),
        )

    slot = columns_of(down_full, d_local)
    source = columns_of(down_in, d_local)
    downs = RingGather(
        at, slot(at.group, None), lambda part: slot(at.group, part), slot, (d_send, d_recv, d_local_sem)
    )

    def load_down(index):
        other = at.group + 1 - 2 * at.core
        ends = ((at.same(at.turn(3)), 0), (at.same(at.turn(1)), 1), (at.group, None), (other, None))
        return pltpu.make_async_copy(
            source(*ends[index]), slot(*ends[index]), down_loads.at[index]
        )

    load(0).start()
    for copy in load_tile(0):
        copy.start()
    for index in range(3):
        load_down(index).start()
    for tile in range(1, 4):
        for copy in load_tile(tile):
            copy.start()
    load(1).start()
    load_down(3).start()
    load(2).start()
    load(3).start()
    base[...] = jnp.zeros(base.shape, F32)
    load(0).wait()

    def project_tile(tile, carry):
        for copy in load_tile(tile):
            copy.wait()
        start = pl.multiple_of(tile * local, local)
        work[...] = contract(ctx[:, pl.ds(start, local)], outs[...], (0, 0))

        def body(rows):
            here = pl.ds(pl.multiple_of(start + rows.start, 64), rows.size)
            value = (first[here].astype(F32) + work[rows]).astype(BF)
            second[here] = value
            value = value.astype(F32)
            mean = jnp.mean(value, axis=-1, keepdims=True)
            away = value - mean
            inverse = lax.rsqrt(jnp.mean(away * away, axis=-1, keepdims=True) + EPS)
            normed_two[here] = (away * inverse).astype(BF)
            stats[0, here] = jnp.broadcast_to(mean, (rows.size, 128))
            stats[1, here] = jnp.broadcast_to(inverse, (rows.size, 128))
            live = lax.broadcasted_iota(jnp.int32, value.shape, 0) + here.start < length
            base[...] += jnp.sum(
                jnp.where(live, value, 0.0).reshape(rows.size // 8, 8, width), axis=0
            )

        add_tiles(local, 64, body)
        turned[:, pl.ds(start, local)] = normed_two[pl.ds(start, local)].T
        return carry

    lax.fori_loop(0, 1, project_tile, 0)
    for index in range(3):
        load_down(index).wait()
    at.ready(peers)
    downs.start_rest()
    lax.fori_loop(1, 4, project_tile, 0)
    load(1).wait()

    def hidden_chunk(step, carry):
        lanes = pl.ds(pl.multiple_of(step * chunk, chunk), chunk)
        pre = jnp.dot(normed_two[...], up_full[:, lanes], preferred_element_type=F32)
        live = lax.broadcasted_iota(jnp.int32, pre.shape, 0) < length
        square = pre * pre
        bend = jnp.tanh(0.7978845608028654 * (pre * (1.0 + 0.044715 * square)))
        part = 0.5 * (1.0 + bend)
        act = (pre * part).astype(BF).astype(F32)
        sums[:, lanes] = jnp.sum(jnp.where(live, act, 0.0), axis=0, keepdims=True)
        inner = 0.7978845608028654 * (1.0 + 3 * 0.044715 * square)
        value = part + 0.5 * pre * (1.0 - bend * bend) * inner
        slope[:, lanes] = jnp.where(live, value, 0.0).astype(BF)
        return carry

    lax.fori_loop(0, units // chunk, hidden_chunk, 0)
    load_down(3).wait()
    downs.near()
    downs.far()
    downs.close_rest()
    hidden_sum = sums[...]
    parts[at.rank] = exact_dot(hidden_sum, down_full[...], (1, 0))
    part_copies = [
        remote(parts.at[at.rank], parts.at[at.rank], (p_send, p_recv), index, peer)
        for index, peer in enumerate(peers[:3])
    ]
    for copy in part_copies:
        copy.start()

    def base_chunk(step, carry):
        lanes = pl.ds(pl.multiple_of(step * chunk, chunk), chunk)
        up_base[:, lanes] = jnp.dot(turned[...], slope[:, lanes], preferred_element_type=F32)
        return carry

    lax.fori_loop(0, units // chunk, base_chunk, 0)
    for copy in part_copies:
        copy.wait()
    count = jnp.full((1, 1), length, jnp.int32).astype(F32)
    total = jnp.sum(base[...], axis=0, keepdims=True)
    for index in range(4):
        total = total + parts[index]
    pooled = total / count
    mean = jnp.mean(pooled, axis=-1, keepdims=True)
    centered = pooled - mean
    norm_scale = lax.rsqrt(jnp.mean(centered * centered, axis=-1, keepdims=True) + EPS)
    final = centered * norm_scale
    logits = exact_dot(final, top_ref[...], (1, 0))
    highest = jnp.max(logits, axis=-1, keepdims=True)
    total_exp = jnp.log(jnp.sum(jnp.exp(logits - highest), axis=-1, keepdims=True)) + highest
    labels = (lax.broadcasted_iota(jnp.int32, logits.shape, 1) == bin_ref[0]).astype(F32)
    loss = total_exp - jnp.sum(logits * labels, axis=-1, keepdims=True)
    g_logits = (jnp.exp(logits - total_exp) - labels) / 8.0
    g_final = exact_dot(g_logits, top_ref[...], (1, 1))
    g_pooled = norm_scale * (
        g_final
        - jnp.mean(g_final, axis=-1, keepdims=True)
        - final * jnp.mean(g_final * final, axis=-1, keepdims=True)
    )
    per_token = g_pooled / count
    rounded = per_token.astype(BF).astype(F32)
    token[...] = per_token / 4.0
    sums[...] = contract(
        jnp.broadcast_to(rounded, (8, width)).astype(BF), down_full[...], (1, 1)
    )[:1]
    small_ref[:, :units] = hidden_sum
    small_ref[:, units : units + width] = rounded
    small_ref[:, units + width : units + 2 * width] = final
    small_ref[:, units + 2 * width : units + 2 * width + bins] = g_logits
    small_ref[:, units + 2 * width + bins :] = jnp.broadcast_to(loss, (1, 128))

    def scale_group(group, carry):
        def body(rows):
            here = pl.ds(pl.multiple_of(group * d_local + rows.start, 32), rows.size)
            up_term[group, rows] = (up_base[here] * sums[...]).astype(BF)

        add_tiles(d_local, 32, body)
        return carry

    lax.fori_loop(0, groups, scale_group, 0)
    up_sum = GroupSum(up_term, up_out, u_pair, u_own, u_far, (u_sem0, u_sem1, u_sem2, u_sem3))
    up_sum.start()

    def small_copies():
        return [
            remote(
                small_ref, smalls.at[at.group], (m_send, m_recv), step - 1,
                {"dp": lax.rem(at.group + step, groups)},
            )
            for step in range(1, groups)
        ]

    for copy in small_copies():
        copy.start()
    smalls[at.group] = small_ref[...]

    def back_tile(tile, carry):
        start = pl.multiple_of(tile * local, local)

        def pre(rows):
            here = pl.ds(pl.multiple_of(start + rows.start, 64), rows.size)
            slope[here] = (slope[here].astype(F32) * sums[...]).astype(BF)

        add_tiles(local, 64, pre)
        work[...] = contract(slope[pl.ds(start, local)], up_full[...], (1, 1))

        def body(rows):
            here = pl.ds(pl.multiple_of(start + rows.start, 64), rows.size)
            grad = work[rows]
            inverse = stats[1, here, :1]
            unit = (second[here].astype(F32) - stats[0, here, :1]) * inverse
            back = inverse * (
                grad
                - jnp.mean(grad, axis=-1, keepdims=True)
                - unit * jnp.mean(grad * unit, axis=-1, keepdims=True)
            )
            live = lax.broadcasted_iota(jnp.int32, grad.shape, 0) + here.start < length
            g_second[here] = (back + jnp.where(live, token[...], 0.0)).astype(BF)

        add_tiles(local, 64, body)
        return carry

    lax.fori_loop(0, 1, back_tile, 0)
    up_sum.middle()
    lax.fori_loop(1, 4, back_tile, 0)

    def folds(one):
        return [
            Fold(
                at, spread, s_held, s_acc, s_last, (s_send, s_recv), one * 6 + part * 3,
                pl.ds(pl.multiple_of(one * HEAD_WIDTH + part * half, half), half), part == 0,
            )
            for part in range(2)
        ]

    out_folds = [
        Fold(
            at, out_sum, o_held, o_acc, o_last, (o_send, o_recv), part * 3,
            pl.ds(part * (e_local // 2), e_local // 2), part == 0,
        )
        for part in range(2)
    ]
    out_group = RelaySum(out_term, o_pair, o_own, o_far, (o_sem0, o_sem1, o_sem2, o_sem3), 64)

    def qkv_sum(one, kind=RelaySum):
        return kind(
            q_term.at[one], q_pair.at[one], q_own.at[one], q_far.at[one],
            (q_sem0.at[one], q_sem1.at[one], q_sem2.at[one], q_sem3.at[one]), q_term.shape[2],
        )

    def put_context(here, total):
        g_ctx[here] = total.astype(BF)

    def put_out(here, total):
        for chip in range(4):
            o_own[chip, here] = total[:, chip * d_local : (chip + 1) * d_local].astype(BF)

    def pair_out():
        for copy in out_group.pair_copies():
            copy.wait()

        def block(one, carry):
            for chip in range(4):

                def body(rows):
                    here = pl.ds(pl.multiple_of(one * e_local + rows.start, 64), rows.size)
                    out_sum[one, rows, chip * d_local : (chip + 1) * d_local] = (
                        out_term[chip * 2 + at.core, here].astype(F32)
                        + o_pair[chip, here].astype(F32)
                    ).astype(BF)

                add_tiles(e_local, 64, body)
            return carry

        lax.fori_loop(0, 4, block, 0)

    def spread_head(one, carry):
        left = jnp.concatenate(
            [
                outs[pl.ds(pl.multiple_of(part * e_local + one * HEAD_WIDTH, HEAD_WIDTH), HEAD_WIDTH)]
                for part in range(4)
            ],
            axis=0,
        )
        result = contract(left, g_second[...], (1, 1)).astype(BF)
        for part in range(4):
            spread[part, pl.ds(pl.multiple_of(one * HEAD_WIDTH, HEAD_WIDTH), HEAD_WIDTH)] = result[
                part * HEAD_WIDTH : (part + 1) * HEAD_WIDTH
            ]
        for fold in folds(one):
            fold.start()
        return carry

    def out_block(one, carry):
        rows = pl.ds(pl.multiple_of(one * e_local, e_local), e_local)
        result = jnp.dot(ctx[rows], g_second[...], preferred_element_type=F32)
        for group in range(groups):
            out_term[group, rows] = result[:, group * d_local : (group + 1) * d_local].astype(BF)
        return carry

    lax.fori_loop(0, 2, spread_head, 0)
    lax.fori_loop(0, 2, out_block, 0)
    for fold in folds(0):
        fold.second()
    lax.fori_loop(2, heads, spread_head, 0)
    for fold in folds(1):
        fold.second()
    lax.fori_loop(2, 4, out_block, 0)
    out_group.start()
    up_sum.relay()
    load(2).wait()
    load(3).wait()

    def back_head(head, carry):
        for fold in folds(head):
            fold.third(put_context)

        mine = pl.ds(pl.multiple_of(head * HEAD_WIDTH, HEAD_WIDTH), HEAD_WIDTH)
        keys, vals = qkv_ref[1, mine], qkv_ref[2, mine]
        g_keys = jnp.zeros((HEAD_WIDTH, span), F32)
        g_vals = jnp.zeros((HEAD_WIDTH, span), F32)
        for index, start in enumerate(range(0, span, local)):
            here = slice(start, start + local)
            query = (qkv_ref[0, mine, here].astype(F32) * scale).astype(BF)
            grad = g_ctx[mine, here]
            probs = jnp.exp(masked_scores(keys, query, length) - lse_ref[head, :, here])
            g_probs = contract(vals, grad, (0, 0))
            weighted = probs * g_probs
            inner = jnp.sum(weighted, axis=0, keepdims=True)
            g_scores = (weighted - probs * inner).astype(BF)
            g_qkv[:HEAD_WIDTH, here] = (contract(keys, g_scores, (1, 0)) * scale).astype(BF)
            g_keys += contract(query, g_scores, (1, 1))
            g_vals += contract(grad, probs.astype(BF), (1, 1))
            if index == 0:

                @pl.when(head > 0)
                def _():
                    qkv_sum(head - 1).middle()

            if index == 3:

                @pl.when(head > 0)
                def _():
                    qkv_sum(head - 1).relay()

                @pl.when(head == end)
                def _():
                    out_group.relay()

                @pl.when(head == 1)
                def _():
                    for fold in out_folds:
                        fold.second()

                @pl.when(head == 2)
                def _():
                    for fold in out_folds:
                        fold.third(put_out)
                    out_group.send()

        g_qkv[HEAD_WIDTH : 2 * HEAD_WIDTH] = g_keys.astype(BF)
        g_qkv[2 * HEAD_WIDTH :] = g_vals.astype(BF)
        result = jnp.dot(g_qkv[...], normed[...], preferred_element_type=F32)
        for group in range(groups):
            q_term[head, group] = result[:, group * d_local : (group + 1) * d_local].astype(BF)
        qkv_sum(head).start()

        @pl.when(head == 0)
        def _():
            def second(one, carry):
                for fold in folds(one):
                    fold.second()
                return carry

            lax.fori_loop(2, heads, second, 0)
            pair_out()
            for fold in out_folds:
                fold.start()
        return carry

    lax.fori_loop(0, heads, back_head, 0)
    qkv_sum(end, DirectSum).middle()
    up_sum.finish()
    for copy in small_copies():
        copy.wait()

    def lines(start, size):
        return [smalls[group, :, pl.ds(start, size)] for group in range(groups)]

    mine_d = pl.multiple_of(at.group * d_local, d_local)
    units_all = split_three(jnp.concatenate(lines(0, units), axis=0))
    tokens_all = jnp.concatenate(lines(units + mine_d, d_local), axis=0)
    down_out[...] = contract(stack_rows(units_all), stack_rows([tokens_all] * 3), (0, 0))
    finals = split_three(jnp.concatenate(lines(units + width + mine_d, d_local), axis=0))
    errors = split_three(jnp.concatenate(lines(units + 2 * width, bins), axis=0))
    order = [(i, j) for i in range(3) for j in range(3) if i + j < 4]
    top_out[...] = contract(
        stack_rows([finals[i] for i, _ in order]), stack_rows([errors[j] for _, j in order]), (0, 0)
    )
    losses = jnp.concatenate(lines(units + 2 * width + bins, 128), axis=0)
    loss_out[...] = jnp.sum(losses, axis=0, keepdims=True) / 8.0

    def drain(one, carry):
        for fold in folds(one):
            fold.finish()
        return carry

    lax.fori_loop(0, heads, drain, 0)
    for fold in out_folds:
        fold.finish()

    def put_final(here, total):
        out_out[here] = total

    out_group.finish(put_final)

    def store(one, kind):
        def put(here, total):
            for kind in range(3):
                q_all[kind, pl.ds(pl.multiple_of(one * HEAD_WIDTH, HEAD_WIDTH), HEAD_WIDTH)] = total[
                    kind * HEAD_WIDTH : (kind + 1) * HEAD_WIDTH
                ]

        qkv_sum(one, kind).finish(put)

    for one in range(end):
        store(one, RelaySum)
    store(end, DirectSum)
    for kind in range(3):
        qkv_out[kind] = q_all[kind].T


def finish(lengths, bins_at, top, lse, first, context, out_full, up, down, qkv, normed, chunk, ident):
    _, width, length = qkv.shape
    full, units = up.shape
    heads = width // HEAD_WIDTH
    groups = lax.axis_size("dp")
    d_local = full // groups
    bins = top.shape[1]
    rows = 3 * HEAD_WIDTH
    small = units + 2 * full + bins + 128
    dma = pltpu.SemaphoreType.DMA
    smem = pl.BlockSpec(memory_space=pltpu.SMEM)
    return pl.pallas_call(
        functools.partial(finish_body, chunk),
        out_shape=(
            jax.ShapeDtypeStruct((3, d_local, width), F32),
            jax.ShapeDtypeStruct((width, d_local), F32),
            jax.ShapeDtypeStruct((d_local, units), F32),
            jax.ShapeDtypeStruct((units, d_local), F32),
            jax.ShapeDtypeStruct((d_local, bins), F32),
            jax.ShapeDtypeStruct((1, 128), F32),
        ),
        in_specs=[smem, smem, vmem_spec(), vmem_spec()] + [any_spec()] * 7,
        out_specs=(vmem_spec(),) * 6,
        scratch_shapes=[
            VMEM((length, full), BF),
            VMEM(context.shape, BF),
            VMEM(out_full.shape, BF),
            VMEM(up.shape, BF),
            VMEM(down.shape, BF),
            VMEM(qkv.shape, BF),
            VMEM(normed.shape, BF),
            dma((4,)),
            dma((4, 2)),
            dma((4,)),
            VMEM((2, length, 128), F32),
            VMEM((length // 4, full), F32),
            VMEM((length, full), BF),
            VMEM((length, full), BF),
            VMEM((full, length), BF),
            VMEM((length, units), BF),
            VMEM((1, units), F32),
            VMEM((8, full), F32),
            VMEM((full, units), F32),
            VMEM((4, 1, full), F32),
            dma((3,)),
            dma((3,)),
            VMEM((1, full), F32),
            VMEM((1, small), F32),
        ]
        + RingGather.scratch()
        + [
            VMEM((length, full), BF),
            VMEM((groups, d_local, units), BF),
            VMEM((4, width, length), BF),
            VMEM((width, length), BF),
            VMEM((2, width, length), BF),
            VMEM((width, length), BF),
            VMEM((width, length), BF),
            dma((heads * 6,)),
            dma((heads * 6,)),
            VMEM((groups, 4 * width, d_local), BF),
            VMEM((4, 4 * width, d_local), BF),
            VMEM((4, width, full // 2), BF),
            VMEM((2, width, full // 2), BF),
            VMEM((width, full // 2), BF),
            VMEM((width, full // 2), BF),
            dma((6,)),
            dma((6,)),
            VMEM((4, width, d_local), BF),
            VMEM((3, width, d_local), BF),
            dma((4,)),
            dma((4,)),
            dma((6,)),
            dma((6,)),
        ]
        + GroupSum.scratch((groups, d_local, units), BF)
        + [
            VMEM((rows, length), BF),
            VMEM((heads, groups, rows, d_local), BF),
            VMEM((heads, 4, rows, d_local), BF),
            VMEM((heads, 4, rows, d_local), BF),
            VMEM((heads, 3, rows, d_local), BF),
            dma((heads, 4)),
            dma((heads, 4)),
            dma((heads, 6)),
            dma((heads, 6)),
            VMEM((groups, 1, small), F32),
            dma((groups - 1,)),
            dma((groups - 1,)),
            VMEM((3, width, d_local), F32),
        ],
        compiler_params=pltpu.CompilerParams(
            collective_id=ident, has_side_effects=True, vmem_limit_bytes=BIG
        ),
        name="finish",
    )(lengths, bins_at, top, lse, first, context, out_full, up, down, qkv, normed)


def hand_over_body(*refs):
    half = len(refs) // 2
    for source, target in zip(refs[:half], refs[half:]):
        target[...] = source[...]


def hand_over(*arrays):
    return pl.pallas_call(
        hand_over_body,
        out_shape=tuple(jax.ShapeDtypeStruct(one.shape, one.dtype) for one in arrays),
        in_specs=[vmem_spec()] * len(arrays),
        out_specs=(vmem_spec(),) * len(arrays),
        name="hand_over",
    )(*arrays)


def per_device_block(
    token_ids,
    lengths,
    teacher_bins,
    embed_table,
    query_key_value_matrix,
    output_matrix,
    up_matrix,
    down_matrix,
    w_head,
):
    ranks = lax.axis_size("tensor")
    rank = lax.axis_index("tensor")
    assert token_ids.shape[0] == 1
    local_len = token_ids.shape[1]
    span = local_len * ranks
    vocab_local, width = embed_table.shape
    _, _, e_local = query_key_value_matrix.shape
    f_local = up_matrix.shape[1]

    all_ids = share_ids(token_ids, 11)
    shifted = all_ids.reshape(span) - rank * vocab_local
    rows = embed_table.at[jnp.clip(shifted, 0, vocab_local - 1)].get(mode="promise_in_bounds")
    chunk = min(256, span)
    first, normed_one, qkv, context, lse, up_full, out_full, down_part, head_full = front(
        all_ids,
        rows.reshape(ranks, local_len, width),
        query_key_value_matrix.transpose(1, 0, 2),
        up_matrix,
        down_matrix,
        w_head,
        output_matrix,
        lengths,
        vocab_local,
        chunk,
        12,
    )
    first = first.reshape(span, width)
    normed_one = normed_one.reshape(span, width)
    context_all = context.reshape(ranks * e_local, span)
    (
        qkv_gradient,
        output_weight_gradient,
        up_weight_gradient,
        down_weight_gradient,
        grad_head,
        losses,
    ) = finish(
        lengths, teacher_bins, head_full, lse, first, context_all, out_full, up_full, down_part,
        qkv, normed_one, min(256, f_local), 15,
    )
    (
        qkv_gradient,
        output_weight_gradient,
        up_weight_gradient,
        down_weight_gradient,
        grad_head,
        losses,
    ) = hand_over(
        qkv_gradient,
        output_weight_gradient,
        up_weight_gradient,
        down_weight_gradient,
        grad_head,
        losses,
    )
    loss = losses[0, 0]
    query_key_value_gradient = qkv_gradient.transpose(1, 0, 2)
    return (
        loss,
        query_key_value_gradient,
        output_weight_gradient,
        up_weight_gradient,
        down_weight_gradient,
        grad_head,
    )


def solution(mesh):
    placed = (
        P("dp", "tensor"),
        P("dp"),
        P("dp"),
        P("tensor", None),
        P("dp", None, "tensor"),
        P("tensor", "dp"),
        P("dp", "tensor"),
        P("tensor", "dp"),
        P("dp", None),
    )
    return jax.shard_map(
        per_device_block if (mesh.shape["tensor"], mesh.shape["dp"]) == (4, 8) else per_device,
        mesh=mesh,
        in_specs=placed,
        out_specs=(
            P(),
            P("dp", None, "tensor"),
            P("tensor", "dp"),
            P("dp", "tensor"),
            P("tensor", "dp"),
            P("dp", None),
        ),
        check_vma=False,
    )
```
